32 devices in a mesh: col: 4 (over z), row: 8 (over y, x, core).
Axes of the slice: x: 2, y: 2, z: 4, core: 2. Of those that a mesh axis runs over, the one named last changes fastest.
Arguments:
- vel_u: float32 [31, 1024, 512], P(None, 'row', 'col')
- vel_v: float32 [31, 1024, 512], P(None, 'row', 'col')
- temperature: float32 [31, 1024, 512], P(None, 'row', 'col')
- salinity: float32 [31, 1024, 512], P(None, 'row', 'col')
- sea_level: float32 [1024, 512], P('row', 'col')
- trans_u: float32 [1024, 512], P('row', 'col')
- trans_v: float32 [1024, 512], P('row', 'col')
- col_depth: float32 [1024, 512], P('row', 'col')
- kmt_levels: int32 [1024, 512], P('row', 'col')
Outputs:
- output 1: float32 [1024, 512], P('row', 'col')
- output 2: float32 [1024, 512], P('row', 'col')
- output 3: float32 [1024, 512], P('row', 'col')
- output 4: float32 [31, 1024, 512], P(None, 'row', 'col')
- output 5: float32 [31, 1024, 512], P(None, 'row', 'col')
- output 6: float32 [31, 1024, 512], P(None, 'row', 'col')
- output 7: float32 [31, 1024, 512], P(None, 'row', 'col')
All inputs are finite; a program needn't handle non-finite values.
Results may differ from the reference program's by a relative error of at most 0.001.
Values sent between devices are 32-bit elements.
A program may use at most 1 GiB of HBM per device.

```python
import jax
import jax.numpy as jnp
from jax import lax

LEVELS = 31
GRID_Y = 1024
GRID_X = 512
SUBCYCLES = 30
ADV_COURANT = 0.25
WAVE_COURANT = 0.5
VISC_NUM = 4.0
DIFF_NUM = 1.0
ALPHA_T = 0.3
BETA_S = 0.6


def setup_inputs(seed: int = 0) -> dict:
    sub_keys = jax.random.split(jax.random.key(seed), 12)
    kmt_draw = jax.random.randint(sub_keys[0], (GRID_Y, GRID_X), LEVELS // 3, LEVELS + 1)
    land_draw = jax.random.randint(sub_keys[1], (GRID_Y, GRID_X), 0, 8)
    kmt_levels = jnp.where(land_draw == 0, 0, kmt_draw).astype(jnp.int32)
    kmt_levels = kmt_levels.at[0, 0].set(0).at[0, 1].set(LEVELS)
    col_depth = jax.random.uniform(sub_keys[2], (GRID_Y, GRID_X), jnp.float32, 0.3, 1.0)
    level_frac = jnp.arange(LEVELS, dtype=jnp.float32)[:, None, None] / LEVELS
    shape_3d = (LEVELS, GRID_Y, GRID_X)
    plane_shape = (1, GRID_Y, GRID_X)
    temperature = 1.5 * (1.0 - 2.0 * level_frac) + jax.random.normal(sub_keys[3], plane_shape, jnp.float32) + 0.5 * jax.random.normal(sub_keys[4], shape_3d, jnp.float32)
    salinity = 0.8 * level_frac + 0.8 * jax.random.normal(sub_keys[5], plane_shape, jnp.float32) + 0.4 * jax.random.normal(sub_keys[6], shape_3d, jnp.float32)
    vel_u = 0.5 * jax.random.normal(sub_keys[7], shape_3d, jnp.float32)
    vel_v = 0.5 * jax.random.normal(sub_keys[8], shape_3d, jnp.float32)
    sea_level = 0.5 * jax.random.normal(sub_keys[9], (GRID_Y, GRID_X), jnp.float32)
    trans_u = 0.4 * jax.random.normal(sub_keys[10], (GRID_Y, GRID_X), jnp.float32)
    trans_v = 0.4 * jax.random.normal(sub_keys[11], (GRID_Y, GRID_X), jnp.float32)
    return {'vel_u': vel_u, 'vel_v': vel_v, 'temperature': temperature, 'salinity': salinity, 'sea_level': sea_level, 'trans_u': trans_u, 'trans_v': trans_v, 'col_depth': col_depth, 'kmt_levels': kmt_levels}


def pad_halo(field_in):
    wide_pad = jnp.concatenate([field_in[..., -1:], field_in, field_in[..., :1]], axis=-1)
    zero_row = jnp.zeros_like(wide_pad[..., :1, :])
    return jnp.concatenate([zero_row, wide_pad, zero_row], axis=-2)


def column_solve(wet_mask, diffusivity, rhs_list):
    link_mask = wet_mask[:-1] * wet_mask[1:]
    zero_level = jnp.zeros_like(wet_mask[:1])
    upper_band = diffusivity * jnp.concatenate([link_mask, zero_level], axis=0)
    lower_band = diffusivity * jnp.concatenate([zero_level, link_mask], axis=0)
    diag_band = 1.0 + upper_band + lower_band

    def forward(state_in, level_in):
        c_prev, d_prev = state_in
        up_k, lo_k, dg_k, rhs_k = level_in
        pivot = dg_k - lo_k * c_prev
        c_ratio = up_k / pivot
        d_new = tuple((r + lo_k * p) / pivot for r, p in zip(rhs_k, d_prev))
        return (c_ratio, d_new), (c_ratio, d_new)

    def backward(x_next, level_in):
        c_k, d_k = level_in
        x_new = tuple(d + c_k * x for d, x in zip(d_k, x_next))
        return x_new, x_new

    zero_plane = jnp.zeros_like(wet_mask[0])
    start_state = (zero_plane, tuple(zero_plane for _ in rhs_list))
    _, (c_all, d_all) = lax.scan(forward, start_state, (upper_band, lower_band, diag_band, tuple(rhs_list)))
    _, x_all = lax.scan(backward, tuple(zero_plane for _ in rhs_list), (c_all, d_all), reverse=True)
    return x_all


def upwind_div(u_pad, v_pad, tracer_pad, face_u, face_v):
    u_face = u_pad[:, 1:-1, :-1]
    flux_e = face_u[:, 1:-1, :] * (jnp.maximum(u_face, 0.0) * tracer_pad[:, 1:-1, :-1] + jnp.minimum(u_face, 0.0) * tracer_pad[:, 1:-1, 1:])
    v_face = v_pad[:, :-1, 1:-1]
    flux_n = face_v[:, :, 1:-1] * (jnp.maximum(v_face, 0.0) * tracer_pad[:, :-1, 1:-1] + jnp.minimum(v_face, 0.0) * tracer_pad[:, 1:, 1:-1])
    return flux_e[:, :, 1:] - flux_e[:, :, :-1] + flux_n[:, 1:, :] - flux_n[:, :-1, :]


def baroclinic(u_pad, v_pad, t_pad, s_pad, kmt_pad, depth_pad):
    level_idx = jnp.arange(u_pad.shape[0], dtype=jnp.int32)[:, None, None]
    cell_p = (level_idx < kmt_pad[None]).astype(jnp.float32)
    kmin_u = jnp.minimum(kmt_pad[:, :-1], kmt_pad[:, 1:])
    kmin_v = jnp.minimum(kmt_pad[:-1, :], kmt_pad[1:, :])
    face_u = (level_idx < kmin_u[None]).astype(jnp.float32)
    face_v = (level_idx < kmin_v[None]).astype(jnp.float32)
    thickness = depth_pad / jnp.maximum(kmt_pad, 1).astype(jnp.float32)
    density = (BETA_S * s_pad - ALPHA_T * t_pad) * cell_p
    pressure = (jnp.cumsum(density, axis=0) - 0.5 * density) * thickness[None]
    u_c = u_pad[:, 1:-1, 1:-1]
    v_c = v_pad[:, 1:-1, 1:-1]
    p_c = pressure[:, 1:-1, 1:-1]
    mask_u = face_u[:, 1:-1, 1:]
    mask_v = face_v[:, 1:, 1:-1]
    cell_c = cell_p[:, 1:-1, 1:-1]
    v_at_u = 0.25 * (v_c + v_pad[:, 1:-1, 2:] + v_pad[:, :-2, 1:-1] + v_pad[:, :-2, 2:])
    u_at_v = 0.25 * (u_c + u_pad[:, 1:-1, :-2] + u_pad[:, 2:, 1:-1] + u_pad[:, 2:, :-2])
    tend_u = mask_u * (p_c - pressure[:, 1:-1, 2:] - 0.5 * (u_c * (u_pad[:, 1:-1, 2:] - u_pad[:, 1:-1, :-2]) + v_at_u * (u_pad[:, 2:, 1:-1] - u_pad[:, :-2, 1:-1])))
    tend_v = mask_v * (p_c - pressure[:, 2:, 1:-1] - 0.5 * (u_at_v * (v_pad[:, 1:-1, 2:] - v_pad[:, 1:-1, :-2]) + v_c * (v_pad[:, 2:, 1:-1] - v_pad[:, :-2, 1:-1])))
    new_u = column_solve(mask_u, VISC_NUM, (mask_u * (u_c + ADV_COURANT * tend_u),))[0]
    new_v = column_solve(mask_v, VISC_NUM, (mask_v * (v_c + ADV_COURANT * tend_v),))[0]
    pred_t = cell_c * (t_pad[:, 1:-1, 1:-1] - ADV_COURANT * upwind_div(u_pad, v_pad, t_pad, face_u, face_v))
    pred_s = cell_c * (s_pad[:, 1:-1, 1:-1] - ADV_COURANT * upwind_div(u_pad, v_pad, s_pad, face_u, face_v))
    new_t, new_s = column_solve(cell_c, DIFF_NUM, (pred_t, pred_s))
    count_u = kmin_u[1:-1, 1:]
    count_v = kmin_v[1:, 1:-1]
    wet_u = (count_u > 0).astype(jnp.float32)
    wet_v = (count_v > 0).astype(jnp.float32)
    wet_c = (kmt_pad[1:-1, 1:-1] > 0).astype(jnp.float32)
    inv_u = 1.0 / jnp.maximum(count_u, 1).astype(jnp.float32)
    inv_v = 1.0 / jnp.maximum(count_v, 1).astype(jnp.float32)
    depth_u = 0.5 * (depth_pad[1:-1, 1:-1] + depth_pad[1:-1, 2:]) * wet_u
    depth_v = 0.5 * (depth_pad[1:-1, 1:-1] + depth_pad[2:, 1:-1]) * wet_v
    force_u = depth_u * inv_u * jnp.sum(tend_u, axis=0)
    force_v = depth_v * inv_v * jnp.sum(tend_v, axis=0)
    base_u = new_u - mask_u * (inv_u * jnp.sum(new_u, axis=0))[None]
    base_v = new_v - mask_v * (inv_v * jnp.sum(new_v, axis=0))[None]
    return (base_u, base_v, mask_u, mask_v, new_t, new_s, force_u, force_v, depth_u, depth_v, wet_u, wet_v, wet_c)


def sm_weights():
    frac_step = jnp.arange(1, SUBCYCLES + 1, dtype=jnp.float32) / (SUBCYCLES + 1)
    raw_shape = frac_step ** 2 * (1.0 - frac_step ** 4)
    return raw_shape / jnp.sum(raw_shape)


def barotropic_whole(sea_level, trans_u, trans_v, force_u, force_v, depth_u, depth_v, wet_u, wet_v, wet_c):
    wave_u = WAVE_COURANT * depth_u
    wave_v = WAVE_COURANT * depth_v
    push_u = (ADV_COURANT / SUBCYCLES) * force_u
    push_v = (ADV_COURANT / SUBCYCLES) * force_v

    def subcycle(state_in, weight):
        level_now, flow_u, flow_v, mean_u, mean_v = state_in
        west_u = jnp.roll(flow_u, 1, axis=1)
        south_v = jnp.concatenate([jnp.zeros_like(flow_v[:1]), flow_v[:-1]], axis=0)
        level_new = wet_c * (level_now - WAVE_COURANT * (flow_u - west_u + flow_v - south_v))
        east_level = jnp.roll(level_new, -1, axis=1)
        north_level = jnp.concatenate([level_new[1:], jnp.zeros_like(level_new[:1])], axis=0)
        flow_u = wet_u * (flow_u - wave_u * (east_level - level_new) + push_u)
        flow_v = wet_v * (flow_v - wave_v * (north_level - level_new) + push_v)
        return (level_new, flow_u, flow_v, mean_u + weight * flow_u, mean_v + weight * flow_v), None

    start_state = (wet_c * sea_level, wet_u * trans_u, wet_v * trans_v, jnp.zeros_like(trans_u), jnp.zeros_like(trans_v))
    final_state, _ = lax.scan(subcycle, start_state, sm_weights())
    return final_state


def finish(base_vel, face_mask, mean_flow, face_depth):
    return base_vel + face_mask * (mean_flow / jnp.where(face_depth > 0, face_depth, 1.0))[None]


def reference(vel_u, vel_v, temperature, salinity, sea_level, trans_u, trans_v, col_depth, kmt_levels):
    (base_u, base_v, mask_u, mask_v, new_t, new_s, force_u, force_v, depth_u, depth_v, wet_u, wet_v, wet_c) = baroclinic(pad_halo(vel_u), pad_halo(vel_v), pad_halo(temperature), pad_halo(salinity), pad_halo(kmt_levels), pad_halo(col_depth))
    level_new, flow_u, flow_v, mean_u, mean_v = barotropic_whole(sea_level, trans_u, trans_v, force_u, force_v, depth_u, depth_v, wet_u, wet_v, wet_c)
    return (level_new, flow_u, flow_v, finish(base_u, mask_u, mean_u, depth_u), finish(base_v, mask_v, mean_v, depth_v), new_t, new_s)
```

```python
import jax
import jax.numpy as jnp
import numpy as np
from jax import lax
from jax.experimental import pallas as pl
from jax.experimental.pallas import tpu as pltpu
from jax.sharding import PartitionSpec as P

MESH = pl.DeviceIdType.MESH
F32 = jnp.float32
SUBCYCLES = 30
LEVELS = 31
VISC_NUM = 4.0
DIFF_NUM = 1.0
N = 128
W = 32
EXT = N + 2 * W
PR = 16
CHUNKS = ((0, 8), (8, 16), (16, 24), (24, 31))


def solve_coefs(nu):
    inner, last, back = [], [], []
    c_prev = 0.0
    for k in range(LEVELS):
        lo = nu if k > 0 else 0.0
        piv = 1.0 + nu + lo - lo * c_prev
        inner.append(1.0 / piv)
        last.append(1.0 / (1.0 + lo - lo * c_prev))
        c_prev = nu / piv
        back.append(c_prev)
    return inner, last, back


VISC = solve_coefs(VISC_NUM)
DIFF = solve_coefs(DIFF_NUM)


def weights():
    s = np.arange(1, SUBCYCLES + 1, dtype=np.float64) / (SUBCYCLES + 1)
    w = s ** 2 * (1.0 - s ** 4)
    return (w / w.sum()).astype(np.float32)


def lane_of(field, k):
    return 2 * ((field % 2) * LEVELS + k) + (field // 2)


def exchange_kernel(ncol, nrow, u_hbm, v_hbm, t_hbm, s_hbm, eta_hbm, tu_hbm, tv_hbm, dep_hbm, kmt_hbm,
                    nu_ref, nv_ref, nt_ref, ns_ref, two_ref, wm_out, we_out, ww_out, fm_out, fe_out, fw_out,
                    fb, ki, kd, edge_e, edge_w, from_w, from_e, cor_nw, cor_se, m1, m2,
                    wm, pk_e, pk_w, we, ww, fm, fk_e, fk_w, fe, fw,
                    ld_sem, in_sem, snd, rcv):
    c = lax.axis_index('col')
    r = lax.axis_index('row')
    east = lax.rem(c + 1, ncol)
    west = lax.rem(c + ncol - 1, ncol)
    north = lax.rem(r + 1, nrow)
    south = lax.rem(r + nrow - 1, nrow)
    has_n = r < nrow - 1
    has_s = r > 0

    src3 = (u_hbm, v_hbm, t_hbm, s_hbm)
    small = [pltpu.make_async_copy(kmt_hbm, ki, in_sem.at[0]),
             pltpu.make_async_copy(dep_hbm, kd.at[1, pl.ds(8, N), :], in_sem.at[1]),
             pltpu.make_async_copy(eta_hbm, wm.at[0, pl.ds(W, N), :], in_sem.at[2]),
             pltpu.make_async_copy(tu_hbm, wm.at[1, pl.ds(W, N), :], in_sem.at[3]),
             pltpu.make_async_copy(tv_hbm, wm.at[2, pl.ds(W, N), :], in_sem.at[4])]
    loads = []
    for ci, (k0, k1) in enumerate(CHUNKS):
        row = [pltpu.make_async_copy(src3[f].at[pl.ds(k0, k1 - k0)], fb.at[f, pl.ds(k0, k1 - k0), pl.ds(8, N), :],
                                     ld_sem.at[f, ci]) for f in range(4)]
        loads.append(row)
        for cp in row:
            cp.start()
        if ci == 0:
            for cp in small:
                cp.start()

    barrier = pltpu.get_barrier_semaphore()
    places = [(east, r), (west, r), (c, north), (c, south), (east, north), (east, south), (west, north), (west, south)]
    for cc, rr in places:
        pl.semaphore_signal(barrier, inc=1, device_id={'col': cc, 'row': rr}, device_id_type=MESH)

    lane = lax.broadcasted_iota(jnp.int32, (N, N), 1)
    for cp in small:
        cp.wait()
    kmt_f = ki[...].astype(F32)
    dep = kd[1, 8:8 + N, :]
    kd[0, 8:8 + N, :] = kmt_f
    wm[3, W:W + N, :] = jnp.where(kmt_f > 0.0, dep, 0.0)

    even = lax.rem(lane, 2) == 0
    pair_a = lane // 2
    pair_b = lax.rem(lane + (N - 1), N) // 2
    acc_a = jnp.zeros((N, N), F32)
    acc_b = jnp.zeros((N, N), F32)

    def put(acc, pair, x, l):
        return jnp.where(pair == l // 2, pltpu.roll(x, (l + 1) % N, 1), acc)

    acc_a = put(acc_a, pair_a, kmt_f, 124)
    acc_b = put(acc_b, pair_b, dep, 125)
    for ci, (k0, k1) in enumerate(CHUNKS):
        for cp in loads[ci]:
            cp.wait()
        for k in range(k0, k1):
            for f in range(2):
                acc_a = put(acc_a, pair_a, fb[f, k, 8:8 + N, :], lane_of(f, k))
                acc_b = put(acc_b, pair_b, fb[f + 2, k, 8:8 + N, :], lane_of(f + 2, k))
    edge_e[...] = jnp.where(even, acc_a, acc_b)
    edge_w[...] = jnp.where(even, acc_b, acc_a)

    pl.semaphore_wait(barrier, len(places))

    def copy(i, src, dst, cc, rr):
        return pltpu.make_async_remote_copy(src_ref=src, dst_ref=dst, send_sem=snd.at[i], recv_sem=rcv.at[i],
                                            device_id={'col': cc, 'row': rr}, device_id_type=MESH)

    thin = [
        (copy(0, fb.at[:, :, pl.ds(8, 1), :], fb.at[:, :, pl.ds(8 + N, 1), :], c, south), has_s, has_n),
        (copy(1, fb.at[:, :, pl.ds(7 + N, 1), :], fb.at[:, :, pl.ds(7, 1), :], c, north), has_n, has_s),
        (copy(2, kd.at[:, pl.ds(8, 1), :], kd.at[:, pl.ds(8 + N, 1), :], c, south), has_s, has_n),
        (copy(3, kd.at[:, pl.ds(7 + N, 1), :], kd.at[:, pl.ds(7, 1), :], c, north), has_n, has_s),
        (copy(4, edge_e, from_w, east, r), None, None),
        (copy(5, edge_w, from_e, west, r), None, None),
        (copy(6, edge_e.at[pl.ds(0, 8), :], cor_nw, east, south), has_s, has_n),
        (copy(7, edge_w.at[pl.ds(N - 8, 8), :], cor_se, west, north), has_n, has_s),
    ]

    def wide_set(base, main, to_e, to_w, got_e, got_w):
        lo, hi = pl.ds(0, W), pl.ds(N - W, W)
        return [
            (copy(base + 0, to_w, got_e.at[pl.ds(W, N), :], west, r), None, None),
            (copy(base + 1, to_e, got_w.at[pl.ds(W, N), :], east, r), None, None),
            (copy(base + 2, main.at[:, pl.ds(W, W), :], main.at[:, pl.ds(W + N, W), :], c, south), has_s, has_n),
            (copy(base + 3, main.at[:, pl.ds(N, W), :], main.at[:, pl.ds(0, W), :], c, north), has_n, has_s),
            (copy(base + 4, to_w.at[lo, :], got_e.at[pl.ds(W + N, W), :], west, south), has_s, has_n),
            (copy(base + 5, to_w.at[hi, :], got_e.at[lo, :], west, north), has_n, has_s),
            (copy(base + 6, to_e.at[lo, :], got_w.at[pl.ds(W + N, W), :], east, south), has_s, has_n),
            (copy(base + 7, to_e.at[hi, :], got_w.at[lo, :], east, north), has_n, has_s),
        ]

    wide = wide_set(8, wm, pk_e, pk_w, we, ww)
    forc = wide_set(16, fm, fk_e, fk_w, fe, fw)

    def run(cond, fn):
        if cond is None:
            fn()
        else:
            pl.when(cond)(fn)

    def start(items):
        for cp, s_if, _ in items:
            run(s_if, cp.start)

    def wait_recv(items):
        for cp, _, r_if in items:
            run(r_if, cp.wait_recv)

    def wait_send(items):
        for cp, s_if, _ in items:
            run(s_if, cp.wait_send)

    start(thin)

    def pack(fields):
        e_acc = jnp.zeros((N, N), F32)
        w_acc = jnp.zeros((N, N), F32)
        for f, x in enumerate(fields):
            slot = lane // W == f
            w_acc = jnp.where(slot, pltpu.roll(x, W * f, 1) if f else x, w_acc)
            sh = (W * (f + 1)) % N
            e_acc = jnp.where(slot, pltpu.roll(x, sh, 1) if sh else x, e_acc)
        return e_acc, w_acc

    e_acc, w_acc = pack([wm[f, W:W + N, :] for f in range(4)])
    pk_e[...] = e_acc
    pk_w[...] = w_acc
    start(wide)

    @pl.when(jnp.logical_not(has_n))
    def _():
        fb[:, :, 8 + N:9 + N, :] = jnp.zeros((4, LEVELS, 1, N), F32)
        kd[:, 8 + N:9 + N, :] = jnp.zeros((2, 1, N), F32)
        cor_nw[...] = jnp.zeros((8, N), F32)

    @pl.when(jnp.logical_not(has_s))
    def _():
        fb[:, :, 7:8, :] = jnp.zeros((4, LEVELS, 1, N), F32)
        kd[:, 7:8, :] = jnp.zeros((2, 1, N), F32)
        cor_se[...] = jnp.zeros((8, N), F32)

    wait_recv(thin)

    got_w = from_w[...]
    got_e = pltpu.roll(from_e[...], N - 2, 1)
    m1[8:8 + N, :] = jnp.where(even, got_w, got_e)
    m2[8:8 + N, :] = jnp.where(even, got_e, got_w)
    m1[8 + N:16 + N, :] = cor_nw[...]
    m1[0:8, :] = pltpu.roll(cor_se[...], N - 2, 1)

    lane_p = lax.broadcasted_iota(jnp.int32, (PR, N), 1)
    is_w = lane_p == 0
    is_e = lane_p == N - 1

    def hal(src, off, base, l):
        return pltpu.roll(src[pl.ds(base + off, PR), :], (N - l) % N, 1)

    def to_e(x, h):
        return jnp.where(is_e, h, pltpu.roll(x, N - 1, 1))

    def to_w(x, h):
        return jnp.where(is_w, h, pltpu.roll(x, 1, 1))

    def force_step(g, _):
        own = pl.multiple_of(g * PR, PR)
        base = own + 8

        def at(f, k, off):
            return fb[f, k, pl.ds(base + off, PR), :]

        kc = kd[0, pl.ds(base, PR), :]
        kn = kd[0, pl.ds(base + 1, PR), :]
        dc = kd[1, pl.ds(base, PR), :]
        dn = kd[1, pl.ds(base + 1, PR), :]
        ke = to_e(kc, hal(m1, 0, base, 124))
        de = to_e(dc, hal(m2, 0, base, 125))
        th_c = dc / jnp.maximum(kc, 1.0)
        th_e = de / jnp.maximum(ke, 1.0)
        th_n = dn / jnp.maximum(kn, 1.0)
        nu_f = jnp.minimum(kc, ke)
        nv_f = jnp.minimum(kc, kn)
        zero = jnp.zeros((PR, N), F32)
        cum_c, cum_e, cum_n, sum_u, sum_v = zero, zero, zero, zero, zero
        for k in range(LEVELS):
            fk = float(k)
            t_c, s_c = at(2, k, 0), at(3, k, 0)
            t_e = to_e(t_c, hal(m2, 0, base, lane_of(2, k)))
            s_e = to_e(s_c, hal(m2, 0, base, lane_of(3, k)))
            t_n, s_n = at(2, k, 1), at(3, k, 1)
            d_c = jnp.where(kc > fk, 0.6 * s_c - 0.3 * t_c, 0.0)
            d_e = jnp.where(ke > fk, 0.6 * s_e - 0.3 * t_e, 0.0)
            d_n = jnp.where(kn > fk, 0.6 * s_n - 0.3 * t_n, 0.0)
            cum_c, cum_e, cum_n = cum_c + d_c, cum_e + d_e, cum_n + d_n
            p_c = (cum_c - 0.5 * d_c) * th_c
            p_e = (cum_e - 0.5 * d_e) * th_e
            p_n = (cum_n - 0.5 * d_n) * th_n
            u_c, v_c = at(0, k, 0), at(1, k, 0)
            u_n, v_n = at(0, k, 1), at(1, k, 1)
            u_s, v_s = at(0, k, -1), at(1, k, -1)
            lu, lv = lane_of(0, k), lane_of(1, k)
            h_u = hal(m1, 0, base, lu)
            h_v = hal(m1, 0, base, lv)
            h_us = pltpu.roll(m1[pl.ds(base, PR), :] + m1[pl.ds(base + 1, PR), :], (N - lu) % N, 1)
            h_vs = pltpu.roll(m1[pl.ds(base, PR), :] + m1[pl.ds(base - 1, PR), :], (N - lv) % N, 1)
            us = u_c + u_n
            vs = v_c + v_s
            v_at_u = 0.25 * (vs + to_e(vs, h_vs))
            u_at_v = 0.25 * (us + to_w(us, h_us))
            du_x = to_e(u_c, h_u) - to_w(u_c, h_u)
            dv_x = to_e(v_c, h_v) - to_w(v_c, h_v)
            wet_u = nu_f > fk
            wet_v = nv_f > fk
            g_u = p_c - p_e - 0.5 * (u_c * du_x + v_at_u * (u_n - u_s))
            g_v = p_c - p_n - 0.5 * (u_at_v * dv_x + v_c * (v_n - v_s))
            sum_u = sum_u + jnp.where(wet_u, g_u, 0.0)
            sum_v = sum_v + jnp.where(wet_v, g_v, 0.0)
            nu_ref[k, pl.ds(own, PR), :] = jnp.where(wet_u, u_c + 0.25 * g_u, 0.0)
            nv_ref[k, pl.ds(own, PR), :] = jnp.where(wet_v, v_c + 0.25 * g_v, 0.0)
        hu = jnp.where(nu_f > 0.0, 0.5 * (dc + de), 0.0)
        hv = jnp.where(nv_f > 0.0, 0.5 * (dc + dn), 0.0)
        fm[0, pl.ds(own + W, PR), :] = hu * (1.0 / jnp.maximum(nu_f, 1.0)) * sum_u
        fm[1, pl.ds(own + W, PR), :] = hv * (1.0 / jnp.maximum(nv_f, 1.0)) * sum_v
        two_ref[0, pl.ds(own, PR), :] = nu_f
        two_ref[1, pl.ds(own, PR), :] = nv_f
        return 0

    lax.fori_loop(0, N // PR, force_step, 0)

    e_acc, w_acc = pack([fm[f, W:W + N, :] for f in range(2)])
    fk_e[...] = e_acc
    fk_w[...] = w_acc
    start(forc)

    def solve_step(g, _):
        own = pl.multiple_of(g * PR, PR)
        base = own + 8

        def at(f, k, off):
            return fb[f, k, pl.ds(base + off, PR), :]

        kc = kd[0, pl.ds(base, PR), :]
        kn = kd[0, pl.ds(base + 1, PR), :]
        ks = kd[0, pl.ds(base - 1, PR), :]
        h_k = hal(m1, 0, base, 124)
        nu_f = jnp.minimum(kc, to_e(kc, h_k))
        nw_f = jnp.minimum(kc, to_w(kc, h_k))
        nv_f = jnp.minimum(kc, kn)
        nq_f = jnp.minimum(kc, ks)
        zero = jnp.zeros((PR, N), F32)
        d_u, d_v, d_t, d_s = zero, zero, zero, zero

        def factor(n_f, k, co):
            return jnp.where(n_f > k + 1.0, co[0][k], jnp.where(n_f > float(k), co[1][k], 0.0))

        for k in range(LEVELS):
            fk = float(k)
            t_c, s_c = at(2, k, 0), at(3, k, 0)
            h_t = hal(m2, 0, base, lane_of(2, k))
            h_s = hal(m2, 0, base, lane_of(3, k))
            u_c, v_c = at(0, k, 0), at(1, k, 0)
            u_e = jnp.where(nu_f > fk, u_c, 0.0)
            u_w = jnp.where(nw_f > fk, to_w(u_c, hal(m1, 0, base, lane_of(0, k))), 0.0)
            v_n = jnp.where(nv_f > fk, v_c, 0.0)
            v_s = jnp.where(nq_f > fk, at(1, k, -1), 0.0)
            a_e = jnp.minimum(u_e, 0.0)
            a_w = jnp.maximum(u_w, 0.0)
            a_n = jnp.minimum(v_n, 0.0)
            a_s = jnp.maximum(v_s, 0.0)
            a_c = (jnp.maximum(u_e, 0.0) - jnp.minimum(u_w, 0.0)) + (jnp.maximum(v_n, 0.0) - jnp.minimum(v_s, 0.0))
            fac = factor(kc, k, DIFF)

            def step(x, h, f):
                div = a_c * x + (a_e * to_e(x, h) - a_w * to_w(x, h)) + (a_n * at(f, k, 1) - a_s * at(f, k, -1))
                return x - 0.25 * div

            d_t = (step(t_c, h_t, 2) + DIFF_NUM * d_t) * fac
            d_s = (step(s_c, h_s, 3) + DIFF_NUM * d_s) * fac
            nt_ref[k, pl.ds(own, PR), :] = d_t
            ns_ref[k, pl.ds(own, PR), :] = d_s
            d_u = (nu_ref[k, pl.ds(own, PR), :] + VISC_NUM * d_u) * factor(nu_f, k, VISC)
            d_v = (nv_ref[k, pl.ds(own, PR), :] + VISC_NUM * d_v) * factor(nv_f, k, VISC)
            nu_ref[k, pl.ds(own, PR), :] = d_u
            nv_ref[k, pl.ds(own, PR), :] = d_v
        sum_u, sum_v = d_u, d_v
        for k in range(LEVELS - 2, -1, -1):
            d_t = nt_ref[k, pl.ds(own, PR), :] + DIFF[2][k] * d_t
            d_s = ns_ref[k, pl.ds(own, PR), :] + DIFF[2][k] * d_s
            d_u = nu_ref[k, pl.ds(own, PR), :] + VISC[2][k] * d_u
            d_v = nv_ref[k, pl.ds(own, PR), :] + VISC[2][k] * d_v
            nt_ref[k, pl.ds(own, PR), :] = d_t
            ns_ref[k, pl.ds(own, PR), :] = d_s
            nu_ref[k, pl.ds(own, PR), :] = d_u
            nv_ref[k, pl.ds(own, PR), :] = d_v
            sum_u, sum_v = sum_u + d_u, sum_v + d_v
        two_ref[2, pl.ds(own, PR), :] = sum_u / jnp.maximum(nu_f, 1.0)
        two_ref[3, pl.ds(own, PR), :] = sum_v / jnp.maximum(nv_f, 1.0)
        return 0

    lax.fori_loop(0, N // PR, solve_step, 0)

    wait_recv(wide)
    wait_recv(forc)
    wm_out[...] = wm[...]
    we_out[...] = we[...]
    ww_out[...] = ww[...]
    fm_out[...] = fm[...]
    fe_out[...] = fe[...]
    fw_out[...] = fw[...]
    wait_send(thin)
    wait_send(wide)
    wait_send(forc)


TOP = EXT + 16


def step_kernel(nrow, nu_ref, nv_ref, nt_ref, ns_ref, two_ref, wm, we, ww, fm, fe, fw,
                eta_out, tu_out, tv_out, u_hbm, v_hbm, t_hbm, s_hbm,
                et, fu, fv, cu, cv, pu, pv, dm, mean, ub, vb, osem):
    r = lax.axis_index('row')
    copies = [pltpu.make_async_copy(nt_ref, t_hbm, osem.at[0]), pltpu.make_async_copy(ns_ref, s_hbm, osem.at[1])]
    for cp in copies:
        cp.start()

    lane = lax.broadcasted_iota(jnp.int32, (EXT, N), 1)
    rows = lax.broadcasted_iota(jnp.int32, (EXT, N), 0)
    last = lane == N - 1
    first = lane == 0
    lo_ok = jnp.where(r > 0, 0, W)
    hi_ok = jnp.where(r < nrow - 1, EXT, W + N)
    real = (rows >= lo_ok) & (rows < hi_ok)
    in_e = lane < W
    in_w = lane >= N - W

    def side(e_ref, w_ref, f):
        e = e_ref[...]
        w = w_ref[...]
        se = (N - W * f) % N
        sw = (2 * N - W * (f + 1)) % N
        e = pltpu.roll(e, se, 1) if se else e
        w = pltpu.roll(w, sw, 1) if sw else w
        return jnp.where(in_e, e, jnp.where(in_w, w, 0.0))

    def east_of(a, b):
        ra, rb = pltpu.roll(a, N - 1, 1), pltpu.roll(b, N - 1, 1)
        return jnp.where(last, rb, ra), jnp.where(last, ra, rb)

    def west_of(a, b):
        ra, rb = pltpu.roll(a, 1, 1), pltpu.roll(b, 1, 1)
        return jnp.where(first, rb, ra), jnp.where(first, ra, rb)

    body = pl.ds(8, EXT)
    zero8 = jnp.zeros((8, N), F32)
    for ref in (et, fu, fv, dm):
        for t in range(2):
            ref[t, 0:8, :] = zero8
            ref[t, 8 + EXT:TOP, :] = zero8

    dms = (jnp.where(real, wm[3], 0.0), jnp.where(real & (in_e | in_w), side(we, ww, 3), 0.0))
    for t in range(2):
        dm[t, body, :] = dms[t]
    dme = east_of(*dms)
    for t in range(2):
        d_c = dms[t]
        d_n = dm[t, 9:9 + EXT, :]
        wet_u = (d_c > 0.0) & (dme[t] > 0.0)
        wet_v = (d_c > 0.0) & (d_n > 0.0)
        pick = (lambda f: wm[f]) if t == 0 else (lambda f: side(we, ww, f))
        fpick = (lambda f: fm[f]) if t == 0 else (lambda f: side(fe, fw, f))
        et[t, body, :] = jnp.where(d_c > 0.0, pick(0), 0.0)
        fu[t, body, :] = jnp.where(wet_u, 0.5 * pick(1), 0.0)
        fv[t, body, :] = jnp.where(wet_v, 0.5 * pick(2), 0.0)
        cu[t] = jnp.where(wet_u, 0.125 * (d_c + dme[t]), 0.0)
        cv[t] = jnp.where(wet_v, 0.125 * (d_c + d_n), 0.0)
        pu[t] = jnp.where(wet_u, (0.125 / SUBCYCLES) * fpick(0), 0.0)
        pv[t] = jnp.where(wet_v, (0.125 / SUBCYCLES) * fpick(1), 0.0)
    mean[...] = jnp.zeros((2, N, N), F32)

    inner = float(SUBCYCLES + 1)
    wsum = 0.0
    for n in range(1, SUBCYCLES + 1):
        wsum += (n / inner) ** 2 * (1.0 - (n / inner) ** 4)

    def cycle(n, _):
        frac = (n + 1).astype(F32) * (1.0 / inner)
        f2 = frac * frac
        wgt = f2 * (1.0 - f2 * f2) * (1.0 / wsum)
        us = (fu[0, body, :], fu[1, body, :])
        uw = west_of(*us)
        new = []
        for t in range(2):
            e = et[t, body, :] - ((us[t] - uw[t]) + (fv[t, body, :] - fv[t, 7:7 + EXT, :]))
            et[t, body, :] = e
            new.append(e)
        ee = east_of(*new)
        for t in range(2):
            u = us[t] - cu[t] * (ee[t] - new[t]) + pu[t]
            v = fv[t, body, :] - cv[t] * (et[t, 9:9 + EXT, :] - new[t]) + pv[t]
            fu[t, body, :] = u
            fv[t, body, :] = v
        mean[0] = mean[0] + wgt * fu[0, 8 + W:8 + W + N, :]
        mean[1] = mean[1] + wgt * fv[0, 8 + W:8 + W + N, :]
        return 0

    lax.fori_loop(0, SUBCYCLES, cycle, 0)

    mid = slice(8 + W, 8 + W + N)
    eta_out[...] = et[0, mid, :]
    tu_out[...] = 2.0 * fu[0, mid, :]
    tv_out[...] = 2.0 * fv[0, mid, :]
    for i, co in ((0, cu), (1, cv)):
        h = co[0, W:W + N, :]
        mean[i] = mean[i] / jnp.where(h > 0.0, 2.0 * h, 1.0) - two_ref[2 + i]

    for ci, (k0, k1) in enumerate(CHUNKS):
        for i, (src, buf, dst) in enumerate(((nu_ref, ub, u_hbm), (nv_ref, vb, v_hbm))):
            for k in range(k0, k1):
                buf[k] = src[k] + jnp.where(two_ref[i] > float(k), mean[i], 0.0)
            cp = pltpu.make_async_copy(buf.at[pl.ds(k0, k1 - k0)], dst.at[pl.ds(k0, k1 - k0)], osem.at[2 + 2 * ci + i])
            cp.start()
            copies.append(cp)
    for cp in copies:
        cp.wait()


def solution(mesh):
    ncol, nrow = mesh.shape['col'], mesh.shape['row']
    vmem = pl.BlockSpec(memory_space=pltpu.VMEM)
    hbm = pl.BlockSpec(memory_space=pltpu.HBM)
    s3 = jax.ShapeDtypeStruct((LEVELS, N, N), F32)
    s2 = jax.ShapeDtypeStruct((N, N), F32)

    def sds(*shape):
        return jax.ShapeDtypeStruct(shape, F32)

    def ocean_step(vel_u, vel_v, temp, salt, eta, tu, tv, dep, kmt):
        def kernel_a(*refs):
            exchange_kernel(ncol, nrow, *refs)

        def kernel_b(*refs):
            step_kernel(nrow, *refs)

        mid = pl.pallas_call(
            kernel_a,
            name='exchange',
            out_shape=(s3, s3, s3, s3, sds(4, N, N), sds(4, EXT, N), sds(EXT, N), sds(EXT, N), sds(2, EXT, N), sds(EXT, N), sds(EXT, N)),
            in_specs=[hbm] * 9,
            out_specs=(vmem,) * 11,
            scratch_shapes=[
                pltpu.VMEM((4, LEVELS, N + 16, N), F32),
                pltpu.VMEM((N, N), jnp.int32),
                pltpu.VMEM((2, N + 16, N), F32),
                pltpu.VMEM((N, N), F32), pltpu.VMEM((N, N), F32),
                pltpu.VMEM((N, N), F32), pltpu.VMEM((N, N), F32),
                pltpu.VMEM((8, N), F32), pltpu.VMEM((8, N), F32),
                pltpu.VMEM((N + 16, N), F32), pltpu.VMEM((N + 16, N), F32),
                pltpu.VMEM((4, EXT, N), F32),
                pltpu.VMEM((N, N), F32), pltpu.VMEM((N, N), F32),
                pltpu.VMEM((EXT, N), F32), pltpu.VMEM((EXT, N), F32),
                pltpu.VMEM((2, EXT, N), F32),
                pltpu.VMEM((N, N), F32), pltpu.VMEM((N, N), F32),
                pltpu.VMEM((EXT, N), F32), pltpu.VMEM((EXT, N), F32),
                pltpu.SemaphoreType.DMA((4, len(CHUNKS))),
                pltpu.SemaphoreType.DMA((5,)),
                pltpu.SemaphoreType.DMA((24,)),
                pltpu.SemaphoreType.DMA((24,)),
            ],
            compiler_params=pltpu.CompilerParams(collective_id=0, has_side_effects=True, vmem_limit_bytes=28 * 2 ** 20),
        )(vel_u, vel_v, temp, salt, eta, tu, tv, dep, kmt)
        st = pltpu.VMEM((2, TOP, N), F32)
        co = pltpu.VMEM((2, EXT, N), F32)
        out = pl.pallas_call(
            kernel_b,
            name='subcycles',
            out_shape=(s2, s2, s2, s3, s3, s3, s3),
            in_specs=[vmem] * 11,
            out_specs=(vmem,) * 3 + (hbm,) * 4,
            scratch_shapes=[st, st, st, co, co, co, co, st, pltpu.VMEM((2, N, N), F32),
                            pltpu.VMEM((LEVELS, N, N), F32), pltpu.VMEM((LEVELS, N, N), F32),
                            pltpu.SemaphoreType.DMA((2 + 2 * len(CHUNKS),))],
            compiler_params=pltpu.CompilerParams(vmem_limit_bytes=28 * 2 ** 20),
        )(*mid)
        return out

    spec_3d = P(None, 'row', 'col')
    spec_2d = P('row', 'col')
    return jax.shard_map(ocean_step, mesh=mesh, in_specs=(spec_3d,) * 4 + (spec_2d,) * 5,
                         out_specs=(spec_2d,) * 3 + (spec_3d,) * 4, check_vma=False)
```

```python
import jax
import jax.numpy as jnp
import numpy as np
from jax import lax
from jax.experimental import pallas as pl
from jax.experimental.pallas import tpu as pltpu
from jax.sharding import PartitionSpec as P

MESH = pl.DeviceIdType.MESH
F32 = jnp.float32
SUBCYCLES = 30
LEVELS = 31
VISC_NUM = 4.0
DIFF_NUM = 1.0
N = 128
W = 32
EXT = N + 2 * W
PR = 16
CHUNKS = ((0, 8), (8, 16), (16, 24), (24, 31))


def solve_coefs(nu):
    inner, last, back = [], [], []
    c_prev = 0.0
    for k in range(LEVELS):
        lo = nu if k > 0 else 0.0
        piv = 1.0 + nu + lo - lo * c_prev
        inner.append(1.0 / piv)
        last.append(1.0 / (1.0 + lo - lo * c_prev))
        c_prev = nu / piv
        back.append(c_prev)
    return inner, last, back


VISC = solve_coefs(VISC_NUM)
DIFF = solve_coefs(DIFF_NUM)


def weights():
    s = np.arange(1, SUBCYCLES + 1, dtype=np.float64) / (SUBCYCLES + 1)
    w = s ** 2 * (1.0 - s ** 4)
    return (w / w.sum()).astype(np.float32)


def lane_of(field, k):
    return 2 * ((field % 2) * LEVELS + k) + (field // 2)


def exchange_kernel(ncol, nrow, u_hbm, v_hbm, t_hbm, s_hbm, eta_hbm, tu_hbm, tv_hbm, dep_hbm, kmt_hbm,
                    nu_ref, nv_ref, nt_ref, ns_ref, two_ref, wm_out, we_out, ww_out, fm_out, fe_out, fw_out,
                    fb, ki, kd, edge_e, edge_w, from_w, from_e, cor_nw, cor_se, m1, m2,
                    wm, pk_e, pk_w, we, ww, fm, fk_e, fk_w, fe, fw,
                    ld_sem, in_sem, snd, rcv):
    c = lax.axis_index('col')
    r = lax.axis_index('row')
    east = lax.rem(c + 1, ncol)
    west = lax.rem(c + ncol - 1, ncol)
    north = lax.rem(r + 1, nrow)
    south = lax.rem(r + nrow - 1, nrow)
    has_n = r < nrow - 1
    has_s = r > 0

    src3 = (u_hbm, v_hbm, t_hbm, s_hbm)
    small = [pltpu.make_async_copy(kmt_hbm, ki, in_sem.at[0]),
             pltpu.make_async_copy(dep_hbm, kd.at[1, pl.ds(8, N), :], in_sem.at[1]),
             pltpu.make_async_copy(eta_hbm, wm.at[0, pl.ds(W, N), :], in_sem.at[2]),
             pltpu.make_async_copy(tu_hbm, wm.at[1, pl.ds(W, N), :], in_sem.at[3]),
             pltpu.make_async_copy(tv_hbm, wm.at[2, pl.ds(W, N), :], in_sem.at[4])]
    loads = []
    for ci, (k0, k1) in enumerate(CHUNKS):
        row = [pltpu.make_async_copy(src3[f].at[pl.ds(k0, k1 - k0)], fb.at[f, pl.ds(k0, k1 - k0), pl.ds(8, N), :],
                                     ld_sem.at[f, ci]) for f in range(4)]
        loads.append(row)
        for cp in row:
            cp.start()
        if ci == 0:
            for cp in small:
                cp.start()

    barrier = pltpu.get_barrier_semaphore()
    places = [(east, r), (west, r), (c, north), (c, south), (east, north), (east, south), (west, north), (west, south)]
    for cc, rr in places:
        pl.semaphore_signal(barrier, inc=1, device_id={'col': cc, 'row': rr}, device_id_type=MESH)

    lane = lax.broadcasted_iota(jnp.int32, (N, N), 1)
    for cp in small:
        cp.wait()
    kmt_f = ki[...].astype(F32)
    dep = kd[1, 8:8 + N, :]
    kd[0, 8:8 + N, :] = kmt_f
    wm[3, W:W + N, :] = jnp.where(kmt_f > 0.0, dep, 0.0)

    even = lax.rem(lane, 2) == 0
    pair_a = lane // 2
    pair_b = lax.rem(lane + (N - 1), N) // 2
    acc_a = jnp.zeros((N, N), F32)
    acc_b = jnp.zeros((N, N), F32)

    def put(acc, pair, x, l):
        return jnp.where(pair == l // 2, pltpu.roll(x, (l + 1) % N, 1), acc)

    acc_a = put(acc_a, pair_a, kmt_f, 124)
    acc_b = put(acc_b, pair_b, dep, 125)
    for ci, (k0, k1) in enumerate(CHUNKS):
        for cp in loads[ci]:
            cp.wait()
        for k in range(k0, k1):
            for f in range(2):
                acc_a = put(acc_a, pair_a, fb[f, k, 8:8 + N, :], lane_of(f, k))
                acc_b = put(acc_b, pair_b, fb[f + 2, k, 8:8 + N, :], lane_of(f + 2, k))
    edge_e[...] = jnp.where(even, acc_a, acc_b)
    edge_w[...] = jnp.where(even, acc_b, acc_a)

    pl.semaphore_wait(barrier, len(places))

    def copy(i, src, dst, cc, rr):
        return pltpu.make_async_remote_copy(src_ref=src, dst_ref=dst, send_sem=snd.at[i], recv_sem=rcv.at[i],
                                            device_id={'col': cc, 'row': rr}, device_id_type=MESH)

    thin = [
        (copy(0, fb.at[:, :, pl.ds(8, 1), :], fb.at[:, :, pl.ds(8 + N, 1), :], c, south), has_s, has_n),
        (copy(1, fb.at[:, :, pl.ds(7 + N, 1), :], fb.at[:, :, pl.ds(7, 1), :], c, north), has_n, has_s),
        (copy(2, kd.at[:, pl.ds(8, 1), :], kd.at[:, pl.ds(8 + N, 1), :], c, south), has_s, has_n),
        (copy(3, kd.at[:, pl.ds(7 + N, 1), :], kd.at[:, pl.ds(7, 1), :], c, north), has_n, has_s),
        (copy(4, edge_e, from_w, east, r), None, None),
        (copy(5, edge_w, from_e, west, r), None, None),
        (copy(6, edge_e.at[pl.ds(0, 8), :], cor_nw, east, south), has_s, has_n),
        (copy(7, edge_w.at[pl.ds(N - 8, 8), :], cor_se, west, north), has_n, has_s),
    ]

    def wide_set(base, main, to_e, to_w, got_e, got_w):
        lo, hi = pl.ds(0, W), pl.ds(N - W, W)
        return [
            (copy(base + 0, to_w, got_e.at[pl.ds(W, N), :], west, r), None, None),
            (copy(base + 1, to_e, got_w.at[pl.ds(W, N), :], east, r), None, None),
            (copy(base + 2, main.at[:, pl.ds(W, W), :], main.at[:, pl.ds(W + N, W), :], c, south), has_s, has_n),
            (copy(base + 3, main.at[:, pl.ds(N, W), :], main.at[:, pl.ds(0, W), :], c, north), has_n, has_s),
            (copy(base + 4, to_w.at[lo, :], got_e.at[pl.ds(W + N, W), :], west, south), has_s, has_n),
            (copy(base + 5, to_w.at[hi, :], got_e.at[lo, :], west, north), has_n, has_s),
            (copy(base + 6, to_e.at[lo, :], got_w.at[pl.ds(W + N, W), :], east, south), has_s, has_n),
            (copy(base + 7, to_e.at[hi, :], got_w.at[lo, :], east, north), has_n, has_s),
        ]

    wide = wide_set(8, wm, pk_e, pk_w, we, ww)
    forc = wide_set(16, fm, fk_e, fk_w, fe, fw)

    def run(cond, fn):
        if cond is None:
            fn()
        else:
            pl.when(cond)(fn)

    def start(items):
        for cp, s_if, _ in items:
            run(s_if, cp.start)

    def wait_recv(items):
        for cp, _, r_if in items:
            run(r_if, cp.wait_recv)

    def wait_send(items):
        for cp, s_if, _ in items:
            run(s_if, cp.wait_send)

    start(thin)

    def pack(fields):
        e_acc = jnp.zeros((N, N), F32)
        w_acc = jnp.zeros((N, N), F32)
        for f, x in enumerate(fields):
            slot = lane // W == f
            w_acc = jnp.where(slot, pltpu.roll(x, W * f, 1) if f else x, w_acc)
            sh = (W * (f + 1)) % N
            e_acc = jnp.where(slot, pltpu.roll(x, sh, 1) if sh else x, e_acc)
        return e_acc, w_acc

    e_acc, w_acc = pack([wm[f, W:W + N, :] for f in range(4)])
    pk_e[...] = e_acc
    pk_w[...] = w_acc
    start(wide)

    @pl.when(jnp.logical_not(has_n))
    def _():
        fb[:, :, 8 + N:9 + N, :] = jnp.zeros((4, LEVELS, 1, N), F32)
        kd[:, 8 + N:9 + N, :] = jnp.zeros((2, 1, N), F32)
        cor_nw[...] = jnp.zeros((8, N), F32)

    @pl.when(jnp.logical_not(has_s))
    def _():
        fb[:, :, 7:8, :] = jnp.zeros((4, LEVELS, 1, N), F32)
        kd[:, 7:8, :] = jnp.zeros((2, 1, N), F32)
        cor_se[...] = jnp.zeros((8, N), F32)

    wait_recv(thin)

    got_w = from_w[...]
    got_e = pltpu.roll(from_e[...], N - 2, 1)
    m1[8:8 + N, :] = jnp.where(even, got_w, got_e)
    m2[8:8 + N, :] = jnp.where(even, got_e, got_w)
    m1[8 + N:16 + N, :] = cor_nw[...]
    m1[0:8, :] = pltpu.roll(cor_se[...], N - 2, 1)

    lane_p = lax.broadcasted_iota(jnp.int32, (PR, N), 1)
    is_w = lane_p == 0
    is_e = lane_p == N - 1

    def hal(src, off, base, l):
        return pltpu.roll(src[pl.ds(base + off, PR), :], (N - l) % N, 1)

    def to_e(x, h):
        return jnp.where(is_e, h, pltpu.roll(x, N - 1, 1))

    def to_w(x, h):
        return jnp.where(is_w, h, pltpu.roll(x, 1, 1))

    def force_step(g, _):
        own = pl.multiple_of(g * PR, PR)
        base = own + 8

        def at(f, k, off):
            return fb[f, k, pl.ds(base + off, PR), :]

        kc = kd[0, pl.ds(base, PR), :]
        kn = kd[0, pl.ds(base + 1, PR), :]
        dc = kd[1, pl.ds(base, PR), :]
        dn = kd[1, pl.ds(base + 1, PR), :]
        ke = to_e(kc, hal(m1, 0, base, 124))
        de = to_e(dc, hal(m2, 0, base, 125))
        th_c = dc / jnp.maximum(kc, 1.0)
        th_e = de / jnp.maximum(ke, 1.0)
        th_n = dn / jnp.maximum(kn, 1.0)
        nu_f = jnp.minimum(kc, ke)
        nv_f = jnp.minimum(kc, kn)
        zero = jnp.zeros((PR, N), F32)
        cum_c, cum_e, cum_n, sum_u, sum_v = zero, zero, zero, zero, zero
        for k in range(LEVELS):
            fk = float(k)
            t_c, s_c = at(2, k, 0), at(3, k, 0)
            t_e = to_e(t_c, hal(m2, 0, base, lane_of(2, k)))
            s_e = to_e(s_c, hal(m2, 0, base, lane_of(3, k)))
            t_n, s_n = at(2, k, 1), at(3, k, 1)
            d_c = jnp.where(kc > fk, 0.6 * s_c - 0.3 * t_c, 0.0)
            d_e = jnp.where(ke > fk, 0.6 * s_e - 0.3 * t_e, 0.0)
            d_n = jnp.where(kn > fk, 0.6 * s_n - 0.3 * t_n, 0.0)
            cum_c, cum_e, cum_n = cum_c + d_c, cum_e + d_e, cum_n + d_n
            p_c = (cum_c - 0.5 * d_c) * th_c
            p_e = (cum_e - 0.5 * d_e) * th_e
            p_n = (cum_n - 0.5 * d_n) * th_n
            u_c, v_c = at(0, k, 0), at(1, k, 0)
            u_n, v_n = at(0, k, 1), at(1, k, 1)
            u_s, v_s = at(0, k, -1), at(1, k, -1)
            lu, lv = lane_of(0, k), lane_of(1, k)
            h_u = hal(m1, 0, base, lu)
            h_v = hal(m1, 0, base, lv)
            h_us = pltpu.roll(m1[pl.ds(base, PR), :] + m1[pl.ds(base + 1, PR), :], (N - lu) % N, 1)
            h_vs = pltpu.roll(m1[pl.ds(base, PR), :] + m1[pl.ds(base - 1, PR), :], (N - lv) % N, 1)
            us = u_c + u_n
            vs = v_c + v_s
            v_at_u = 0.25 * (vs + to_e(vs, h_vs))
            u_at_v = 0.25 * (us + to_w(us, h_us))
            du_x = to_e(u_c, h_u) - to_w(u_c, h_u)
            dv_x = to_e(v_c, h_v) - to_w(v_c, h_v)
            wet_u = nu_f > fk
            wet_v = nv_f > fk
            g_u = p_c - p_e - 0.5 * (u_c * du_x + v_at_u * (u_n - u_s))
            g_v = p_c - p_n - 0.5 * (u_at_v * dv_x + v_c * (v_n - v_s))
            sum_u = sum_u + jnp.where(wet_u, g_u, 0.0)
            sum_v = sum_v + jnp.where(wet_v, g_v, 0.0)
            nu_ref[k, pl.ds(own, PR), :] = jnp.where(wet_u, u_c + 0.25 * g_u, 0.0)
            nv_ref[k, pl.ds(own, PR), :] = jnp.where(wet_v, v_c + 0.25 * g_v, 0.0)
        hu = jnp.where(nu_f > 0.0, 0.5 * (dc + de), 0.0)
        hv = jnp.where(nv_f > 0.0, 0.5 * (dc + dn), 0.0)
        fm[0, pl.ds(own + W, PR), :] = hu * (1.0 / jnp.maximum(nu_f, 1.0)) * sum_u
        fm[1, pl.ds(own + W, PR), :] = hv * (1.0 / jnp.maximum(nv_f, 1.0)) * sum_v
        two_ref[0, pl.ds(own, PR), :] = nu_f
        two_ref[1, pl.ds(own, PR), :] = nv_f
        return 0

    lax.fori_loop(0, N // PR, force_step, 0)

    e_acc, w_acc = pack([fm[f, W:W + N, :] for f in range(2)])
    fk_e[...] = e_acc
    fk_w[...] = w_acc
    start(forc)

    def solve_step(g, _):
        own = pl.multiple_of(g * PR, PR)
        base = own + 8

        def at(f, k, off):
            return fb[f, k, pl.ds(base + off, PR), :]

        kc = kd[0, pl.ds(base, PR), :]
        kn = kd[0, pl.ds(base + 1, PR), :]
        ks = kd[0, pl.ds(base - 1, PR), :]
        h_k = hal(m1, 0, base, 124)
        nu_f = jnp.minimum(kc, to_e(kc, h_k))
        nw_f = jnp.minimum(kc, to_w(kc, h_k))
        nv_f = jnp.minimum(kc, kn)
        nq_f = jnp.minimum(kc, ks)
        zero = jnp.zeros((PR, N), F32)
        d_u, d_v, d_t, d_s = zero, zero, zero, zero

        def factor(n_f, k, co):
            return jnp.where(n_f > k + 1.0, co[0][k], jnp.where(n_f > float(k), co[1][k], 0.0))

        for k in range(LEVELS):
            fk = float(k)
            t_c, s_c = at(2, k, 0), at(3, k, 0)
            h_t = hal(m2, 0, base, lane_of(2, k))
            h_s = hal(m2, 0, base, lane_of(3, k))
            u_c, v_c = at(0, k, 0), at(1, k, 0)
            u_e = jnp.where(nu_f > fk, u_c, 0.0)
            u_w = jnp.where(nw_f > fk, to_w(u_c, hal(m1, 0, base, lane_of(0, k))), 0.0)
            v_n = jnp.where(nv_f > fk, v_c, 0.0)
            v_s = jnp.where(nq_f > fk, at(1, k, -1), 0.0)
            a_e = jnp.minimum(u_e, 0.0)
            a_w = jnp.maximum(u_w, 0.0)
            a_n = jnp.minimum(v_n, 0.0)
            a_s = jnp.maximum(v_s, 0.0)
            a_c = (jnp.maximum(u_e, 0.0) - jnp.minimum(u_w, 0.0)) + (jnp.maximum(v_n, 0.0) - jnp.minimum(v_s, 0.0))
            fac = factor(kc, k, DIFF)

            def step(x, h, f):
                div = a_c * x + (a_e * to_e(x, h) - a_w * to_w(x, h)) + (a_n * at(f, k, 1) - a_s * at(f, k, -1))
                return x - 0.25 * div

            d_t = (step(t_c, h_t, 2) + DIFF_NUM * d_t) * fac
            d_s = (step(s_c, h_s, 3) + DIFF_NUM * d_s) * fac
            nt_ref[k, pl.ds(own, PR), :] = d_t
            ns_ref[k, pl.ds(own, PR), :] = d_s
            d_u = (nu_ref[k, pl.ds(own, PR), :] + VISC_NUM * d_u) * factor(nu_f, k, VISC)
            d_v = (nv_ref[k, pl.ds(own, PR), :] + VISC_NUM * d_v) * factor(nv_f, k, VISC)
            nu_ref[k, pl.ds(own, PR), :] = d_u
            nv_ref[k, pl.ds(own, PR), :] = d_v
        sum_u, sum_v = d_u, d_v
        for k in range(LEVELS - 2, -1, -1):
            d_t = nt_ref[k, pl.ds(own, PR), :] + DIFF[2][k] * d_t
            d_s = ns_ref[k, pl.ds(own, PR), :] + DIFF[2][k] * d_s
            d_u = nu_ref[k, pl.ds(own, PR), :] + VISC[2][k] * d_u
            d_v = nv_ref[k, pl.ds(own, PR), :] + VISC[2][k] * d_v
            nt_ref[k, pl.ds(own, PR), :] = d_t
            ns_ref[k, pl.ds(own, PR), :] = d_s
            nu_ref[k, pl.ds(own, PR), :] = d_u
            nv_ref[k, pl.ds(own, PR), :] = d_v
            sum_u, sum_v = sum_u + d_u, sum_v + d_v
        two_ref[2, pl.ds(own, PR), :] = sum_u / jnp.maximum(nu_f, 1.0)
        two_ref[3, pl.ds(own, PR), :] = sum_v / jnp.maximum(nv_f, 1.0)
        return 0

    lax.fori_loop(0, N // PR, solve_step, 0)

    wait_recv(wide)
    wait_recv(forc)
    wm_out[...] = wm[...]
    we_out[...] = we[...]
    ww_out[...] = ww[...]
    fm_out[...] = fm[...]
    fe_out[...] = fe[...]
    fw_out[...] = fw[...]
    wait_send(thin)
    wait_send(wide)
    wait_send(forc)


TOP = EXT + 16


def step_kernel(nrow, nu_ref, nv_ref, nt_ref, ns_ref, two_ref, wm, we, ww, fm, fe, fw,
                eta_out, tu_out, tv_out, u_hbm, v_hbm, t_hbm, s_hbm,
                et, fu, fv, cu, cv, pu, pv, dm, mean, ub, vb, osem):
    r = lax.axis_index('row')
    copies = [pltpu.make_async_copy(nt_ref, t_hbm, osem.at[0]), pltpu.make_async_copy(ns_ref, s_hbm, osem.at[1])]
    for cp in copies:
        cp.start()

    lane = lax.broadcasted_iota(jnp.int32, (EXT, N), 1)
    rows = lax.broadcasted_iota(jnp.int32, (EXT, N), 0)
    last = lane == N - 1
    first = lane == 0
    lo_ok = jnp.where(r > 0, 0, W)
    hi_ok = jnp.where(r < nrow - 1, EXT, W + N)
    real = (rows >= lo_ok) & (rows < hi_ok)
    in_e = lane < W
    in_w = lane >= N - W

    def side(e_ref, w_ref, f):
        e = e_ref[...]
        w = w_ref[...]
        se = (N - W * f) % N
        sw = (2 * N - W * (f + 1)) % N
        e = pltpu.roll(e, se, 1) if se else e
        w = pltpu.roll(w, sw, 1) if sw else w
        return jnp.where(in_e, e, jnp.where(in_w, w, 0.0))

    def east_of(a, b):
        ra, rb = pltpu.roll(a, N - 1, 1), pltpu.roll(b, N - 1, 1)
        return jnp.where(last, rb, ra), jnp.where(last, ra, rb)

    def west_of(a, b):
        ra, rb = pltpu.roll(a, 1, 1), pltpu.roll(b, 1, 1)
        return jnp.where(first, rb, ra), jnp.where(first, ra, rb)

    body = pl.ds(8, EXT)
    zero8 = jnp.zeros((8, N), F32)
    for ref in (et, fu, fv, dm):
        for t in range(2):
            ref[t, 0:8, :] = zero8
            ref[t, 8 + EXT:TOP, :] = zero8

    dms = (jnp.where(real, wm[3], 0.0), jnp.where(real & (in_e | in_w), side(we, ww, 3), 0.0))
    for t in range(2):
        dm[t, body, :] = dms[t]
    dme = east_of(*dms)
    for t in range(2):
        d_c = dms[t]
        d_n = dm[t, 9:9 + EXT, :]
        wet_u = (d_c > 0.0) & (dme[t] > 0.0)
        wet_v = (d_c > 0.0) & (d_n > 0.0)
        pick = (lambda f: wm[f]) if t == 0 else (lambda f: side(we, ww, f))
        fpick = (lambda f: fm[f]) if t == 0 else (lambda f: side(fe, fw, f))
        et[t, body, :] = jnp.where(d_c > 0.0, pick(0), 0.0)
        fu[t, body, :] = jnp.where(wet_u, 0.5 * pick(1), 0.0)
        fv[t, body, :] = jnp.where(wet_v, 0.5 * pick(2), 0.0)
        cu[t] = jnp.where(wet_u, 0.125 * (d_c + dme[t]), 0.0)
        cv[t] = jnp.where(wet_v, 0.125 * (d_c + d_n), 0.0)
        pu[t] = jnp.where(wet_u, (0.125 / SUBCYCLES) * fpick(0), 0.0)
        pv[t] = jnp.where(wet_v, (0.125 / SUBCYCLES) * fpick(1), 0.0)
    mean[...] = jnp.zeros((2, N, N), F32)

    inner = float(SUBCYCLES + 1)
    wsum = 0.0
    for n in range(1, SUBCYCLES + 1):
        wsum += (n / inner) ** 2 * (1.0 - (n / inner) ** 4)

    def cycle(n, _):
        frac = (n + 1).astype(F32) * (1.0 / inner)
        f2 = frac * frac
        wgt = f2 * (1.0 - f2 * f2) * (1.0 / wsum)
        us = (fu[0, body, :], fu[1, body, :])
        uw = west_of(*us)
        new = []
        for t in range(2):
            e = et[t, body, :] - ((us[t] - uw[t]) + (fv[t, body, :] - fv[t, 7:7 + EXT, :]))
            et[t, body, :] = e
            new.append(e)
        ee = east_of(*new)
        for t in range(2):
            u = us[t] - cu[t] * (ee[t] - new[t]) + pu[t]
            v = fv[t, body, :] - cv[t] * (et[t, 9:9 + EXT, :] - new[t]) + pv[t]
            fu[t, body, :] = u
            fv[t, body, :] = v
        mean[0] = mean[0] + wgt * fu[0, 8 + W:8 + W + N, :]
        mean[1] = mean[1] + wgt * fv[0, 8 + W:8 + W + N, :]
        return 0

    lax.fori_loop(0, SUBCYCLES, cycle, 0)

    mid = slice(8 + W, 8 + W + N)
    eta_out[...] = et[0, mid, :]
    tu_out[...] = 2.0 * fu[0, mid, :]
    tv_out[...] = 2.0 * fv[0, mid, :]
    for i, co in ((0, cu), (1, cv)):
        h = co[0, W:W + N, :]
        mean[i] = mean[i] / jnp.where(h > 0.0, 2.0 * h, 1.0) - two_ref[2 + i]

    for ci, (k0, k1) in enumerate(CHUNKS):
        for i, (src, buf, dst) in enumerate(((nu_ref, ub, u_hbm), (nv_ref, vb, v_hbm))):
            for k in range(k0, k1):
                buf[k] = src[k] + jnp.where(two_ref[i] > float(k), mean[i], 0.0)
            cp = pltpu.make_async_copy(buf.at[pl.ds(k0, k1 - k0)], dst.at[pl.ds(k0, k1 - k0)], osem.at[2 + 2 * ci + i])
            cp.start()
            copies.append(cp)
    for cp in copies:
        cp.wait()


def solution(mesh):
    ncol, nrow = mesh.shape['col'], mesh.shape['row']
    vmem = pl.BlockSpec(memory_space=pltpu.VMEM)
    hbm = pl.BlockSpec(memory_space=pl.ANY)
    s3 = jax.ShapeDtypeStruct((LEVELS, N, N), F32)
    s2 = jax.ShapeDtypeStruct((N, N), F32)

    def sds(*shape):
        return jax.ShapeDtypeStruct(shape, F32)

    def ocean_step(vel_u, vel_v, temp, salt, eta, tu, tv, dep, kmt):
        def kernel_a(*refs):
            exchange_kernel(ncol, nrow, *refs)

        def kernel_b(*refs):
            step_kernel(nrow, *refs)

        mid = pl.pallas_call(
            kernel_a,
            name='exchange',
            out_shape=(s3, s3, s3, s3, sds(4, N, N), sds(4, EXT, N), sds(EXT, N), sds(EXT, N), sds(2, EXT, N), sds(EXT, N), sds(EXT, N)),
            in_specs=[hbm] * 9,
            out_specs=(vmem,) * 11,
            scratch_shapes=[
                pltpu.VMEM((4, LEVELS, N + 16, N), F32),
                pltpu.VMEM((N, N), jnp.int32),
                pltpu.VMEM((2, N + 16, N), F32),
                pltpu.VMEM((N, N), F32), pltpu.VMEM((N, N), F32),
                pltpu.VMEM((N, N), F32), pltpu.VMEM((N, N), F32),
                pltpu.VMEM((8, N), F32), pltpu.VMEM((8, N), F32),
                pltpu.VMEM((N + 16, N), F32), pltpu.VMEM((N + 16, N), F32),
                pltpu.VMEM((4, EXT, N), F32),
                pltpu.VMEM((N, N), F32), pltpu.VMEM((N, N), F32),
                pltpu.VMEM((EXT, N), F32), pltpu.VMEM((EXT, N), F32),
                pltpu.VMEM((2, EXT, N), F32),
                pltpu.VMEM((N, N), F32), pltpu.VMEM((N, N), F32),
                pltpu.VMEM((EXT, N), F32), pltpu.VMEM((EXT, N), F32),
                pltpu.SemaphoreType.DMA((4, len(CHUNKS))),
                pltpu.SemaphoreType.DMA((5,)),
                pltpu.SemaphoreType.DMA((24,)),
                pltpu.SemaphoreType.DMA((24,)),
            ],
            compiler_params=pltpu.CompilerParams(collective_id=0, has_side_effects=True, vmem_limit_bytes=28 * 2 ** 20),
        )(*[pltpu.with_memory_space_constraint(x, pltpu.HBM) for x in (vel_u, vel_v, temp, salt, eta, tu, tv, dep, kmt)])
        st = pltpu.VMEM((2, TOP, N), F32)
        co = pltpu.VMEM((2, EXT, N), F32)
        out = pl.pallas_call(
            kernel_b,
            name='subcycles',
            out_shape=(s2, s2, s2, s3, s3, s3, s3),
            in_specs=[vmem] * 11,
            out_specs=(vmem,) * 3 + (hbm,) * 4,
            scratch_shapes=[st, st, st, co, co, co, co, st, pltpu.VMEM((2, N, N), F32),
                            pltpu.VMEM((LEVELS, N, N), F32), pltpu.VMEM((LEVELS, N, N), F32),
                            pltpu.SemaphoreType.DMA((2 + 2 * len(CHUNKS),))],
            compiler_params=pltpu.CompilerParams(vmem_limit_bytes=28 * 2 ** 20),
        )(*mid)
        return out

    spec_3d = P(None, 'row', 'col')
    spec_2d = P('row', 'col')
    return jax.shard_map(ocean_step, mesh=mesh, in_specs=(spec_3d,) * 4 + (spec_2d,) * 5,
                         out_specs=(spec_2d,) * 3 + (spec_3d,) * 4, check_vma=False)
```

```python
import jax
import jax.numpy as jnp
import numpy as np
from jax import lax
from jax.experimental import pallas as pl
from jax.experimental.pallas import tpu as pltpu
from jax.sharding import PartitionSpec as P

MESH = pl.DeviceIdType.MESH
F32 = jnp.float32
SUBCYCLES = 30
LEVELS = 31
VISC_NUM = 4.0
DIFF_NUM = 1.0
N = 128
W = 32
EXT = N + 2 * W
PR = 16
CHUNKS = ((0, 8), (8, 16), (16, 24), (24, 31))


def solve_coefs(nu):
    inner, last, back = [], [], []
    c_prev = 0.0
    for k in range(LEVELS):
        lo = nu if k > 0 else 0.0
        piv = 1.0 + nu + lo - lo * c_prev
        inner.append(1.0 / piv)
        last.append(1.0 / (1.0 + lo - lo * c_prev))
        c_prev = nu / piv
        back.append(c_prev)
    return inner, last, back


VISC = solve_coefs(VISC_NUM)
DIFF = solve_coefs(DIFF_NUM)


def weights():
    s = np.arange(1, SUBCYCLES + 1, dtype=np.float64) / (SUBCYCLES + 1)
    w = s ** 2 * (1.0 - s ** 4)
    return (w / w.sum()).astype(np.float32)


def exchange_kernel(ncol, nrow, u_hbm, v_hbm, t_hbm, s_hbm, eta_hbm, tu_hbm, tv_hbm, dep_hbm, kmt_hbm,
                    nu_ref, nv_ref, nt_ref, ns_ref, two_ref, wm_out, we_out, ww_out, fm_out, fe_out, fw_out,
                    fb, ki, kd, qs, msg_e, msg_w, got_w, got_e, xe, xw, ed,
                    wm, pk_e, pk_w, we, ww, fm, fk_e, fk_w, fe, fw,
                    ld_sem, in_sem, snd, rcv):
    c = lax.axis_index('col')
    r = lax.axis_index('row')
    east = lax.rem(c + 1, ncol)
    west = lax.rem(c + ncol - 1, ncol)
    north = lax.rem(r + 1, nrow)
    south = lax.rem(r + nrow - 1, nrow)
    has_n = r < nrow - 1
    has_s = r > 0

    src3 = (u_hbm, v_hbm, t_hbm, s_hbm)
    small = [pltpu.make_async_copy(kmt_hbm, ki, in_sem.at[0]),
             pltpu.make_async_copy(dep_hbm, kd.at[1, pl.ds(8, N), :], in_sem.at[1]),
             pltpu.make_async_copy(eta_hbm, wm.at[0, pl.ds(W, N), :], in_sem.at[2]),
             pltpu.make_async_copy(tu_hbm, wm.at[1, pl.ds(W, N), :], in_sem.at[3]),
             pltpu.make_async_copy(tv_hbm, wm.at[2, pl.ds(W, N), :], in_sem.at[4])]
    loads = []
    for ci, (k0, k1) in enumerate(CHUNKS):
        row = [pltpu.make_async_copy(src3[f].at[pl.ds(k0, k1 - k0)], fb.at[f, pl.ds(k0, k1 - k0), pl.ds(8, N), :],
                                     ld_sem.at[f, ci]) for f in range(4)]
        loads.append(row)
        for cp in row:
            cp.start()
        if ci == 0:
            for cp in small:
                cp.start()

    barrier = pltpu.get_barrier_semaphore()
    places = [(east, r), (west, r), (c, north), (c, south), (east, north), (east, south), (west, north), (west, south)]
    for cc, rr in places:
        pl.semaphore_signal(barrier, inc=1, device_id={'col': cc, 'row': rr}, device_id_type=MESH)

    def copy(i, src, dst, cc, rr):
        return pltpu.make_async_remote_copy(src_ref=src, dst_ref=dst, send_sem=snd.at[i], recv_sem=rcv.at[i],
                                            device_id={'col': cc, 'row': rr}, device_id_type=MESH)

    rows = [
        (copy(0, fb.at[:, :, pl.ds(8, 1), :], fb.at[:, :, pl.ds(8 + N, 1), :], c, south), has_s, has_n),
        (copy(1, fb.at[:, :, pl.ds(7 + N, 1), :], fb.at[:, :, pl.ds(7, 1), :], c, north), has_n, has_s),
        (copy(2, kd.at[:, pl.ds(8, 1), :], kd.at[:, pl.ds(8 + N, 1), :], c, south), has_s, has_n),
        (copy(3, kd.at[:, pl.ds(7 + N, 1), :], kd.at[:, pl.ds(7, 1), :], c, north), has_n, has_s),
    ]
    cols = [
        (copy(4, msg_e, got_w.at[pl.ds(8, N), :], east, r), None, None),
        (copy(5, msg_w, got_e.at[pl.ds(8, N), :], west, r), None, None),
        (copy(6, msg_e.at[pl.ds(0, 8), :], got_w.at[pl.ds(8 + N, 8), :], east, south), has_s, has_n),
        (copy(7, msg_w.at[pl.ds(N - 8, 8), :], got_e.at[pl.ds(0, 8), :], west, north), has_n, has_s),
    ]

    def wide_set(base, main, to_e, to_w, in_e, in_w):
        lo, hi = pl.ds(0, W), pl.ds(N - W, W)
        return [
            (copy(base + 0, to_w, in_e.at[pl.ds(W, N), :], west, r), None, None),
            (copy(base + 1, to_e, in_w.at[pl.ds(W, N), :], east, r), None, None),
            (copy(base + 2, main.at[:, pl.ds(W, W), :], main.at[:, pl.ds(W + N, W), :], c, south), has_s, has_n),
            (copy(base + 3, main.at[:, pl.ds(N, W), :], main.at[:, pl.ds(0, W), :], c, north), has_n, has_s),
            (copy(base + 4, to_w.at[lo, :], in_e.at[pl.ds(W + N, W), :], west, south), has_s, has_n),
            (copy(base + 5, to_w.at[hi, :], in_e.at[lo, :], west, north), has_n, has_s),
            (copy(base + 6, to_e.at[lo, :], in_w.at[pl.ds(W + N, W), :], east, south), has_s, has_n),
            (copy(base + 7, to_e.at[hi, :], in_w.at[lo, :], east, north), has_n, has_s),
        ]

    wide = wide_set(8, wm, pk_e, pk_w, we, ww)
    forc = wide_set(16, fm, fk_e, fk_w, fe, fw)

    def run(cond, fn):
        if cond is None:
            fn()
        else:
            pl.when(cond)(fn)

    def start(items):
        for cp, s_if, _ in items:
            run(s_if, cp.start)

    def wait_recv(items):
        for cp, _, r_if in items:
            run(r_if, cp.wait_recv)

    def wait_send(items):
        for cp, s_if, _ in items:
            run(s_if, cp.wait_send)

    lane = lax.broadcasted_iota(jnp.int32, (N, N), 1)
    part = lax.rem(lane, 4)
    slot = lane // 4

    def roll(x, s):
        s %= N
        return pltpu.roll(x, s, 1) if s else x

    for cp in small:
        cp.wait()
    kmt_f = ki[...].astype(F32)
    dep = kd[1, 8:8 + N, :]
    kd[0, 8:8 + N, :] = kmt_f
    wm[3, W:W + N, :] = jnp.where(kmt_f > 0.0, dep, 0.0)

    acc = [jnp.zeros((N, N), F32)] * 4
    for ci, (k0, k1) in enumerate(CHUNKS):
        for cp in loads[ci]:
            cp.wait()
        if ci == len(CHUNKS) - 1:
            pl.semaphore_wait(barrier, len(places))
            start(rows)
        for f in range(4):
            x = acc[f]
            for k in range(k0, k1):
                x = jnp.where(slot == k, roll(fb[f, k, 8:8 + N, :], 4 * k + 2), x)
            acc[f] = x
    out_e = jnp.where(lane == 124, roll(kmt_f, -3), roll(dep, -2))
    out_w = jnp.where(lane == 124, roll(kmt_f, 124), roll(dep, 125))
    for f in range(4):
        qs[f, 8:8 + N, :] = acc[f]
        pick = (part == f) & (slot < LEVELS)
        out_e = jnp.where(pick, roll(acc[f], f - 1), out_e)
        out_w = jnp.where(pick, roll(acc[f], f - 2), out_w)
    msg_e[...] = out_e
    msg_w[...] = out_w

    def pack(fields):
        e_acc = jnp.zeros((N, N), F32)
        w_acc = jnp.zeros((N, N), F32)
        for f, x in enumerate(fields):
            here = lane // W == f
            w_acc = jnp.where(here, roll(x, W * f), w_acc)
            e_acc = jnp.where(here, roll(x, W * (f + 1)), e_acc)
        return e_acc, w_acc

    e_acc, w_acc = pack([wm[f, W:W + N, :] for f in range(4)])
    start(cols)
    pk_e[...] = e_acc
    pk_w[...] = w_acc

    @pl.when(jnp.logical_not(has_n))
    def _():
        fb[:, :, 8 + N:9 + N, :] = jnp.zeros((4, LEVELS, 1, N), F32)
        kd[:, 8 + N:9 + N, :] = jnp.zeros((2, 1, N), F32)
        got_w[8 + N:16 + N, :] = jnp.zeros((8, N), F32)

    @pl.when(jnp.logical_not(has_s))
    def _():
        fb[:, :, 7:8, :] = jnp.zeros((4, LEVELS, 1, N), F32)
        kd[:, 7:8, :] = jnp.zeros((2, 1, N), F32)
        got_e[0:8, :] = jnp.zeros((8, N), F32)

    start(wide)

    lane_p = lax.broadcasted_iota(jnp.int32, (PR, N), 1)
    edge = (lane_p == 0) | (lane_p == N - 1)

    def thick(k, d):
        return d / jnp.maximum(k, 1.0)

    def force(p_c, p_e, p_n, u_c, u_n, u_s, v_c, v_n, v_s):
        us, vs = u_c + u_n, v_c + v_s
        v_at_u = 0.25 * (vs + roll(vs, -1))
        u_at_v = 0.25 * (us + roll(us, 1))
        u_w = roll(u_c, 1)
        g_u = p_c - p_e - 0.5 * (u_c * (roll(u_c, -1) - u_w) + v_at_u * (u_n - u_s))
        g_v = p_c - p_n - 0.5 * (u_at_v * (roll(v_c, -1) - roll(v_c, 1)) + v_c * (v_n - v_s))
        return g_u, g_v, u_w

    def advect(ok_e, ok_w, ok_n, ok_s, u_c, u_w, v_c, v_s, tracers):
        u_e, u_w = jnp.where(ok_e, u_c, 0.0), jnp.where(ok_w, u_w, 0.0)
        v_n, v_s = jnp.where(ok_n, v_c, 0.0), jnp.where(ok_s, v_s, 0.0)
        a_e, a_w = jnp.minimum(u_e, 0.0), jnp.maximum(u_w, 0.0)
        a_n, a_s = jnp.minimum(v_n, 0.0), jnp.maximum(v_s, 0.0)
        a_c = (jnp.maximum(u_e, 0.0) - jnp.minimum(u_w, 0.0)) + (jnp.maximum(v_n, 0.0) - jnp.minimum(v_s, 0.0))
        out = []
        for x, x_n, x_s in tracers:
            div = a_c * x + (a_e * roll(x, -1) - a_w * roll(x, 1)) + (a_n * x_n - a_s * x_s)
            out.append(x - 0.25 * div)
        return out

    def main_step(i, _):
        @pl.when(i == N // PR - 2)
        def _():
            wait_recv(rows)

        own = pl.multiple_of(lax.rem(i + 1, N // PR) * PR, PR)
        base = own + 8

        def at(f, k, off):
            return fb[f, k, pl.ds(base + off, PR), :]

        kc = kd[0, pl.ds(base, PR), :]
        kn = kd[0, pl.ds(base + 1, PR), :]
        ks = kd[0, pl.ds(base - 1, PR), :]
        dc = kd[1, pl.ds(base, PR), :]
        dn = kd[1, pl.ds(base + 1, PR), :]
        th_c, th_n = thick(kc, dc), thick(kn, dn)
        nu_f = jnp.minimum(kc, roll(kc, -1))
        nw_f = jnp.minimum(kc, roll(kc, 1))
        nv_f = jnp.minimum(kc, kn)
        nq_f = jnp.minimum(kc, ks)
        zero = jnp.zeros((PR, N), F32)
        cum_c, cum_n, sum_u, sum_v = zero, zero, zero, zero
        for k in range(LEVELS):
            fk = float(k)
            t_c, s_c = at(2, k, 0), at(3, k, 0)
            t_n, s_n = at(2, k, 1), at(3, k, 1)
            d_c = jnp.where(kc > fk, 0.6 * s_c - 0.3 * t_c, 0.0)
            d_n = jnp.where(kn > fk, 0.6 * s_n - 0.3 * t_n, 0.0)
            cum_c, cum_n = cum_c + d_c, cum_n + d_n
            p_c = (cum_c - 0.5 * d_c) * th_c
            p_n = (cum_n - 0.5 * d_n) * th_n
            u_c, v_c, v_s = at(0, k, 0), at(1, k, 0), at(1, k, -1)
            g_u, g_v, u_w = force(p_c, roll(p_c, -1), p_n, u_c, at(0, k, 1), at(0, k, -1), v_c, at(1, k, 1), v_s)
            wet_u, wet_v = nu_f > fk, nv_f > fk
            sum_u = sum_u + jnp.where(wet_u, g_u, 0.0)
            sum_v = sum_v + jnp.where(wet_v, g_v, 0.0)
            nu_ref[k, pl.ds(own, PR), :] = jnp.where(wet_u, u_c + 0.25 * g_u, 0.0)
            nv_ref[k, pl.ds(own, PR), :] = jnp.where(wet_v, v_c + 0.25 * g_v, 0.0)
            t1, s1 = advect(wet_u, nw_f > fk, wet_v, nq_f > fk, u_c, u_w, v_c, v_s,
                            ((t_c, t_n, at(2, k, -1)), (s_c, s_n, at(3, k, -1))))
            nt_ref[k, pl.ds(own, PR), :] = t1
            ns_ref[k, pl.ds(own, PR), :] = s1
        hu = jnp.where(nu_f > 0.0, 0.5 * (dc + roll(dc, -1)), 0.0)
        hv = jnp.where(nv_f > 0.0, 0.5 * (dc + dn), 0.0)
        fm[0, pl.ds(own + W, PR), :] = hu * (1.0 / jnp.maximum(nu_f, 1.0)) * sum_u
        fm[1, pl.ds(own + W, PR), :] = hv * (1.0 / jnp.maximum(nv_f, 1.0)) * sum_v
        return 0

    lax.fori_loop(0, N // PR, main_step, 0)

    lane8 = lax.broadcasted_iota(jnp.int32, (8, N), 1)
    for f in range(4):
        for lo in (0, 8 + N):
            x = jnp.zeros((8, N), F32)
            for k in range(LEVELS):
                x = jnp.where(lane8 // 4 == k, roll(fb[f, k, lo:lo + 8, :], 4 * k + 2), x)
            qs[f, lo:lo + 8, :] = x

    wait_recv(cols)

    part_x = lax.rem(lax.broadcasted_iota(jnp.int32, (N + 16, N), 1), 4)
    for f in range(4):
        q = qs[f]
        xe[f] = jnp.where(part_x == 2, roll(got_e[...], 2 - f), q)
        xw[f] = jnp.where(part_x == 1, roll(got_w[...], 1 - f), q)
    for f in range(2):
        q = kd[f]
        b = [jnp.broadcast_to(q[:, j:j + 1], q.shape) for j in (N - 2, N - 1, 0, 1)]
        h_e = jnp.broadcast_to(got_e[:, 124 + f:125 + f], q.shape)
        h_w = jnp.broadcast_to(got_w[:, 124 + f:125 + f], q.shape)
        xe[4 + f] = jnp.where(part_x == 0, b[0], jnp.where(part_x == 1, b[1], h_e))
        xw[4 + f] = jnp.where(part_x == 1, h_w, jnp.where(part_x == 2, b[2], b[3]))

    lev = slot.astype(F32)

    def prefix(x):
        for s in (1, 2, 4, 8, 16):
            x = x + jnp.where(slot >= s, roll(x, 4 * s), 0.0)
        return x

    def total(x):
        for s in (1, 2, 4, 8, 16):
            x = x + roll(x, 4 * s)
        return x

    def strip(x):
        def at(f, off):
            return x[f, 8 + off:8 + off + N, :]

        kc, kn, ks = at(4, 0), at(4, 1), at(4, -1)
        dc, dn = at(5, 0), at(5, 1)
        nu_f, nw_f = jnp.minimum(kc, roll(kc, -1)), jnp.minimum(kc, roll(kc, 1))
        nv_f, nq_f = jnp.minimum(kc, kn), jnp.minimum(kc, ks)
        t_c, s_c, t_n, s_n = at(2, 0), at(3, 0), at(2, 1), at(3, 1)
        d_c = jnp.where(kc > lev, 0.6 * s_c - 0.3 * t_c, 0.0)
        d_n = jnp.where(kn > lev, 0.6 * s_n - 0.3 * t_n, 0.0)
        p_c = (prefix(d_c) - 0.5 * d_c) * thick(kc, dc)
        p_n = (prefix(d_n) - 0.5 * d_n) * thick(kn, dn)
        u_c, v_c, v_s = at(0, 0), at(1, 0), at(1, -1)
        g_u, g_v, u_w = force(p_c, roll(p_c, -1), p_n, u_c, at(0, 1), at(0, -1), v_c, at(1, 1), v_s)
        wet_u, wet_v = nu_f > lev, nv_f > lev
        hu = jnp.where(nu_f > 0.0, 0.5 * (dc + roll(dc, -1)), 0.0)
        hv = jnp.where(nv_f > 0.0, 0.5 * (dc + dn), 0.0)
        f_u = hu * (1.0 / jnp.maximum(nu_f, 1.0)) * total(jnp.where(wet_u, g_u, 0.0))
        f_v = hv * (1.0 / jnp.maximum(nv_f, 1.0)) * total(jnp.where(wet_v, g_v, 0.0))
        r_u = jnp.where(wet_u, u_c + 0.25 * g_u, 0.0)
        r_v = jnp.where(wet_v, v_c + 0.25 * g_v, 0.0)
        t1, s1 = advect(wet_u, nw_f > lev, wet_v, nq_f > lev, u_c, u_w, v_c, v_s,
                        ((t_c, t_n, at(2, -1)), (s_c, s_n, at(3, -1))))
        return f_u, f_v, r_u, r_v, t1, s1

    both = [jnp.where(part == 1, a, b) for a, b in zip(strip(xe), strip(xw))]
    rim = (lane == 0) | (lane == N - 1)
    forces = []
    for f in range(2):
        x = jnp.where(rim, roll(both[f], 2), fm[f, W:W + N, :])
        fm[f, W:W + N, :] = x
        forces.append(x)
    e_acc, w_acc = pack(forces)
    fk_e[...] = e_acc
    fk_w[...] = w_acc
    for f in range(4):
        ed[f] = both[2 + f]
    start(forc)

    def solve_step(g, _):
        own = pl.multiple_of(g * PR, PR)
        base = own + 8
        here = pl.ds(own, PR)
        kc = kd[0, pl.ds(base, PR), :]
        kn = kd[0, pl.ds(base + 1, PR), :]
        nu_f = jnp.minimum(kc, jnp.where(lane_p == N - 1, roll(got_e[pl.ds(base, PR), :], 3), roll(kc, -1)))
        nv_f = jnp.minimum(kc, kn)
        two_ref[0, here, :] = nu_f
        two_ref[1, here, :] = nv_f
        zero = jnp.zeros((PR, N), F32)
        refs = (nu_ref, nv_ref, nt_ref, ns_ref)
        nus = (VISC_NUM, VISC_NUM, DIFF_NUM, DIFF_NUM)
        cos = (VISC, VISC, DIFF, DIFF)
        d = [zero] * 4

        def factor(n_f, k, co):
            return jnp.where(n_f > k + 1.0, co[0][k], jnp.where(n_f > float(k), co[1][k], 0.0))

        for k in range(LEVELS):
            f_t = factor(kc, k, DIFF)
            facs = (factor(nu_f, k, VISC), factor(nv_f, k, VISC), f_t, f_t)
            for q in range(4):
                x = jnp.where(edge, roll(ed[q, here, :], 126 - 4 * k), refs[q][k, here, :])
                d[q] = (x + nus[q] * d[q]) * facs[q]
                refs[q][k, here, :] = d[q]
        sum_u, sum_v = d[0], d[1]
        for k in range(LEVELS - 2, -1, -1):
            for q in range(4):
                d[q] = refs[q][k, here, :] + cos[q][2][k] * d[q]
                refs[q][k, here, :] = d[q]
            sum_u, sum_v = sum_u + d[0], sum_v + d[1]
        two_ref[2, here, :] = sum_u / jnp.maximum(nu_f, 1.0)
        two_ref[3, here, :] = sum_v / jnp.maximum(nv_f, 1.0)
        return 0

    lax.fori_loop(0, N // PR, solve_step, 0)

    wait_recv(wide)
    wait_recv(forc)
    wm_out[...] = wm[...]
    we_out[...] = we[...]
    ww_out[...] = ww[...]
    fm_out[...] = fm[...]
    fe_out[...] = fe[...]
    fw_out[...] = fw[...]
    wait_send(rows)
    wait_send(cols)
    wait_send(wide)
    wait_send(forc)


TOP = EXT + 16


def step_kernel(nrow, nu_ref, nv_ref, nt_ref, ns_ref, two_ref, wm, we, ww, fm, fe, fw,
                eta_out, tu_out, tv_out, u_hbm, v_hbm, t_hbm, s_hbm,
                et, fu, fv, cu, cv, pu, pv, dm, mean, ub, vb, osem):
    r = lax.axis_index('row')
    copies = [pltpu.make_async_copy(nt_ref, t_hbm, osem.at[0]), pltpu.make_async_copy(ns_ref, s_hbm, osem.at[1])]
    for cp in copies:
        cp.start()

    lane = lax.broadcasted_iota(jnp.int32, (EXT, N), 1)
    rows = lax.broadcasted_iota(jnp.int32, (EXT, N), 0)
    last = lane == N - 1
    first = lane == 0
    lo_ok = jnp.where(r > 0, 0, W)
    hi_ok = jnp.where(r < nrow - 1, EXT, W + N)
    real = (rows >= lo_ok) & (rows < hi_ok)
    in_e = lane < W
    in_w = lane >= N - W

    def side(e_ref, w_ref, f):
        e = e_ref[...]
        w = w_ref[...]
        se = (N - W * f) % N
        sw = (2 * N - W * (f + 1)) % N
        e = pltpu.roll(e, se, 1) if se else e
        w = pltpu.roll(w, sw, 1) if sw else w
        return jnp.where(in_e, e, jnp.where(in_w, w, 0.0))

    def east_of(a, b):
        ra, rb = pltpu.roll(a, N - 1, 1), pltpu.roll(b, N - 1, 1)
        return jnp.where(last, rb, ra), jnp.where(last, ra, rb)

    def west_of(a, b):
        ra, rb = pltpu.roll(a, 1, 1), pltpu.roll(b, 1, 1)
        return jnp.where(first, rb, ra), jnp.where(first, ra, rb)

    body = pl.ds(8, EXT)
    zero8 = jnp.zeros((8, N), F32)
    for ref in (et, fu, fv, dm):
        for t in range(2):
            ref[t, 0:8, :] = zero8
            ref[t, 8 + EXT:TOP, :] = zero8

    dms = (jnp.where(real, wm[3], 0.0), jnp.where(real & (in_e | in_w), side(we, ww, 3), 0.0))
    for t in range(2):
        dm[t, body, :] = dms[t]
    dme = east_of(*dms)
    for t in range(2):
        d_c = dms[t]
        d_n = dm[t, 9:9 + EXT, :]
        wet_u = (d_c > 0.0) & (dme[t] > 0.0)
        wet_v = (d_c > 0.0) & (d_n > 0.0)
        pick = (lambda f: wm[f]) if t == 0 else (lambda f: side(we, ww, f))
        fpick = (lambda f: fm[f]) if t == 0 else (lambda f: side(fe, fw, f))
        et[t, body, :] = jnp.where(d_c > 0.0, pick(0), 0.0)
        fu[t, body, :] = jnp.where(wet_u, 0.5 * pick(1), 0.0)
        fv[t, body, :] = jnp.where(wet_v, 0.5 * pick(2), 0.0)
        cu[t] = jnp.where(wet_u, 0.125 * (d_c + dme[t]), 0.0)
        cv[t] = jnp.where(wet_v, 0.125 * (d_c + d_n), 0.0)
        pu[t] = jnp.where(wet_u, (0.125 / SUBCYCLES) * fpick(0), 0.0)
        pv[t] = jnp.where(wet_v, (0.125 / SUBCYCLES) * fpick(1), 0.0)
    mean[...] = jnp.zeros((2, N, N), F32)

    inner = float(SUBCYCLES + 1)
    wsum = 0.0
    for n in range(1, SUBCYCLES + 1):
        wsum += (n / inner) ** 2 * (1.0 - (n / inner) ** 4)

    def cycle(n, _):
        frac = (n + 1).astype(F32) * (1.0 / inner)
        f2 = frac * frac
        wgt = f2 * (1.0 - f2 * f2) * (1.0 / wsum)
        us = (fu[0, body, :], fu[1, body, :])
        uw = west_of(*us)
        new = []
        for t in range(2):
            e = et[t, body, :] - ((us[t] - uw[t]) + (fv[t, body, :] - fv[t, 7:7 + EXT, :]))
            et[t, body, :] = e
            new.append(e)
        ee = east_of(*new)
        for t in range(2):
            u = us[t] - cu[t] * (ee[t] - new[t]) + pu[t]
            v = fv[t, body, :] - cv[t] * (et[t, 9:9 + EXT, :] - new[t]) + pv[t]
            fu[t, body, :] = u
            fv[t, body, :] = v
        mean[0] = mean[0] + wgt * fu[0, 8 + W:8 + W + N, :]
        mean[1] = mean[1] + wgt * fv[0, 8 + W:8 + W + N, :]
        return 0

    lax.fori_loop(0, SUBCYCLES, cycle, 0)

    mid = slice(8 + W, 8 + W + N)
    eta_out[...] = et[0, mid, :]
    tu_out[...] = 2.0 * fu[0, mid, :]
    tv_out[...] = 2.0 * fv[0, mid, :]
    for i, co in ((0, cu), (1, cv)):
        h = co[0, W:W + N, :]
        mean[i] = mean[i] / jnp.where(h > 0.0, 2.0 * h, 1.0) - two_ref[2 + i]

    for ci, (k0, k1) in enumerate(CHUNKS):
        for i, (src, buf, dst) in enumerate(((nu_ref, ub, u_hbm), (nv_ref, vb, v_hbm))):
            for k in range(k0, k1):
                buf[k] = src[k] + jnp.where(two_ref[i] > float(k), mean[i], 0.0)
            cp = pltpu.make_async_copy(buf.at[pl.ds(k0, k1 - k0)], dst.at[pl.ds(k0, k1 - k0)], osem.at[2 + 2 * ci + i])
            cp.start()
            copies.append(cp)
    for cp in copies:
        cp.wait()


def solution(mesh):
    ncol, nrow = mesh.shape['col'], mesh.shape['row']
    vmem = pl.BlockSpec(memory_space=pltpu.VMEM)
    hbm = pl.BlockSpec(memory_space=pl.ANY)
    s3 = jax.ShapeDtypeStruct((LEVELS, N, N), F32)
    s2 = jax.ShapeDtypeStruct((N, N), F32)

    def sds(*shape):
        return jax.ShapeDtypeStruct(shape, F32)

    def ocean_step(vel_u, vel_v, temp, salt, eta, tu, tv, dep, kmt):
        def kernel_a(*refs):
            exchange_kernel(ncol, nrow, *refs)

        def kernel_b(*refs):
            step_kernel(nrow, *refs)

        mid = pl.pallas_call(
            kernel_a,
            name='exchange',
            out_shape=(s3, s3, s3, s3, sds(4, N, N), sds(4, EXT, N), sds(EXT, N), sds(EXT, N), sds(2, EXT, N), sds(EXT, N), sds(EXT, N)),
            in_specs=[hbm] * 9,
            out_specs=(vmem,) * 11,
            scratch_shapes=[
                pltpu.VMEM((4, LEVELS, N + 16, N), F32),
                pltpu.VMEM((N, N), jnp.int32),
                pltpu.VMEM((2, N + 16, N), F32),
                pltpu.VMEM((4, N + 16, N), F32),
                pltpu.VMEM((N, N), F32), pltpu.VMEM((N, N), F32),
                pltpu.VMEM((N + 16, N), F32), pltpu.VMEM((N + 16, N), F32),
                pltpu.VMEM((6, N + 16, N), F32), pltpu.VMEM((6, N + 16, N), F32),
                pltpu.VMEM((4, N, N), F32),
                pltpu.VMEM((4, EXT, N), F32),
                pltpu.VMEM((N, N), F32), pltpu.VMEM((N, N), F32),
                pltpu.VMEM((EXT, N), F32), pltpu.VMEM((EXT, N), F32),
                pltpu.VMEM((2, EXT, N), F32),
                pltpu.VMEM((N, N), F32), pltpu.VMEM((N, N), F32),
                pltpu.VMEM((EXT, N), F32), pltpu.VMEM((EXT, N), F32),
                pltpu.SemaphoreType.DMA((4, len(CHUNKS))),
                pltpu.SemaphoreType.DMA((5,)),
                pltpu.SemaphoreType.DMA((24,)),
                pltpu.SemaphoreType.DMA((24,)),
            ],
            compiler_params=pltpu.CompilerParams(collective_id=0, has_side_effects=True, vmem_limit_bytes=28 * 2 ** 20),
        )(*[pltpu.with_memory_space_constraint(x, pltpu.HBM) for x in (vel_u, vel_v, temp, salt, eta, tu, tv, dep, kmt)])
        st = pltpu.VMEM((2, TOP, N), F32)
        co = pltpu.VMEM((2, EXT, N), F32)
        out = pl.pallas_call(
            kernel_b,
            name='subcycles',
            out_shape=(s2, s2, s2, s3, s3, s3, s3),
            in_specs=[vmem] * 11,
            out_specs=(vmem,) * 3 + (hbm,) * 4,
            scratch_shapes=[st, st, st, co, co, co, co, st, pltpu.VMEM((2, N, N), F32),
                            pltpu.VMEM((LEVELS, N, N), F32), pltpu.VMEM((LEVELS, N, N), F32),
                            pltpu.SemaphoreType.DMA((2 + 2 * len(CHUNKS),))],
            compiler_params=pltpu.CompilerParams(vmem_limit_bytes=28 * 2 ** 20),
        )(*mid)
        return out

    spec_3d = P(None, 'row', 'col')
    spec_2d = P('row', 'col')
    return jax.shard_map(ocean_step, mesh=mesh, in_specs=(spec_3d,) * 4 + (spec_2d,) * 5,
                         out_specs=(spec_2d,) * 3 + (spec_3d,) * 4, check_vma=False)
```

```python
import jax
import jax.numpy as jnp
import numpy as np
from jax import lax
from jax.experimental import pallas as pl
from jax.experimental.pallas import tpu as pltpu
from jax.sharding import PartitionSpec as P

MESH = pl.DeviceIdType.MESH
F32 = jnp.float32
SUBCYCLES = 30
LEVELS = 31
VISC_NUM = 4.0
DIFF_NUM = 1.0
N = 128
W = 32
EXT = N + 2 * W
PR = 16
CHUNKS = ((0, 8), (8, 16), (16, 24), (24, 31))


def solve_coefs(nu):
    inner, last, back = [], [], []
    c_prev = 0.0
    for k in range(LEVELS):
        lo = nu if k > 0 else 0.0
        piv = 1.0 + nu + lo - lo * c_prev
        inner.append(1.0 / piv)
        last.append(1.0 / (1.0 + lo - lo * c_prev))
        c_prev = nu / piv
        back.append(c_prev)
    return inner, last, back


VISC = solve_coefs(VISC_NUM)
DIFF = solve_coefs(DIFF_NUM)


def weights():
    s = np.arange(1, SUBCYCLES + 1, dtype=np.float64) / (SUBCYCLES + 1)
    w = s ** 2 * (1.0 - s ** 4)
    return (w / w.sum()).astype(np.float32)


def exchange_kernel(ncol, nrow, u_hbm, v_hbm, t_hbm, s_hbm, eta_hbm, tu_hbm, tv_hbm, dep_hbm, kmt_hbm,
                    nu_ref, nv_ref, nt_ref, ns_ref, two_ref, wm_out, we_out, ww_out, fm_out, fe_out, fw_out,
                    fb, ki, kd, qs, msg_e, msg_w, got_w, got_e, xe, xw, ed,
                    wm, pk_e, pk_w, we, ww, fm, fk_e, fk_w, fe, fw,
                    ld_sem, in_sem, snd, rcv):
    c = lax.axis_index('col')
    r = lax.axis_index('row')
    east = lax.rem(c + 1, ncol)
    west = lax.rem(c + ncol - 1, ncol)
    north = lax.rem(r + 1, nrow)
    south = lax.rem(r + nrow - 1, nrow)
    has_n = r < nrow - 1
    has_s = r > 0

    src3 = (u_hbm, v_hbm, t_hbm, s_hbm)
    small = [pltpu.make_async_copy(kmt_hbm, ki, in_sem.at[0]),
             pltpu.make_async_copy(dep_hbm, kd.at[1, pl.ds(8, N), :], in_sem.at[1]),
             pltpu.make_async_copy(eta_hbm, wm.at[0, pl.ds(W, N), :], in_sem.at[2]),
             pltpu.make_async_copy(tu_hbm, wm.at[1, pl.ds(W, N), :], in_sem.at[3]),
             pltpu.make_async_copy(tv_hbm, wm.at[2, pl.ds(W, N), :], in_sem.at[4])]
    loads = []
    for ci, (k0, k1) in enumerate(CHUNKS):
        row = [pltpu.make_async_copy(src3[f].at[pl.ds(k0, k1 - k0)], fb.at[f, pl.ds(k0, k1 - k0), pl.ds(8, N), :],
                                     ld_sem.at[f, ci]) for f in range(4)]
        loads.append(row)
        for cp in row:
            cp.start()
        if ci == 0:
            for cp in small:
                cp.start()

    barrier = pltpu.get_barrier_semaphore()
    places = [(east, r), (west, r), (c, north), (c, south), (east, north), (east, south), (west, north), (west, south)]
    for cc, rr in places:
        pl.semaphore_signal(barrier, inc=1, device_id={'col': cc, 'row': rr}, device_id_type=MESH)

    def copy(i, src, dst, cc, rr):
        return pltpu.make_async_remote_copy(src_ref=src, dst_ref=dst, send_sem=snd.at[i], recv_sem=rcv.at[i],
                                            device_id={'col': cc, 'row': rr}, device_id_type=MESH)

    rows = [
        (copy(0, fb.at[:, :, pl.ds(8, 1), :], fb.at[:, :, pl.ds(8 + N, 1), :], c, south), has_s, has_n),
        (copy(1, fb.at[:, :, pl.ds(7 + N, 1), :], fb.at[:, :, pl.ds(7, 1), :], c, north), has_n, has_s),
        (copy(2, kd.at[:, pl.ds(8, 1), :], kd.at[:, pl.ds(8 + N, 1), :], c, south), has_s, has_n),
        (copy(3, kd.at[:, pl.ds(7 + N, 1), :], kd.at[:, pl.ds(7, 1), :], c, north), has_n, has_s),
    ]
    cols = [
        (copy(4, msg_e, got_w.at[pl.ds(8, N), :], east, r), None, None),
        (copy(5, msg_w, got_e.at[pl.ds(8, N), :], west, r), None, None),
        (copy(6, msg_e.at[pl.ds(0, 8), :], got_w.at[pl.ds(8 + N, 8), :], east, south), has_s, has_n),
        (copy(7, msg_w.at[pl.ds(N - 8, 8), :], got_e.at[pl.ds(0, 8), :], west, north), has_n, has_s),
    ]

    def wide_set(base, main, to_e, to_w, in_e, in_w):
        lo, hi = pl.ds(0, W), pl.ds(N - W, W)
        return [
            (copy(base + 0, to_w, in_e.at[pl.ds(W, N), :], west, r), None, None),
            (copy(base + 1, to_e, in_w.at[pl.ds(W, N), :], east, r), None, None),
            (copy(base + 2, main.at[:, pl.ds(W, W), :], main.at[:, pl.ds(W + N, W), :], c, south), has_s, has_n),
            (copy(base + 3, main.at[:, pl.ds(N, W), :], main.at[:, pl.ds(0, W), :], c, north), has_n, has_s),
            (copy(base + 4, to_w.at[lo, :], in_e.at[pl.ds(W + N, W), :], west, south), has_s, has_n),
            (copy(base + 5, to_w.at[hi, :], in_e.at[lo, :], west, north), has_n, has_s),
            (copy(base + 6, to_e.at[lo, :], in_w.at[pl.ds(W + N, W), :], east, south), has_s, has_n),
            (copy(base + 7, to_e.at[hi, :], in_w.at[lo, :], east, north), has_n, has_s),
        ]

    wide = wide_set(8, wm, pk_e, pk_w, we, ww)
    forc = wide_set(16, fm, fk_e, fk_w, fe, fw)

    def run(cond, fn):
        if cond is None:
            fn()
        else:
            pl.when(cond)(fn)

    def start(items):
        for cp, s_if, _ in items:
            run(s_if, cp.start)

    def wait_recv(items):
        for cp, _, r_if in items:
            run(r_if, cp.wait_recv)

    def wait_send(items):
        for cp, s_if, _ in items:
            run(s_if, cp.wait_send)

    lane = lax.broadcasted_iota(jnp.int32, (N, N), 1)
    part = lax.rem(lane, 4)
    slot = lane // 4

    def roll(x, s):
        s %= N
        return pltpu.roll(x, s, 1) if s else x

    for cp in small:
        cp.wait()
    kmt_f = ki[...].astype(F32)
    dep = kd[1, 8:8 + N, :]
    kd[0, 8:8 + N, :] = kmt_f
    wm[3, W:W + N, :] = jnp.where(kmt_f > 0.0, dep, 0.0)

    acc = [jnp.zeros((N, N), F32)] * 4
    for ci, (k0, k1) in enumerate(CHUNKS):
        for cp in loads[ci]:
            cp.wait()
        if ci == len(CHUNKS) - 1:
            pl.semaphore_wait(barrier, len(places))
            start(rows)
        for f in range(4):
            x = acc[f]
            for k in range(k0, k1):
                x = jnp.where(slot == k, roll(fb[f, k, 8:8 + N, :], 4 * k + 2), x)
            acc[f] = x
    out_e = jnp.where(lane == 124, roll(kmt_f, -3), roll(dep, -2))
    out_w = jnp.where(lane == 124, roll(kmt_f, 124), roll(dep, 125))
    for f in range(4):
        qs[f, 8:8 + N, :] = acc[f]
        pick = (part == f) & (slot < LEVELS)
        out_e = jnp.where(pick, roll(acc[f], f - 1), out_e)
        out_w = jnp.where(pick, roll(acc[f], f - 2), out_w)
    msg_e[...] = out_e
    msg_w[...] = out_w

    def pack(fields):
        e_acc = jnp.zeros((N, N), F32)
        w_acc = jnp.zeros((N, N), F32)
        for f, x in enumerate(fields):
            here = lane // W == f
            w_acc = jnp.where(here, roll(x, W * f), w_acc)
            e_acc = jnp.where(here, roll(x, W * (f + 1)), e_acc)
        return e_acc, w_acc

    e_acc, w_acc = pack([wm[f, W:W + N, :] for f in range(4)])
    start(cols)
    pk_e[...] = e_acc
    pk_w[...] = w_acc

    @pl.when(jnp.logical_not(has_n))
    def _():
        fb[:, :, 8 + N:9 + N, :] = jnp.zeros((4, LEVELS, 1, N), F32)
        kd[:, 8 + N:9 + N, :] = jnp.zeros((2, 1, N), F32)
        got_w[8 + N:16 + N, :] = jnp.zeros((8, N), F32)

    @pl.when(jnp.logical_not(has_s))
    def _():
        fb[:, :, 7:8, :] = jnp.zeros((4, LEVELS, 1, N), F32)
        kd[:, 7:8, :] = jnp.zeros((2, 1, N), F32)
        got_e[0:8, :] = jnp.zeros((8, N), F32)

    start(wide)

    lane_p = lax.broadcasted_iota(jnp.int32, (PR, N), 1)
    edge = (lane_p == 0) | (lane_p == N - 1)

    def thick(k, d):
        return d / jnp.maximum(k, 1.0)

    def force(p_c, p_e, p_n, u_c, u_n, u_s, v_c, v_n, v_s):
        us, vs = u_c + u_n, v_c + v_s
        v_at_u = 0.25 * (vs + roll(vs, -1))
        u_at_v = 0.25 * (us + roll(us, 1))
        u_w = roll(u_c, 1)
        g_u = p_c - p_e - 0.5 * (u_c * (roll(u_c, -1) - u_w) + v_at_u * (u_n - u_s))
        g_v = p_c - p_n - 0.5 * (u_at_v * (roll(v_c, -1) - roll(v_c, 1)) + v_c * (v_n - v_s))
        return g_u, g_v, u_w

    def advect(ok_e, ok_w, ok_n, ok_s, u_c, u_w, v_c, v_s, tracers):
        u_e, u_w = jnp.where(ok_e, u_c, 0.0), jnp.where(ok_w, u_w, 0.0)
        v_n, v_s = jnp.where(ok_n, v_c, 0.0), jnp.where(ok_s, v_s, 0.0)
        a_e, a_w = jnp.minimum(u_e, 0.0), jnp.maximum(u_w, 0.0)
        a_n, a_s = jnp.minimum(v_n, 0.0), jnp.maximum(v_s, 0.0)
        a_c = (jnp.maximum(u_e, 0.0) - jnp.minimum(u_w, 0.0)) + (jnp.maximum(v_n, 0.0) - jnp.minimum(v_s, 0.0))
        out = []
        for x, x_n, x_s in tracers:
            div = a_c * x + (a_e * roll(x, -1) - a_w * roll(x, 1)) + (a_n * x_n - a_s * x_s)
            out.append(x - 0.25 * div)
        return out

    def main_step(i, _):
        @pl.when(i == N // PR - 2)
        def _():
            wait_recv(rows)

        own = pl.multiple_of(lax.rem(i + 1, N // PR) * PR, PR)
        base = own + 8

        def at(f, k, off):
            return fb[f, k, pl.ds(base + off, PR), :]

        kc = kd[0, pl.ds(base, PR), :]
        kn = kd[0, pl.ds(base + 1, PR), :]
        ks = kd[0, pl.ds(base - 1, PR), :]
        dc = kd[1, pl.ds(base, PR), :]
        dn = kd[1, pl.ds(base + 1, PR), :]
        th_c, th_n = thick(kc, dc), thick(kn, dn)
        nu_f = jnp.minimum(kc, roll(kc, -1))
        nw_f = jnp.minimum(kc, roll(kc, 1))
        nv_f = jnp.minimum(kc, kn)
        nq_f = jnp.minimum(kc, ks)
        zero = jnp.zeros((PR, N), F32)
        cum_c, cum_n, sum_u, sum_v = zero, zero, zero, zero
        for k in range(LEVELS):
            fk = float(k)
            t_c, s_c = at(2, k, 0), at(3, k, 0)
            t_n, s_n = at(2, k, 1), at(3, k, 1)
            d_c = jnp.where(kc > fk, 0.6 * s_c - 0.3 * t_c, 0.0)
            d_n = jnp.where(kn > fk, 0.6 * s_n - 0.3 * t_n, 0.0)
            cum_c, cum_n = cum_c + d_c, cum_n + d_n
            p_c = (cum_c - 0.5 * d_c) * th_c
            p_n = (cum_n - 0.5 * d_n) * th_n
            u_c, v_c, v_s = at(0, k, 0), at(1, k, 0), at(1, k, -1)
            g_u, g_v, u_w = force(p_c, roll(p_c, -1), p_n, u_c, at(0, k, 1), at(0, k, -1), v_c, at(1, k, 1), v_s)
            wet_u, wet_v = nu_f > fk, nv_f > fk
            sum_u = sum_u + jnp.where(wet_u, g_u, 0.0)
            sum_v = sum_v + jnp.where(wet_v, g_v, 0.0)
            nu_ref[k, pl.ds(own, PR), :] = jnp.where(wet_u, u_c + 0.25 * g_u, 0.0)
            nv_ref[k, pl.ds(own, PR), :] = jnp.where(wet_v, v_c + 0.25 * g_v, 0.0)
            t1, s1 = advect(wet_u, nw_f > fk, wet_v, nq_f > fk, u_c, u_w, v_c, v_s,
                            ((t_c, t_n, at(2, k, -1)), (s_c, s_n, at(3, k, -1))))
            nt_ref[k, pl.ds(own, PR), :] = t1
            ns_ref[k, pl.ds(own, PR), :] = s1
        hu = jnp.where(nu_f > 0.0, 0.5 * (dc + roll(dc, -1)), 0.0)
        hv = jnp.where(nv_f > 0.0, 0.5 * (dc + dn), 0.0)
        fm[0, pl.ds(own + W, PR), :] = hu * (1.0 / jnp.maximum(nu_f, 1.0)) * sum_u
        fm[1, pl.ds(own + W, PR), :] = hv * (1.0 / jnp.maximum(nv_f, 1.0)) * sum_v
        return 0

    lax.fori_loop(0, N // PR, main_step, 0)

    lane8 = lax.broadcasted_iota(jnp.int32, (8, N), 1)
    for f in range(4):
        for lo in (0, 8 + N):
            x = jnp.zeros((8, N), F32)
            for k in range(LEVELS):
                x = jnp.where(lane8 // 4 == k, roll(fb[f, k, lo:lo + 8, :], 4 * k + 2), x)
            qs[f, lo:lo + 8, :] = x

    wait_recv(cols)

    part_x = lax.rem(lax.broadcasted_iota(jnp.int32, (N + 16, N), 1), 4)
    for f in range(4):
        q = qs[f]
        xe[f] = jnp.where(part_x == 2, roll(got_e[...], 2 - f), q)
        xw[f] = jnp.where(part_x == 1, roll(got_w[...], 1 - f), q)
    for f in range(2):
        q = kd[f]
        b = [jnp.broadcast_to(q[:, j:j + 1], q.shape) for j in (N - 2, N - 1, 0, 1)]
        h_e = jnp.broadcast_to(got_e[:, 124 + f:125 + f], q.shape)
        h_w = jnp.broadcast_to(got_w[:, 124 + f:125 + f], q.shape)
        xe[4 + f] = jnp.where(part_x == 0, b[0], jnp.where(part_x == 1, b[1], h_e))
        xw[4 + f] = jnp.where(part_x == 1, h_w, jnp.where(part_x == 2, b[2], b[3]))

    lev = slot.astype(F32)

    def prefix(x):
        for s in (1, 2, 4, 8, 16):
            x = x + jnp.where(slot >= s, roll(x, 4 * s), 0.0)
        return x

    def total(x):
        for s in (1, 2, 4, 8, 16):
            x = x + roll(x, 4 * s)
        return x

    def strip(x):
        def at(f, off):
            return x[f, 8 + off:8 + off + N, :]

        kc, kn, ks = at(4, 0), at(4, 1), at(4, -1)
        dc, dn = at(5, 0), at(5, 1)
        nu_f, nw_f = jnp.minimum(kc, roll(kc, -1)), jnp.minimum(kc, roll(kc, 1))
        nv_f, nq_f = jnp.minimum(kc, kn), jnp.minimum(kc, ks)
        t_c, s_c, t_n, s_n = at(2, 0), at(3, 0), at(2, 1), at(3, 1)
        d_c = jnp.where(kc > lev, 0.6 * s_c - 0.3 * t_c, 0.0)
        d_n = jnp.where(kn > lev, 0.6 * s_n - 0.3 * t_n, 0.0)
        p_c = (prefix(d_c) - 0.5 * d_c) * thick(kc, dc)
        p_n = (prefix(d_n) - 0.5 * d_n) * thick(kn, dn)
        u_c, v_c, v_s = at(0, 0), at(1, 0), at(1, -1)
        g_u, g_v, u_w = force(p_c, roll(p_c, -1), p_n, u_c, at(0, 1), at(0, -1), v_c, at(1, 1), v_s)
        wet_u, wet_v = nu_f > lev, nv_f > lev
        hu = jnp.where(nu_f > 0.0, 0.5 * (dc + roll(dc, -1)), 0.0)
        hv = jnp.where(nv_f > 0.0, 0.5 * (dc + dn), 0.0)
        f_u = hu * (1.0 / jnp.maximum(nu_f, 1.0)) * total(jnp.where(wet_u, g_u, 0.0))
        f_v = hv * (1.0 / jnp.maximum(nv_f, 1.0)) * total(jnp.where(wet_v, g_v, 0.0))
        r_u = jnp.where(wet_u, u_c + 0.25 * g_u, 0.0)
        r_v = jnp.where(wet_v, v_c + 0.25 * g_v, 0.0)
        t1, s1 = advect(wet_u, nw_f > lev, wet_v, nq_f > lev, u_c, u_w, v_c, v_s,
                        ((t_c, t_n, at(2, -1)), (s_c, s_n, at(3, -1))))
        return f_u, f_v, r_u, r_v, t1, s1

    both = [jnp.where(part == 1, a, b) for a, b in zip(strip(xe), strip(xw))]
    rim = (lane == 0) | (lane == N - 1)
    forces = []
    for f in range(2):
        x = jnp.where(rim, roll(both[f], 2), fm[f, W:W + N, :])
        fm[f, W:W + N, :] = x
        forces.append(x)
    e_acc, w_acc = pack(forces)
    fk_e[...] = e_acc
    fk_w[...] = w_acc
    for f in range(4):
        ed[f] = both[2 + f]
    start(forc)

    def solve_step(g, _):
        own = pl.multiple_of(g * PR, PR)
        base = own + 8
        here = pl.ds(own, PR)
        kc = kd[0, pl.ds(base, PR), :]
        kn = kd[0, pl.ds(base + 1, PR), :]
        nu_f = jnp.minimum(kc, jnp.where(lane_p == N - 1, roll(got_e[pl.ds(base, PR), :], 3), roll(kc, -1)))
        nv_f = jnp.minimum(kc, kn)
        two_ref[0, here, :] = nu_f
        two_ref[1, here, :] = nv_f
        zero = jnp.zeros((PR, N), F32)
        refs = (nu_ref, nv_ref, nt_ref, ns_ref)
        nus = (VISC_NUM, VISC_NUM, DIFF_NUM, DIFF_NUM)
        cos = (VISC, VISC, DIFF, DIFF)
        d = [zero] * 4

        def factor(n_f, k, co):
            return jnp.where(n_f > k + 1.0, co[0][k], jnp.where(n_f > float(k), co[1][k], 0.0))

        for k in range(LEVELS):
            f_t = factor(kc, k, DIFF)
            facs = (factor(nu_f, k, VISC), factor(nv_f, k, VISC), f_t, f_t)
            for q in range(4):
                x = jnp.where(edge, roll(ed[q, here, :], 126 - 4 * k), refs[q][k, here, :])
                d[q] = (x + nus[q] * d[q]) * facs[q]
                refs[q][k, here, :] = d[q]
        sum_u, sum_v = d[0], d[1]
        for k in range(LEVELS - 2, -1, -1):
            for q in range(4):
                d[q] = refs[q][k, here, :] + cos[q][2][k] * d[q]
                refs[q][k, here, :] = d[q]
            sum_u, sum_v = sum_u + d[0], sum_v + d[1]
        two_ref[2, here, :] = sum_u / jnp.maximum(nu_f, 1.0)
        two_ref[3, here, :] = sum_v / jnp.maximum(nv_f, 1.0)
        return 0

    lax.fori_loop(0, N // PR, solve_step, 0)

    wait_recv(wide)
    wait_recv(forc)
    wm_out[...] = wm[...]
    we_out[...] = we[...]
    ww_out[...] = ww[...]
    fm_out[...] = fm[...]
    fe_out[...] = fe[...]
    fw_out[...] = fw[...]
    wait_send(rows)
    wait_send(cols)
    wait_send(wide)
    wait_send(forc)


TOP = EXT + 16


def step_kernel(nrow, nu_ref, nv_ref, nt_ref, ns_ref, two_ref, wm, we, ww, fm, fe, fw,
                eta_out, tu_out, tv_out, u_hbm, v_hbm, t_hbm, s_hbm,
                et, fu, fv, cu, cv, pu, pv, dm, mean, ub, vb, osem):
    r = lax.axis_index('row')
    copies = [pltpu.make_async_copy(nt_ref, t_hbm, osem.at[0]), pltpu.make_async_copy(ns_ref, s_hbm, osem.at[1])]
    for cp in copies:
        cp.start()

    lane = lax.broadcasted_iota(jnp.int32, (EXT, N), 1)
    rows = lax.broadcasted_iota(jnp.int32, (EXT, N), 0)
    last = lane == N - 1
    first = lane == 0
    lo_ok = jnp.where(r > 0, 0, W)
    hi_ok = jnp.where(r < nrow - 1, EXT, W + N)
    real = (rows >= lo_ok) & (rows < hi_ok)
    in_e = lane < W
    in_w = lane >= N - W

    def side(e_ref, w_ref, f):
        e = e_ref[...]
        w = w_ref[...]
        se = (N - W * f) % N
        sw = (2 * N - W * (f + 1)) % N
        e = pltpu.roll(e, se, 1) if se else e
        w = pltpu.roll(w, sw, 1) if sw else w
        return jnp.where(in_e, e, jnp.where(in_w, w, 0.0))

    def east_of(a, b):
        ra, rb = pltpu.roll(a, N - 1, 1), pltpu.roll(b, N - 1, 1)
        return jnp.where(last, rb, ra), jnp.where(last, ra, rb)

    def west_of(a, b):
        ra, rb = pltpu.roll(a, 1, 1), pltpu.roll(b, 1, 1)
        return jnp.where(first, rb, ra), jnp.where(first, ra, rb)

    body = pl.ds(8, EXT)
    zero8 = jnp.zeros((8, N), F32)
    for ref in (et, fu, fv, dm):
        for t in range(2):
            ref[t, 0:8, :] = zero8
            ref[t, 8 + EXT:TOP, :] = zero8

    dms = (jnp.where(real, wm[3], 0.0), jnp.where(real & (in_e | in_w), side(we, ww, 3), 0.0))
    for t in range(2):
        dm[t, body, :] = dms[t]
    dme = east_of(*dms)
    for t in range(2):
        d_c = dms[t]
        d_n = dm[t, 9:9 + EXT, :]
        wet_u = (d_c > 0.0) & (dme[t] > 0.0)
        wet_v = (d_c > 0.0) & (d_n > 0.0)
        pick = (lambda f: wm[f]) if t == 0 else (lambda f: side(we, ww, f))
        fpick = (lambda f: fm[f]) if t == 0 else (lambda f: side(fe, fw, f))
        et[t, body, :] = jnp.where(d_c > 0.0, pick(0), 0.0)
        fu[t, body, :] = jnp.where(wet_u, 0.5 * pick(1), 0.0)
        fv[t, body, :] = jnp.where(wet_v, 0.5 * pick(2), 0.0)
        cu[t] = jnp.where(wet_u, 0.125 * (d_c + dme[t]), 0.0)
        cv[t] = jnp.where(wet_v, 0.125 * (d_c + d_n), 0.0)
        pu[t] = jnp.where(wet_u, (0.125 / SUBCYCLES) * fpick(0), 0.0)
        pv[t] = jnp.where(wet_v, (0.125 / SUBCYCLES) * fpick(1), 0.0)
    wgt = weights()
    lane8 = lax.broadcasted_iota(jnp.int32, (8, N), 1)
    first8, last8 = lane8 == 0, lane8 == N - 1

    def west8(x):
        a, b = pltpu.roll(x[0], 1, 1), pltpu.roll(x[1], 1, 1)
        return jnp.where(first8, b, a), jnp.where(first8, a, b)

    def east8(x):
        a, b = pltpu.roll(x[0], N - 1, 1), pltpu.roll(x[1], N - 1, 1)
        return jnp.where(last8, b, a), jnp.where(last8, a, b)

    for n in range(1, SUBCYCLES + 1):
        lo = 8 * (n // 8)
        groups = range(lo, EXT - lo, 8)
        for g in groups:
            us = (fu[0, 8 + g:16 + g, :], fu[1, 8 + g:16 + g, :])
            uw = west8(us)
            for t in range(2):
                et[t, 8 + g:16 + g, :] = et[t, 8 + g:16 + g, :] - (
                    (us[t] - uw[t]) + (fv[t, 8 + g:16 + g, :] - fv[t, 7 + g:15 + g, :]))
        for g in groups:
            es = (et[0, 8 + g:16 + g, :], et[1, 8 + g:16 + g, :])
            ee = east8(es)
            for t in range(2):
                u = fu[t, 8 + g:16 + g, :] - cu[t, g:g + 8, :] * (ee[t] - es[t]) + pu[t, g:g + 8, :]
                v = fv[t, 8 + g:16 + g, :] - cv[t, g:g + 8, :] * (et[t, 9 + g:17 + g, :] - es[t]) + pv[t, g:g + 8, :]
                fu[t, 8 + g:16 + g, :] = u
                fv[t, 8 + g:16 + g, :] = v
                if t == 0 and W <= g < W + N:
                    at = slice(g - W, g - W + 8)
                    w = float(wgt[n - 1])
                    mean[0, at, :] = w * u if n == 1 else mean[0, at, :] + w * u
                    mean[1, at, :] = w * v if n == 1 else mean[1, at, :] + w * v

    mid = slice(8 + W, 8 + W + N)
    eta_out[...] = et[0, mid, :]
    tu_out[...] = 2.0 * fu[0, mid, :]
    tv_out[...] = 2.0 * fv[0, mid, :]
    for i, co in ((0, cu), (1, cv)):
        h = co[0, W:W + N, :]
        mean[i] = mean[i] / jnp.where(h > 0.0, 2.0 * h, 1.0) - two_ref[2 + i]

    for ci, (k0, k1) in enumerate(CHUNKS):
        for i, (src, buf, dst) in enumerate(((nu_ref, ub, u_hbm), (nv_ref, vb, v_hbm))):
            for k in range(k0, k1):
                buf[k] = src[k] + jnp.where(two_ref[i] > float(k), mean[i], 0.0)
            cp = pltpu.make_async_copy(buf.at[pl.ds(k0, k1 - k0)], dst.at[pl.ds(k0, k1 - k0)], osem.at[2 + 2 * ci + i])
            cp.start()
            copies.append(cp)
    for cp in copies:
        cp.wait()


def solution(mesh):
    ncol, nrow = mesh.shape['col'], mesh.shape['row']
    vmem = pl.BlockSpec(memory_space=pltpu.VMEM)
    hbm = pl.BlockSpec(memory_space=pl.ANY)
    s3 = jax.ShapeDtypeStruct((LEVELS, N, N), F32)
    s2 = jax.ShapeDtypeStruct((N, N), F32)

    def sds(*shape):
        return jax.ShapeDtypeStruct(shape, F32)

    def ocean_step(vel_u, vel_v, temp, salt, eta, tu, tv, dep, kmt):
        def kernel_a(*refs):
            exchange_kernel(ncol, nrow, *refs)

        def kernel_b(*refs):
            step_kernel(nrow, *refs)

        mid = pl.pallas_call(
            kernel_a,
            name='exchange',
            out_shape=(s3, s3, s3, s3, sds(4, N, N), sds(4, EXT, N), sds(EXT, N), sds(EXT, N), sds(2, EXT, N), sds(EXT, N), sds(EXT, N)),
            in_specs=[hbm] * 9,
            out_specs=(vmem,) * 11,
            scratch_shapes=[
                pltpu.VMEM((4, LEVELS, N + 16, N), F32),
                pltpu.VMEM((N, N), jnp.int32),
                pltpu.VMEM((2, N + 16, N), F32),
                pltpu.VMEM((4, N + 16, N), F32),
                pltpu.VMEM((N, N), F32), pltpu.VMEM((N, N), F32),
                pltpu.VMEM((N + 16, N), F32), pltpu.VMEM((N + 16, N), F32),
                pltpu.VMEM((6, N + 16, N), F32), pltpu.VMEM((6, N + 16, N), F32),
                pltpu.VMEM((4, N, N), F32),
                pltpu.VMEM((4, EXT, N), F32),
                pltpu.VMEM((N, N), F32), pltpu.VMEM((N, N), F32),
                pltpu.VMEM((EXT, N), F32), pltpu.VMEM((EXT, N), F32),
                pltpu.VMEM((2, EXT, N), F32),
                pltpu.VMEM((N, N), F32), pltpu.VMEM((N, N), F32),
                pltpu.VMEM((EXT, N), F32), pltpu.VMEM((EXT, N), F32),
                pltpu.SemaphoreType.DMA((4, len(CHUNKS))),
                pltpu.SemaphoreType.DMA((5,)),
                pltpu.SemaphoreType.DMA((24,)),
                pltpu.SemaphoreType.DMA((24,)),
            ],
            compiler_params=pltpu.CompilerParams(collective_id=0, has_side_effects=True, vmem_limit_bytes=28 * 2 ** 20),
        )(*[pltpu.with_memory_space_constraint(x, pltpu.HBM) for x in (vel_u, vel_v, temp, salt, eta, tu, tv, dep, kmt)])
        st = pltpu.VMEM((2, TOP, N), F32)
        co = pltpu.VMEM((2, EXT, N), F32)
        out = pl.pallas_call(
            kernel_b,
            name='subcycles',
            out_shape=(s2, s2, s2, s3, s3, s3, s3),
            in_specs=[vmem] * 11,
            out_specs=(vmem,) * 3 + (hbm,) * 4,
            scratch_shapes=[st, st, st, co, co, co, co, st, pltpu.VMEM((2, N, N), F32),
                            pltpu.VMEM((LEVELS, N, N), F32), pltpu.VMEM((LEVELS, N, N), F32),
                            pltpu.SemaphoreType.DMA((2 + 2 * len(CHUNKS),))],
            compiler_params=pltpu.CompilerParams(vmem_limit_bytes=28 * 2 ** 20),
        )(*mid)
        return out

    spec_3d = P(None, 'row', 'col')
    spec_2d = P('row', 'col')
    return jax.shard_map(ocean_step, mesh=mesh, in_specs=(spec_3d,) * 4 + (spec_2d,) * 5,
                         out_specs=(spec_2d,) * 3 + (spec_3d,) * 4, check_vma=False)
```

```python
import jax
import jax.numpy as jnp
import numpy as np
from jax import lax
from jax.experimental import pallas as pl
from jax.experimental.pallas import tpu as pltpu
from jax.sharding import PartitionSpec as P

MESH = pl.DeviceIdType.MESH
F32 = jnp.float32
SUBCYCLES = 30
LEVELS = 31
VISC_NUM = 4.0
DIFF_NUM = 1.0
N = 128
W = 32
EXT = N + 2 * W
TOP = EXT + 16
PR = 16
CHUNKS = ((0, 9), (9, 18), (18, 26), (26, 31))


def solve_coefs(nu):
    inner, last, back = [], [], []
    c_prev = 0.0
    for k in range(LEVELS):
        lo = nu if k > 0 else 0.0
        piv = 1.0 + nu + lo - lo * c_prev
        inner.append(1.0 / piv)
        last.append(1.0 / (1.0 + lo - lo * c_prev))
        c_prev = nu / piv
        back.append(c_prev)
    return inner, last, back


VISC = solve_coefs(VISC_NUM)
DIFF = solve_coefs(DIFF_NUM)


def weights():
    s = np.arange(1, SUBCYCLES + 1, dtype=np.float64) / (SUBCYCLES + 1)
    w = s ** 2 * (1.0 - s ** 4)
    return (w / w.sum()).astype(np.float32)


def exchange_kernel(ncol, nrow, u_hbm, v_hbm, t_hbm, s_hbm, eta_hbm, tu_hbm, tv_hbm, dep_hbm, kmt_hbm,
                    nu_ref, nv_ref, nt_ref, ns_ref, two_ref, et, fu, fv, cu, cv, fm_out, fe_out, fw_out,
                    fb, ki, kd, qs, msg_e, msg_w, got_w, got_e, xe, xw, ed,
                    wm, pk_e, pk_w, we, ww, fm, fk_e, fk_w, fe, fw,
                    ld_sem, in_sem, snd, rcv):
    c = lax.axis_index('col')
    r = lax.axis_index('row')
    east = lax.rem(c + 1, ncol)
    west = lax.rem(c + ncol - 1, ncol)
    north = lax.rem(r + 1, nrow)
    south = lax.rem(r + nrow - 1, nrow)
    has_n = r < nrow - 1
    has_s = r > 0

    src3 = (u_hbm, v_hbm, t_hbm, s_hbm)
    small = [pltpu.make_async_copy(kmt_hbm, ki, in_sem.at[0]),
             pltpu.make_async_copy(dep_hbm, kd.at[1, pl.ds(8, N), :], in_sem.at[1]),
             pltpu.make_async_copy(eta_hbm, wm.at[0, pl.ds(W, N), :], in_sem.at[2]),
             pltpu.make_async_copy(tu_hbm, wm.at[1, pl.ds(W, N), :], in_sem.at[3]),
             pltpu.make_async_copy(tv_hbm, wm.at[2, pl.ds(W, N), :], in_sem.at[4])]
    loads = []
    for ci, (k0, k1) in enumerate(CHUNKS):
        row = [pltpu.make_async_copy(src3[f].at[pl.ds(k0, k1 - k0)], fb.at[f, pl.ds(k0, k1 - k0), pl.ds(8, N), :],
                                     ld_sem.at[f, ci]) for f in range(4)]
        loads.append(row)
        for cp in row:
            cp.start()
        if ci == 0:
            for cp in small:
                cp.start()

    barrier = pltpu.get_barrier_semaphore()
    places = [(east, r), (west, r), (c, north), (c, south), (east, north), (east, south), (west, north), (west, south)]
    for cc, rr in places:
        pl.semaphore_signal(barrier, inc=1, device_id={'col': cc, 'row': rr}, device_id_type=MESH)

    def copy(i, src, dst, cc, rr):
        return pltpu.make_async_remote_copy(src_ref=src, dst_ref=dst, send_sem=snd.at[i], recv_sem=rcv.at[i],
                                            device_id={'col': cc, 'row': rr}, device_id_type=MESH)

    rows = [
        (copy(0, fb.at[:, :, pl.ds(8, 1), :], fb.at[:, :, pl.ds(8 + N, 1), :], c, south), has_s, has_n),
        (copy(1, fb.at[:, :, pl.ds(7 + N, 1), :], fb.at[:, :, pl.ds(7, 1), :], c, north), has_n, has_s),
        (copy(2, kd.at[:, pl.ds(8, 1), :], kd.at[:, pl.ds(8 + N, 1), :], c, south), has_s, has_n),
        (copy(3, kd.at[:, pl.ds(7 + N, 1), :], kd.at[:, pl.ds(7, 1), :], c, north), has_n, has_s),
    ]
    cols = [
        (copy(4, msg_e, got_w.at[pl.ds(8, N), :], east, r), None, None),
        (copy(5, msg_w, got_e.at[pl.ds(8, N), :], west, r), None, None),
        (copy(6, msg_e.at[pl.ds(0, 8), :], got_w.at[pl.ds(8 + N, 8), :], east, south), has_s, has_n),
        (copy(7, msg_w.at[pl.ds(N - 8, 8), :], got_e.at[pl.ds(0, 8), :], west, north), has_n, has_s),
    ]

    def wide_set(base, main, to_e, to_w, in_e, in_w, n):
        lo, hi = pl.ds(0, W), pl.ds(n - W, W)
        return [
            (copy(base + 0, to_w, in_e.at[pl.ds(W, n), :], west, r), None, None),
            (copy(base + 1, to_e, in_w.at[pl.ds(W, n), :], east, r), None, None),
            (copy(base + 2, main.at[:, pl.ds(W, W), :], main.at[:, pl.ds(W + N, W), :], c, south), has_s, has_n),
            (copy(base + 3, main.at[:, pl.ds(N, W), :], main.at[:, pl.ds(0, W), :], c, north), has_n, has_s),
            (copy(base + 4, to_w.at[lo, :], in_e.at[pl.ds(W + n, W), :], west, south), has_s, has_n),
            (copy(base + 5, to_w.at[hi, :], in_e.at[lo, :], west, north), has_n, has_s),
            (copy(base + 6, to_e.at[lo, :], in_w.at[pl.ds(W + n, W), :], east, south), has_s, has_n),
            (copy(base + 7, to_e.at[hi, :], in_w.at[lo, :], east, north), has_n, has_s),
        ]

    wide = wide_set(8, wm, pk_e, pk_w, we, ww, N)
    forc = wide_set(16, fm, fk_e, fk_w, fe, fw, N // 2)

    def run(cond, fn):
        if cond is None:
            fn()
        else:
            pl.when(cond)(fn)

    def start(items):
        for cp, s_if, _ in items:
            run(s_if, cp.start)

    def wait_recv(items):
        for cp, _, r_if in items:
            run(r_if, cp.wait_recv)

    def wait_send(items):
        for cp, s_if, _ in items:
            run(s_if, cp.wait_send)

    lane = lax.broadcasted_iota(jnp.int32, (N, N), 1)
    part = lax.rem(lane, 4)
    slot = lane // 4

    def roll(x, s):
        s %= N
        return pltpu.roll(x, s, 1) if s else x

    for cp in small:
        cp.wait()
    kmt_f = ki[...].astype(F32)
    dep = kd[1, 8:8 + N, :]
    kd[0, 8:8 + N, :] = kmt_f
    wm[3, W:W + N, :] = jnp.where(kmt_f > 0.0, dep, 0.0)

    def pack(fields):
        e_acc = jnp.zeros((N, N), F32)
        w_acc = jnp.zeros((N, N), F32)
        for f, x in enumerate(fields):
            here = lane // W == f
            w_acc = jnp.where(here, roll(x, W * f), w_acc)
            e_acc = jnp.where(here, roll(x, W * (f + 1)), e_acc)
        return e_acc, w_acc

    e_acc, w_acc = pack([wm[f, W:W + N, :] for f in range(4)])
    pk_e[...] = e_acc
    pk_w[...] = w_acc

    acc = [jnp.zeros((N, N), F32)] * 4
    for ci, (k0, k1) in enumerate(CHUNKS):
        for cp in loads[ci]:
            cp.wait()
        if ci == 0:
            pl.semaphore_wait(barrier, len(places))
            start(wide)
        if ci == len(CHUNKS) - 1:
            start(rows)
        for f in range(4):
            x = acc[f]
            for k in range(k0, k1):
                x = jnp.where(slot == k, roll(fb[f, k, 8:8 + N, :], 4 * k + 2), x)
            acc[f] = x
    out_e = jnp.where(lane == 124, roll(kmt_f, -3), roll(dep, -2))
    out_w = jnp.where(lane == 124, roll(kmt_f, 124), roll(dep, 125))
    for f in range(4):
        qs[f, 8:8 + N, :] = acc[f]
        pick = (part == f) & (slot < LEVELS)
        out_e = jnp.where(pick, roll(acc[f], f - 1), out_e)
        out_w = jnp.where(pick, roll(acc[f], f - 2), out_w)
    msg_e[...] = out_e
    msg_w[...] = out_w

    start(cols)

    @pl.when(jnp.logical_not(has_n))
    def _():
        fb[:, :, 8 + N:9 + N, :] = jnp.zeros((4, LEVELS, 1, N), F32)
        kd[:, 8 + N:9 + N, :] = jnp.zeros((2, 1, N), F32)
        got_w[8 + N:16 + N, :] = jnp.zeros((8, N), F32)

    @pl.when(jnp.logical_not(has_s))
    def _():
        fb[:, :, 7:8, :] = jnp.zeros((4, LEVELS, 1, N), F32)
        kd[:, 7:8, :] = jnp.zeros((2, 1, N), F32)
        got_e[0:8, :] = jnp.zeros((8, N), F32)

    lane_p = lax.broadcasted_iota(jnp.int32, (PR, N), 1)
    edge = (lane_p == 0) | (lane_p == N - 1)

    def thick(k, d):
        return d / jnp.maximum(k, 1.0)

    def force(p_c, p_e, p_n, u_c, u_n, u_s, v_c, v_n, v_s):
        us, vs = u_c + u_n, v_c + v_s
        v_at_u = 0.25 * (vs + roll(vs, -1))
        u_at_v = 0.25 * (us + roll(us, 1))
        u_w = roll(u_c, 1)
        g_u = p_c - p_e - 0.5 * (u_c * (roll(u_c, -1) - u_w) + v_at_u * (u_n - u_s))
        g_v = p_c - p_n - 0.5 * (u_at_v * (roll(v_c, -1) - roll(v_c, 1)) + v_c * (v_n - v_s))
        return g_u, g_v, u_w

    def advect(ok_e, ok_w, ok_n, ok_s, u_c, u_w, v_c, v_s, tracers):
        u_e, u_w = jnp.where(ok_e, u_c, 0.0), jnp.where(ok_w, u_w, 0.0)
        v_n, v_s = jnp.where(ok_n, v_c, 0.0), jnp.where(ok_s, v_s, 0.0)
        a_e, a_w = jnp.minimum(u_e, 0.0), jnp.maximum(u_w, 0.0)
        a_n, a_s = jnp.minimum(v_n, 0.0), jnp.maximum(v_s, 0.0)
        a_c = (jnp.maximum(u_e, 0.0) - jnp.minimum(u_w, 0.0)) + (jnp.maximum(v_n, 0.0) - jnp.minimum(v_s, 0.0))
        out = []
        for x, x_n, x_s in tracers:
            div = a_c * x + (a_e * roll(x, -1) - a_w * roll(x, 1)) + (a_n * x_n - a_s * x_s)
            out.append(x - 0.25 * div)
        return out

    def main_step(i, _):
        @pl.when(i == N // PR - 2)
        def _():
            wait_recv(rows)

        own = pl.multiple_of(lax.rem(i + 1, N // PR) * PR, PR)
        base = own + 8

        def at(f, k, off):
            return fb[f, k, pl.ds(base + off, PR), :]

        kc = kd[0, pl.ds(base, PR), :]
        kn = kd[0, pl.ds(base + 1, PR), :]
        ks = kd[0, pl.ds(base - 1, PR), :]
        dc = kd[1, pl.ds(base, PR), :]
        dn = kd[1, pl.ds(base + 1, PR), :]
        th_c, th_n = thick(kc, dc), thick(kn, dn)
        nu_f = jnp.minimum(kc, roll(kc, -1))
        nw_f = jnp.minimum(kc, roll(kc, 1))
        nv_f = jnp.minimum(kc, kn)
        nq_f = jnp.minimum(kc, ks)
        zero = jnp.zeros((PR, N), F32)
        cum_c, cum_n, sum_u, sum_v = zero, zero, zero, zero
        for k in range(LEVELS):
            fk = float(k)
            t_c, s_c = at(2, k, 0), at(3, k, 0)
            t_n, s_n = at(2, k, 1), at(3, k, 1)
            d_c = jnp.where(kc > fk, 0.6 * s_c - 0.3 * t_c, 0.0)
            d_n = jnp.where(kn > fk, 0.6 * s_n - 0.3 * t_n, 0.0)
            cum_c, cum_n = cum_c + d_c, cum_n + d_n
            p_c = (cum_c - 0.5 * d_c) * th_c
            p_n = (cum_n - 0.5 * d_n) * th_n
            u_c, v_c, v_s = at(0, k, 0), at(1, k, 0), at(1, k, -1)
            g_u, g_v, u_w = force(p_c, roll(p_c, -1), p_n, u_c, at(0, k, 1), at(0, k, -1), v_c, at(1, k, 1), v_s)
            wet_u, wet_v = nu_f > fk, nv_f > fk
            sum_u = sum_u + jnp.where(wet_u, g_u, 0.0)
            sum_v = sum_v + jnp.where(wet_v, g_v, 0.0)
            nu_ref[k, pl.ds(own, PR), :] = jnp.where(wet_u, u_c + 0.25 * g_u, 0.0)
            nv_ref[k, pl.ds(own, PR), :] = jnp.where(wet_v, v_c + 0.25 * g_v, 0.0)
            t1, s1 = advect(wet_u, nw_f > fk, wet_v, nq_f > fk, u_c, u_w, v_c, v_s,
                            ((t_c, t_n, at(2, k, -1)), (s_c, s_n, at(3, k, -1))))
            nt_ref[k, pl.ds(own, PR), :] = t1
            ns_ref[k, pl.ds(own, PR), :] = s1
        hu = jnp.where(nu_f > 0.0, 0.5 * (dc + roll(dc, -1)), 0.0)
        hv = jnp.where(nv_f > 0.0, 0.5 * (dc + dn), 0.0)
        fm[0, pl.ds(own + W, PR), :] = hu * (1.0 / jnp.maximum(nu_f, 1.0)) * sum_u
        fm[1, pl.ds(own + W, PR), :] = hv * (1.0 / jnp.maximum(nv_f, 1.0)) * sum_v
        return 0

    lax.fori_loop(0, N // PR, main_step, 0)

    lane8 = lax.broadcasted_iota(jnp.int32, (8, N), 1)
    for f in range(4):
        for lo in (0, 8 + N):
            x = jnp.zeros((8, N), F32)
            for k in range(LEVELS):
                x = jnp.where(lane8 // 4 == k, roll(fb[f, k, lo:lo + 8, :], 4 * k + 2), x)
            qs[f, lo:lo + 8, :] = x

    wait_recv(cols)

    part_x = lax.rem(lax.broadcasted_iota(jnp.int32, (N + 16, N), 1), 4)
    for f in range(4):
        q = qs[f]
        xe[f] = jnp.where(part_x == 2, roll(got_e[...], 2 - f), q)
        xw[f] = jnp.where(part_x == 1, roll(got_w[...], 1 - f), q)
    for f in range(2):
        q = kd[f]
        b = [jnp.broadcast_to(q[:, j:j + 1], q.shape) for j in (N - 2, N - 1, 0, 1)]
        h_e = jnp.broadcast_to(got_e[:, 124 + f:125 + f], q.shape)
        h_w = jnp.broadcast_to(got_w[:, 124 + f:125 + f], q.shape)
        xe[4 + f] = jnp.where(part_x == 0, b[0], jnp.where(part_x == 1, b[1], h_e))
        xw[4 + f] = jnp.where(part_x == 1, h_w, jnp.where(part_x == 2, b[2], b[3]))

    lev = slot.astype(F32)

    row_i = lax.broadcasted_iota(jnp.int32, (N, N), 0)
    same = lax.rem(row_i, 4) == part
    below = jnp.where(same & (row_i // 4 <= slot), 1.0, 0.0)
    every = jnp.where(same, 1.0, 0.0)

    def mix(x, m):
        return jnp.dot(x, m, precision=lax.Precision.HIGHEST, preferred_element_type=F32)

    def strip_force(x):
        def at(f, off):
            return x[f, 8 + off:8 + off + N, :]

        kc, kn = at(4, 0), at(4, 1)
        dc, dn = at(5, 0), at(5, 1)
        nu_f, nv_f = jnp.minimum(kc, roll(kc, -1)), jnp.minimum(kc, kn)
        d_c = jnp.where(kc > lev, 0.6 * at(3, 0) - 0.3 * at(2, 0), 0.0)
        d_n = jnp.where(kn > lev, 0.6 * at(3, 1) - 0.3 * at(2, 1), 0.0)
        p_c = (mix(d_c, below) - 0.5 * d_c) * thick(kc, dc)
        p_n = (mix(d_n, below) - 0.5 * d_n) * thick(kn, dn)
        u_c, v_c = at(0, 0), at(1, 0)
        g_u, g_v, u_w = force(p_c, roll(p_c, -1), p_n, u_c, at(0, 1), at(0, -1), v_c, at(1, 1), at(1, -1))
        wet_u, wet_v = nu_f > lev, nv_f > lev
        hu = jnp.where(nu_f > 0.0, 0.5 * (dc + roll(dc, -1)), 0.0) / jnp.maximum(nu_f, 1.0)
        hv = jnp.where(nv_f > 0.0, 0.5 * (dc + dn), 0.0) / jnp.maximum(nv_f, 1.0)
        r_u = jnp.where(wet_u, u_c + 0.25 * g_u, 0.0)
        r_v = jnp.where(wet_v, v_c + 0.25 * g_v, 0.0)
        return hu, hv, jnp.where(wet_u, g_u, 0.0), jnp.where(wet_v, g_v, 0.0), r_u, r_v

    def strip_tracer(x):
        def at(f, off):
            return x[f, 8 + off:8 + off + N, :]

        kc, kn, ks = at(4, 0), at(4, 1), at(4, -1)
        u_c = at(0, 0)
        return advect(jnp.minimum(kc, roll(kc, -1)) > lev, jnp.minimum(kc, roll(kc, 1)) > lev,
                      jnp.minimum(kc, kn) > lev, jnp.minimum(kc, ks) > lev, u_c, roll(u_c, 1), at(1, 0), at(1, -1),
                      ((at(2, 0), at(2, 1), at(2, -1)), (at(3, 0), at(3, 1), at(3, -1))))

    def merge(fn):
        return [jnp.where(part == 1, a, b) for a, b in zip(fn(xe), fn(xw))]

    hu, hv, g_u, g_v, r_u, r_v = merge(strip_force)
    rim = (lane == 0) | (lane == N - 1)
    forces = []
    for f, (h, g) in enumerate(((hu, g_u), (hv, g_v))):
        x = jnp.where(rim, roll(h * mix(g, every), 2), fm[f, W:W + N, :])
        fm[f, W:W + N, :] = x
        forces.append(x)
    half = lax.broadcasted_iota(jnp.int32, (N // 2, N), 1) < N // 2
    for ref, x in zip((fk_e, fk_w), pack(forces)):
        ref[...] = jnp.where(half, x[:N // 2], roll(x[N // 2:], N // 2))
    start(forc)
    ed[0] = r_u
    ed[1] = r_v
    t1, s1 = merge(strip_tracer)
    ed[2] = t1
    ed[3] = s1

    def solve_step(g, _):
        own = pl.multiple_of(g * PR, PR)
        base = own + 8
        here = pl.ds(own, PR)
        kc = kd[0, pl.ds(base, PR), :]
        kn = kd[0, pl.ds(base + 1, PR), :]
        nu_f = jnp.minimum(kc, jnp.where(lane_p == N - 1, roll(got_e[pl.ds(base, PR), :], 3), roll(kc, -1)))
        nv_f = jnp.minimum(kc, kn)
        two_ref[0, here, :] = nu_f
        two_ref[1, here, :] = nv_f
        zero = jnp.zeros((PR, N), F32)
        refs = (nu_ref, nv_ref, nt_ref, ns_ref)
        nus = (VISC_NUM, VISC_NUM, DIFF_NUM, DIFF_NUM)
        cos = (VISC, VISC, DIFF, DIFF)
        d = [zero] * 4

        def factor(n_f, k, co):
            return jnp.where(n_f > k + 1.0, co[0][k], jnp.where(n_f > float(k), co[1][k], 0.0))

        for k in range(LEVELS):
            f_t = factor(kc, k, DIFF)
            facs = (factor(nu_f, k, VISC), factor(nv_f, k, VISC), f_t, f_t)
            for q in range(4):
                x = jnp.where(edge, roll(ed[q, here, :], 126 - 4 * k), refs[q][k, here, :])
                d[q] = (x + nus[q] * d[q]) * facs[q]
                refs[q][k, here, :] = d[q]
        sum_u, sum_v = d[0], d[1]
        for k in range(LEVELS - 2, -1, -1):
            for q in range(4):
                d[q] = refs[q][k, here, :] + cos[q][2][k] * d[q]
                refs[q][k, here, :] = d[q]
            sum_u, sum_v = sum_u + d[0], sum_v + d[1]
        two_ref[2, here, :] = sum_u / jnp.maximum(nu_f, 1.0)
        two_ref[3, here, :] = sum_v / jnp.maximum(nv_f, 1.0)
        return 0

    lax.fori_loop(0, N // PR, solve_step, 0)

    wait_recv(wide)
    lane_x = lax.broadcasted_iota(jnp.int32, (EXT, N), 1)
    row_x = lax.broadcasted_iota(jnp.int32, (EXT, N), 0)
    real = (row_x >= jnp.where(has_s, 0, W)) & (row_x < jnp.where(has_n, EXT, W + N))
    in_e, in_w = lane_x < W, lane_x >= N - W

    def side(f):
        return jnp.where(in_e, roll(we[...], -W * f), roll(ww[...], -W * (f + 1)))

    dms = (jnp.where(real, wm[3], 0.0), jnp.where(real & (in_e | in_w), side(3), 0.0))
    zero8 = jnp.zeros((8, N), F32)
    for ref in (et, fu, fv):
        for t in range(2):
            ref[t, 0:8, :] = zero8
            ref[t, 8 + EXT:TOP, :] = zero8
    for t in range(2):
        et[t, 8:8 + EXT, :] = dms[t]
    ra, rb = roll(dms[0], -1), roll(dms[1], -1)
    dme = (jnp.where(lane_x == N - 1, rb, ra), jnp.where(lane_x == N - 1, ra, rb))
    for t in range(2):
        d_c = dms[t]
        d_n = et[t, 9:9 + EXT, :]
        wet_u = (d_c > 0.0) & (dme[t] > 0.0)
        wet_v = (d_c > 0.0) & (d_n > 0.0)
        pick = (lambda f: wm[f]) if t == 0 else side
        et[t, 8:8 + EXT, :] = jnp.where(d_c > 0.0, pick(0), 0.0)
        fu[t, 8:8 + EXT, :] = jnp.where(wet_u, 0.5 * pick(1), 0.0)
        fv[t, 8:8 + EXT, :] = jnp.where(wet_v, 0.5 * pick(2), 0.0)
        cu[t] = jnp.where(wet_u, 0.125 * (d_c + dme[t]), 0.0)
        cv[t] = jnp.where(wet_v, 0.125 * (d_c + d_n), 0.0)
    wait_send(rows)
    wait_send(cols)
    wait_send(wide)
    wait_recv(forc)
    fm_out[...] = fm[...]
    h = N // 2
    for out, got in ((fe_out, fe), (fw_out, fw)):
        out[0:W, :] = roll(got[0:W, :], h)
        out[W:W + h, :] = got[W:W + h, :]
        out[W + h:W + N, :] = roll(got[W:W + h, :], h)
        out[W + N:EXT, :] = got[W + h:N, :]
    wait_send(forc)


def step_kernel(nu_ref, nv_ref, nt_ref, ns_ref, two_ref, et0, fu0, fv0, cu, cv, fm, fe, fw,
                eta_out, tu_out, tv_out, u_hbm, v_hbm, t_hbm, s_hbm,
                et1, fu1, fv1, pu, pv, mean, ub, vb, osem):
    copies = [pltpu.make_async_copy(nt_ref, t_hbm, osem.at[0]), pltpu.make_async_copy(ns_ref, s_hbm, osem.at[1])]
    for cp in copies:
        cp.start()

    lane = lax.broadcasted_iota(jnp.int32, (EXT, N), 1)

    def side(f):
        e, w = fe[...], fw[...]
        e = pltpu.roll(e, N - W * f, 1) if f else e
        w = pltpu.roll(w, N - W * (f + 1), 1)
        return jnp.where(lane < W, e, w)

    for f, (p, co) in enumerate(((pu, cu), (pv, cv))):
        for t in range(2):
            x = fm[f] if t == 0 else side(f)
            p[t] = jnp.where(co[t] > 0.0, (0.125 / SUBCYCLES) * x, 0.0)
    zero8 = jnp.zeros((8, N), F32)
    for ref in (et1, fv1):
        for t in range(2):
            ref[t, 0:8, :] = zero8
            ref[t, 8 + EXT:TOP, :] = zero8

    wgt = weights()
    lane8 = lax.broadcasted_iota(jnp.int32, (8, N), 1)
    first8, last8 = lane8 == 0, lane8 == N - 1

    def west8(x):
        a, b = pltpu.roll(x[0], 1, 1), pltpu.roll(x[1], 1, 1)
        return jnp.where(first8, b, a), jnp.where(first8, a, b)

    def east8(x):
        a, b = pltpu.roll(x[0], N - 1, 1), pltpu.roll(x[1], N - 1, 1)
        return jnp.where(last8, b, a), jnp.where(last8, a, b)

    for n in range(1, SUBCYCLES + 1):
        lo = 8 * (n // 8)
        groups = range(lo, EXT - lo, 8)
        et, fu, fv = (et1, fu1, fv1) if n > 1 else (et0, fu0, fv0)
        for g in groups:
            us = (fu[0, 8 + g:16 + g, :], fu[1, 8 + g:16 + g, :])
            uw = west8(us)
            for t in range(2):
                et1[t, 8 + g:16 + g, :] = et[t, 8 + g:16 + g, :] - (
                    (us[t] - uw[t]) + (fv[t, 8 + g:16 + g, :] - fv[t, 7 + g:15 + g, :]))
        for g in groups:
            es = (et1[0, 8 + g:16 + g, :], et1[1, 8 + g:16 + g, :])
            ee = east8(es)
            for t in range(2):
                u = fu[t, 8 + g:16 + g, :] - cu[t, g:g + 8, :] * (ee[t] - es[t]) + pu[t, g:g + 8, :]
                v = fv[t, 8 + g:16 + g, :] - cv[t, g:g + 8, :] * (et1[t, 9 + g:17 + g, :] - es[t]) + pv[t, g:g + 8, :]
                fu1[t, 8 + g:16 + g, :] = u
                fv1[t, 8 + g:16 + g, :] = v
                if t == 0 and W <= g < W + N:
                    at = slice(g - W, g - W + 8)
                    w = float(wgt[n - 1])
                    mean[0, at, :] = w * u if n == 1 else mean[0, at, :] + w * u
                    mean[1, at, :] = w * v if n == 1 else mean[1, at, :] + w * v

    mid = slice(8 + W, 8 + W + N)
    eta_out[...] = et1[0, mid, :]
    tu_out[...] = 2.0 * fu1[0, mid, :]
    tv_out[...] = 2.0 * fv1[0, mid, :]
    for i, co in ((0, cu), (1, cv)):
        h = co[0, W:W + N, :]
        mean[i] = mean[i] / jnp.where(h > 0.0, 2.0 * h, 1.0) - two_ref[2 + i]

    for ci, (k0, k1) in enumerate(CHUNKS):
        for i, (src, buf, dst) in enumerate(((nu_ref, ub, u_hbm), (nv_ref, vb, v_hbm))):
            for k in range(k0, k1):
                buf[k] = src[k] + jnp.where(two_ref[i] > float(k), mean[i], 0.0)
            cp = pltpu.make_async_copy(buf.at[pl.ds(k0, k1 - k0)], dst.at[pl.ds(k0, k1 - k0)], osem.at[2 + 2 * ci + i])
            cp.start()
            copies.append(cp)
    for cp in copies:
        cp.wait()


def solution(mesh):
    ncol, nrow = mesh.shape['col'], mesh.shape['row']
    vmem = pl.BlockSpec(memory_space=pltpu.VMEM)
    hbm = pl.BlockSpec(memory_space=pl.ANY)
    s3 = jax.ShapeDtypeStruct((LEVELS, N, N), F32)
    s2 = jax.ShapeDtypeStruct((N, N), F32)

    def sds(*shape):
        return jax.ShapeDtypeStruct(shape, F32)

    def ocean_step(vel_u, vel_v, temp, salt, eta, tu, tv, dep, kmt):
        def kernel_a(*refs):
            exchange_kernel(ncol, nrow, *refs)

        def kernel_b(*refs):
            step_kernel(*refs)

        mid = pl.pallas_call(
            kernel_a,
            name='exchange',
            out_shape=(s3, s3, s3, s3, sds(4, N, N), sds(2, TOP, N), sds(2, TOP, N), sds(2, TOP, N), sds(2, EXT, N),
                       sds(2, EXT, N), sds(2, EXT, N), sds(EXT, N), sds(EXT, N)),
            in_specs=[hbm] * 9,
            out_specs=(vmem,) * 13,
            scratch_shapes=[
                pltpu.VMEM((4, LEVELS, N + 16, N), F32),
                pltpu.VMEM((N, N), jnp.int32),
                pltpu.VMEM((2, N + 16, N), F32),
                pltpu.VMEM((4, N + 16, N), F32),
                pltpu.VMEM((N, N), F32), pltpu.VMEM((N, N), F32),
                pltpu.VMEM((N + 16, N), F32), pltpu.VMEM((N + 16, N), F32),
                pltpu.VMEM((6, N + 16, N), F32), pltpu.VMEM((6, N + 16, N), F32),
                pltpu.VMEM((4, N, N), F32),
                pltpu.VMEM((4, EXT, N), F32),
                pltpu.VMEM((N, N), F32), pltpu.VMEM((N, N), F32),
                pltpu.VMEM((EXT, N), F32), pltpu.VMEM((EXT, N), F32),
                pltpu.VMEM((2, EXT, N), F32),
                pltpu.VMEM((N // 2, N), F32), pltpu.VMEM((N // 2, N), F32),
                pltpu.VMEM((N, N), F32), pltpu.VMEM((N, N), F32),
                pltpu.SemaphoreType.DMA((4, len(CHUNKS))),
                pltpu.SemaphoreType.DMA((5,)),
                pltpu.SemaphoreType.DMA((24,)),
                pltpu.SemaphoreType.DMA((24,)),
            ],
            compiler_params=pltpu.CompilerParams(collective_id=0, has_side_effects=True, vmem_limit_bytes=28 * 2 ** 20),
        )(*[pltpu.with_memory_space_constraint(x, pltpu.HBM) for x in (vel_u, vel_v, temp, salt, eta, tu, tv, dep, kmt)])
        st = pltpu.VMEM((2, TOP, N), F32)
        co = pltpu.VMEM((2, EXT, N), F32)
        out = pl.pallas_call(
            kernel_b,
            name='subcycles',
            out_shape=(s2, s2, s2, s3, s3, s3, s3),
            in_specs=[vmem] * 13,
            out_specs=(vmem,) * 3 + (hbm,) * 4,
            scratch_shapes=[st, st, st, co, co, pltpu.VMEM((2, N, N), F32),
                            pltpu.VMEM((LEVELS, N, N), F32), pltpu.VMEM((LEVELS, N, N), F32),
                            pltpu.SemaphoreType.DMA((2 + 2 * len(CHUNKS),))],
            compiler_params=pltpu.CompilerParams(vmem_limit_bytes=28 * 2 ** 20),
        )(*mid)
        return out

    spec_3d = P(None, 'row', 'col')
    spec_2d = P('row', 'col')
    return jax.shard_map(ocean_step, mesh=mesh, in_specs=(spec_3d,) * 4 + (spec_2d,) * 5,
                         out_specs=(spec_2d,) * 3 + (spec_3d,) * 4, check_vma=False)
```

```python
import jax
import jax.numpy as jnp
import numpy as np
from jax import lax
from jax.experimental import pallas as pl
from jax.experimental.pallas import tpu as pltpu
from jax.sharding import PartitionSpec as P

MESH = pl.DeviceIdType.MESH
F32 = jnp.float32
SUBCYCLES = 30
LEVELS = 31
VISC_NUM = 4.0
DIFF_NUM = 1.0
N = 128
W = 32
EXT = N + 2 * W
TOP = EXT + 16
PR = 32
QR = 16
CHUNKS = ((0, 9), (9, 18), (18, 26), (26, 31))


def solve_coefs(nu):
    inner, last, back = [], [], []
    c_prev = 0.0
    for k in range(LEVELS):
        lo = nu if k > 0 else 0.0
        piv = 1.0 + nu + lo - lo * c_prev
        inner.append(1.0 / piv)
        last.append(1.0 / (1.0 + lo - lo * c_prev))
        c_prev = nu / piv
        back.append(c_prev)
    return inner, last, back


VISC = solve_coefs(VISC_NUM)
DIFF = solve_coefs(DIFF_NUM)


def weights():
    s = np.arange(1, SUBCYCLES + 1, dtype=np.float64) / (SUBCYCLES + 1)
    w = s ** 2 * (1.0 - s ** 4)
    return (w / w.sum()).astype(np.float32)


def exchange_kernel(ncol, nrow, u_hbm, v_hbm, t_hbm, s_hbm, eta_hbm, tu_hbm, tv_hbm, dep_hbm, kmt_hbm,
                    nu_ref, nv_ref, nt_ref, ns_ref, two_ref, et, fu, fv, cu, cv, fm_out, fe_out, fw_out,
                    fb, ki, kd, qs, msg_e, msg_w, got_w, got_e, xe, xw, ed,
                    wm, pk_e, pk_w, we, ww, fm, fk_e, fk_w, fe, fw,
                    ld_sem, in_sem, snd, rcv):
    c = lax.axis_index('col')
    r = lax.axis_index('row')
    east = lax.rem(c + 1, ncol)
    west = lax.rem(c + ncol - 1, ncol)
    north = lax.rem(r + 1, nrow)
    south = lax.rem(r + nrow - 1, nrow)
    has_n = r < nrow - 1
    has_s = r > 0

    src3 = (u_hbm, v_hbm, t_hbm, s_hbm)
    small = [pltpu.make_async_copy(kmt_hbm, ki, in_sem.at[0]),
             pltpu.make_async_copy(dep_hbm, kd.at[1, pl.ds(8, N), :], in_sem.at[1]),
             pltpu.make_async_copy(eta_hbm, wm.at[0, pl.ds(W, N), :], in_sem.at[2]),
             pltpu.make_async_copy(tu_hbm, wm.at[1, pl.ds(W, N), :], in_sem.at[3]),
             pltpu.make_async_copy(tv_hbm, wm.at[2, pl.ds(W, N), :], in_sem.at[4])]
    loads = []
    for ci, (k0, k1) in enumerate(CHUNKS):
        row = [pltpu.make_async_copy(src3[f].at[pl.ds(k0, k1 - k0)], fb.at[f, pl.ds(k0, k1 - k0), pl.ds(8, N), :],
                                     ld_sem.at[f, ci]) for f in range(4)]
        loads.append(row)
        for cp in row:
            cp.start()
        if ci == 0:
            for cp in small:
                cp.start()

    barrier = pltpu.get_barrier_semaphore()
    places = [(east, r), (west, r), (c, north), (c, south), (east, north), (east, south), (west, north), (west, south)]
    for cc, rr in places:
        pl.semaphore_signal(barrier, inc=1, device_id={'col': cc, 'row': rr}, device_id_type=MESH)

    def copy(i, src, dst, cc, rr):
        return pltpu.make_async_remote_copy(src_ref=src, dst_ref=dst, send_sem=snd.at[i], recv_sem=rcv.at[i],
                                            device_id={'col': cc, 'row': rr}, device_id_type=MESH)

    rows = [
        (copy(0, fb.at[:, :, pl.ds(8, 1), :], fb.at[:, :, pl.ds(8 + N, 1), :], c, south), has_s, has_n),
        (copy(1, fb.at[:, :, pl.ds(7 + N, 1), :], fb.at[:, :, pl.ds(7, 1), :], c, north), has_n, has_s),
        (copy(2, kd.at[:, pl.ds(8, 1), :], kd.at[:, pl.ds(8 + N, 1), :], c, south), has_s, has_n),
        (copy(3, kd.at[:, pl.ds(7 + N, 1), :], kd.at[:, pl.ds(7, 1), :], c, north), has_n, has_s),
    ]
    cols = [
        (copy(4, msg_e, got_w.at[pl.ds(8, N), :], east, r), None, None),
        (copy(5, msg_w, got_e.at[pl.ds(8, N), :], west, r), None, None),
        (copy(6, msg_e.at[pl.ds(0, 8), :], got_w.at[pl.ds(8 + N, 8), :], east, south), has_s, has_n),
        (copy(7, msg_w.at[pl.ds(N - 8, 8), :], got_e.at[pl.ds(0, 8), :], west, north), has_n, has_s),
    ]

    def wide_set(base, main, to_e, to_w, in_e, in_w, n):
        lo, hi = pl.ds(0, W), pl.ds(n - W, W)
        return [
            (copy(base + 0, to_w, in_e.at[pl.ds(W, n), :], west, r), None, None),
            (copy(base + 1, to_e, in_w.at[pl.ds(W, n), :], east, r), None, None),
            (copy(base + 2, main.at[:, pl.ds(W, W), :], main.at[:, pl.ds(W + N, W), :], c, south), has_s, has_n),
            (copy(base + 3, main.at[:, pl.ds(N, W), :], main.at[:, pl.ds(0, W), :], c, north), has_n, has_s),
            (copy(base + 4, to_w.at[lo, :], in_e.at[pl.ds(W + n, W), :], west, south), has_s, has_n),
            (copy(base + 5, to_w.at[hi, :], in_e.at[lo, :], west, north), has_n, has_s),
            (copy(base + 6, to_e.at[lo, :], in_w.at[pl.ds(W + n, W), :], east, south), has_s, has_n),
            (copy(base + 7, to_e.at[hi, :], in_w.at[lo, :], east, north), has_n, has_s),
        ]

    wide = wide_set(8, wm, pk_e, pk_w, we, ww, N)
    forc = wide_set(16, fm, fk_e, fk_w, fe, fw, N // 2)

    def run(cond, fn):
        if cond is None:
            fn()
        else:
            pl.when(cond)(fn)

    def start(items):
        for cp, s_if, _ in items:
            run(s_if, cp.start)

    def wait_recv(items):
        for cp, _, r_if in items:
            run(r_if, cp.wait_recv)

    def wait_send(items):
        for cp, s_if, _ in items:
            run(s_if, cp.wait_send)

    lane = lax.broadcasted_iota(jnp.int32, (N, N), 1)
    part = lax.rem(lane, 4)
    slot = lane // 4

    def roll(x, s):
        s %= N
        return pltpu.roll(x, s, 1) if s else x

    for cp in small:
        cp.wait()
    kmt_f = ki[...].astype(F32)
    dep = kd[1, 8:8 + N, :]
    kd[0, 8:8 + N, :] = kmt_f
    wm[3, W:W + N, :] = jnp.where(kmt_f > 0.0, dep, 0.0)

    def pack(fields):
        e_acc = jnp.zeros((N, N), F32)
        w_acc = jnp.zeros((N, N), F32)
        for f, x in enumerate(fields):
            here = lane // W == f
            w_acc = jnp.where(here, roll(x, W * f), w_acc)
            e_acc = jnp.where(here, roll(x, W * (f + 1)), e_acc)
        return e_acc, w_acc

    e_acc, w_acc = pack([wm[f, W:W + N, :] for f in range(4)])
    pk_e[...] = e_acc
    pk_w[...] = w_acc

    acc = [jnp.zeros((N, N), F32)] * 4
    for ci, (k0, k1) in enumerate(CHUNKS):
        for cp in loads[ci]:
            cp.wait()
        if ci == 0:
            pl.semaphore_wait(barrier, len(places))
            start(wide)
        if ci == len(CHUNKS) - 1:
            start(rows)
        for f in range(4):
            x = acc[f]
            for k in range(k0, k1):
                x = jnp.where(slot == k, roll(fb[f, k, 8:8 + N, :], 4 * k + 2), x)
            acc[f] = x
    out_e = jnp.where(lane == 124, roll(kmt_f, -3), roll(dep, -2))
    out_w = jnp.where(lane == 124, roll(kmt_f, 124), roll(dep, 125))
    for f in range(4):
        qs[f, 8:8 + N, :] = acc[f]
        pick = (part == f) & (slot < LEVELS)
        out_e = jnp.where(pick, roll(acc[f], f - 1), out_e)
        out_w = jnp.where(pick, roll(acc[f], f - 2), out_w)
    msg_e[...] = out_e
    msg_w[...] = out_w

    start(cols)

    @pl.when(jnp.logical_not(has_n))
    def _():
        fb[:, :, 8 + N:9 + N, :] = jnp.zeros((4, LEVELS, 1, N), F32)
        kd[:, 8 + N:9 + N, :] = jnp.zeros((2, 1, N), F32)
        got_w[8 + N:16 + N, :] = jnp.zeros((8, N), F32)

    @pl.when(jnp.logical_not(has_s))
    def _():
        fb[:, :, 7:8, :] = jnp.zeros((4, LEVELS, 1, N), F32)
        kd[:, 7:8, :] = jnp.zeros((2, 1, N), F32)
        got_e[0:8, :] = jnp.zeros((8, N), F32)

    def thick(k, d):
        return 0.6 * d / jnp.maximum(k, 1.0)

    def force(wet_u, wet_v, q_c, q_e, q_n, u_c, u_n, u_s, v_c, v_n, v_s):
        us, vs = u_c + u_n, v_c + v_s
        v_at_u = 0.25 * (vs + roll(vs, -1))
        u_at_v = 0.25 * (us + roll(us, 1))
        u_w = roll(u_c, 1)
        g_u = jnp.where(wet_u, u_c * (roll(u_c, -1) - u_w) + v_at_u * (u_n - u_s) + (q_e - q_c), 0.0)
        g_v = jnp.where(wet_v, u_at_v * (roll(v_c, -1) - roll(v_c, 1)) + v_c * (v_n - v_s) + (q_n - q_c), 0.0)
        u_m, v_m = jnp.where(wet_u, u_c, 0.0), jnp.where(wet_v, v_c, 0.0)
        return g_u, g_v, u_m - 0.125 * g_u, v_m - 0.125 * g_v, u_m, v_m, u_w

    def advect(u_e, u_w, v_n, v_s, tracers):
        a_e, a_w = jnp.minimum(u_e, 0.0), jnp.maximum(u_w, 0.0)
        a_n, a_s = jnp.minimum(v_n, 0.0), jnp.maximum(v_s, 0.0)
        a_c = (jnp.maximum(u_e, 0.0) - jnp.minimum(u_w, 0.0)) + (jnp.maximum(v_n, 0.0) - jnp.minimum(v_s, 0.0))
        b_c = 4.0 - a_c
        return [b_c * x + ((a_w * roll(x, 1) - a_e * roll(x, -1)) + (a_s * x_s - a_n * x_n)) for x, x_n, x_s in tracers]

    def main_step(i, _):
        @pl.when(i == N // PR - 2)
        def _():
            wait_recv(rows)

        own = pl.multiple_of(lax.rem(i + 1, N // PR) * PR, PR)
        base = own + 8

        def at(f, k, off):
            return fb[f, k, pl.ds(base + off, PR), :]

        kc = kd[0, pl.ds(base, PR), :]
        kn = kd[0, pl.ds(base + 1, PR), :]
        ks = kd[0, pl.ds(base - 1, PR), :]
        dc = kd[1, pl.ds(base, PR), :]
        dn = kd[1, pl.ds(base + 1, PR), :]
        th_c, th_n = thick(kc, dc), thick(kn, dn)
        nu_f = jnp.minimum(kc, roll(kc, -1))
        nw_f = jnp.minimum(kc, roll(kc, 1))
        nv_f = jnp.minimum(kc, kn)
        nq_f = jnp.minimum(kc, ks)
        zero = jnp.zeros((PR, N), F32)
        cum_c, cum_n, sum_u, sum_v = zero, zero, zero, zero
        for k in range(LEVELS):
            fk = float(k)
            t_c, s_c = at(2, k, 0), at(3, k, 0)
            t_n, s_n = at(2, k, 1), at(3, k, 1)
            h_c = s_c - 0.5 * t_c
            h_n = s_n - 0.5 * t_n
            mid_c, mid_n = cum_c + h_c, cum_n + h_n
            cum_c, cum_n = mid_c + h_c, mid_n + h_n
            q_c = mid_c * th_c
            u_c, v_c, v_s = at(0, k, 0), at(1, k, 0), at(1, k, -1)
            g_u, g_v, r_u, r_v, u_m, v_m, u_w = force(
                nu_f > fk, nv_f > fk, q_c, roll(q_c, -1), mid_n * th_n,
                u_c, at(0, k, 1), at(0, k, -1), v_c, at(1, k, 1), v_s)
            sum_u, sum_v = sum_u + g_u, sum_v + g_v
            nu_ref[k, pl.ds(own, PR), :] = r_u
            nv_ref[k, pl.ds(own, PR), :] = r_v
            t1, s1 = advect(u_m, jnp.where(nw_f > fk, u_w, 0.0), v_m, jnp.where(nq_f > fk, v_s, 0.0),
                            ((t_c, t_n, at(2, k, -1)), (s_c, s_n, at(3, k, -1))))
            nt_ref[k, pl.ds(own, PR), :] = t1
            ns_ref[k, pl.ds(own, PR), :] = s1
        hu = jnp.where(nu_f > 0.0, 0.5 * (dc + roll(dc, -1)), 0.0)
        hv = jnp.where(nv_f > 0.0, 0.5 * (dc + dn), 0.0)
        fm[0, pl.ds(own + W, PR), :] = hu / jnp.maximum(nu_f, 1.0) * (-0.5 * sum_u)
        fm[1, pl.ds(own + W, PR), :] = hv / jnp.maximum(nv_f, 1.0) * (-0.5 * sum_v)
        return 0

    lax.fori_loop(0, N // PR, main_step, 0)

    lane8 = lax.broadcasted_iota(jnp.int32, (8, N), 1)
    for f in range(4):
        for lo in (0, 8 + N):
            x = jnp.zeros((8, N), F32)
            for k in range(LEVELS):
                x = jnp.where(lane8 // 4 == k, roll(fb[f, k, lo:lo + 8, :], 4 * k + 2), x)
            qs[f, lo:lo + 8, :] = x

    wait_recv(cols)

    part_x = lax.rem(lax.broadcasted_iota(jnp.int32, (N + 16, N), 1), 4)
    for f in range(4):
        q = qs[f]
        xe[f] = jnp.where(part_x == 2, roll(got_e[...], 2 - f), q)
        xw[f] = jnp.where(part_x == 1, roll(got_w[...], 1 - f), q)
    for f in range(2):
        q = kd[f]
        b = [jnp.broadcast_to(q[:, j:j + 1], q.shape) for j in (N - 2, N - 1, 0, 1)]
        h_e = jnp.broadcast_to(got_e[:, 124 + f:125 + f], q.shape)
        h_w = jnp.broadcast_to(got_w[:, 124 + f:125 + f], q.shape)
        xe[4 + f] = jnp.where(part_x == 0, b[0], jnp.where(part_x == 1, b[1], h_e))
        xw[4 + f] = jnp.where(part_x == 1, h_w, jnp.where(part_x == 2, b[2], b[3]))

    lev = slot.astype(F32)

    row_i = lax.broadcasted_iota(jnp.int32, (N, N), 0)
    same = lax.rem(row_i, 4) == part
    below = jnp.where(same & (row_i // 4 <= slot), 1.0, 0.0)
    every = jnp.where(same, 1.0, 0.0)

    def mix(x, m):
        return jnp.dot(x, m, precision=lax.Precision.HIGHEST, preferred_element_type=F32)

    def strip_force(x):
        def at(f, off):
            return x[f, 8 + off:8 + off + N, :]

        kc, kn = at(4, 0), at(4, 1)
        dc, dn = at(5, 0), at(5, 1)
        nu_f, nv_f = jnp.minimum(kc, roll(kc, -1)), jnp.minimum(kc, kn)
        h_c = at(3, 0) - 0.5 * at(2, 0)
        h_n = at(3, 1) - 0.5 * at(2, 1)
        q_c = (2.0 * mix(h_c, below) - h_c) * thick(kc, dc)
        q_n = (2.0 * mix(h_n, below) - h_n) * thick(kn, dn)
        g_u, g_v, r_u, r_v = force(nu_f > lev, nv_f > lev, q_c, roll(q_c, -1), q_n,
                                   at(0, 0), at(0, 1), at(0, -1), at(1, 0), at(1, 1), at(1, -1))[:4]
        hu = jnp.where(nu_f > 0.0, -0.25 * (dc + roll(dc, -1)), 0.0) / jnp.maximum(nu_f, 1.0)
        hv = jnp.where(nv_f > 0.0, -0.25 * (dc + dn), 0.0) / jnp.maximum(nv_f, 1.0)
        return hu, hv, g_u, g_v, r_u, r_v

    def strip_tracer(x):
        def at(f, off):
            return x[f, 8 + off:8 + off + N, :]

        kc, kn, ks = at(4, 0), at(4, 1), at(4, -1)
        u_m = jnp.where(jnp.minimum(kc, roll(kc, -1)) > lev, at(0, 0), 0.0)
        u_w = jnp.where(jnp.minimum(kc, roll(kc, 1)) > lev, roll(at(0, 0), 1), 0.0)
        v_m = jnp.where(jnp.minimum(kc, kn) > lev, at(1, 0), 0.0)
        v_s = jnp.where(jnp.minimum(kc, ks) > lev, at(1, -1), 0.0)
        return advect(u_m, u_w, v_m, v_s, ((at(2, 0), at(2, 1), at(2, -1)), (at(3, 0), at(3, 1), at(3, -1))))

    def merge(fn):
        return [jnp.where(part == 1, a, b) for a, b in zip(fn(xe), fn(xw))]

    hu, hv, g_u, g_v, r_u, r_v = merge(strip_force)
    rim = (lane == 0) | (lane == N - 1)
    forces = []
    for f, (h, g) in enumerate(((hu, g_u), (hv, g_v))):
        x = jnp.where(rim, roll(h * mix(g, every), 2), fm[f, W:W + N, :])
        fm[f, W:W + N, :] = x
        forces.append(x)
    half = lax.broadcasted_iota(jnp.int32, (N // 2, N), 1) < N // 2
    for ref, x in zip((fk_e, fk_w), pack(forces)):
        ref[...] = jnp.where(half, x[:N // 2], roll(x[N // 2:], N // 2))
    start(forc)
    ed[0] = r_u
    ed[1] = r_v
    t1, s1 = merge(strip_tracer)
    ed[2] = t1
    ed[3] = s1

    lane_q = lax.broadcasted_iota(jnp.int32, (QR, N), 1)
    edge_q = (lane_q == 0) | (lane_q == N - 1)

    def solve_step(g, _):
        own = pl.multiple_of(g * QR, QR)
        base = own + 8
        here = pl.ds(own, QR)
        kc = kd[0, pl.ds(base, QR), :]
        kn = kd[0, pl.ds(base + 1, QR), :]
        nu_f = jnp.minimum(kc, jnp.where(lane_q == N - 1, roll(got_e[pl.ds(base, QR), :], 3), roll(kc, -1)))
        nv_f = jnp.minimum(kc, kn)
        two_ref[0, here, :] = nu_f
        two_ref[1, here, :] = nv_f
        zero = jnp.zeros((QR, N), F32)
        refs = (nu_ref, nv_ref, nt_ref, ns_ref)
        cos = (VISC, VISC, DIFF, DIFF)
        d = [zero] * 4

        def factor(n_f, k, co, nu):
            return jnp.where(n_f > k + 1.0, nu * co[0][k], jnp.where(n_f > float(k), nu * co[1][k], 0.0))

        for k in range(LEVELS):
            f_t = factor(kc, k, DIFF, DIFF_NUM)
            facs = (factor(nu_f, k, VISC, VISC_NUM), factor(nv_f, k, VISC, VISC_NUM), f_t, f_t)
            for q in range(4):
                x = jnp.where(edge_q, roll(ed[q, here, :], 126 - 4 * k), refs[q][k, here, :])
                d[q] = (x + d[q]) * facs[q]
                if k == LEVELS - 1 and q > 1:
                    refs[q][k, here, :] = 0.25 * d[q]
                else:
                    refs[q][k, here, :] = d[q]
        sum_u, sum_v = d[0], d[1]
        for k in range(LEVELS - 2, -1, -1):
            for q in range(4):
                d[q] = refs[q][k, here, :] + cos[q][2][k] * d[q]
                refs[q][k, here, :] = d[q] if q < 2 else 0.25 * d[q]
            sum_u, sum_v = sum_u + d[0], sum_v + d[1]
        two_ref[2, here, :] = sum_u / (VISC_NUM * jnp.maximum(nu_f, 1.0))
        two_ref[3, here, :] = sum_v / (VISC_NUM * jnp.maximum(nv_f, 1.0))
        return 0

    lax.fori_loop(0, N // QR, solve_step, 0)

    wait_recv(wide)
    lane_x = lax.broadcasted_iota(jnp.int32, (EXT, N), 1)
    row_x = lax.broadcasted_iota(jnp.int32, (EXT, N), 0)
    real = (row_x >= jnp.where(has_s, 0, W)) & (row_x < jnp.where(has_n, EXT, W + N))
    in_e, in_w = lane_x < W, lane_x >= N - W

    def side(f):
        return jnp.where(in_e, roll(we[...], -W * f), roll(ww[...], -W * (f + 1)))

    dms = (jnp.where(real, wm[3], 0.0), jnp.where(real & (in_e | in_w), side(3), 0.0))
    zero8 = jnp.zeros((8, N), F32)
    for ref in (et, fu, fv):
        for t in range(2):
            ref[t, 0:8, :] = zero8
            ref[t, 8 + EXT:TOP, :] = zero8
    for t in range(2):
        et[t, 8:8 + EXT, :] = dms[t]
    ra, rb = roll(dms[0], -1), roll(dms[1], -1)
    dme = (jnp.where(lane_x == N - 1, rb, ra), jnp.where(lane_x == N - 1, ra, rb))
    for t in range(2):
        d_c = dms[t]
        d_n = et[t, 9:9 + EXT, :]
        wet_u = (d_c > 0.0) & (dme[t] > 0.0)
        wet_v = (d_c > 0.0) & (d_n > 0.0)
        pick = (lambda f: wm[f]) if t == 0 else side
        et[t, 8:8 + EXT, :] = jnp.where(d_c > 0.0, pick(0), 0.0)
        fu[t, 8:8 + EXT, :] = jnp.where(wet_u, 0.5 * pick(1), 0.0)
        fv[t, 8:8 + EXT, :] = jnp.where(wet_v, 0.5 * pick(2), 0.0)
        cu[t] = jnp.where(wet_u, 0.125 * (d_c + dme[t]), 0.0)
        cv[t] = jnp.where(wet_v, 0.125 * (d_c + d_n), 0.0)
    wait_send(rows)
    wait_send(cols)
    wait_send(wide)
    wait_recv(forc)
    fm_out[...] = fm[...]
    h = N // 2
    for out, got in ((fe_out, fe), (fw_out, fw)):
        out[0:W, :] = roll(got[0:W, :], h)
        out[W:W + h, :] = got[W:W + h, :]
        out[W + h:W + N, :] = roll(got[W:W + h, :], h)
        out[W + N:EXT, :] = got[W + h:N, :]
    wait_send(forc)


def step_kernel(nu_ref, nv_ref, nt_ref, ns_ref, two_ref, et0, fu0, fv0, cu, cv, fm, fe, fw,
                eta_out, tu_out, tv_out, u_hbm, v_hbm, t_hbm, s_hbm,
                et1, fu1, fv1, pu, pv, mean, ub, vb, osem):
    copies = [pltpu.make_async_copy(nt_ref, t_hbm, osem.at[0]), pltpu.make_async_copy(ns_ref, s_hbm, osem.at[1])]
    for cp in copies:
        cp.start()

    lane = lax.broadcasted_iota(jnp.int32, (EXT, N), 1)

    def side(f):
        e, w = fe[...], fw[...]
        e = pltpu.roll(e, N - W * f, 1) if f else e
        w = pltpu.roll(w, N - W * (f + 1), 1)
        return jnp.where(lane < W, e, w)

    for f, (p, co) in enumerate(((pu, cu), (pv, cv))):
        for t in range(2):
            x = fm[f] if t == 0 else side(f)
            p[t] = jnp.where(co[t] > 0.0, (0.125 / SUBCYCLES) * x, 0.0)
    zero8 = jnp.zeros((8, N), F32)
    for ref in (et1, fv1):
        for t in range(2):
            ref[t, 0:8, :] = zero8
            ref[t, 8 + EXT:TOP, :] = zero8

    wgt = weights()
    lane8 = lax.broadcasted_iota(jnp.int32, (8, N), 1)
    first8, last8 = lane8 == 0, lane8 == N - 1

    def west8(x):
        a, b = pltpu.roll(x[0], 1, 1), pltpu.roll(x[1], 1, 1)
        return jnp.where(first8, b, a), jnp.where(first8, a, b)

    def east8(x):
        a, b = pltpu.roll(x[0], N - 1, 1), pltpu.roll(x[1], N - 1, 1)
        return jnp.where(last8, b, a), jnp.where(last8, a, b)

    for n in range(1, SUBCYCLES + 1):
        lo = 8 * (n // 8)
        groups = range(lo, EXT - lo, 8)
        et, fu, fv = (et1, fu1, fv1) if n > 1 else (et0, fu0, fv0)
        for g in groups:
            us = (fu[0, 8 + g:16 + g, :], fu[1, 8 + g:16 + g, :])
            uw = west8(us)
            for t in range(2):
                et1[t, 8 + g:16 + g, :] = et[t, 8 + g:16 + g, :] - (
                    (us[t] - uw[t]) + (fv[t, 8 + g:16 + g, :] - fv[t, 7 + g:15 + g, :]))
        for g in groups:
            es = (et1[0, 8 + g:16 + g, :], et1[1, 8 + g:16 + g, :])
            ee = east8(es)
            for t in range(2):
                u = fu[t, 8 + g:16 + g, :] - cu[t, g:g + 8, :] * (ee[t] - es[t]) + pu[t, g:g + 8, :]
                v = fv[t, 8 + g:16 + g, :] - cv[t, g:g + 8, :] * (et1[t, 9 + g:17 + g, :] - es[t]) + pv[t, g:g + 8, :]
                fu1[t, 8 + g:16 + g, :] = u
                fv1[t, 8 + g:16 + g, :] = v
                if t == 0 and W <= g < W + N:
                    at = slice(g - W, g - W + 8)
                    w = float(wgt[n - 1])
                    mean[0, at, :] = w * u if n == 1 else mean[0, at, :] + w * u
                    mean[1, at, :] = w * v if n == 1 else mean[1, at, :] + w * v

    mid = slice(8 + W, 8 + W + N)
    eta_out[...] = et1[0, mid, :]
    tu_out[...] = 2.0 * fu1[0, mid, :]
    tv_out[...] = 2.0 * fv1[0, mid, :]
    for i, co in ((0, cu), (1, cv)):
        h = co[0, W:W + N, :]
        mean[i] = mean[i] / jnp.where(h > 0.0, 2.0 * h, 1.0) - two_ref[2 + i]

    for ci, (k0, k1) in enumerate(CHUNKS):
        for i, (src, buf, dst) in enumerate(((nu_ref, ub, u_hbm), (nv_ref, vb, v_hbm))):
            for k in range(k0, k1):
                buf[k] = (1.0 / VISC_NUM) * src[k] + jnp.where(two_ref[i] > float(k), mean[i], 0.0)
            cp = pltpu.make_async_copy(buf.at[pl.ds(k0, k1 - k0)], dst.at[pl.ds(k0, k1 - k0)], osem.at[2 + 2 * ci + i])
            cp.start()
            copies.append(cp)
    for cp in copies:
        cp.wait()


def solution(mesh):
    ncol, nrow = mesh.shape['col'], mesh.shape['row']
    vmem = pl.BlockSpec(memory_space=pltpu.VMEM)
    hbm = pl.BlockSpec(memory_space=pl.ANY)
    s3 = jax.ShapeDtypeStruct((LEVELS, N, N), F32)
    s2 = jax.ShapeDtypeStruct((N, N), F32)

    def sds(*shape):
        return jax.ShapeDtypeStruct(shape, F32)

    def ocean_step(vel_u, vel_v, temp, salt, eta, tu, tv, dep, kmt):
        def kernel_a(*refs):
            exchange_kernel(ncol, nrow, *refs)

        def kernel_b(*refs):
            step_kernel(*refs)

        mid = pl.pallas_call(
            kernel_a,
            name='exchange',
            out_shape=(s3, s3, s3, s3, sds(4, N, N), sds(2, TOP, N), sds(2, TOP, N), sds(2, TOP, N), sds(2, EXT, N),
                       sds(2, EXT, N), sds(2, EXT, N), sds(EXT, N), sds(EXT, N)),
            in_specs=[hbm] * 9,
            out_specs=(vmem,) * 13,
            scratch_shapes=[
                pltpu.VMEM((4, LEVELS, N + 16, N), F32),
                pltpu.VMEM((N, N), jnp.int32),
                pltpu.VMEM((2, N + 16, N), F32),
                pltpu.VMEM((4, N + 16, N), F32),
                pltpu.VMEM((N, N), F32), pltpu.VMEM((N, N), F32),
                pltpu.VMEM((N + 16, N), F32), pltpu.VMEM((N + 16, N), F32),
                pltpu.VMEM((6, N + 16, N), F32), pltpu.VMEM((6, N + 16, N), F32),
                pltpu.VMEM((4, N, N), F32),
                pltpu.VMEM((4, EXT, N), F32),
                pltpu.VMEM((N, N), F32), pltpu.VMEM((N, N), F32),
                pltpu.VMEM((EXT, N), F32), pltpu.VMEM((EXT, N), F32),
                pltpu.VMEM((2, EXT, N), F32),
                pltpu.VMEM((N // 2, N), F32), pltpu.VMEM((N // 2, N), F32),
                pltpu.VMEM((N, N), F32), pltpu.VMEM((N, N), F32),
                pltpu.SemaphoreType.DMA((4, len(CHUNKS))),
                pltpu.SemaphoreType.DMA((5,)),
                pltpu.SemaphoreType.DMA((24,)),
                pltpu.SemaphoreType.DMA((24,)),
            ],
            compiler_params=pltpu.CompilerParams(collective_id=0, has_side_effects=True, vmem_limit_bytes=28 * 2 ** 20),
        )(*[pltpu.with_memory_space_constraint(x, pltpu.HBM) for x in (vel_u, vel_v, temp, salt, eta, tu, tv, dep, kmt)])
        st = pltpu.VMEM((2, TOP, N), F32)
        co = pltpu.VMEM((2, EXT, N), F32)
        out = pl.pallas_call(
            kernel_b,
            name='subcycles',
            out_shape=(s2, s2, s2, s3, s3, s3, s3),
            in_specs=[vmem] * 13,
            out_specs=(vmem,) * 3 + (hbm,) * 4,
            scratch_shapes=[st, st, st, co, co, pltpu.VMEM((2, N, N), F32),
                            pltpu.VMEM((LEVELS, N, N), F32), pltpu.VMEM((LEVELS, N, N), F32),
                            pltpu.SemaphoreType.DMA((2 + 2 * len(CHUNKS),))],
            compiler_params=pltpu.CompilerParams(vmem_limit_bytes=28 * 2 ** 20),
        )(*mid)
        return out

    spec_3d = P(None, 'row', 'col')
    spec_2d = P('row', 'col')
    return jax.shard_map(ocean_step, mesh=mesh, in_specs=(spec_3d,) * 4 + (spec_2d,) * 5,
                         out_specs=(spec_2d,) * 3 + (spec_3d,) * 4, check_vma=False)
```

```python
import jax
import jax.numpy as jnp
import numpy as np
from jax import lax
from jax.experimental import pallas as pl
from jax.experimental.pallas import tpu as pltpu
from jax.sharding import PartitionSpec as P

MESH = pl.DeviceIdType.MESH
F32 = jnp.float32
SUBCYCLES = 30
LEVELS = 31
VISC_NUM = 4.0
DIFF_NUM = 1.0
N = 128
W = 32
EXT = N + 2 * W
TOP = EXT + 16
PR = 16
QR = 32
CHUNKS = ((0, 9), (9, 18), (18, 26), (26, 31))


def solve_coefs(nu):
    inner, last, back = [], [], []
    c_prev = 0.0
    for k in range(LEVELS):
        lo = nu if k > 0 else 0.0
        piv = 1.0 + nu + lo - lo * c_prev
        inner.append(1.0 / piv)
        last.append(1.0 / (1.0 + lo - lo * c_prev))
        c_prev = nu / piv
        back.append(c_prev)
    return inner, last, back


VISC = solve_coefs(VISC_NUM)
DIFF = solve_coefs(DIFF_NUM)


def weights():
    s = np.arange(1, SUBCYCLES + 1, dtype=np.float64) / (SUBCYCLES + 1)
    w = s ** 2 * (1.0 - s ** 4)
    return (w / w.sum()).astype(np.float32)


def exchange_kernel(ncol, nrow, u_hbm, v_hbm, t_hbm, s_hbm, eta_hbm, tu_hbm, tv_hbm, dep_hbm, kmt_hbm,
                    nu_ref, nv_ref, nt_ref, ns_ref, two_ref, et, fu, fv, cu, cv, fm_out, fe_out, fw_out,
                    fb, ki, kd, cr, qs, msg_e, msg_w, got_w, got_e, xe, xw, ed,
                    wm, pk_e, pk_w, we, ww, fm, fk_e, fk_w, fe, fw,
                    ld_sem, in_sem, snd, rcv):
    c = lax.axis_index('col')
    r = lax.axis_index('row')
    east = lax.rem(c + 1, ncol)
    west = lax.rem(c + ncol - 1, ncol)
    north = lax.rem(r + 1, nrow)
    south = lax.rem(r + nrow - 1, nrow)
    has_n = r < nrow - 1
    has_s = r > 0

    src3 = (u_hbm, v_hbm, t_hbm, s_hbm)
    small = [pltpu.make_async_copy(kmt_hbm, ki, in_sem.at[0]),
             pltpu.make_async_copy(dep_hbm, kd.at[1, pl.ds(8, N), :], in_sem.at[1]),
             pltpu.make_async_copy(eta_hbm, wm.at[0, pl.ds(W, N), :], in_sem.at[2]),
             pltpu.make_async_copy(tu_hbm, wm.at[1, pl.ds(W, N), :], in_sem.at[3]),
             pltpu.make_async_copy(tv_hbm, wm.at[2, pl.ds(W, N), :], in_sem.at[4])]
    loads = []
    for ci, (k0, k1) in enumerate(CHUNKS):
        row = [pltpu.make_async_copy(src3[f].at[pl.ds(k0, k1 - k0)], fb.at[f, pl.ds(k0, k1 - k0), pl.ds(8, N), :],
                                     ld_sem.at[f, ci]) for f in range(4)]
        loads.append(row)
        for cp in row:
            cp.start()
        if ci == 0:
            for cp in small:
                cp.start()

    barrier = pltpu.get_barrier_semaphore()
    places = [(east, r), (west, r), (c, north), (c, south), (east, north), (east, south), (west, north), (west, south)]
    for cc, rr in places:
        pl.semaphore_signal(barrier, inc=1, device_id={'col': cc, 'row': rr}, device_id_type=MESH)

    def copy(i, src, dst, cc, rr):
        return pltpu.make_async_remote_copy(src_ref=src, dst_ref=dst, send_sem=snd.at[i], recv_sem=rcv.at[i],
                                            device_id={'col': cc, 'row': rr}, device_id_type=MESH)

    rows = [
        (copy(0, fb.at[:, :, pl.ds(8, 1), :], fb.at[:, :, pl.ds(8 + N, 1), :], c, south), has_s, has_n),
        (copy(1, fb.at[:, :, pl.ds(7 + N, 1), :], fb.at[:, :, pl.ds(7, 1), :], c, north), has_n, has_s),
        (copy(2, kd.at[:, pl.ds(8, 1), :], kd.at[:, pl.ds(8 + N, 1), :], c, south), has_s, has_n),
        (copy(3, kd.at[:, pl.ds(7 + N, 1), :], kd.at[:, pl.ds(7, 1), :], c, north), has_n, has_s),
    ]
    cols = [
        (copy(4, msg_e, got_w.at[pl.ds(8, N), :], east, r), None, None),
        (copy(5, msg_w, got_e.at[pl.ds(8, N), :], west, r), None, None),
        (copy(6, msg_e.at[pl.ds(0, 8), :], got_w.at[pl.ds(8 + N, 8), :], east, south), has_s, has_n),
        (copy(7, msg_w.at[pl.ds(N - 8, 8), :], got_e.at[pl.ds(0, 8), :], west, north), has_n, has_s),
    ]

    def wide_set(base, main, to_e, to_w, in_e, in_w, n):
        lo, hi = pl.ds(0, W), pl.ds(n - W, W)
        return [
            (copy(base + 0, to_w, in_e.at[pl.ds(W, n), :], west, r), None, None),
            (copy(base + 1, to_e, in_w.at[pl.ds(W, n), :], east, r), None, None),
            (copy(base + 2, main.at[:, pl.ds(W, W), :], main.at[:, pl.ds(W + N, W), :], c, south), has_s, has_n),
            (copy(base + 3, main.at[:, pl.ds(N, W), :], main.at[:, pl.ds(0, W), :], c, north), has_n, has_s),
            (copy(base + 4, to_w.at[lo, :], in_e.at[pl.ds(W + n, W), :], west, south), has_s, has_n),
            (copy(base + 5, to_w.at[hi, :], in_e.at[lo, :], west, north), has_n, has_s),
            (copy(base + 6, to_e.at[lo, :], in_w.at[pl.ds(W + n, W), :], east, south), has_s, has_n),
            (copy(base + 7, to_e.at[hi, :], in_w.at[lo, :], east, north), has_n, has_s),
        ]

    wide = wide_set(8, wm, pk_e, pk_w, we, ww, N)
    forc = wide_set(16, fm, fk_e, fk_w, fe, fw, N // 2)

    def run(cond, fn):
        if cond is None:
            fn()
        else:
            pl.when(cond)(fn)

    def start(items):
        for cp, s_if, _ in items:
            run(s_if, cp.start)

    def wait_recv(items):
        for cp, _, r_if in items:
            run(r_if, cp.wait_recv)

    def wait_send(items):
        for cp, s_if, _ in items:
            run(s_if, cp.wait_send)

    lane = lax.broadcasted_iota(jnp.int32, (N, N), 1)
    part = lax.rem(lane, 4)
    slot = lane // 4

    def roll(x, s):
        s %= N
        return pltpu.roll(x, s, 1) if s else x

    for cp in small:
        cp.wait()
    kmt_f = ki[...].astype(F32)
    dep = kd[1, 8:8 + N, :]
    kd[0, 8:8 + N, :] = kmt_f
    wm[3, W:W + N, :] = jnp.where(kmt_f > 0.0, dep, 0.0)

    def pack(fields):
        e_acc = jnp.zeros((N, N), F32)
        w_acc = jnp.zeros((N, N), F32)
        for f, x in enumerate(fields):
            here = lane // W == f
            w_acc = jnp.where(here, roll(x, W * f), w_acc)
            e_acc = jnp.where(here, roll(x, W * (f + 1)), e_acc)
        return e_acc, w_acc

    e_acc, w_acc = pack([wm[f, W:W + N, :] for f in range(4)])
    pk_e[...] = e_acc
    pk_w[...] = w_acc

    def thick(k, d):
        return 0.6 * d / jnp.maximum(k, 1.0)

    def force(wet_u, wet_v, q_c, q_e, q_n, u_c, u_n, u_s, v_c, v_n, v_s):
        us, vs = u_c + u_n, v_c + v_s
        v_at_u = 0.25 * (vs + roll(vs, -1))
        u_at_v = 0.25 * (us + roll(us, 1))
        u_w = roll(u_c, 1)
        g_u = jnp.where(wet_u, u_c * (roll(u_c, -1) - u_w) + v_at_u * (u_n - u_s) + (q_e - q_c), 0.0)
        g_v = jnp.where(wet_v, u_at_v * (roll(v_c, -1) - roll(v_c, 1)) + v_c * (v_n - v_s) + (q_n - q_c), 0.0)
        u_m, v_m = jnp.where(wet_u, u_c, 0.0), jnp.where(wet_v, v_c, 0.0)
        return g_u, g_v, u_m - 0.125 * g_u, v_m - 0.125 * g_v, u_m, v_m, u_w

    def advect(u_e, u_w, v_n, v_s, tracers):
        a_e, a_w = jnp.minimum(u_e, 0.0), jnp.maximum(u_w, 0.0)
        a_n, a_s = jnp.minimum(v_n, 0.0), jnp.maximum(v_s, 0.0)
        a_c = (jnp.maximum(u_e, 0.0) - jnp.minimum(u_w, 0.0)) + (jnp.maximum(v_n, 0.0) - jnp.minimum(v_s, 0.0))
        b_c = 4.0 - a_c
        return [b_c * x + ((a_w * roll(x, 1) - a_e * roll(x, -1)) + (a_s * x_s - a_n * x_n)) for x, x_n, x_s in tracers]

    def main_part(own, k0, k1):
        here = pl.ds(own, PR)
        base = own + 8

        def at(f, k, off):
            return fb[f, k, pl.ds(base + off, PR), :]

        kc = kd[0, pl.ds(base, PR), :]
        kn = kd[0, pl.ds(base + 1, PR), :]
        ks = kd[0, pl.ds(base - 1, PR), :]
        dc = kd[1, pl.ds(base, PR), :]
        dn = kd[1, pl.ds(base + 1, PR), :]
        th_c, th_n = thick(kc, dc), thick(kn, dn)
        nu_f = jnp.minimum(kc, roll(kc, -1))
        nw_f = jnp.minimum(kc, roll(kc, 1))
        nv_f = jnp.minimum(kc, kn)
        nq_f = jnp.minimum(kc, ks)
        if k0 == 0:
            cum_c = cum_n = sum_u = sum_v = jnp.zeros((PR, N), F32)
        else:
            cum_c, cum_n, sum_u, sum_v = [cr[q, here, :] for q in range(4)]
        for k in range(k0, k1):
            fk = float(k)
            t_c, s_c = at(2, k, 0), at(3, k, 0)
            t_n, s_n = at(2, k, 1), at(3, k, 1)
            h_c = s_c - 0.5 * t_c
            h_n = s_n - 0.5 * t_n
            mid_c, mid_n = cum_c + h_c, cum_n + h_n
            cum_c, cum_n = mid_c + h_c, mid_n + h_n
            q_c = mid_c * th_c
            u_c, v_c, v_s = at(0, k, 0), at(1, k, 0), at(1, k, -1)
            g_u, g_v, r_u, r_v, u_m, v_m, u_w = force(
                nu_f > fk, nv_f > fk, q_c, roll(q_c, -1), mid_n * th_n,
                u_c, at(0, k, 1), at(0, k, -1), v_c, at(1, k, 1), v_s)
            sum_u, sum_v = sum_u + g_u, sum_v + g_v
            nu_ref[k, pl.ds(own, PR), :] = r_u
            nv_ref[k, pl.ds(own, PR), :] = r_v
            t1, s1 = advect(u_m, jnp.where(nw_f > fk, u_w, 0.0), v_m, jnp.where(nq_f > fk, v_s, 0.0),
                            ((t_c, t_n, at(2, k, -1)), (s_c, s_n, at(3, k, -1))))
            nt_ref[k, pl.ds(own, PR), :] = t1
            ns_ref[k, pl.ds(own, PR), :] = s1
        if k1 < LEVELS:
            for q, x in enumerate((cum_c, cum_n, sum_u, sum_v)):
                cr[q, here, :] = x
            return
        hu = jnp.where(nu_f > 0.0, 0.5 * (dc + roll(dc, -1)), 0.0)
        hv = jnp.where(nv_f > 0.0, 0.5 * (dc + dn), 0.0)
        fm[0, pl.ds(own + W, PR), :] = hu / jnp.maximum(nu_f, 1.0) * (-0.5 * sum_u)
        fm[1, pl.ds(own + W, PR), :] = hv / jnp.maximum(nv_f, 1.0) * (-0.5 * sum_v)

    def early_step(i, _):
        main_part(pl.multiple_of((i + 1) * PR, PR), 0, CHUNKS[0][1])
        return 0

    def main_step(i, _):
        own = pl.multiple_of(lax.rem(i + 1, N // PR) * PR, PR)

        @pl.when(i == N // PR - 2)
        def _():
            wait_recv(rows)

        @pl.when(i >= N // PR - 2)
        def _():
            main_part(own, 0, CHUNKS[0][1])

        main_part(own, CHUNKS[0][1], LEVELS)
        return 0

    for ci, (k0, k1) in enumerate(CHUNKS):
        for cp in loads[ci]:
            cp.wait()
        if ci == 0:
            pl.semaphore_wait(barrier, len(places))
            start(wide)
        if ci == len(CHUNKS) - 1:
            start(rows)
        for f in range(4):
            x = qs[f, 8:8 + N, :] if ci else jnp.zeros((N, N), F32)
            for k in range(k0, k1):
                x = jnp.where(slot == k, roll(fb[f, k, 8:8 + N, :], 4 * k + 2), x)
            qs[f, 8:8 + N, :] = x
        if ci == 0:
            lax.fori_loop(0, N // PR - 2, early_step, 0)
    out_e = jnp.where(lane == 124, roll(kmt_f, -3), roll(dep, -2))
    out_w = jnp.where(lane == 124, roll(kmt_f, 124), roll(dep, 125))
    for f in range(4):
        x = qs[f, 8:8 + N, :]
        pick = (part == f) & (slot < LEVELS)
        out_e = jnp.where(pick, roll(x, f - 1), out_e)
        out_w = jnp.where(pick, roll(x, f - 2), out_w)
    msg_e[...] = out_e
    msg_w[...] = out_w

    start(cols)

    @pl.when(jnp.logical_not(has_n))
    def _():
        fb[:, :, 8 + N:9 + N, :] = jnp.zeros((4, LEVELS, 1, N), F32)
        kd[:, 8 + N:9 + N, :] = jnp.zeros((2, 1, N), F32)
        got_w[8 + N:16 + N, :] = jnp.zeros((8, N), F32)

    @pl.when(jnp.logical_not(has_s))
    def _():
        fb[:, :, 7:8, :] = jnp.zeros((4, LEVELS, 1, N), F32)
        kd[:, 7:8, :] = jnp.zeros((2, 1, N), F32)
        got_e[0:8, :] = jnp.zeros((8, N), F32)

    lax.fori_loop(0, N // PR, main_step, 0)

    lane8 = lax.broadcasted_iota(jnp.int32, (8, N), 1)
    for f in range(4):
        for lo in (0, 8 + N):
            x = jnp.zeros((8, N), F32)
            for k in range(LEVELS):
                x = jnp.where(lane8 // 4 == k, roll(fb[f, k, lo:lo + 8, :], 4 * k + 2), x)
            qs[f, lo:lo + 8, :] = x

    wait_recv(cols)

    part_x = lax.rem(lax.broadcasted_iota(jnp.int32, (N + 16, N), 1), 4)
    for f in range(4):
        q = qs[f]
        xe[f] = jnp.where(part_x == 2, roll(got_e[...], 2 - f), q)
        xw[f] = jnp.where(part_x == 1, roll(got_w[...], 1 - f), q)
    for f in range(2):
        q = kd[f]
        b = [jnp.broadcast_to(q[:, j:j + 1], q.shape) for j in (N - 2, N - 1, 0, 1)]
        h_e = jnp.broadcast_to(got_e[:, 124 + f:125 + f], q.shape)
        h_w = jnp.broadcast_to(got_w[:, 124 + f:125 + f], q.shape)
        xe[4 + f] = jnp.where(part_x == 0, b[0], jnp.where(part_x == 1, b[1], h_e))
        xw[4 + f] = jnp.where(part_x == 1, h_w, jnp.where(part_x == 2, b[2], b[3]))

    lev = slot.astype(F32)

    row_i = lax.broadcasted_iota(jnp.int32, (N, N), 0)
    same = lax.rem(row_i, 4) == part
    below = jnp.where(same & (row_i // 4 <= slot), 1.0, 0.0)
    every = jnp.where(same, 1.0, 0.0)

    def mix(x, m):
        return jnp.dot(x, m, precision=lax.Precision.HIGHEST, preferred_element_type=F32)

    def strip_force(x):
        def at(f, off):
            return x[f, 8 + off:8 + off + N, :]

        kc, kn = at(4, 0), at(4, 1)
        dc, dn = at(5, 0), at(5, 1)
        nu_f, nv_f = jnp.minimum(kc, roll(kc, -1)), jnp.minimum(kc, kn)
        h_c = at(3, 0) - 0.5 * at(2, 0)
        h_n = at(3, 1) - 0.5 * at(2, 1)
        q_c = (2.0 * mix(h_c, below) - h_c) * thick(kc, dc)
        q_n = (2.0 * mix(h_n, below) - h_n) * thick(kn, dn)
        g_u, g_v, r_u, r_v = force(nu_f > lev, nv_f > lev, q_c, roll(q_c, -1), q_n,
                                   at(0, 0), at(0, 1), at(0, -1), at(1, 0), at(1, 1), at(1, -1))[:4]
        hu = jnp.where(nu_f > 0.0, -0.25 * (dc + roll(dc, -1)), 0.0) / jnp.maximum(nu_f, 1.0)
        hv = jnp.where(nv_f > 0.0, -0.25 * (dc + dn), 0.0) / jnp.maximum(nv_f, 1.0)
        return hu, hv, g_u, g_v, r_u, r_v

    def strip_tracer(x):
        def at(f, off):
            return x[f, 8 + off:8 + off + N, :]

        kc, kn, ks = at(4, 0), at(4, 1), at(4, -1)
        u_m = jnp.where(jnp.minimum(kc, roll(kc, -1)) > lev, at(0, 0), 0.0)
        u_w = jnp.where(jnp.minimum(kc, roll(kc, 1)) > lev, roll(at(0, 0), 1), 0.0)
        v_m = jnp.where(jnp.minimum(kc, kn) > lev, at(1, 0), 0.0)
        v_s = jnp.where(jnp.minimum(kc, ks) > lev, at(1, -1), 0.0)
        return advect(u_m, u_w, v_m, v_s, ((at(2, 0), at(2, 1), at(2, -1)), (at(3, 0), at(3, 1), at(3, -1))))

    def merge(fn):
        return [jnp.where(part == 1, a, b) for a, b in zip(fn(xe), fn(xw))]

    hu, hv, g_u, g_v, r_u, r_v = merge(strip_force)
    rim = (lane == 0) | (lane == N - 1)
    forces = []
    for f, (h, g) in enumerate(((hu, g_u), (hv, g_v))):
        x = jnp.where(rim, roll(h * mix(g, every), 2), fm[f, W:W + N, :])
        fm[f, W:W + N, :] = x
        forces.append(x)
    half = lax.broadcasted_iota(jnp.int32, (N // 2, N), 1) < N // 2
    for ref, x in zip((fk_e, fk_w), pack(forces)):
        ref[...] = jnp.where(half, x[:N // 2], roll(x[N // 2:], N // 2))
    start(forc)
    ed[0] = r_u
    ed[1] = r_v
    t1, s1 = merge(strip_tracer)
    ed[2] = t1
    ed[3] = s1

    lane_q = lax.broadcasted_iota(jnp.int32, (QR, N), 1)
    edge_q = (lane_q == 0) | (lane_q == N - 1)

    def solve_step(g, _):
        own = pl.multiple_of(g * QR, QR)
        base = own + 8
        here = pl.ds(own, QR)
        kc = kd[0, pl.ds(base, QR), :]
        kn = kd[0, pl.ds(base + 1, QR), :]
        nu_f = jnp.minimum(kc, jnp.where(lane_q == N - 1, roll(got_e[pl.ds(base, QR), :], 3), roll(kc, -1)))
        nv_f = jnp.minimum(kc, kn)
        two_ref[0, here, :] = nu_f
        two_ref[1, here, :] = nv_f
        zero = jnp.zeros((QR, N), F32)
        refs = (nu_ref, nv_ref, nt_ref, ns_ref)
        cos = (VISC, VISC, DIFF, DIFF)
        d = [zero] * 4

        def factor(n_f, k, co, nu):
            return jnp.where(n_f > k + 1.0, nu * co[0][k], jnp.where(n_f > float(k), nu * co[1][k], 0.0))

        for k in range(LEVELS):
            f_t = factor(kc, k, DIFF, DIFF_NUM)
            facs = (factor(nu_f, k, VISC, VISC_NUM), factor(nv_f, k, VISC, VISC_NUM), f_t, f_t)
            for q in range(4):
                x = jnp.where(edge_q, roll(ed[q, here, :], 126 - 4 * k), refs[q][k, here, :])
                d[q] = (x + d[q]) * facs[q]
                if k == LEVELS - 1 and q > 1:
                    refs[q][k, here, :] = 0.25 * d[q]
                else:
                    refs[q][k, here, :] = d[q]
        sum_u, sum_v = d[0], d[1]
        for k in range(LEVELS - 2, -1, -1):
            for q in range(4):
                d[q] = refs[q][k, here, :] + cos[q][2][k] * d[q]
                refs[q][k, here, :] = d[q] if q < 2 else 0.25 * d[q]
            sum_u, sum_v = sum_u + d[0], sum_v + d[1]
        two_ref[2, here, :] = sum_u / (VISC_NUM * jnp.maximum(nu_f, 1.0))
        two_ref[3, here, :] = sum_v / (VISC_NUM * jnp.maximum(nv_f, 1.0))
        return 0

    lax.fori_loop(0, N // QR, solve_step, 0)

    wait_recv(wide)
    lane_x = lax.broadcasted_iota(jnp.int32, (EXT, N), 1)
    row_x = lax.broadcasted_iota(jnp.int32, (EXT, N), 0)
    real = (row_x >= jnp.where(has_s, 0, W)) & (row_x < jnp.where(has_n, EXT, W + N))
    in_e, in_w = lane_x < W, lane_x >= N - W

    def side(f):
        return jnp.where(in_e, roll(we[...], -W * f), roll(ww[...], -W * (f + 1)))

    dms = (jnp.where(real, wm[3], 0.0), jnp.where(real & (in_e | in_w), side(3), 0.0))
    zero8 = jnp.zeros((8, N), F32)
    for ref in (et, fu, fv):
        for t in range(2):
            ref[t, 0:8, :] = zero8
            ref[t, 8 + EXT:TOP, :] = zero8
    for t in range(2):
        et[t, 8:8 + EXT, :] = dms[t]
    ra, rb = roll(dms[0], -1), roll(dms[1], -1)
    dme = (jnp.where(lane_x == N - 1, rb, ra), jnp.where(lane_x == N - 1, ra, rb))
    for t in range(2):
        d_c = dms[t]
        d_n = et[t, 9:9 + EXT, :]
        wet_u = (d_c > 0.0) & (dme[t] > 0.0)
        wet_v = (d_c > 0.0) & (d_n > 0.0)
        pick = (lambda f: wm[f]) if t == 0 else side
        et[t, 8:8 + EXT, :] = jnp.where(d_c > 0.0, pick(0), 0.0)
        fu[t, 8:8 + EXT, :] = jnp.where(wet_u, 0.5 * pick(1), 0.0)
        fv[t, 8:8 + EXT, :] = jnp.where(wet_v, 0.5 * pick(2), 0.0)
        cu[t] = jnp.where(wet_u, 0.125 * (d_c + dme[t]), 0.0)
        cv[t] = jnp.where(wet_v, 0.125 * (d_c + d_n), 0.0)
    wait_send(rows)
    wait_send(cols)
    wait_send(wide)
    wait_recv(forc)
    fm_out[...] = fm[...]
    h = N // 2
    for out, got in ((fe_out, fe), (fw_out, fw)):
        out[0:W, :] = roll(got[0:W, :], h)
        out[W:W + h, :] = got[W:W + h, :]
        out[W + h:W + N, :] = roll(got[W:W + h, :], h)
        out[W + N:EXT, :] = got[W + h:N, :]
    wait_send(forc)


def step_kernel(nu_ref, nv_ref, nt_ref, ns_ref, two_ref, et0, fu0, fv0, cu, cv, fm, fe, fw,
                eta_out, tu_out, tv_out, u_hbm, v_hbm, t_hbm, s_hbm,
                et1, fu1, fv1, pu, pv, mean, ub, vb, osem):
    copies = [pltpu.make_async_copy(nt_ref, t_hbm, osem.at[0]), pltpu.make_async_copy(ns_ref, s_hbm, osem.at[1])]
    for cp in copies:
        cp.start()

    lane = lax.broadcasted_iota(jnp.int32, (EXT, N), 1)

    def side(f):
        e, w = fe[...], fw[...]
        e = pltpu.roll(e, N - W * f, 1) if f else e
        w = pltpu.roll(w, N - W * (f + 1), 1)
        return jnp.where(lane < W, e, w)

    for f, (p, co) in enumerate(((pu, cu), (pv, cv))):
        for t in range(2):
            x = fm[f] if t == 0 else side(f)
            p[t] = jnp.where(co[t] > 0.0, (0.125 / SUBCYCLES) * x, 0.0)
    zero8 = jnp.zeros((8, N), F32)
    for ref in (et1, fv1):
        for t in range(2):
            ref[t, 0:8, :] = zero8
            ref[t, 8 + EXT:TOP, :] = zero8

    wgt = weights()
    lane8 = lax.broadcasted_iota(jnp.int32, (8, N), 1)
    first8, last8 = lane8 == 0, lane8 == N - 1

    def west8(x):
        a, b = pltpu.roll(x[0], 1, 1), pltpu.roll(x[1], 1, 1)
        return jnp.where(first8, b, a), jnp.where(first8, a, b)

    def east8(x):
        a, b = pltpu.roll(x[0], N - 1, 1), pltpu.roll(x[1], N - 1, 1)
        return jnp.where(last8, b, a), jnp.where(last8, a, b)

    for n in range(1, SUBCYCLES + 1):
        lo = 8 * (n // 8)
        groups = range(lo, EXT - lo, 8)
        et, fu, fv = (et1, fu1, fv1) if n > 1 else (et0, fu0, fv0)
        for g in groups:
            us = (fu[0, 8 + g:16 + g, :], fu[1, 8 + g:16 + g, :])
            uw = west8(us)
            for t in range(2):
                et1[t, 8 + g:16 + g, :] = et[t, 8 + g:16 + g, :] - (
                    (us[t] - uw[t]) + (fv[t, 8 + g:16 + g, :] - fv[t, 7 + g:15 + g, :]))
        for g in groups:
            es = (et1[0, 8 + g:16 + g, :], et1[1, 8 + g:16 + g, :])
            ee = east8(es)
            for t in range(2):
                u = fu[t, 8 + g:16 + g, :] - cu[t, g:g + 8, :] * (ee[t] - es[t]) + pu[t, g:g + 8, :]
                v = fv[t, 8 + g:16 + g, :] - cv[t, g:g + 8, :] * (et1[t, 9 + g:17 + g, :] - es[t]) + pv[t, g:g + 8, :]
                fu1[t, 8 + g:16 + g, :] = u
                fv1[t, 8 + g:16 + g, :] = v
                if t == 0 and W <= g < W + N:
                    at = slice(g - W, g - W + 8)
                    w = float(wgt[n - 1])
                    mean[0, at, :] = w * u if n == 1 else mean[0, at, :] + w * u
                    mean[1, at, :] = w * v if n == 1 else mean[1, at, :] + w * v

    mid = slice(8 + W, 8 + W + N)
    eta_out[...] = et1[0, mid, :]
    tu_out[...] = 2.0 * fu1[0, mid, :]
    tv_out[...] = 2.0 * fv1[0, mid, :]
    for i, co in ((0, cu), (1, cv)):
        h = co[0, W:W + N, :]
        mean[i] = mean[i] / jnp.where(h > 0.0, 2.0 * h, 1.0) - two_ref[2 + i]

    for ci, (k0, k1) in enumerate(CHUNKS):
        for i, (src, buf, dst) in enumerate(((nu_ref, ub, u_hbm), (nv_ref, vb, v_hbm))):
            for g in range(0, N, 8):
                at = slice(g, g + 8)
                n_f, m = two_ref[i, at, :], mean[i, at, :]
                for k in range(k0, k1):
                    buf[k, at, :] = (1.0 / VISC_NUM) * src[k, at, :] + jnp.where(n_f > float(k), m, 0.0)
            cp = pltpu.make_async_copy(buf.at[pl.ds(k0, k1 - k0)], dst.at[pl.ds(k0, k1 - k0)], osem.at[2 + 2 * ci + i])
            cp.start()
            copies.append(cp)
    for cp in copies:
        cp.wait()


def solution(mesh):
    ncol, nrow = mesh.shape['col'], mesh.shape['row']
    vmem = pl.BlockSpec(memory_space=pltpu.VMEM)
    hbm = pl.BlockSpec(memory_space=pl.ANY)
    s3 = jax.ShapeDtypeStruct((LEVELS, N, N), F32)
    s2 = jax.ShapeDtypeStruct((N, N), F32)

    def sds(*shape):
        return jax.ShapeDtypeStruct(shape, F32)

    def ocean_step(vel_u, vel_v, temp, salt, eta, tu, tv, dep, kmt):
        def kernel_a(*refs):
            exchange_kernel(ncol, nrow, *refs)

        def kernel_b(*refs):
            step_kernel(*refs)

        mid = pl.pallas_call(
            kernel_a,
            name='exchange',
            out_shape=(s3, s3, s3, s3, sds(4, N, N), sds(2, TOP, N), sds(2, TOP, N), sds(2, TOP, N), sds(2, EXT, N),
                       sds(2, EXT, N), sds(2, EXT, N), sds(EXT, N), sds(EXT, N)),
            in_specs=[hbm] * 9,
            out_specs=(vmem,) * 13,
            scratch_shapes=[
                pltpu.VMEM((4, LEVELS, N + 16, N), F32),
                pltpu.VMEM((N, N), jnp.int32),
                pltpu.VMEM((2, N + 16, N), F32),
                pltpu.VMEM((4, N, N), F32),
                pltpu.VMEM((4, N + 16, N), F32),
                pltpu.VMEM((N, N), F32), pltpu.VMEM((N, N), F32),
                pltpu.VMEM((N + 16, N), F32), pltpu.VMEM((N + 16, N), F32),
                pltpu.VMEM((6, N + 16, N), F32), pltpu.VMEM((6, N + 16, N), F32),
                pltpu.VMEM((4, N, N), F32),
                pltpu.VMEM((4, EXT, N), F32),
                pltpu.VMEM((N, N), F32), pltpu.VMEM((N, N), F32),
                pltpu.VMEM((EXT, N), F32), pltpu.VMEM((EXT, N), F32),
                pltpu.VMEM((2, EXT, N), F32),
                pltpu.VMEM((N // 2, N), F32), pltpu.VMEM((N // 2, N), F32),
                pltpu.VMEM((N, N), F32), pltpu.VMEM((N, N), F32),
                pltpu.SemaphoreType.DMA((4, len(CHUNKS))),
                pltpu.SemaphoreType.DMA((5,)),
                pltpu.SemaphoreType.DMA((24,)),
                pltpu.SemaphoreType.DMA((24,)),
            ],
            compiler_params=pltpu.CompilerParams(collective_id=0, has_side_effects=True, vmem_limit_bytes=28 * 2 ** 20),
        )(*[pltpu.with_memory_space_constraint(x, pltpu.HBM) for x in (vel_u, vel_v, temp, salt, eta, tu, tv, dep, kmt)])
        st = pltpu.VMEM((2, TOP, N), F32)
        co = pltpu.VMEM((2, EXT, N), F32)
        out = pl.pallas_call(
            kernel_b,
            name='subcycles',
            out_shape=(s2, s2, s2, s3, s3, s3, s3),
            in_specs=[vmem] * 13,
            out_specs=(vmem,) * 3 + (hbm,) * 4,
            scratch_shapes=[st, st, st, co, co, pltpu.VMEM((2, N, N), F32),
                            pltpu.VMEM((LEVELS, N, N), F32), pltpu.VMEM((LEVELS, N, N), F32),
                            pltpu.SemaphoreType.DMA((2 + 2 * len(CHUNKS),))],
            compiler_params=pltpu.CompilerParams(vmem_limit_bytes=28 * 2 ** 20),
        )(*mid)
        return out

    spec_3d = P(None, 'row', 'col')
    spec_2d = P('row', 'col')
    return jax.shard_map(ocean_step, mesh=mesh, in_specs=(spec_3d,) * 4 + (spec_2d,) * 5,
                         out_specs=(spec_2d,) * 3 + (spec_3d,) * 4, check_vma=False)
```

```python
import jax
import jax.numpy as jnp
import numpy as np
from jax import lax
from jax.experimental import pallas as pl
from jax.experimental.pallas import tpu as pltpu
from jax.sharding import PartitionSpec as P

MESH = pl.DeviceIdType.MESH
F32 = jnp.float32
SUBCYCLES = 30
LEVELS = 31
VISC_NUM = 4.0
DIFF_NUM = 1.0
N = 128
W = 32
EXT = N + 2 * W
TOP = EXT + 16
PR = 16
QR = 32
CHUNKS = ((0, 9), (9, 18), (18, 26), (26, 31))


def solve_coefs(nu):
    inner, last, back = [], [], []
    c_prev = 0.0
    for k in range(LEVELS):
        lo = nu if k > 0 else 0.0
        piv = 1.0 + nu + lo - lo * c_prev
        inner.append(1.0 / piv)
        last.append(1.0 / (1.0 + lo - lo * c_prev))
        c_prev = nu / piv
        back.append(c_prev)
    return inner, last, back


VISC = solve_coefs(VISC_NUM)
DIFF = solve_coefs(DIFF_NUM)


def weights():
    s = np.arange(1, SUBCYCLES + 1, dtype=np.float64) / (SUBCYCLES + 1)
    w = s ** 2 * (1.0 - s ** 4)
    return (w / w.sum()).astype(np.float32)


def exchange_kernel(ncol, nrow, u_hbm, v_hbm, t_hbm, s_hbm, eta_hbm, tu_hbm, tv_hbm, dep_hbm, kmt_hbm,
                    nu_ref, nv_ref, nt_ref, ns_ref, two_ref, et, fu, fv, cu, cv, fm_out, fe_out, fw_out,
                    fb, ki, kd, cr, qs, msg_e, msg_w, got_w, got_e, xe, xw, ed,
                    wm, pk_e, pk_w, we, ww, fm, fk_e, fk_w, fe, fw,
                    ld_sem, in_sem, snd, rcv):
    c = lax.axis_index('col')
    r = lax.axis_index('row')
    east = lax.rem(c + 1, ncol)
    west = lax.rem(c + ncol - 1, ncol)
    north = lax.rem(r + 1, nrow)
    south = lax.rem(r + nrow - 1, nrow)
    has_n = r < nrow - 1
    has_s = r > 0

    src3 = (u_hbm, v_hbm, t_hbm, s_hbm)
    small = [pltpu.make_async_copy(kmt_hbm, ki, in_sem.at[0]),
             pltpu.make_async_copy(dep_hbm, kd.at[1, pl.ds(8, N), :], in_sem.at[1]),
             pltpu.make_async_copy(eta_hbm, wm.at[0, pl.ds(W, N), :], in_sem.at[2]),
             pltpu.make_async_copy(tu_hbm, wm.at[1, pl.ds(W, N), :], in_sem.at[3]),
             pltpu.make_async_copy(tv_hbm, wm.at[2, pl.ds(W, N), :], in_sem.at[4])]
    loads = []
    for ci, (k0, k1) in enumerate(CHUNKS):
        row = [pltpu.make_async_copy(src3[f].at[pl.ds(k0, k1 - k0)], fb.at[f, pl.ds(k0, k1 - k0), pl.ds(8, N), :],
                                     ld_sem.at[f, ci]) for f in range(4)]
        loads.append(row)
        for cp in row:
            cp.start()
        if ci == 0:
            for cp in small:
                cp.start()

    barrier = pltpu.get_barrier_semaphore()
    places = [(east, r), (west, r), (c, north), (c, south), (east, north), (east, south), (west, north), (west, south)]
    for cc, rr in places:
        pl.semaphore_signal(barrier, inc=1, device_id={'col': cc, 'row': rr}, device_id_type=MESH)

    def copy(i, src, dst, cc, rr):
        return pltpu.make_async_remote_copy(src_ref=src, dst_ref=dst, send_sem=snd.at[i], recv_sem=rcv.at[i],
                                            device_id={'col': cc, 'row': rr}, device_id_type=MESH)

    rows = [
        (copy(0, fb.at[:, :, pl.ds(8, 1), :], fb.at[:, :, pl.ds(8 + N, 1), :], c, south), has_s, has_n),
        (copy(1, fb.at[:, :, pl.ds(7 + N, 1), :], fb.at[:, :, pl.ds(7, 1), :], c, north), has_n, has_s),
        (copy(2, kd.at[:, pl.ds(8, 1), :], kd.at[:, pl.ds(8 + N, 1), :], c, south), has_s, has_n),
        (copy(3, kd.at[:, pl.ds(7 + N, 1), :], kd.at[:, pl.ds(7, 1), :], c, north), has_n, has_s),
    ]
    cols = [
        (copy(4, msg_e, got_w.at[pl.ds(8, N), :], east, r), None, None),
        (copy(5, msg_w, got_e.at[pl.ds(8, N), :], west, r), None, None),
        (copy(6, msg_e.at[pl.ds(0, 8), :], got_w.at[pl.ds(8 + N, 8), :], east, south), has_s, has_n),
        (copy(7, msg_w.at[pl.ds(N - 8, 8), :], got_e.at[pl.ds(0, 8), :], west, north), has_n, has_s),
    ]

    def wide_set(base, main, to_e, to_w, in_e, in_w, n):
        lo, hi = pl.ds(0, W), pl.ds(n - W, W)
        return [
            (copy(base + 0, to_w, in_e.at[pl.ds(W, n), :], west, r), None, None),
            (copy(base + 1, to_e, in_w.at[pl.ds(W, n), :], east, r), None, None),
            (copy(base + 2, main.at[:, pl.ds(W, W), :], main.at[:, pl.ds(W + N, W), :], c, south), has_s, has_n),
            (copy(base + 3, main.at[:, pl.ds(N, W), :], main.at[:, pl.ds(0, W), :], c, north), has_n, has_s),
            (copy(base + 4, to_w.at[lo, :], in_e.at[pl.ds(W + n, W), :], west, south), has_s, has_n),
            (copy(base + 5, to_w.at[hi, :], in_e.at[lo, :], west, north), has_n, has_s),
            (copy(base + 6, to_e.at[lo, :], in_w.at[pl.ds(W + n, W), :], east, south), has_s, has_n),
            (copy(base + 7, to_e.at[hi, :], in_w.at[lo, :], east, north), has_n, has_s),
        ]

    wide = wide_set(8, wm, pk_e, pk_w, we, ww, N)
    forc = wide_set(16, fm, fk_e, fk_w, fe, fw, N // 2)

    def run(cond, fn):
        if cond is None:
            fn()
        else:
            pl.when(cond)(fn)

    def start(items):
        for cp, s_if, _ in items:
            run(s_if, cp.start)

    def wait_recv(items):
        for cp, _, r_if in items:
            run(r_if, cp.wait_recv)

    def wait_send(items):
        for cp, s_if, _ in items:
            run(s_if, cp.wait_send)

    lane = lax.broadcasted_iota(jnp.int32, (N, N), 1)
    part = lax.rem(lane, 4)
    slot = lane // 4

    def roll(x, s):
        s %= N
        return pltpu.roll(x, s, 1) if s else x

    for cp in small:
        cp.wait()
    kmt_f = ki[...].astype(F32)
    dep = kd[1, 8:8 + N, :]
    kd[0, 8:8 + N, :] = kmt_f
    wm[3, W:W + N, :] = jnp.where(kmt_f > 0.0, dep, 0.0)

    def pack(fields):
        e_acc = jnp.zeros((N, N), F32)
        w_acc = jnp.zeros((N, N), F32)
        for f, x in enumerate(fields):
            here = lane // W == f
            w_acc = jnp.where(here, roll(x, W * f), w_acc)
            e_acc = jnp.where(here, roll(x, W * (f + 1)), e_acc)
        return e_acc, w_acc

    e_acc, w_acc = pack([wm[f, W:W + N, :] for f in range(4)])
    pk_e[...] = e_acc
    pk_w[...] = w_acc

    def thick(k, d):
        return 0.6 * d / jnp.maximum(k, 1.0)

    def force(wet_u, wet_v, q_c, q_e, q_n, u_c, u_n, u_s, v_c, v_n, v_s):
        us, vs = u_c + u_n, v_c + v_s
        v_at_u = 0.25 * (vs + roll(vs, -1))
        u_at_v = 0.25 * (us + roll(us, 1))
        u_w = roll(u_c, 1)
        g_u = jnp.where(wet_u, u_c * (roll(u_c, -1) - u_w) + v_at_u * (u_n - u_s) + (q_e - q_c), 0.0)
        g_v = jnp.where(wet_v, u_at_v * (roll(v_c, -1) - roll(v_c, 1)) + v_c * (v_n - v_s) + (q_n - q_c), 0.0)
        u_m, v_m = jnp.where(wet_u, u_c, 0.0), jnp.where(wet_v, v_c, 0.0)
        return g_u, g_v, u_m - 0.125 * g_u, v_m - 0.125 * g_v, u_m, v_m, u_w

    def advect(u_e, u_w, v_n, v_s, tracers):
        a_e, a_w = jnp.minimum(u_e, 0.0), jnp.maximum(u_w, 0.0)
        a_n, a_s = jnp.minimum(v_n, 0.0), jnp.maximum(v_s, 0.0)
        a_c = (jnp.maximum(u_e, 0.0) - jnp.minimum(u_w, 0.0)) + (jnp.maximum(v_n, 0.0) - jnp.minimum(v_s, 0.0))
        b_c = 4.0 - a_c
        return [b_c * x + ((a_w * roll(x, 1) - a_e * roll(x, -1)) + (a_s * x_s - a_n * x_n)) for x, x_n, x_s in tracers]

    def main_part(own, k0, k1):
        here = pl.ds(own, PR)
        base = own + 8

        def at(f, k, off):
            return fb[f, k, pl.ds(base + off, PR), :]

        kc = kd[0, pl.ds(base, PR), :]
        kn = kd[0, pl.ds(base + 1, PR), :]
        ks = kd[0, pl.ds(base - 1, PR), :]
        dc = kd[1, pl.ds(base, PR), :]
        dn = kd[1, pl.ds(base + 1, PR), :]
        th_c, th_n = thick(kc, dc), thick(kn, dn)
        nu_f = jnp.minimum(kc, roll(kc, -1))
        nw_f = jnp.minimum(kc, roll(kc, 1))
        nv_f = jnp.minimum(kc, kn)
        nq_f = jnp.minimum(kc, ks)
        if k0 == 0:
            cum_c = cum_n = sum_u = sum_v = jnp.zeros((PR, N), F32)
        else:
            cum_c, cum_n, sum_u, sum_v = [cr[q, here, :] for q in range(4)]
        for k in range(k0, k1):
            fk = float(k)
            t_c, s_c = at(2, k, 0), at(3, k, 0)
            t_n, s_n = at(2, k, 1), at(3, k, 1)
            h_c = s_c - 0.5 * t_c
            h_n = s_n - 0.5 * t_n
            mid_c, mid_n = cum_c + h_c, cum_n + h_n
            cum_c, cum_n = mid_c + h_c, mid_n + h_n
            q_c = mid_c * th_c
            u_c, v_c, v_s = at(0, k, 0), at(1, k, 0), at(1, k, -1)
            g_u, g_v, r_u, r_v, u_m, v_m, u_w = force(
                nu_f > fk, nv_f > fk, q_c, roll(q_c, -1), mid_n * th_n,
                u_c, at(0, k, 1), at(0, k, -1), v_c, at(1, k, 1), v_s)
            sum_u, sum_v = sum_u + g_u, sum_v + g_v
            nu_ref[k, pl.ds(own, PR), :] = r_u
            nv_ref[k, pl.ds(own, PR), :] = r_v
            t1, s1 = advect(u_m, jnp.where(nw_f > fk, u_w, 0.0), v_m, jnp.where(nq_f > fk, v_s, 0.0),
                            ((t_c, t_n, at(2, k, -1)), (s_c, s_n, at(3, k, -1))))
            nt_ref[k, pl.ds(own, PR), :] = t1
            ns_ref[k, pl.ds(own, PR), :] = s1
        if k1 < LEVELS:
            for q, x in enumerate((cum_c, cum_n, sum_u, sum_v)):
                cr[q, here, :] = x
            return
        hu = jnp.where(nu_f > 0.0, 0.5 * (dc + roll(dc, -1)), 0.0)
        hv = jnp.where(nv_f > 0.0, 0.5 * (dc + dn), 0.0)
        fm[0, pl.ds(own + W, PR), :] = hu / jnp.maximum(nu_f, 1.0) * (-0.5 * sum_u)
        fm[1, pl.ds(own + W, PR), :] = hv / jnp.maximum(nv_f, 1.0) * (-0.5 * sum_v)

    def early_step(i, _):
        main_part(pl.multiple_of((i + 1) * PR, PR), 0, CHUNKS[0][1])
        return 0

    def main_step(i, _):
        own = pl.multiple_of(lax.rem(i + 1, N // PR) * PR, PR)

        @pl.when(i == N // PR - 2)
        def _():
            wait_recv(rows)

        @pl.when(i >= N // PR - 2)
        def _():
            main_part(own, 0, CHUNKS[0][1])

        main_part(own, CHUNKS[0][1], LEVELS)
        return 0

    for ci, (k0, k1) in enumerate(CHUNKS):
        for cp in loads[ci]:
            cp.wait()
        for f in range(4):
            x = qs[f, 8:8 + N, :] if ci else jnp.zeros((N, N), F32)
            for k in range(k0, k1):
                x = jnp.where(slot == k, roll(fb[f, k, 8:8 + N, :], 4 * k + 2), x)
            qs[f, 8:8 + N, :] = x
        if ci == 0:
            lax.fori_loop(0, N // PR - 2, early_step, 0)
    out_e = jnp.where(lane == 124, roll(kmt_f, -3), roll(dep, -2))
    out_w = jnp.where(lane == 124, roll(kmt_f, 124), roll(dep, 125))
    for f in range(4):
        x = qs[f, 8:8 + N, :]
        pick = (part == f) & (slot < LEVELS)
        out_e = jnp.where(pick, roll(x, f - 1), out_e)
        out_w = jnp.where(pick, roll(x, f - 2), out_w)
    msg_e[...] = out_e
    msg_w[...] = out_w
    pl.semaphore_wait(barrier, len(places))
    start(rows)

    start(cols)
    start(wide)

    @pl.when(jnp.logical_not(has_n))
    def _():
        fb[:, :, 8 + N:9 + N, :] = jnp.zeros((4, LEVELS, 1, N), F32)
        kd[:, 8 + N:9 + N, :] = jnp.zeros((2, 1, N), F32)
        got_w[8 + N:16 + N, :] = jnp.zeros((8, N), F32)

    @pl.when(jnp.logical_not(has_s))
    def _():
        fb[:, :, 7:8, :] = jnp.zeros((4, LEVELS, 1, N), F32)
        kd[:, 7:8, :] = jnp.zeros((2, 1, N), F32)
        got_e[0:8, :] = jnp.zeros((8, N), F32)

    lax.fori_loop(0, N // PR, main_step, 0)

    lane8 = lax.broadcasted_iota(jnp.int32, (8, N), 1)
    for f in range(4):
        for lo in (0, 8 + N):
            x = jnp.zeros((8, N), F32)
            for k in range(LEVELS):
                x = jnp.where(lane8 // 4 == k, roll(fb[f, k, lo:lo + 8, :], 4 * k + 2), x)
            qs[f, lo:lo + 8, :] = x

    wait_recv(cols)

    part_x = lax.rem(lax.broadcasted_iota(jnp.int32, (N + 16, N), 1), 4)
    for f in range(4):
        q = qs[f]
        xe[f] = jnp.where(part_x == 2, roll(got_e[...], 2 - f), q)
        xw[f] = jnp.where(part_x == 1, roll(got_w[...], 1 - f), q)
    for f in range(2):
        q = kd[f]
        b = [jnp.broadcast_to(q[:, j:j + 1], q.shape) for j in (N - 2, N - 1, 0, 1)]
        h_e = jnp.broadcast_to(got_e[:, 124 + f:125 + f], q.shape)
        h_w = jnp.broadcast_to(got_w[:, 124 + f:125 + f], q.shape)
        xe[4 + f] = jnp.where(part_x == 0, b[0], jnp.where(part_x == 1, b[1], h_e))
        xw[4 + f] = jnp.where(part_x == 1, h_w, jnp.where(part_x == 2, b[2], b[3]))

    lev = slot.astype(F32)

    row_i = lax.broadcasted_iota(jnp.int32, (N, N), 0)
    same = lax.rem(row_i, 4) == part
    below = jnp.where(same & (row_i // 4 <= slot), 1.0, 0.0)
    every = jnp.where(same, 1.0, 0.0)

    def mix(x, m):
        return jnp.dot(x, m, precision=lax.Precision.HIGHEST, preferred_element_type=F32)

    def strip_force(x):
        def at(f, off):
            return x[f, 8 + off:8 + off + N, :]

        kc, kn = at(4, 0), at(4, 1)
        dc, dn = at(5, 0), at(5, 1)
        nu_f, nv_f = jnp.minimum(kc, roll(kc, -1)), jnp.minimum(kc, kn)
        h_c = at(3, 0) - 0.5 * at(2, 0)
        h_n = at(3, 1) - 0.5 * at(2, 1)
        q_c = (2.0 * mix(h_c, below) - h_c) * thick(kc, dc)
        q_n = (2.0 * mix(h_n, below) - h_n) * thick(kn, dn)
        g_u, g_v, r_u, r_v = force(nu_f > lev, nv_f > lev, q_c, roll(q_c, -1), q_n,
                                   at(0, 0), at(0, 1), at(0, -1), at(1, 0), at(1, 1), at(1, -1))[:4]
        hu = jnp.where(nu_f > 0.0, -0.25 * (dc + roll(dc, -1)), 0.0) / jnp.maximum(nu_f, 1.0)
        hv = jnp.where(nv_f > 0.0, -0.25 * (dc + dn), 0.0) / jnp.maximum(nv_f, 1.0)
        return hu, hv, g_u, g_v, r_u, r_v

    def strip_tracer(x):
        def at(f, off):
            return x[f, 8 + off:8 + off + N, :]

        kc, kn, ks = at(4, 0), at(4, 1), at(4, -1)
        u_m = jnp.where(jnp.minimum(kc, roll(kc, -1)) > lev, at(0, 0), 0.0)
        u_w = jnp.where(jnp.minimum(kc, roll(kc, 1)) > lev, roll(at(0, 0), 1), 0.0)
        v_m = jnp.where(jnp.minimum(kc, kn) > lev, at(1, 0), 0.0)
        v_s = jnp.where(jnp.minimum(kc, ks) > lev, at(1, -1), 0.0)
        return advect(u_m, u_w, v_m, v_s, ((at(2, 0), at(2, 1), at(2, -1)), (at(3, 0), at(3, 1), at(3, -1))))

    def merge(fn):
        return [jnp.where(part == 1, a, b) for a, b in zip(fn(xe), fn(xw))]

    hu, hv, g_u, g_v, r_u, r_v = merge(strip_force)
    rim = (lane == 0) | (lane == N - 1)
    forces = []
    for f, (h, g) in enumerate(((hu, g_u), (hv, g_v))):
        x = jnp.where(rim, roll(h * mix(g, every), 2), fm[f, W:W + N, :])
        fm[f, W:W + N, :] = x
        forces.append(x)
    half = lax.broadcasted_iota(jnp.int32, (N // 2, N), 1) < N // 2
    for ref, x in zip((fk_e, fk_w), pack(forces)):
        ref[...] = jnp.where(half, x[:N // 2], roll(x[N // 2:], N // 2))
    start(forc)
    ed[0] = r_u
    ed[1] = r_v
    t1, s1 = merge(strip_tracer)
    ed[2] = t1
    ed[3] = s1

    lane_q = lax.broadcasted_iota(jnp.int32, (QR, N), 1)
    edge_q = (lane_q == 0) | (lane_q == N - 1)

    def solve_step(g, _):
        own = pl.multiple_of(g * QR, QR)
        base = own + 8
        here = pl.ds(own, QR)
        kc = kd[0, pl.ds(base, QR), :]
        kn = kd[0, pl.ds(base + 1, QR), :]
        nu_f = jnp.minimum(kc, jnp.where(lane_q == N - 1, roll(got_e[pl.ds(base, QR), :], 3), roll(kc, -1)))
        nv_f = jnp.minimum(kc, kn)
        two_ref[0, here, :] = nu_f
        two_ref[1, here, :] = nv_f
        zero = jnp.zeros((QR, N), F32)
        refs = (nu_ref, nv_ref, nt_ref, ns_ref)
        cos = (VISC, VISC, DIFF, DIFF)
        d = [zero] * 4

        def factor(n_f, k, co, nu):
            return jnp.where(n_f > k + 1.0, nu * co[0][k], jnp.where(n_f > float(k), nu * co[1][k], 0.0))

        for k in range(LEVELS):
            f_t = factor(kc, k, DIFF, DIFF_NUM)
            facs = (factor(nu_f, k, VISC, VISC_NUM), factor(nv_f, k, VISC, VISC_NUM), f_t, f_t)
            for q in range(4):
                x = jnp.where(edge_q, roll(ed[q, here, :], 126 - 4 * k), refs[q][k, here, :])
                d[q] = (x + d[q]) * facs[q]
                if k == LEVELS - 1:
                    refs[q][k, here, :] = 0.25 * d[q]
                else:
                    refs[q][k, here, :] = d[q]
        sum_u, sum_v = d[0], d[1]
        for k in range(LEVELS - 2, -1, -1):
            for q in range(4):
                d[q] = refs[q][k, here, :] + cos[q][2][k] * d[q]
                refs[q][k, here, :] = 0.25 * d[q]
            sum_u, sum_v = sum_u + d[0], sum_v + d[1]
        two_ref[2, here, :] = sum_u / (VISC_NUM * jnp.maximum(nu_f, 1.0))
        two_ref[3, here, :] = sum_v / (VISC_NUM * jnp.maximum(nv_f, 1.0))
        return 0

    lax.fori_loop(0, N // QR, solve_step, 0)

    wait_recv(wide)
    lane_x = lax.broadcasted_iota(jnp.int32, (EXT, N), 1)
    row_x = lax.broadcasted_iota(jnp.int32, (EXT, N), 0)
    real = (row_x >= jnp.where(has_s, 0, W)) & (row_x < jnp.where(has_n, EXT, W + N))
    in_e, in_w = lane_x < W, lane_x >= N - W

    def side(f):
        return jnp.where(in_e, roll(we[...], -W * f), roll(ww[...], -W * (f + 1)))

    dms = (jnp.where(real, wm[3], 0.0), jnp.where(real & (in_e | in_w), side(3), 0.0))
    zero8 = jnp.zeros((8, N), F32)
    for ref in (et, fu, fv):
        for t in range(2):
            ref[t, 0:8, :] = zero8
            ref[t, 8 + EXT:TOP, :] = zero8
    for t in range(2):
        et[t, 8:8 + EXT, :] = dms[t]
    ra, rb = roll(dms[0], -1), roll(dms[1], -1)
    dme = (jnp.where(lane_x == N - 1, rb, ra), jnp.where(lane_x == N - 1, ra, rb))
    for t in range(2):
        d_c = dms[t]
        d_n = et[t, 9:9 + EXT, :]
        wet_u = (d_c > 0.0) & (dme[t] > 0.0)
        wet_v = (d_c > 0.0) & (d_n > 0.0)
        pick = (lambda f: wm[f]) if t == 0 else side
        et[t, 8:8 + EXT, :] = jnp.where(d_c > 0.0, pick(0), 0.0)
        fu[t, 8:8 + EXT, :] = jnp.where(wet_u, 0.5 * pick(1), 0.0)
        fv[t, 8:8 + EXT, :] = jnp.where(wet_v, 0.5 * pick(2), 0.0)
        cu[t] = jnp.where(wet_u, 0.125 * (d_c + dme[t]), 0.0)
        cv[t] = jnp.where(wet_v, 0.125 * (d_c + d_n), 0.0)
    wait_send(rows)
    wait_send(cols)
    wait_send(wide)
    wait_recv(forc)
    fm_out[...] = fm[...]
    h = N // 2
    for out, got in ((fe_out, fe), (fw_out, fw)):
        out[0:W, :] = roll(got[0:W, :], h)
        out[W:W + h, :] = got[W:W + h, :]
        out[W + h:W + N, :] = roll(got[W:W + h, :], h)
        out[W + N:EXT, :] = got[W + h:N, :]
    wait_send(forc)


def step_kernel(nu_ref, nv_ref, nt_ref, ns_ref, two_ref, et0, fu0, fv0, cu, cv, fm, fe, fw,
                eta_out, tu_out, tv_out, u_hbm, v_hbm, t_hbm, s_hbm,
                et1, fu1, fv1, pu, pv, mean, ub, vb, osem):
    copies = [pltpu.make_async_copy(nt_ref, t_hbm, osem.at[0]), pltpu.make_async_copy(ns_ref, s_hbm, osem.at[1])]
    for cp in copies:
        cp.start()

    lane = lax.broadcasted_iota(jnp.int32, (EXT, N), 1)

    def side(f):
        e, w = fe[...], fw[...]
        e = pltpu.roll(e, N - W * f, 1) if f else e
        w = pltpu.roll(w, N - W * (f + 1), 1)
        return jnp.where(lane < W, e, w)

    for f, (p, co) in enumerate(((pu, cu), (pv, cv))):
        for t in range(2):
            x = fm[f] if t == 0 else side(f)
            p[t] = jnp.where(co[t] > 0.0, (0.125 / SUBCYCLES) * x, 0.0)
    zero8 = jnp.zeros((8, N), F32)
    for ref in (et1, fv1):
        for t in range(2):
            ref[t, 0:8, :] = zero8
            ref[t, 8 + EXT:TOP, :] = zero8

    wgt = weights()
    lane8 = lax.broadcasted_iota(jnp.int32, (8, N), 1)
    first8, last8 = lane8 == 0, lane8 == N - 1

    def west8(x):
        a, b = pltpu.roll(x[0], 1, 1), pltpu.roll(x[1], 1, 1)
        return jnp.where(first8, b, a), jnp.where(first8, a, b)

    def east8(x):
        a, b = pltpu.roll(x[0], N - 1, 1), pltpu.roll(x[1], N - 1, 1)
        return jnp.where(last8, b, a), jnp.where(last8, a, b)

    for n in range(1, SUBCYCLES + 1):
        lo = 8 * (n // 8)
        groups = range(lo, EXT - lo, 8)
        et, fu, fv = (et1, fu1, fv1) if n > 1 else (et0, fu0, fv0)
        for g in groups:
            us = (fu[0, 8 + g:16 + g, :], fu[1, 8 + g:16 + g, :])
            uw = west8(us)
            for t in range(2):
                et1[t, 8 + g:16 + g, :] = et[t, 8 + g:16 + g, :] - (
                    (us[t] - uw[t]) + (fv[t, 8 + g:16 + g, :] - fv[t, 7 + g:15 + g, :]))
        for g in groups:
            es = (et1[0, 8 + g:16 + g, :], et1[1, 8 + g:16 + g, :])
            ee = east8(es)
            for t in range(2):
                u = fu[t, 8 + g:16 + g, :] - cu[t, g:g + 8, :] * (ee[t] - es[t]) + pu[t, g:g + 8, :]
                v = fv[t, 8 + g:16 + g, :] - cv[t, g:g + 8, :] * (et1[t, 9 + g:17 + g, :] - es[t]) + pv[t, g:g + 8, :]
                fu1[t, 8 + g:16 + g, :] = u
                fv1[t, 8 + g:16 + g, :] = v
                if t == 0 and W <= g < W + N:
                    at = slice(g - W, g - W + 8)
                    w = float(wgt[n - 1])
                    mean[0, at, :] = w * u if n == 1 else mean[0, at, :] + w * u
                    mean[1, at, :] = w * v if n == 1 else mean[1, at, :] + w * v

    mid = slice(8 + W, 8 + W + N)
    eta_out[...] = et1[0, mid, :]
    tu_out[...] = 2.0 * fu1[0, mid, :]
    tv_out[...] = 2.0 * fv1[0, mid, :]
    for i, co in ((0, cu), (1, cv)):
        h = co[0, W:W + N, :]
        mean[i] = mean[i] / jnp.where(h > 0.0, 2.0 * h, 1.0) - two_ref[2 + i]

    for ci, (k0, k1) in enumerate(CHUNKS):
        for i, (src, buf, dst) in enumerate(((nu_ref, ub, u_hbm), (nv_ref, vb, v_hbm))):
            for g in range(0, N, 8):
                at = slice(g, g + 8)
                n_f, m = two_ref[i, at, :], mean[i, at, :]
                for k in range(k0, k1):
                    buf[k, at, :] = src[k, at, :] + jnp.where(n_f > float(k), m, 0.0)
            cp = pltpu.make_async_copy(buf.at[pl.ds(k0, k1 - k0)], dst.at[pl.ds(k0, k1 - k0)], osem.at[2 + 2 * ci + i])
            cp.start()
            copies.append(cp)
    for cp in copies:
        cp.wait()


def solution(mesh):
    ncol, nrow = mesh.shape['col'], mesh.shape['row']
    vmem = pl.BlockSpec(memory_space=pltpu.VMEM)
    hbm = pl.BlockSpec(memory_space=pl.ANY)
    s3 = jax.ShapeDtypeStruct((LEVELS, N, N), F32)
    s2 = jax.ShapeDtypeStruct((N, N), F32)

    def sds(*shape):
        return jax.ShapeDtypeStruct(shape, F32)

    def ocean_step(vel_u, vel_v, temp, salt, eta, tu, tv, dep, kmt):
        def kernel_a(*refs):
            exchange_kernel(ncol, nrow, *refs)

        def kernel_b(*refs):
            step_kernel(*refs)

        mid = pl.pallas_call(
            kernel_a,
            name='exchange',
            out_shape=(s3, s3, s3, s3, sds(4, N, N), sds(2, TOP, N), sds(2, TOP, N), sds(2, TOP, N), sds(2, EXT, N),
                       sds(2, EXT, N), sds(2, EXT, N), sds(EXT, N), sds(EXT, N)),
            in_specs=[hbm] * 9,
            out_specs=(vmem,) * 13,
            scratch_shapes=[
                pltpu.VMEM((4, LEVELS, N + 16, N), F32),
                pltpu.VMEM((N, N), jnp.int32),
                pltpu.VMEM((2, N + 16, N), F32),
                pltpu.VMEM((4, N, N), F32),
                pltpu.VMEM((4, N + 16, N), F32),
                pltpu.VMEM((N, N), F32), pltpu.VMEM((N, N), F32),
                pltpu.VMEM((N + 16, N), F32), pltpu.VMEM((N + 16, N), F32),
                pltpu.VMEM((6, N + 16, N), F32), pltpu.VMEM((6, N + 16, N), F32),
                pltpu.VMEM((4, N, N), F32),
                pltpu.VMEM((4, EXT, N), F32),
                pltpu.VMEM((N, N), F32), pltpu.VMEM((N, N), F32),
                pltpu.VMEM((EXT, N), F32), pltpu.VMEM((EXT, N), F32),
                pltpu.VMEM((2, EXT, N), F32),
                pltpu.VMEM((N // 2, N), F32), pltpu.VMEM((N // 2, N), F32),
                pltpu.VMEM((N, N), F32), pltpu.VMEM((N, N), F32),
                pltpu.SemaphoreType.DMA((4, len(CHUNKS))),
                pltpu.SemaphoreType.DMA((5,)),
                pltpu.SemaphoreType.DMA((24,)),
                pltpu.SemaphoreType.DMA((24,)),
            ],
            compiler_params=pltpu.CompilerParams(collective_id=0, has_side_effects=True, vmem_limit_bytes=28 * 2 ** 20),
        )(*[pltpu.with_memory_space_constraint(x, pltpu.HBM) for x in (vel_u, vel_v, temp, salt, eta, tu, tv, dep, kmt)])
        st = pltpu.VMEM((2, TOP, N), F32)
        co = pltpu.VMEM((2, EXT, N), F32)
        out = pl.pallas_call(
            kernel_b,
            name='subcycles',
            out_shape=(s2, s2, s2, s3, s3, s3, s3),
            in_specs=[vmem] * 13,
            out_specs=(vmem,) * 3 + (hbm,) * 4,
            scratch_shapes=[st, st, st, co, co, pltpu.VMEM((2, N, N), F32),
                            pltpu.VMEM((LEVELS, N, N), F32), pltpu.VMEM((LEVELS, N, N), F32),
                            pltpu.SemaphoreType.DMA((2 + 2 * len(CHUNKS),))],
            compiler_params=pltpu.CompilerParams(vmem_limit_bytes=28 * 2 ** 20),
        )(*mid)
        return out

    spec_3d = P(None, 'row', 'col')
    spec_2d = P('row', 'col')
    return jax.shard_map(ocean_step, mesh=mesh, in_specs=(spec_3d,) * 4 + (spec_2d,) * 5,
                         out_specs=(spec_2d,) * 3 + (spec_3d,) * 4, check_vma=False)
```

```python
import jax
import jax.numpy as jnp
import numpy as np
from jax import lax
from jax.experimental import pallas as pl
from jax.experimental.pallas import tpu as pltpu
from jax.sharding import PartitionSpec as P

MESH = pl.DeviceIdType.MESH
F32 = jnp.float32
SUBCYCLES = 30
LEVELS = 31
VISC_NUM = 4.0
DIFF_NUM = 1.0
N = 128
W = 32
EXT = N + 2 * W
TOP = EXT + 16
PR = 16
QR = 32
CHUNKS = ((0, 9), (9, 18), (18, 26), (26, 31))


def solve_coefs(nu):
    inner, last, back = [], [], []
    c_prev = 0.0
    for k in range(LEVELS):
        lo = nu if k > 0 else 0.0
        piv = 1.0 + nu + lo - lo * c_prev
        inner.append(1.0 / piv)
        last.append(1.0 / (1.0 + lo - lo * c_prev))
        c_prev = nu / piv
        back.append(c_prev)
    return inner, last, back


VISC = solve_coefs(VISC_NUM)
DIFF = solve_coefs(DIFF_NUM)


def weights():
    s = np.arange(1, SUBCYCLES + 1, dtype=np.float64) / (SUBCYCLES + 1)
    w = s ** 2 * (1.0 - s ** 4)
    return (w / w.sum()).astype(np.float32)


def exchange_kernel(ncol, nrow, u_hbm, v_hbm, t_hbm, s_hbm, eta_hbm, tu_hbm, tv_hbm, dep_hbm, kmt_hbm,
                    nu_ref, nv_ref, nt_ref, ns_ref, two_ref, et, fu, fv, cu, cv, fm_out, fe_out, fw_out,
                    fb, ki, kd, qs, msg_e, msg_w, got_w, got_e, xe, xw, ed,
                    wm, pk_e, pk_w, we, ww, fm, fk_e, fk_w, fe, fw,
                    ld_sem, in_sem, snd, rcv):
    c = lax.axis_index('col')
    r = lax.axis_index('row')
    east = lax.rem(c + 1, ncol)
    west = lax.rem(c + ncol - 1, ncol)
    north = lax.rem(r + 1, nrow)
    south = lax.rem(r + nrow - 1, nrow)
    has_n = r < nrow - 1
    has_s = r > 0

    src3 = (u_hbm, v_hbm, t_hbm, s_hbm)
    small = [pltpu.make_async_copy(kmt_hbm, ki, in_sem.at[0]),
             pltpu.make_async_copy(dep_hbm, kd.at[1, pl.ds(8, N), :], in_sem.at[1]),
             pltpu.make_async_copy(eta_hbm, wm.at[0, pl.ds(W, N), :], in_sem.at[2]),
             pltpu.make_async_copy(tu_hbm, wm.at[1, pl.ds(W, N), :], in_sem.at[3]),
             pltpu.make_async_copy(tv_hbm, wm.at[2, pl.ds(W, N), :], in_sem.at[4])]
    loads = []
    for ci, (k0, k1) in enumerate(CHUNKS):
        row = [pltpu.make_async_copy(src3[f].at[pl.ds(k0, k1 - k0)], fb.at[f, pl.ds(k0, k1 - k0), pl.ds(8, N), :],
                                     ld_sem.at[f, ci]) for f in range(4)]
        loads.append(row)
        for cp in row:
            cp.start()
        if ci == 0:
            for cp in small:
                cp.start()

    barrier = pltpu.get_barrier_semaphore()
    places = [(east, r), (west, r), (c, north), (c, south), (east, north), (east, south), (west, north), (west, south)]
    for cc, rr in places:
        pl.semaphore_signal(barrier, inc=1, device_id={'col': cc, 'row': rr}, device_id_type=MESH)

    def copy(i, src, dst, cc, rr):
        return pltpu.make_async_remote_copy(src_ref=src, dst_ref=dst, send_sem=snd.at[i], recv_sem=rcv.at[i],
                                            device_id={'col': cc, 'row': rr}, device_id_type=MESH)

    rows = [
        (copy(0, fb.at[:, :, pl.ds(8, 1), :], fb.at[:, :, pl.ds(8 + N, 1), :], c, south), has_s, has_n),
        (copy(1, fb.at[:, :, pl.ds(7 + N, 1), :], fb.at[:, :, pl.ds(7, 1), :], c, north), has_n, has_s),
        (copy(2, kd.at[:, pl.ds(8, 1), :], kd.at[:, pl.ds(8 + N, 1), :], c, south), has_s, has_n),
        (copy(3, kd.at[:, pl.ds(7 + N, 1), :], kd.at[:, pl.ds(7, 1), :], c, north), has_n, has_s),
    ]
    cols = [
        (copy(4, msg_e, got_w.at[pl.ds(8, N), :], east, r), None, None),
        (copy(5, msg_w, got_e.at[pl.ds(8, N), :], west, r), None, None),
        (copy(6, msg_e.at[pl.ds(0, 8), :], got_w.at[pl.ds(8 + N, 8), :], east, south), has_s, has_n),
        (copy(7, msg_w.at[pl.ds(N - 8, 8), :], got_e.at[pl.ds(0, 8), :], west, north), has_n, has_s),
    ]

    def main_rows(base, main):
        return [
            (copy(base, main.at[:, pl.ds(W, W), :], main.at[:, pl.ds(W + N, W), :], c, south), has_s, has_n),
            (copy(base + 1, main.at[:, pl.ds(N, W), :], main.at[:, pl.ds(0, W), :], c, north), has_n, has_s),
        ]

    def side_cols(base, to_e, to_w, in_e, in_w, w, n):
        return [
            (copy(base, to_w, in_e.at[pl.ds(w, n), :], west, r), None, None),
            (copy(base + 1, to_e, in_w.at[pl.ds(w, n), :], east, r), None, None),
        ]

    wide_side = side_cols(8, pk_e, pk_w, we, ww, W, N)
    wide_main = main_rows(10, wm)
    wide_pass = []
    for i, buf in ((12, we), (14, ww)):
        wide_pass += [
            (copy(i, buf.at[pl.ds(W, W), :], buf.at[pl.ds(W + N, W), :], c, south), has_s, has_n),
            (copy(i + 1, buf.at[pl.ds(N, W), :], buf.at[pl.ds(0, W), :], c, north), has_n, has_s),
        ]
    h = W // 2
    n2 = N // 2
    lo, hi = pl.ds(0, h), pl.ds(n2 - h, h)
    forc = side_cols(16, fk_e, fk_w, fe, fw, h, n2) + main_rows(18, fm) + [
        (copy(20, fk_w.at[lo, :], fe.at[pl.ds(h + n2, h), :], west, south), has_s, has_n),
        (copy(21, fk_w.at[hi, :], fe.at[lo, :], west, north), has_n, has_s),
        (copy(22, fk_e.at[lo, :], fw.at[pl.ds(h + n2, h), :], east, south), has_s, has_n),
        (copy(23, fk_e.at[hi, :], fw.at[lo, :], east, north), has_n, has_s),
    ]

    def run(cond, fn):
        if cond is None:
            fn()
        else:
            pl.when(cond)(fn)

    def start(items):
        for cp, s_if, _ in items:
            run(s_if, cp.start)

    def wait_recv(items):
        for cp, _, r_if in items:
            run(r_if, cp.wait_recv)

    def wait_send(items):
        for cp, s_if, _ in items:
            run(s_if, cp.wait_send)

    lane = lax.broadcasted_iota(jnp.int32, (N, N), 1)
    part = lax.rem(lane, 4)
    slot = lane // 4

    def roll(x, s):
        s %= N
        return pltpu.roll(x, s, 1) if s else x

    for cp in small:
        cp.wait()
    kmt_f = ki[...].astype(F32)
    dep = kd[1, 8:8 + N, :]
    kd[0, 8:8 + N, :] = kmt_f
    wm[3, W:W + N, :] = jnp.where(kmt_f > 0.0, dep, 0.0)

    def pack(fields):
        e_acc = jnp.zeros((N, N), F32)
        w_acc = jnp.zeros((N, N), F32)
        for f, x in enumerate(fields):
            here = lane // W == f
            w_acc = jnp.where(here, roll(x, W * f), w_acc)
            e_acc = jnp.where(here, roll(x, W * (f + 1)), e_acc)
        return e_acc, w_acc

    e_acc, w_acc = pack([wm[f, W:W + N, :] for f in range(4)])
    pk_e[...] = e_acc
    pk_w[...] = w_acc

    acc = [jnp.zeros((N, N), F32)] * 4
    for ci, (k0, k1) in enumerate(CHUNKS):
        for cp in loads[ci]:
            cp.wait()
        if ci == 0:
            pl.semaphore_wait(barrier, len(places))
            start(wide_side)
            start(wide_main)
        if ci == len(CHUNKS) - 1:
            start(rows)
        for f in range(4):
            x = acc[f]
            for k in range(k0, k1):
                x = jnp.where(slot == k, roll(fb[f, k, 8:8 + N, :], 4 * k + 2), x)
            acc[f] = x
    out_e = jnp.where(lane == 124, roll(kmt_f, -3), roll(dep, -2))
    out_w = jnp.where(lane == 124, roll(kmt_f, 124), roll(dep, 125))
    for f in range(4):
        qs[f, 8:8 + N, :] = acc[f]
        pick = (part == f) & (slot < LEVELS)
        out_e = jnp.where(pick, roll(acc[f], f - 1), out_e)
        out_w = jnp.where(pick, roll(acc[f], f - 2), out_w)
    msg_e[...] = out_e
    msg_w[...] = out_w

    start(cols)

    @pl.when(jnp.logical_not(has_n))
    def _():
        fb[:, :, 8 + N:9 + N, :] = jnp.zeros((4, LEVELS, 1, N), F32)
        kd[:, 8 + N:9 + N, :] = jnp.zeros((2, 1, N), F32)
        got_w[8 + N:16 + N, :] = jnp.zeros((8, N), F32)

    @pl.when(jnp.logical_not(has_s))
    def _():
        fb[:, :, 7:8, :] = jnp.zeros((4, LEVELS, 1, N), F32)
        kd[:, 7:8, :] = jnp.zeros((2, 1, N), F32)
        got_e[0:8, :] = jnp.zeros((8, N), F32)

    def thick(k, d):
        return 0.6 * d / jnp.maximum(k, 1.0)

    def force(wet_u, wet_v, q_c, q_e, q_n, u_c, u_n, u_s, v_c, v_n, v_s):
        us, vs = u_c + u_n, v_c + v_s
        v_at_u = 0.25 * (vs + roll(vs, -1))
        u_at_v = 0.25 * (us + roll(us, 1))
        u_w = roll(u_c, 1)
        g_u = jnp.where(wet_u, u_c * (roll(u_c, -1) - u_w) + v_at_u * (u_n - u_s) + (q_e - q_c), 0.0)
        g_v = jnp.where(wet_v, u_at_v * (roll(v_c, -1) - roll(v_c, 1)) + v_c * (v_n - v_s) + (q_n - q_c), 0.0)
        u_m, v_m = jnp.where(wet_u, u_c, 0.0), jnp.where(wet_v, v_c, 0.0)
        return g_u, g_v, u_m - 0.125 * g_u, v_m - 0.125 * g_v, u_m, v_m, u_w

    def advect(u_e, u_w, v_n, v_s, tracers):
        a_e, a_w = jnp.minimum(u_e, 0.0), jnp.maximum(u_w, 0.0)
        a_n, a_s = jnp.minimum(v_n, 0.0), jnp.maximum(v_s, 0.0)
        a_c = (jnp.maximum(u_e, 0.0) - jnp.minimum(u_w, 0.0)) + (jnp.maximum(v_n, 0.0) - jnp.minimum(v_s, 0.0))
        b_c = 4.0 - a_c
        return [b_c * x + ((a_w * roll(x, 1) - a_e * roll(x, -1)) + (a_s * x_s - a_n * x_n)) for x, x_n, x_s in tracers]

    def main_step(i, _):
        @pl.when(i == N // PR - 2)
        def _():
            wait_recv(rows)
            wait_recv(wide_side)
            start(wide_pass)

        own = pl.multiple_of(lax.rem(i + 1, N // PR) * PR, PR)
        base = own + 8

        def at(f, k, off):
            return fb[f, k, pl.ds(base + off, PR), :]

        kc = kd[0, pl.ds(base, PR), :]
        kn = kd[0, pl.ds(base + 1, PR), :]
        ks = kd[0, pl.ds(base - 1, PR), :]
        dc = kd[1, pl.ds(base, PR), :]
        dn = kd[1, pl.ds(base + 1, PR), :]
        th_c, th_n = thick(kc, dc), thick(kn, dn)
        nu_f = jnp.minimum(kc, roll(kc, -1))
        nw_f = jnp.minimum(kc, roll(kc, 1))
        nv_f = jnp.minimum(kc, kn)
        nq_f = jnp.minimum(kc, ks)
        zero = jnp.zeros((PR, N), F32)
        cum_c, cum_n, sum_u, sum_v = zero, zero, zero, zero
        for k in range(LEVELS):
            fk = float(k)
            t_c, s_c = at(2, k, 0), at(3, k, 0)
            t_n, s_n = at(2, k, 1), at(3, k, 1)
            h_c = s_c - 0.5 * t_c
            h_n = s_n - 0.5 * t_n
            mid_c, mid_n = cum_c + h_c, cum_n + h_n
            cum_c, cum_n = mid_c + h_c, mid_n + h_n
            q_c = mid_c * th_c
            u_c, v_c, v_s = at(0, k, 0), at(1, k, 0), at(1, k, -1)
            g_u, g_v, r_u, r_v, u_m, v_m, u_w = force(
                nu_f > fk, nv_f > fk, q_c, roll(q_c, -1), mid_n * th_n,
                u_c, at(0, k, 1), at(0, k, -1), v_c, at(1, k, 1), v_s)
            sum_u, sum_v = sum_u + g_u, sum_v + g_v
            nu_ref[k, pl.ds(own, PR), :] = r_u
            nv_ref[k, pl.ds(own, PR), :] = r_v
            t1, s1 = advect(u_m, jnp.where(nw_f > fk, u_w, 0.0), v_m, jnp.where(nq_f > fk, v_s, 0.0),
                            ((t_c, t_n, at(2, k, -1)), (s_c, s_n, at(3, k, -1))))
            nt_ref[k, pl.ds(own, PR), :] = t1
            ns_ref[k, pl.ds(own, PR), :] = s1
        hu = jnp.where(nu_f > 0.0, 0.5 * (dc + roll(dc, -1)), 0.0)
        hv = jnp.where(nv_f > 0.0, 0.5 * (dc + dn), 0.0)
        fm[0, pl.ds(own + W, PR), :] = hu / jnp.maximum(nu_f, 1.0) * (-0.5 * sum_u)
        fm[1, pl.ds(own + W, PR), :] = hv / jnp.maximum(nv_f, 1.0) * (-0.5 * sum_v)
        return 0

    lax.fori_loop(0, N // PR, main_step, 0)

    lane8 = lax.broadcasted_iota(jnp.int32, (8, N), 1)
    for f in range(4):
        for lo in (0, 8 + N):
            x = jnp.zeros((8, N), F32)
            for k in range(LEVELS):
                x = jnp.where(lane8 // 4 == k, roll(fb[f, k, lo:lo + 8, :], 4 * k + 2), x)
            qs[f, lo:lo + 8, :] = x

    wait_recv(cols)

    part_x = lax.rem(lax.broadcasted_iota(jnp.int32, (N + 16, N), 1), 4)
    for f in range(4):
        q = qs[f]
        xe[f] = jnp.where(part_x == 2, roll(got_e[...], 2 - f), q)
        xw[f] = jnp.where(part_x == 1, roll(got_w[...], 1 - f), q)
    for f in range(2):
        q = kd[f]
        b = [jnp.broadcast_to(q[:, j:j + 1], q.shape) for j in (N - 2, N - 1, 0, 1)]
        h_e = jnp.broadcast_to(got_e[:, 124 + f:125 + f], q.shape)
        h_w = jnp.broadcast_to(got_w[:, 124 + f:125 + f], q.shape)
        xe[4 + f] = jnp.where(part_x == 0, b[0], jnp.where(part_x == 1, b[1], h_e))
        xw[4 + f] = jnp.where(part_x == 1, h_w, jnp.where(part_x == 2, b[2], b[3]))

    lev = slot.astype(F32)

    row_i = lax.broadcasted_iota(jnp.int32, (N, N), 0)
    same = lax.rem(row_i, 4) == part
    below = jnp.where(same & (row_i // 4 <= slot), 1.0, 0.0)
    every = jnp.where(same, 1.0, 0.0)

    def mix(x, m):
        return jnp.dot(x, m, precision=lax.Precision.HIGHEST, preferred_element_type=F32)

    def strip_force(x):
        def at(f, off):
            return x[f, 8 + off:8 + off + N, :]

        kc, kn = at(4, 0), at(4, 1)
        dc, dn = at(5, 0), at(5, 1)
        nu_f, nv_f = jnp.minimum(kc, roll(kc, -1)), jnp.minimum(kc, kn)
        h_c = at(3, 0) - 0.5 * at(2, 0)
        h_n = at(3, 1) - 0.5 * at(2, 1)
        q_c = (2.0 * mix(h_c, below) - h_c) * thick(kc, dc)
        q_n = (2.0 * mix(h_n, below) - h_n) * thick(kn, dn)
        g_u, g_v, r_u, r_v = force(nu_f > lev, nv_f > lev, q_c, roll(q_c, -1), q_n,
                                   at(0, 0), at(0, 1), at(0, -1), at(1, 0), at(1, 1), at(1, -1))[:4]
        hu = jnp.where(nu_f > 0.0, -0.25 * (dc + roll(dc, -1)), 0.0) / jnp.maximum(nu_f, 1.0)
        hv = jnp.where(nv_f > 0.0, -0.25 * (dc + dn), 0.0) / jnp.maximum(nv_f, 1.0)
        return hu, hv, g_u, g_v, r_u, r_v

    def strip_tracer(x):
        def at(f, off):
            return x[f, 8 + off:8 + off + N, :]

        kc, kn, ks = at(4, 0), at(4, 1), at(4, -1)
        u_m = jnp.where(jnp.minimum(kc, roll(kc, -1)) > lev, at(0, 0), 0.0)
        u_w = jnp.where(jnp.minimum(kc, roll(kc, 1)) > lev, roll(at(0, 0), 1), 0.0)
        v_m = jnp.where(jnp.minimum(kc, kn) > lev, at(1, 0), 0.0)
        v_s = jnp.where(jnp.minimum(kc, ks) > lev, at(1, -1), 0.0)
        return advect(u_m, u_w, v_m, v_s, ((at(2, 0), at(2, 1), at(2, -1)), (at(3, 0), at(3, 1), at(3, -1))))

    def merge(fn):
        return [jnp.where(part == 1, a, b) for a, b in zip(fn(xe), fn(xw))]

    hu, hv, g_u, g_v, r_u, r_v = merge(strip_force)
    rim = (lane == 0) | (lane == N - 1)
    forces = []
    for f, (hf, g) in enumerate(((hu, g_u), (hv, g_v))):
        x = jnp.where(rim, roll(hf * mix(g, every), 2), fm[f, W:W + N, :])
        fm[f, W:W + N, :] = x
        forces.append(x)
    half = lax.broadcasted_iota(jnp.int32, (h, N), 1) < n2
    for ref, x in zip((fk_e, fk_w), pack(forces)):
        for b in range(N // W):
            ref[h * b:h * b + h, :] = jnp.where(half, x[W * b:W * b + h], roll(x[W * b + h:W * b + W], n2))
    start(forc)
    ed[0] = r_u
    ed[1] = r_v
    t1, s1 = merge(strip_tracer)
    ed[2] = t1
    ed[3] = s1

    lane_q = lax.broadcasted_iota(jnp.int32, (QR, N), 1)
    edge_q = (lane_q == 0) | (lane_q == N - 1)

    def solve_step(g, _):
        own = pl.multiple_of(g * QR, QR)
        base = own + 8
        here = pl.ds(own, QR)
        kc = kd[0, pl.ds(base, QR), :]
        kn = kd[0, pl.ds(base + 1, QR), :]
        nu_f = jnp.minimum(kc, jnp.where(lane_q == N - 1, roll(got_e[pl.ds(base, QR), :], 3), roll(kc, -1)))
        nv_f = jnp.minimum(kc, kn)
        two_ref[0, here, :] = nu_f
        two_ref[1, here, :] = nv_f
        zero = jnp.zeros((QR, N), F32)
        refs = (nu_ref, nv_ref, nt_ref, ns_ref)
        cos = (VISC, VISC, DIFF, DIFF)
        d = [zero] * 4

        def factor(n_f, k, co, nu):
            return jnp.where(n_f > k + 1.0, nu * co[0][k], jnp.where(n_f > float(k), nu * co[1][k], 0.0))

        for k in range(LEVELS):
            f_t = factor(kc, k, DIFF, DIFF_NUM)
            facs = (factor(nu_f, k, VISC, VISC_NUM), factor(nv_f, k, VISC, VISC_NUM), f_t, f_t)
            for q in range(4):
                x = jnp.where(edge_q, roll(ed[q, here, :], 126 - 4 * k), refs[q][k, here, :])
                d[q] = (x + d[q]) * facs[q]
                if k == LEVELS - 1:
                    refs[q][k, here, :] = 0.25 * d[q]
                else:
                    refs[q][k, here, :] = d[q]
        sum_u, sum_v = d[0], d[1]
        for k in range(LEVELS - 2, -1, -1):
            for q in range(4):
                d[q] = refs[q][k, here, :] + cos[q][2][k] * d[q]
                refs[q][k, here, :] = 0.25 * d[q]
            sum_u, sum_v = sum_u + d[0], sum_v + d[1]
        two_ref[2, here, :] = sum_u / (VISC_NUM * jnp.maximum(nu_f, 1.0))
        two_ref[3, here, :] = sum_v / (VISC_NUM * jnp.maximum(nv_f, 1.0))
        return 0

    lax.fori_loop(0, N // QR, solve_step, 0)

    wait_recv(wide_main)
    wait_recv(wide_pass)
    lane_x = lax.broadcasted_iota(jnp.int32, (EXT, N), 1)
    row_x = lax.broadcasted_iota(jnp.int32, (EXT, N), 0)
    real = (row_x >= jnp.where(has_s, 0, W)) & (row_x < jnp.where(has_n, EXT, W + N))
    in_e, in_w = lane_x < W, lane_x >= N - W

    def side(f):
        return jnp.where(in_e, roll(we[...], -W * f), roll(ww[...], -W * (f + 1)))

    dms = (jnp.where(real, wm[3], 0.0), jnp.where(real & (in_e | in_w), side(3), 0.0))
    zero8 = jnp.zeros((8, N), F32)
    for ref in (et, fu, fv):
        for t in range(2):
            ref[t, 0:8, :] = zero8
            ref[t, 8 + EXT:TOP, :] = zero8
    for t in range(2):
        et[t, 8:8 + EXT, :] = dms[t]
    ra, rb = roll(dms[0], -1), roll(dms[1], -1)
    dme = (jnp.where(lane_x == N - 1, rb, ra), jnp.where(lane_x == N - 1, ra, rb))
    for t in range(2):
        d_c = dms[t]
        d_n = et[t, 9:9 + EXT, :]
        wet_u = (d_c > 0.0) & (dme[t] > 0.0)
        wet_v = (d_c > 0.0) & (d_n > 0.0)
        pick = (lambda f: wm[f]) if t == 0 else side
        et[t, 8:8 + EXT, :] = jnp.where(d_c > 0.0, pick(0), 0.0)
        fu[t, 8:8 + EXT, :] = jnp.where(wet_u, 0.5 * pick(1), 0.0)
        fv[t, 8:8 + EXT, :] = jnp.where(wet_v, 0.5 * pick(2), 0.0)
        cu[t] = jnp.where(wet_u, 0.125 * (d_c + dme[t]), 0.0)
        cv[t] = jnp.where(wet_v, 0.125 * (d_c + d_n), 0.0)
    wait_send(rows)
    wait_send(cols)
    wait_send(wide_side)
    wait_send(wide_main)
    wait_send(wide_pass)
    wait_recv(forc)
    fm_out[...] = fm[...]
    for out, got in ((fe_out, fe), (fw_out, fw)):
        for b in range(EXT // W):
            x = got[h * b:h * b + h, :]
            out[W * b:W * b + h, :] = x
            out[W * b + h:W * b + W, :] = roll(x, n2)
    wait_send(forc)


def step_kernel(nu_ref, nv_ref, nt_ref, ns_ref, two_ref, et0, fu0, fv0, cu, cv, fm, fe, fw,
                eta_out, tu_out, tv_out, u_hbm, v_hbm, t_hbm, s_hbm,
                et1, fu1, fv1, pu, pv, mean, ub, vb, osem):
    copies = [pltpu.make_async_copy(nt_ref, t_hbm, osem.at[0]), pltpu.make_async_copy(ns_ref, s_hbm, osem.at[1])]
    for cp in copies:
        cp.start()

    lane = lax.broadcasted_iota(jnp.int32, (EXT, N), 1)

    def side(f):
        e, w = fe[...], fw[...]
        e = pltpu.roll(e, N - W * f, 1) if f else e
        w = pltpu.roll(w, N - W * (f + 1), 1)
        return jnp.where(lane < W, e, w)

    for f, (p, co) in enumerate(((pu, cu), (pv, cv))):
        for t in range(2):
            x = fm[f] if t == 0 else side(f)
            p[t] = jnp.where(co[t] > 0.0, (0.125 / SUBCYCLES) * x, 0.0)
    zero8 = jnp.zeros((8, N), F32)
    for ref in (et1, fv1):
        for t in range(2):
            ref[t, 0:8, :] = zero8
            ref[t, 8 + EXT:TOP, :] = zero8

    wgt = weights()
    lane8 = lax.broadcasted_iota(jnp.int32, (8, N), 1)
    first8, last8 = lane8 == 0, lane8 == N - 1

    def west8(x):
        a, b = pltpu.roll(x[0], 1, 1), pltpu.roll(x[1], 1, 1)
        return jnp.where(first8, b, a), jnp.where(first8, a, b)

    def east8(x):
        a, b = pltpu.roll(x[0], N - 1, 1), pltpu.roll(x[1], N - 1, 1)
        return jnp.where(last8, b, a), jnp.where(last8, a, b)

    for n in range(1, SUBCYCLES + 1):
        lo = 8 * (n // 8)
        groups = range(lo, EXT - lo, 8)
        et, fu, fv = (et1, fu1, fv1) if n > 1 else (et0, fu0, fv0)
        for g in groups:
            us = (fu[0, 8 + g:16 + g, :], fu[1, 8 + g:16 + g, :])
            uw = west8(us)
            for t in range(2):
                et1[t, 8 + g:16 + g, :] = et[t, 8 + g:16 + g, :] - (
                    (us[t] - uw[t]) + (fv[t, 8 + g:16 + g, :] - fv[t, 7 + g:15 + g, :]))
        for g in groups:
            es = (et1[0, 8 + g:16 + g, :], et1[1, 8 + g:16 + g, :])
            ee = east8(es)
            for t in range(2):
                u = fu[t, 8 + g:16 + g, :] - cu[t, g:g + 8, :] * (ee[t] - es[t]) + pu[t, g:g + 8, :]
                v = fv[t, 8 + g:16 + g, :] - cv[t, g:g + 8, :] * (et1[t, 9 + g:17 + g, :] - es[t]) + pv[t, g:g + 8, :]
                fu1[t, 8 + g:16 + g, :] = u
                fv1[t, 8 + g:16 + g, :] = v
                if t == 0 and W <= g < W + N:
                    at = slice(g - W, g - W + 8)
                    w = float(wgt[n - 1])
                    mean[0, at, :] = w * u if n == 1 else mean[0, at, :] + w * u
                    mean[1, at, :] = w * v if n == 1 else mean[1, at, :] + w * v

    mid = slice(8 + W, 8 + W + N)
    eta_out[...] = et1[0, mid, :]
    tu_out[...] = 2.0 * fu1[0, mid, :]
    tv_out[...] = 2.0 * fv1[0, mid, :]
    for i, co in ((0, cu), (1, cv)):
        h = co[0, W:W + N, :]
        mean[i] = mean[i] / jnp.where(h > 0.0, 2.0 * h, 1.0) - two_ref[2 + i]

    for ci, (k0, k1) in enumerate(CHUNKS):
        for i, (src, buf, dst) in enumerate(((nu_ref, ub, u_hbm), (nv_ref, vb, v_hbm))):
            for g in range(0, N, 8):
                at = slice(g, g + 8)
                n_f, m = two_ref[i, at, :], mean[i, at, :]
                for k in range(k0, k1):
                    buf[k, at, :] = src[k, at, :] + jnp.where(n_f > float(k), m, 0.0)
            cp = pltpu.make_async_copy(buf.at[pl.ds(k0, k1 - k0)], dst.at[pl.ds(k0, k1 - k0)], osem.at[2 + 2 * ci + i])
            cp.start()
            copies.append(cp)
    for cp in copies:
        cp.wait()


def solution(mesh):
    ncol, nrow = mesh.shape['col'], mesh.shape['row']
    vmem = pl.BlockSpec(memory_space=pltpu.VMEM)
    hbm = pl.BlockSpec(memory_space=pl.ANY)
    s3 = jax.ShapeDtypeStruct((LEVELS, N, N), F32)
    s2 = jax.ShapeDtypeStruct((N, N), F32)

    def sds(*shape):
        return jax.ShapeDtypeStruct(shape, F32)

    def ocean_step(vel_u, vel_v, temp, salt, eta, tu, tv, dep, kmt):
        def kernel_a(*refs):
            exchange_kernel(ncol, nrow, *refs)

        def kernel_b(*refs):
            step_kernel(*refs)

        mid = pl.pallas_call(
            kernel_a,
            name='exchange',
            out_shape=(s3, s3, s3, s3, sds(4, N, N), sds(2, TOP, N), sds(2, TOP, N), sds(2, TOP, N), sds(2, EXT, N),
                       sds(2, EXT, N), sds(2, EXT, N), sds(EXT, N), sds(EXT, N)),
            in_specs=[hbm] * 9,
            out_specs=(vmem,) * 13,
            scratch_shapes=[
                pltpu.VMEM((4, LEVELS, N + 16, N), F32),
                pltpu.VMEM((N, N), jnp.int32),
                pltpu.VMEM((2, N + 16, N), F32),
                pltpu.VMEM((4, N + 16, N), F32),
                pltpu.VMEM((N, N), F32), pltpu.VMEM((N, N), F32),
                pltpu.VMEM((N + 16, N), F32), pltpu.VMEM((N + 16, N), F32),
                pltpu.VMEM((6, N + 16, N), F32), pltpu.VMEM((6, N + 16, N), F32),
                pltpu.VMEM((4, N, N), F32),
                pltpu.VMEM((4, EXT, N), F32),
                pltpu.VMEM((N, N), F32), pltpu.VMEM((N, N), F32),
                pltpu.VMEM((EXT, N), F32), pltpu.VMEM((EXT, N), F32),
                pltpu.VMEM((2, EXT, N), F32),
                pltpu.VMEM((N // 2, N), F32), pltpu.VMEM((N // 2, N), F32),
                pltpu.VMEM((EXT // 2, N), F32), pltpu.VMEM((EXT // 2, N), F32),
                pltpu.SemaphoreType.DMA((4, len(CHUNKS))),
                pltpu.SemaphoreType.DMA((5,)),
                pltpu.SemaphoreType.DMA((24,)),
                pltpu.SemaphoreType.DMA((24,)),
            ],
            compiler_params=pltpu.CompilerParams(collective_id=0, has_side_effects=True, vmem_limit_bytes=28 * 2 ** 20),
        )(*[pltpu.with_memory_space_constraint(x, pltpu.HBM) for x in (vel_u, vel_v, temp, salt, eta, tu, tv, dep, kmt)])
        st = pltpu.VMEM((2, TOP, N), F32)
        co = pltpu.VMEM((2, EXT, N), F32)
        out = pl.pallas_call(
            kernel_b,
            name='subcycles',
            out_shape=(s2, s2, s2, s3, s3, s3, s3),
            in_specs=[vmem] * 13,
            out_specs=(vmem,) * 3 + (hbm,) * 4,
            scratch_shapes=[st, st, st, co, co, pltpu.VMEM((2, N, N), F32),
                            pltpu.VMEM((LEVELS, N, N), F32), pltpu.VMEM((LEVELS, N, N), F32),
                            pltpu.SemaphoreType.DMA((2 + 2 * len(CHUNKS),))],
            compiler_params=pltpu.CompilerParams(vmem_limit_bytes=28 * 2 ** 20),
        )(*mid)
        return out

    spec_3d = P(None, 'row', 'col')
    spec_2d = P('row', 'col')
    return jax.shard_map(ocean_step, mesh=mesh, in_specs=(spec_3d,) * 4 + (spec_2d,) * 5,
                         out_specs=(spec_2d,) * 3 + (spec_3d,) * 4, check_vma=False)
```

```python
import jax
import jax.numpy as jnp
import numpy as np
from jax import lax
from jax.experimental import pallas as pl
from jax.experimental.pallas import tpu as pltpu
from jax.sharding import PartitionSpec as P

MESH = pl.DeviceIdType.MESH
F32 = jnp.float32
SUBCYCLES = 30
LEVELS = 31
VISC_NUM = 4.0
DIFF_NUM = 1.0
N = 128
W = 32
EXT = N + 2 * W
TOP = EXT + 16
PR = 16
QR = 32
CHUNKS = ((0, 9), (9, 18), (18, 26), (26, 31))
OUT_CHUNKS = ((0, 3), (3, 9), (9, 17), (17, 25), (25, 31))


def solve_coefs(nu):
    inner, last, back = [], [], []
    c_prev = 0.0
    for k in range(LEVELS):
        lo = nu if k > 0 else 0.0
        piv = 1.0 + nu + lo - lo * c_prev
        inner.append(1.0 / piv)
        last.append(1.0 / (1.0 + lo - lo * c_prev))
        c_prev = nu / piv
        back.append(c_prev)
    return inner, last, back


VISC = solve_coefs(VISC_NUM)
DIFF = solve_coefs(DIFF_NUM)


def weights():
    s = np.arange(1, SUBCYCLES + 1, dtype=np.float64) / (SUBCYCLES + 1)
    w = s ** 2 * (1.0 - s ** 4)
    return (w / w.sum()).astype(np.float32)


def exchange_kernel(ncol, nrow, u_hbm, v_hbm, t_hbm, s_hbm, eta_hbm, tu_hbm, tv_hbm, dep_hbm, kmt_hbm,
                    nu_ref, nv_ref, nt_ref, ns_ref, two_ref, et, fu, fv, cu, cv, fm_out, fe_out, fw_out,
                    fb, ki, kd, cr, qs, msg_e, msg_w, got_w, got_e, xe, xw, ed,
                    wm, pk_e, pk_w, we, ww, fm, fk_e, fk_w, fe, fw,
                    ld_sem, in_sem, snd, rcv):
    c = lax.axis_index('col')
    r = lax.axis_index('row')
    east = lax.rem(c + 1, ncol)
    west = lax.rem(c + ncol - 1, ncol)
    north = lax.rem(r + 1, nrow)
    south = lax.rem(r + nrow - 1, nrow)
    has_n = r < nrow - 1
    has_s = r > 0

    barrier = pltpu.get_barrier_semaphore()
    places = [(east, r), (west, r), (c, north), (c, south), (east, north), (east, south), (west, north), (west, south)]
    for cc, rr in places:
        pl.semaphore_signal(barrier, inc=1, device_id={'col': cc, 'row': rr}, device_id_type=MESH)

    src3 = (u_hbm, v_hbm, t_hbm, s_hbm)
    small = [pltpu.make_async_copy(kmt_hbm, ki, in_sem.at[0]),
             pltpu.make_async_copy(dep_hbm, kd.at[1, pl.ds(8, N), :], in_sem.at[1]),
             pltpu.make_async_copy(eta_hbm, wm.at[0, pl.ds(W, N), :], in_sem.at[2]),
             pltpu.make_async_copy(tu_hbm, wm.at[1, pl.ds(W, N), :], in_sem.at[3]),
             pltpu.make_async_copy(tv_hbm, wm.at[2, pl.ds(W, N), :], in_sem.at[4])]
    loads = []
    for ci, (k0, k1) in enumerate(CHUNKS):
        row = [pltpu.make_async_copy(src3[f].at[pl.ds(k0, k1 - k0)], fb.at[f, pl.ds(k0, k1 - k0), pl.ds(8, N), :],
                                     ld_sem.at[f, ci]) for f in range(4)]
        loads.append(row)
        for cp in row:
            cp.start()
        if ci == 0:
            for cp in small:
                cp.start()

    def copy(i, src, dst, cc, rr):
        return pltpu.make_async_remote_copy(src_ref=src, dst_ref=dst, send_sem=snd.at[i], recv_sem=rcv.at[i],
                                            device_id={'col': cc, 'row': rr}, device_id_type=MESH)

    rows = [
        (copy(0, fb.at[:, :, pl.ds(8, 1), :], fb.at[:, :, pl.ds(8 + N, 1), :], c, south), has_s, has_n),
        (copy(1, fb.at[:, :, pl.ds(7 + N, 1), :], fb.at[:, :, pl.ds(7, 1), :], c, north), has_n, has_s),
        (copy(2, kd.at[:, pl.ds(8, 1), :], kd.at[:, pl.ds(8 + N, 1), :], c, south), has_s, has_n),
        (copy(3, kd.at[:, pl.ds(7 + N, 1), :], kd.at[:, pl.ds(7, 1), :], c, north), has_n, has_s),
    ]
    cols = [
        (copy(4, msg_e, got_w.at[pl.ds(8, N), :], east, r), None, None),
        (copy(5, msg_w, got_e.at[pl.ds(8, N), :], west, r), None, None),
        (copy(6, msg_e.at[pl.ds(0, 8), :], got_w.at[pl.ds(8 + N, 8), :], east, south), has_s, has_n),
        (copy(7, msg_w.at[pl.ds(N - 8, 8), :], got_e.at[pl.ds(0, 8), :], west, north), has_n, has_s),
    ]

    def main_rows(base, main):
        return [
            (copy(base, main.at[:, pl.ds(W, W), :], main.at[:, pl.ds(W + N, W), :], c, south), has_s, has_n),
            (copy(base + 1, main.at[:, pl.ds(N, W), :], main.at[:, pl.ds(0, W), :], c, north), has_n, has_s),
        ]

    def side_cols(base, to_e, to_w, in_e, in_w, w, n):
        return [
            (copy(base, to_w, in_e.at[pl.ds(w, n), :], west, r), None, None),
            (copy(base + 1, to_e, in_w.at[pl.ds(w, n), :], east, r), None, None),
        ]

    wide_side = side_cols(8, pk_e, pk_w, we, ww, W, N)
    wide_main = main_rows(10, wm)
    wide_pass = []
    for i, buf in ((12, we), (14, ww)):
        wide_pass += [
            (copy(i, buf.at[pl.ds(W, W), :], buf.at[pl.ds(W + N, W), :], c, south), has_s, has_n),
            (copy(i + 1, buf.at[pl.ds(N, W), :], buf.at[pl.ds(0, W), :], c, north), has_n, has_s),
        ]
    h = W // 2
    n2 = N // 2
    lo, hi = pl.ds(0, h), pl.ds(n2 - h, h)
    forc = side_cols(16, fk_e, fk_w, fe, fw, h, n2) + main_rows(18, fm) + [
        (copy(20, fk_w.at[lo, :], fe.at[pl.ds(h + n2, h), :], west, south), has_s, has_n),
        (copy(21, fk_w.at[hi, :], fe.at[lo, :], west, north), has_n, has_s),
        (copy(22, fk_e.at[lo, :], fw.at[pl.ds(h + n2, h), :], east, south), has_s, has_n),
        (copy(23, fk_e.at[hi, :], fw.at[lo, :], east, north), has_n, has_s),
    ]

    def run(cond, fn):
        if cond is None:
            fn()
        else:
            pl.when(cond)(fn)

    def start(items):
        for cp, s_if, _ in items:
            run(s_if, cp.start)

    def wait_recv(items):
        for cp, _, r_if in items:
            run(r_if, cp.wait_recv)

    def wait_send(items):
        for cp, s_if, _ in items:
            run(s_if, cp.wait_send)

    lane = lax.broadcasted_iota(jnp.int32, (N, N), 1)
    part = lax.rem(lane, 4)
    slot = lane // 4

    def roll(x, s):
        s %= N
        return pltpu.roll(x, s, 1) if s else x

    for cp in small:
        cp.wait()
    kmt_f = ki[...].astype(F32)
    dep = kd[1, 8:8 + N, :]
    kd[0, 8:8 + N, :] = kmt_f
    wm[3, W:W + N, :] = jnp.where(kmt_f > 0.0, dep, 0.0)

    def pack(fields):
        e_acc = jnp.zeros((N, N), F32)
        w_acc = jnp.zeros((N, N), F32)
        for f, x in enumerate(fields):
            here = lane // W == f
            w_acc = jnp.where(here, roll(x, W * f), w_acc)
            e_acc = jnp.where(here, roll(x, W * (f + 1)), e_acc)
        return e_acc, w_acc

    e_acc, w_acc = pack([wm[f, W:W + N, :] for f in range(4)])
    pk_e[...] = e_acc
    pk_w[...] = w_acc

    def thick(k, d):
        return 0.6 * d / jnp.maximum(k, 1.0)

    def force(wet_u, wet_v, q_c, q_e, q_n, u_c, u_n, u_s, v_c, v_n, v_s):
        us, vs = u_c + u_n, v_c + v_s
        v_at_u = 0.25 * (vs + roll(vs, -1))
        u_at_v = 0.25 * (us + roll(us, 1))
        u_w = roll(u_c, 1)
        g_u = jnp.where(wet_u, u_c * (roll(u_c, -1) - u_w) + v_at_u * (u_n - u_s) + (q_e - q_c), 0.0)
        g_v = jnp.where(wet_v, u_at_v * (roll(v_c, -1) - roll(v_c, 1)) + v_c * (v_n - v_s) + (q_n - q_c), 0.0)
        u_m, v_m = jnp.where(wet_u, u_c, 0.0), jnp.where(wet_v, v_c, 0.0)
        return g_u, g_v, u_m - 0.125 * g_u, v_m - 0.125 * g_v, u_m, v_m, u_w

    def advect(u_e, u_w, v_n, v_s, tracers):
        a_e, a_w = jnp.minimum(u_e, 0.0), jnp.maximum(u_w, 0.0)
        a_n, a_s = jnp.minimum(v_n, 0.0), jnp.maximum(v_s, 0.0)
        a_c = (jnp.maximum(u_e, 0.0) - jnp.minimum(u_w, 0.0)) + (jnp.maximum(v_n, 0.0) - jnp.minimum(v_s, 0.0))
        b_c = 4.0 - a_c
        return [b_c * x + ((a_w * roll(x, 1) - a_e * roll(x, -1)) + (a_s * x_s - a_n * x_n)) for x, x_n, x_s in tracers]

    def main_part(own, k0, k1):
        here = pl.ds(own, PR)
        base = own + 8

        def at(f, k, off):
            return fb[f, k, pl.ds(base + off, PR), :]

        kc = kd[0, pl.ds(base, PR), :]
        kn = kd[0, pl.ds(base + 1, PR), :]
        ks = kd[0, pl.ds(base - 1, PR), :]
        dc = kd[1, pl.ds(base, PR), :]
        dn = kd[1, pl.ds(base + 1, PR), :]
        th_c, th_n = thick(kc, dc), thick(kn, dn)
        nu_f = jnp.minimum(kc, roll(kc, -1))
        nw_f = jnp.minimum(kc, roll(kc, 1))
        nv_f = jnp.minimum(kc, kn)
        nq_f = jnp.minimum(kc, ks)
        if k0 == 0:
            cum_c = cum_n = sum_u = sum_v = jnp.zeros((PR, N), F32)
        else:
            cum_c, cum_n, sum_u, sum_v = [cr[q, here, :] for q in range(4)]
        for k in range(k0, k1):
            fk = float(k)
            t_c, s_c = at(2, k, 0), at(3, k, 0)
            t_n, s_n = at(2, k, 1), at(3, k, 1)
            h_c = s_c - 0.5 * t_c
            h_n = s_n - 0.5 * t_n
            mid_c, mid_n = cum_c + h_c, cum_n + h_n
            cum_c, cum_n = mid_c + h_c, mid_n + h_n
            q_c = mid_c * th_c
            u_c, v_c, v_s = at(0, k, 0), at(1, k, 0), at(1, k, -1)
            g_u, g_v, r_u, r_v, u_m, v_m, u_w = force(
                nu_f > fk, nv_f > fk, q_c, roll(q_c, -1), mid_n * th_n,
                u_c, at(0, k, 1), at(0, k, -1), v_c, at(1, k, 1), v_s)
            sum_u, sum_v = sum_u + g_u, sum_v + g_v
            nu_ref[k, pl.ds(own, PR), :] = r_u
            nv_ref[k, pl.ds(own, PR), :] = r_v
            t1, s1 = advect(u_m, jnp.where(nw_f > fk, u_w, 0.0), v_m, jnp.where(nq_f > fk, v_s, 0.0),
                            ((t_c, t_n, at(2, k, -1)), (s_c, s_n, at(3, k, -1))))
            nt_ref[k, pl.ds(own, PR), :] = t1
            ns_ref[k, pl.ds(own, PR), :] = s1
        if k1 < LEVELS:
            for q, x in enumerate((cum_c, cum_n, sum_u, sum_v)):
                cr[q, here, :] = x
            return
        hu = jnp.where(nu_f > 0.0, 0.5 * (dc + roll(dc, -1)), 0.0)
        hv = jnp.where(nv_f > 0.0, 0.5 * (dc + dn), 0.0)
        fm[0, pl.ds(own + W, PR), :] = hu / jnp.maximum(nu_f, 1.0) * (-0.5 * sum_u)
        fm[1, pl.ds(own + W, PR), :] = hv / jnp.maximum(nv_f, 1.0) * (-0.5 * sum_v)

    def early_step(i, _):
        main_part(pl.multiple_of((i + 1) * PR, PR), 0, CHUNKS[0][1])
        return 0

    def main_step(i, _):
        own = pl.multiple_of(lax.rem(i + 1, N // PR) * PR, PR)

        @pl.when(i == N // PR - 2)
        def _():
            wait_recv(rows)
            wait_recv(wide_side)
            start(wide_pass)

        @pl.when(i >= N // PR - 2)
        def _():
            main_part(own, 0, CHUNKS[0][1])

        main_part(own, CHUNKS[0][1], LEVELS)
        return 0

    for ci, (k0, k1) in enumerate(CHUNKS):
        for cp in loads[ci]:
            cp.wait()
        if ci == len(CHUNKS) - 1:
            start(rows)
        for f in range(4):
            x = qs[f, 8:8 + N, :] if ci else jnp.zeros((N, N), F32)
            for k in range(k0, k1):
                x = jnp.where(slot == k, roll(fb[f, k, 8:8 + N, :], 4 * k + 2), x)
            qs[f, 8:8 + N, :] = x
        if ci == 0:
            lax.fori_loop(0, N // PR - 2, early_step, 0)
            pl.semaphore_wait(barrier, len(places))
            start(wide_side)
            start(wide_main)
    out_e = jnp.where(lane == 124, roll(kmt_f, -3), roll(dep, -2))
    out_w = jnp.where(lane == 124, roll(kmt_f, 124), roll(dep, 125))
    for f in range(4):
        x = qs[f, 8:8 + N, :]
        pick = (part == f) & (slot < LEVELS)
        out_e = jnp.where(pick, roll(x, f - 1), out_e)
        out_w = jnp.where(pick, roll(x, f - 2), out_w)
    msg_e[...] = out_e
    msg_w[...] = out_w

    start(cols)

    @pl.when(jnp.logical_not(has_n))
    def _():
        fb[:, :, 8 + N:9 + N, :] = jnp.zeros((4, LEVELS, 1, N), F32)
        kd[:, 8 + N:9 + N, :] = jnp.zeros((2, 1, N), F32)
        got_w[8 + N:16 + N, :] = jnp.zeros((8, N), F32)

    @pl.when(jnp.logical_not(has_s))
    def _():
        fb[:, :, 7:8, :] = jnp.zeros((4, LEVELS, 1, N), F32)
        kd[:, 7:8, :] = jnp.zeros((2, 1, N), F32)
        got_e[0:8, :] = jnp.zeros((8, N), F32)

    lax.fori_loop(0, N // PR, main_step, 0)

    lane8 = lax.broadcasted_iota(jnp.int32, (8, N), 1)
    for f in range(4):
        for lo in (0, 8 + N):
            x = jnp.zeros((8, N), F32)
            for k in range(LEVELS):
                x = jnp.where(lane8 // 4 == k, roll(fb[f, k, lo:lo + 8, :], 4 * k + 2), x)
            qs[f, lo:lo + 8, :] = x

    wait_recv(cols)

    part_x = lax.rem(lax.broadcasted_iota(jnp.int32, (N + 16, N), 1), 4)
    for f in range(4):
        q = qs[f]
        xe[f] = jnp.where(part_x == 2, roll(got_e[...], 2 - f), q)
        xw[f] = jnp.where(part_x == 1, roll(got_w[...], 1 - f), q)
    for f in range(2):
        q = kd[f]
        b = [jnp.broadcast_to(q[:, j:j + 1], q.shape) for j in (N - 2, N - 1, 0, 1)]
        h_e = jnp.broadcast_to(got_e[:, 124 + f:125 + f], q.shape)
        h_w = jnp.broadcast_to(got_w[:, 124 + f:125 + f], q.shape)
        xe[4 + f] = jnp.where(part_x == 0, b[0], jnp.where(part_x == 1, b[1], h_e))
        xw[4 + f] = jnp.where(part_x == 1, h_w, jnp.where(part_x == 2, b[2], b[3]))

    lev = slot.astype(F32)

    row_i = lax.broadcasted_iota(jnp.int32, (N, N), 0)
    same = lax.rem(row_i, 4) == part
    below = jnp.where(same & (row_i // 4 <= slot), 1.0, 0.0)
    every = jnp.where(same, 1.0, 0.0)

    def mix(x, m):
        return jnp.dot(x, m, precision=lax.Precision.HIGHEST, preferred_element_type=F32)

    def strip_force(x):
        def at(f, off):
            return x[f, 8 + off:8 + off + N, :]

        kc, kn = at(4, 0), at(4, 1)
        dc, dn = at(5, 0), at(5, 1)
        nu_f, nv_f = jnp.minimum(kc, roll(kc, -1)), jnp.minimum(kc, kn)
        h_c = at(3, 0) - 0.5 * at(2, 0)
        h_n = at(3, 1) - 0.5 * at(2, 1)
        q_c = (2.0 * mix(h_c, below) - h_c) * thick(kc, dc)
        q_n = (2.0 * mix(h_n, below) - h_n) * thick(kn, dn)
        g_u, g_v, r_u, r_v = force(nu_f > lev, nv_f > lev, q_c, roll(q_c, -1), q_n,
                                   at(0, 0), at(0, 1), at(0, -1), at(1, 0), at(1, 1), at(1, -1))[:4]
        hu = jnp.where(nu_f > 0.0, -0.25 * (dc + roll(dc, -1)), 0.0) / jnp.maximum(nu_f, 1.0)
        hv = jnp.where(nv_f > 0.0, -0.25 * (dc + dn), 0.0) / jnp.maximum(nv_f, 1.0)
        return hu, hv, g_u, g_v, r_u, r_v

    def strip_tracer(x):
        def at(f, off):
            return x[f, 8 + off:8 + off + N, :]

        kc, kn, ks = at(4, 0), at(4, 1), at(4, -1)
        u_m = jnp.where(jnp.minimum(kc, roll(kc, -1)) > lev, at(0, 0), 0.0)
        u_w = jnp.where(jnp.minimum(kc, roll(kc, 1)) > lev, roll(at(0, 0), 1), 0.0)
        v_m = jnp.where(jnp.minimum(kc, kn) > lev, at(1, 0), 0.0)
        v_s = jnp.where(jnp.minimum(kc, ks) > lev, at(1, -1), 0.0)
        return advect(u_m, u_w, v_m, v_s, ((at(2, 0), at(2, 1), at(2, -1)), (at(3, 0), at(3, 1), at(3, -1))))

    def merge(fn):
        return [jnp.where(part == 1, a, b) for a, b in zip(fn(xe), fn(xw))]

    hu, hv, g_u, g_v, r_u, r_v = merge(strip_force)
    rim = (lane == 0) | (lane == N - 1)
    forces = []
    for f, (hf, g) in enumerate(((hu, g_u), (hv, g_v))):
        x = jnp.where(rim, roll(hf * mix(g, every), 2), fm[f, W:W + N, :])
        fm[f, W:W + N, :] = x
        forces.append(x)
    half = lax.broadcasted_iota(jnp.int32, (h, N), 1) < n2
    for ref, x in zip((fk_e, fk_w), pack(forces)):
        for b in range(N // W):
            ref[h * b:h * b + h, :] = jnp.where(half, x[W * b:W * b + h], roll(x[W * b + h:W * b + W], n2))
    start(forc)
    ed[0] = r_u
    ed[1] = r_v
    t1, s1 = merge(strip_tracer)
    ed[2] = t1
    ed[3] = s1

    lane_q = lax.broadcasted_iota(jnp.int32, (QR, N), 1)
    edge_q = (lane_q == 0) | (lane_q == N - 1)

    def solve_step(g, _):
        own = pl.multiple_of(g * QR, QR)
        base = own + 8
        here = pl.ds(own, QR)
        kc = kd[0, pl.ds(base, QR), :]
        kn = kd[0, pl.ds(base + 1, QR), :]
        nu_f = jnp.minimum(kc, jnp.where(lane_q == N - 1, roll(got_e[pl.ds(base, QR), :], 3), roll(kc, -1)))
        nv_f = jnp.minimum(kc, kn)
        two_ref[0, here, :] = nu_f
        two_ref[1, here, :] = nv_f
        zero = jnp.zeros((QR, N), F32)
        refs = (nu_ref, nv_ref, nt_ref, ns_ref)
        cos = (VISC, VISC, DIFF, DIFF)
        d = [zero] * 4

        def factor(n_f, k, co, nu):
            return jnp.where(n_f > k + 1.0, nu * co[0][k], jnp.where(n_f > float(k), nu * co[1][k], 0.0))

        for k in range(LEVELS):
            f_t = factor(kc, k, DIFF, DIFF_NUM)
            facs = (factor(nu_f, k, VISC, VISC_NUM), factor(nv_f, k, VISC, VISC_NUM), f_t, f_t)
            for q in range(4):
                x = jnp.where(edge_q, roll(ed[q, here, :], 126 - 4 * k), refs[q][k, here, :])
                d[q] = (x + d[q]) * facs[q]
                if k == LEVELS - 1:
                    refs[q][k, here, :] = 0.25 * d[q]
                else:
                    refs[q][k, here, :] = d[q]
        sum_u, sum_v = d[0], d[1]
        for k in range(LEVELS - 2, -1, -1):
            for q in range(4):
                d[q] = refs[q][k, here, :] + cos[q][2][k] * d[q]
                refs[q][k, here, :] = 0.25 * d[q]
            sum_u, sum_v = sum_u + d[0], sum_v + d[1]
        two_ref[2, here, :] = sum_u / (VISC_NUM * jnp.maximum(nu_f, 1.0))
        two_ref[3, here, :] = sum_v / (VISC_NUM * jnp.maximum(nv_f, 1.0))
        return 0

    lax.fori_loop(0, N // QR, solve_step, 0)

    wait_recv(wide_main)
    wait_recv(wide_pass)
    lane_x = lax.broadcasted_iota(jnp.int32, (EXT, N), 1)
    row_x = lax.broadcasted_iota(jnp.int32, (EXT, N), 0)
    real = (row_x >= jnp.where(has_s, 0, W)) & (row_x < jnp.where(has_n, EXT, W + N))
    in_e, in_w = lane_x < W, lane_x >= N - W

    def side(f):
        return jnp.where(in_e, roll(we[...], -W * f), roll(ww[...], -W * (f + 1)))

    dms = (jnp.where(real, wm[3], 0.0), jnp.where(real & (in_e | in_w), side(3), 0.0))
    zero8 = jnp.zeros((8, N), F32)
    for ref in (et, fu, fv):
        for t in range(2):
            ref[t, 0:8, :] = zero8
            ref[t, 8 + EXT:TOP, :] = zero8
    for t in range(2):
        et[t, 8:8 + EXT, :] = dms[t]
    ra, rb = roll(dms[0], -1), roll(dms[1], -1)
    dme = (jnp.where(lane_x == N - 1, rb, ra), jnp.where(lane_x == N - 1, ra, rb))
    for t in range(2):
        d_c = dms[t]
        d_n = et[t, 9:9 + EXT, :]
        wet_u = (d_c > 0.0) & (dme[t] > 0.0)
        wet_v = (d_c > 0.0) & (d_n > 0.0)
        pick = (lambda f: wm[f]) if t == 0 else side
        et[t, 8:8 + EXT, :] = jnp.where(d_c > 0.0, pick(0), 0.0)
        fu[t, 8:8 + EXT, :] = jnp.where(wet_u, 0.5 * pick(1), 0.0)
        fv[t, 8:8 + EXT, :] = jnp.where(wet_v, 0.5 * pick(2), 0.0)
        cu[t] = jnp.where(wet_u, 0.125 * (d_c + dme[t]), 0.0)
        cv[t] = jnp.where(wet_v, 0.125 * (d_c + d_n), 0.0)
    wait_send(rows)
    wait_send(cols)
    wait_send(wide_side)
    wait_send(wide_main)
    wait_send(wide_pass)
    wait_recv(forc)
    fm_out[...] = fm[...]
    for out, got in ((fe_out, fe), (fw_out, fw)):
        for b in range(EXT // W):
            x = got[h * b:h * b + h, :]
            out[W * b:W * b + h, :] = x
            out[W * b + h:W * b + W, :] = roll(x, n2)
    wait_send(forc)


def step_kernel(nu_ref, nv_ref, nt_ref, ns_ref, two_ref, et0, fu0, fv0, cu, cv, fm, fe, fw,
                eta_out, tu_out, tv_out, u_hbm, v_hbm, t_hbm, s_hbm,
                et1, fu1, fv1, pu, pv, mean, ub, vb, flat, osem):
    copies = [pltpu.make_async_copy(nt_ref, t_hbm, osem.at[0]), pltpu.make_async_copy(ns_ref, s_hbm, osem.at[1])]
    for cp in copies:
        cp.start()

    lane = lax.broadcasted_iota(jnp.int32, (EXT, N), 1)

    def side(f):
        e, w = fe[...], fw[...]
        e = pltpu.roll(e, N - W * f, 1) if f else e
        w = pltpu.roll(w, N - W * (f + 1), 1)
        return jnp.where(lane < W, e, w)

    for f, (p, co) in enumerate(((pu, cu), (pv, cv))):
        for t in range(2):
            x = fm[f] if t == 0 else side(f)
            p[t] = jnp.where(co[t] > 0.0, (0.125 / SUBCYCLES) * x, 0.0)
    zero8 = jnp.zeros((8, N), F32)
    for ref in (et1, fv1):
        for t in range(2):
            ref[t, 0:8, :] = zero8
            ref[t, 8 + EXT:TOP, :] = zero8

    wgt = weights()
    lane8 = lax.broadcasted_iota(jnp.int32, (8, N), 1)
    first8, last8 = lane8 == 0, lane8 == N - 1

    def west8(x):
        a, b = pltpu.roll(x[0], 1, 1), pltpu.roll(x[1], 1, 1)
        return jnp.where(first8, b, a), jnp.where(first8, a, b)

    def east8(x):
        a, b = pltpu.roll(x[0], N - 1, 1), pltpu.roll(x[1], N - 1, 1)
        return jnp.where(last8, b, a), jnp.where(last8, a, b)

    for n in range(1, SUBCYCLES + 1):
        lo = 8 * (n // 8)
        groups = range(lo, EXT - lo, 8)
        et, fu, fv = (et1, fu1, fv1) if n > 1 else (et0, fu0, fv0)
        for g in groups:
            us = (fu[0, 8 + g:16 + g, :], fu[1, 8 + g:16 + g, :])
            uw = west8(us)
            for t in range(2):
                et1[t, 8 + g:16 + g, :] = et[t, 8 + g:16 + g, :] - (
                    (us[t] - uw[t]) + (fv[t, 8 + g:16 + g, :] - fv[t, 7 + g:15 + g, :]))
        for g in groups:
            es = (et1[0, 8 + g:16 + g, :], et1[1, 8 + g:16 + g, :])
            ee = east8(es)
            for t in range(2):
                u = fu[t, 8 + g:16 + g, :] - cu[t, g:g + 8, :] * (ee[t] - es[t]) + pu[t, g:g + 8, :]
                v = fv[t, 8 + g:16 + g, :] - cv[t, g:g + 8, :] * (et1[t, 9 + g:17 + g, :] - es[t]) + pv[t, g:g + 8, :]
                fu1[t, 8 + g:16 + g, :] = u
                fv1[t, 8 + g:16 + g, :] = v
                if t == 0 and W <= g < W + N:
                    at = slice(g - W, g - W + 8)
                    w = float(wgt[n - 1])
                    mean[0, at, :] = w * u if n == 1 else mean[0, at, :] + w * u
                    mean[1, at, :] = w * v if n == 1 else mean[1, at, :] + w * v

    mid = slice(8 + W, 8 + W + N)
    flat[0] = et1[0, mid, :]
    flat[1] = 2.0 * fu1[0, mid, :]
    flat[2] = 2.0 * fv1[0, mid, :]
    for i, out in enumerate((eta_out, tu_out, tv_out)):
        cp = pltpu.make_async_copy(flat.at[i], out, osem.at[2 + i])
        cp.start()
        copies.append(cp)
    for i, co in ((0, cu), (1, cv)):
        h = co[0, W:W + N, :]
        mean[i] = mean[i] / jnp.where(h > 0.0, 2.0 * h, 1.0) - two_ref[2 + i]

    for ci, (k0, k1) in enumerate(OUT_CHUNKS):
        for i, (src, buf, dst) in enumerate(((nu_ref, ub, u_hbm), (nv_ref, vb, v_hbm))):
            for g in range(0, N, 8):
                at = slice(g, g + 8)
                n_f, m = two_ref[i, at, :], mean[i, at, :]
                for k in range(k0, k1):
                    buf[k, at, :] = src[k, at, :] + jnp.where(n_f > float(k), m, 0.0)
            cp = pltpu.make_async_copy(buf.at[pl.ds(k0, k1 - k0)], dst.at[pl.ds(k0, k1 - k0)], osem.at[5 + 2 * ci + i])
            cp.start()
            copies.append(cp)
    for cp in copies:
        cp.wait()


def solution(mesh):
    ncol, nrow = mesh.shape['col'], mesh.shape['row']
    vmem = pl.BlockSpec(memory_space=pltpu.VMEM)
    hbm = pl.BlockSpec(memory_space=pl.ANY)
    s3 = jax.ShapeDtypeStruct((LEVELS, N, N), F32)
    s2 = jax.ShapeDtypeStruct((N, N), F32)

    def sds(*shape):
        return jax.ShapeDtypeStruct(shape, F32)

    def ocean_step(vel_u, vel_v, temp, salt, eta, tu, tv, dep, kmt):
        def kernel_a(*refs):
            exchange_kernel(ncol, nrow, *refs)

        def kernel_b(*refs):
            step_kernel(*refs)

        mid = pl.pallas_call(
            kernel_a,
            name='exchange',
            out_shape=(s3, s3, s3, s3, sds(4, N, N), sds(2, TOP, N), sds(2, TOP, N), sds(2, TOP, N), sds(2, EXT, N),
                       sds(2, EXT, N), sds(2, EXT, N), sds(EXT, N), sds(EXT, N)),
            in_specs=[hbm] * 9,
            out_specs=(vmem,) * 13,
            scratch_shapes=[
                pltpu.VMEM((4, LEVELS, N + 16, N), F32),
                pltpu.VMEM((N, N), jnp.int32),
                pltpu.VMEM((2, N + 16, N), F32),
                pltpu.VMEM((4, N, N), F32),
                pltpu.VMEM((4, N + 16, N), F32),
                pltpu.VMEM((N, N), F32), pltpu.VMEM((N, N), F32),
                pltpu.VMEM((N + 16, N), F32), pltpu.VMEM((N + 16, N), F32),
                pltpu.VMEM((6, N + 16, N), F32), pltpu.VMEM((6, N + 16, N), F32),
                pltpu.VMEM((4, N, N), F32),
                pltpu.VMEM((4, EXT, N), F32),
                pltpu.VMEM((N, N), F32), pltpu.VMEM((N, N), F32),
                pltpu.VMEM((EXT, N), F32), pltpu.VMEM((EXT, N), F32),
                pltpu.VMEM((2, EXT, N), F32),
                pltpu.VMEM((N // 2, N), F32), pltpu.VMEM((N // 2, N), F32),
                pltpu.VMEM((EXT // 2, N), F32), pltpu.VMEM((EXT // 2, N), F32),
                pltpu.SemaphoreType.DMA((4, len(CHUNKS))),
                pltpu.SemaphoreType.DMA((5,)),
                pltpu.SemaphoreType.DMA((24,)),
                pltpu.SemaphoreType.DMA((24,)),
            ],
            compiler_params=pltpu.CompilerParams(collective_id=0, has_side_effects=True, vmem_limit_bytes=28 * 2 ** 20),
        )(*[pltpu.with_memory_space_constraint(x, pltpu.HBM) for x in (vel_u, vel_v, temp, salt, eta, tu, tv, dep, kmt)])
        st = pltpu.VMEM((2, TOP, N), F32)
        co = pltpu.VMEM((2, EXT, N), F32)
        out = pl.pallas_call(
            kernel_b,
            name='subcycles',
            out_shape=(s2, s2, s2, s3, s3, s3, s3),
            in_specs=[vmem] * 13,
            out_specs=(hbm,) * 7,
            scratch_shapes=[st, st, st, co, co, pltpu.VMEM((2, N, N), F32),
                            pltpu.VMEM((LEVELS, N, N), F32), pltpu.VMEM((LEVELS, N, N), F32),
                            pltpu.VMEM((3, N, N), F32), pltpu.SemaphoreType.DMA((5 + 2 * len(OUT_CHUNKS),))],
            compiler_params=pltpu.CompilerParams(vmem_limit_bytes=28 * 2 ** 20),
        )(*mid)
        return out

    spec_3d = P(None, 'row', 'col')
    spec_2d = P('row', 'col')
    return jax.shard_map(ocean_step, mesh=mesh, in_specs=(spec_3d,) * 4 + (spec_2d,) * 5,
                         out_specs=(spec_2d,) * 3 + (spec_3d,) * 4, check_vma=False)
```

```python
import jax
import jax.numpy as jnp
import numpy as np
from jax import lax
from jax.experimental import pallas as pl
from jax.experimental.pallas import tpu as pltpu
from jax.sharding import PartitionSpec as P

MESH = pl.DeviceIdType.MESH
F32 = jnp.float32
SUBCYCLES = 30
LEVELS = 31
VISC_NUM = 4.0
DIFF_NUM = 1.0
N = 128
W = 32
EXT = N + 2 * W
TOP = EXT + 16
PR = 16
QR = 32
CHUNKS = ((0, 9), (9, 18), (18, 26), (26, 31))
OUT_CHUNKS = ((0, 3), (3, 9), (9, 17), (17, 25), (25, 31))


def solve_coefs(nu):
    inner, last, back = [], [], []
    c_prev = 0.0
    for k in range(LEVELS):
        lo = nu if k > 0 else 0.0
        piv = 1.0 + nu + lo - lo * c_prev
        inner.append(1.0 / piv)
        last.append(1.0 / (1.0 + lo - lo * c_prev))
        c_prev = nu / piv
        back.append(c_prev)
    return inner, last, back


VISC = solve_coefs(VISC_NUM)
DIFF = solve_coefs(DIFF_NUM)


def weights():
    s = np.arange(1, SUBCYCLES + 1, dtype=np.float64) / (SUBCYCLES + 1)
    w = s ** 2 * (1.0 - s ** 4)
    return (w / w.sum()).astype(np.float32)


def exchange_kernel(ncol, nrow, u_hbm, v_hbm, t_hbm, s_hbm, eta_hbm, tu_hbm, tv_hbm, dep_hbm, kmt_hbm,
                    nu_ref, nv_ref, nt_ref, ns_ref, two_ref, et, fu, fv, cu, cv, fm_out, fe_out, fw_out,
                    fb, ki, kd, qs, msg_e, msg_w, got_w, got_e, xe, xw, ed,
                    wm, pk_e, pk_w, we, ww, fm, fk_e, fk_w, fe, fw,
                    ld_sem, in_sem, snd, rcv):
    c = lax.axis_index('col')
    r = lax.axis_index('row')
    east = lax.rem(c + 1, ncol)
    west = lax.rem(c + ncol - 1, ncol)
    north = lax.rem(r + 1, nrow)
    south = lax.rem(r + nrow - 1, nrow)
    has_n = r < nrow - 1
    has_s = r > 0

    barrier = pltpu.get_barrier_semaphore()
    places = [(east, r), (west, r), (c, north), (c, south), (east, north), (east, south), (west, north), (west, south)]
    for cc, rr in places:
        pl.semaphore_signal(barrier, inc=1, device_id={'col': cc, 'row': rr}, device_id_type=MESH)

    src3 = (u_hbm, v_hbm, t_hbm, s_hbm)
    small = [pltpu.make_async_copy(kmt_hbm, ki, in_sem.at[0]),
             pltpu.make_async_copy(dep_hbm, kd.at[1, pl.ds(8, N), :], in_sem.at[1]),
             pltpu.make_async_copy(eta_hbm, wm.at[0, pl.ds(W, N), :], in_sem.at[2]),
             pltpu.make_async_copy(tu_hbm, wm.at[1, pl.ds(W, N), :], in_sem.at[3]),
             pltpu.make_async_copy(tv_hbm, wm.at[2, pl.ds(W, N), :], in_sem.at[4])]
    loads = []
    for ci, (k0, k1) in enumerate(CHUNKS):
        row = [pltpu.make_async_copy(src3[f].at[pl.ds(k0, k1 - k0)], fb.at[f, pl.ds(k0, k1 - k0), pl.ds(8, N), :],
                                     ld_sem.at[f, ci]) for f in range(4)]
        loads.append(row)
        for cp in row:
            cp.start()
        if ci == 0:
            for cp in small:
                cp.start()

    def copy(i, src, dst, cc, rr):
        return pltpu.make_async_remote_copy(src_ref=src, dst_ref=dst, send_sem=snd.at[i], recv_sem=rcv.at[i],
                                            device_id={'col': cc, 'row': rr}, device_id_type=MESH)

    rows = [
        (copy(0, fb.at[:, :, pl.ds(8, 1), :], fb.at[:, :, pl.ds(8 + N, 1), :], c, south), has_s, has_n),
        (copy(1, fb.at[:, :, pl.ds(7 + N, 1), :], fb.at[:, :, pl.ds(7, 1), :], c, north), has_n, has_s),
        (copy(2, kd.at[:, pl.ds(8, 1), :], kd.at[:, pl.ds(8 + N, 1), :], c, south), has_s, has_n),
        (copy(3, kd.at[:, pl.ds(7 + N, 1), :], kd.at[:, pl.ds(7, 1), :], c, north), has_n, has_s),
    ]
    cols = [
        (copy(4, msg_e, got_w.at[pl.ds(8, N), :], east, r), None, None),
        (copy(5, msg_w, got_e.at[pl.ds(8, N), :], west, r), None, None),
        (copy(6, msg_e.at[pl.ds(0, 8), :], got_w.at[pl.ds(8 + N, 8), :], east, south), has_s, has_n),
        (copy(7, msg_w.at[pl.ds(N - 8, 8), :], got_e.at[pl.ds(0, 8), :], west, north), has_n, has_s),
    ]

    def main_rows(base, main):
        return [
            (copy(base, main.at[:, pl.ds(W, W), :], main.at[:, pl.ds(W + N, W), :], c, south), has_s, has_n),
            (copy(base + 1, main.at[:, pl.ds(N, W), :], main.at[:, pl.ds(0, W), :], c, north), has_n, has_s),
        ]

    def side_cols(base, to_e, to_w, in_e, in_w, w, n):
        return [
            (copy(base, to_w, in_e.at[pl.ds(w, n), :], west, r), None, None),
            (copy(base + 1, to_e, in_w.at[pl.ds(w, n), :], east, r), None, None),
        ]

    wide_side = side_cols(8, pk_e, pk_w, we, ww, W, N)
    wide_main = main_rows(10, wm)
    wide_pass = []
    for i, buf in ((12, we), (14, ww)):
        wide_pass += [
            (copy(i, buf.at[pl.ds(W, W), :], buf.at[pl.ds(W + N, W), :], c, south), has_s, has_n),
            (copy(i + 1, buf.at[pl.ds(N, W), :], buf.at[pl.ds(0, W), :], c, north), has_n, has_s),
        ]
    h = W // 2
    n2 = N // 2
    lo, hi = pl.ds(0, h), pl.ds(n2 - h, h)
    forc = side_cols(16, fk_e, fk_w, fe, fw, h, n2) + main_rows(18, fm) + [
        (copy(20, fk_w.at[lo, :], fe.at[pl.ds(h + n2, h), :], west, south), has_s, has_n),
        (copy(21, fk_w.at[hi, :], fe.at[lo, :], west, north), has_n, has_s),
        (copy(22, fk_e.at[lo, :], fw.at[pl.ds(h + n2, h), :], east, south), has_s, has_n),
        (copy(23, fk_e.at[hi, :], fw.at[lo, :], east, north), has_n, has_s),
    ]

    def run(cond, fn):
        if cond is None:
            fn()
        else:
            pl.when(cond)(fn)

    def start(items):
        for cp, s_if, _ in items:
            run(s_if, cp.start)

    def wait_recv(items):
        for cp, _, r_if in items:
            run(r_if, cp.wait_recv)

    def wait_send(items):
        for cp, s_if, _ in items:
            run(s_if, cp.wait_send)

    lane = lax.broadcasted_iota(jnp.int32, (N, N), 1)
    part = lax.rem(lane, 4)
    slot = lane // 4

    def roll(x, s):
        s %= N
        return pltpu.roll(x, s, 1) if s else x

    for cp in small:
        cp.wait()
    kmt_f = ki[...].astype(F32)
    dep = kd[1, 8:8 + N, :]
    kd[0, 8:8 + N, :] = kmt_f
    wm[3, W:W + N, :] = jnp.where(kmt_f > 0.0, dep, 0.0)

    def pack(fields):
        e_acc = jnp.zeros((N, N), F32)
        w_acc = jnp.zeros((N, N), F32)
        for f, x in enumerate(fields):
            here = lane // W == f
            w_acc = jnp.where(here, roll(x, W * f), w_acc)
            e_acc = jnp.where(here, roll(x, W * (f + 1)), e_acc)
        return e_acc, w_acc

    e_acc, w_acc = pack([wm[f, W:W + N, :] for f in range(4)])
    pk_e[...] = e_acc
    pk_w[...] = w_acc

    acc = [jnp.zeros((N, N), F32)] * 4
    for ci, (k0, k1) in enumerate(CHUNKS):
        for cp in loads[ci]:
            cp.wait()
        if ci == 0:
            pl.semaphore_wait(barrier, len(places))
            start(wide_side)
            start(wide_main)
        if ci == len(CHUNKS) - 1:
            start(rows)
        for f in range(4):
            x = acc[f]
            for k in range(k0, k1):
                x = jnp.where(slot == k, roll(fb[f, k, 8:8 + N, :], 4 * k + 2), x)
            acc[f] = x
    out_e = jnp.where(lane == 124, roll(kmt_f, -3), roll(dep, -2))
    out_w = jnp.where(lane == 124, roll(kmt_f, 124), roll(dep, 125))
    for f in range(4):
        qs[f, 8:8 + N, :] = acc[f]
        pick = (part == f) & (slot < LEVELS)
        out_e = jnp.where(pick, roll(acc[f], f - 1), out_e)
        out_w = jnp.where(pick, roll(acc[f], f - 2), out_w)
    msg_e[...] = out_e
    msg_w[...] = out_w

    start(cols)

    @pl.when(jnp.logical_not(has_n))
    def _():
        fb[:, :, 8 + N:9 + N, :] = jnp.zeros((4, LEVELS, 1, N), F32)
        kd[:, 8 + N:9 + N, :] = jnp.zeros((2, 1, N), F32)
        got_w[8 + N:16 + N, :] = jnp.zeros((8, N), F32)

    @pl.when(jnp.logical_not(has_s))
    def _():
        fb[:, :, 7:8, :] = jnp.zeros((4, LEVELS, 1, N), F32)
        kd[:, 7:8, :] = jnp.zeros((2, 1, N), F32)
        got_e[0:8, :] = jnp.zeros((8, N), F32)

    def thick(k, d):
        return 0.6 * d / jnp.maximum(k, 1.0)

    def force(wet_u, wet_v, q_c, q_e, q_n, u_c, u_n, u_s, v_c, v_n, v_s):
        us, vs = u_c + u_n, v_c + v_s
        v_at_u = 0.25 * (vs + roll(vs, -1))
        u_at_v = 0.25 * (us + roll(us, 1))
        u_w = roll(u_c, 1)
        g_u = jnp.where(wet_u, u_c * (roll(u_c, -1) - u_w) + v_at_u * (u_n - u_s) + (q_e - q_c), 0.0)
        g_v = jnp.where(wet_v, u_at_v * (roll(v_c, -1) - roll(v_c, 1)) + v_c * (v_n - v_s) + (q_n - q_c), 0.0)
        u_m, v_m = jnp.where(wet_u, u_c, 0.0), jnp.where(wet_v, v_c, 0.0)
        return g_u, g_v, u_m - 0.125 * g_u, v_m - 0.125 * g_v, u_m, v_m, u_w

    def advect(u_e, u_w, v_n, v_s, tracers):
        a_e, a_w = jnp.minimum(u_e, 0.0), jnp.maximum(u_w, 0.0)
        a_n, a_s = jnp.minimum(v_n, 0.0), jnp.maximum(v_s, 0.0)
        a_c = (jnp.maximum(u_e, 0.0) - jnp.minimum(u_w, 0.0)) + (jnp.maximum(v_n, 0.0) - jnp.minimum(v_s, 0.0))
        b_c = 4.0 - a_c
        return [b_c * x + ((a_w * roll(x, 1) - a_e * roll(x, -1)) + (a_s * x_s - a_n * x_n)) for x, x_n, x_s in tracers]

    def main_step(i, _):
        @pl.when(i == N // PR - 2)
        def _():
            wait_recv(rows)
            wait_recv(wide_side)
            start(wide_pass)

        own = pl.multiple_of(lax.rem(i + 1, N // PR) * PR, PR)
        base = own + 8

        def at(f, k, off):
            return fb[f, k, pl.ds(base + off, PR), :]

        kc = kd[0, pl.ds(base, PR), :]
        kn = kd[0, pl.ds(base + 1, PR), :]
        ks = kd[0, pl.ds(base - 1, PR), :]
        dc = kd[1, pl.ds(base, PR), :]
        dn = kd[1, pl.ds(base + 1, PR), :]
        th_c, th_n = thick(kc, dc), thick(kn, dn)
        nu_f = jnp.minimum(kc, roll(kc, -1))
        nw_f = jnp.minimum(kc, roll(kc, 1))
        nv_f = jnp.minimum(kc, kn)
        nq_f = jnp.minimum(kc, ks)
        zero = jnp.zeros((PR, N), F32)
        cum_c, cum_n, sum_u, sum_v = zero, zero, zero, zero
        for k in range(LEVELS):
            fk = float(k)
            t_c, s_c = at(2, k, 0), at(3, k, 0)
            t_n, s_n = at(2, k, 1), at(3, k, 1)
            h_c = s_c - 0.5 * t_c
            h_n = s_n - 0.5 * t_n
            mid_c, mid_n = cum_c + h_c, cum_n + h_n
            cum_c, cum_n = mid_c + h_c, mid_n + h_n
            q_c = mid_c * th_c
            u_c, v_c, v_s = at(0, k, 0), at(1, k, 0), at(1, k, -1)
            g_u, g_v, r_u, r_v, u_m, v_m, u_w = force(
                nu_f > fk, nv_f > fk, q_c, roll(q_c, -1), mid_n * th_n,
                u_c, at(0, k, 1), at(0, k, -1), v_c, at(1, k, 1), v_s)
            sum_u, sum_v = sum_u + g_u, sum_v + g_v
            nu_ref[k, pl.ds(own, PR), :] = r_u
            nv_ref[k, pl.ds(own, PR), :] = r_v
            t1, s1 = advect(u_m, jnp.where(nw_f > fk, u_w, 0.0), v_m, jnp.where(nq_f > fk, v_s, 0.0),
                            ((t_c, t_n, at(2, k, -1)), (s_c, s_n, at(3, k, -1))))
            nt_ref[k, pl.ds(own, PR), :] = t1
            ns_ref[k, pl.ds(own, PR), :] = s1
        hu = jnp.where(nu_f > 0.0, 0.5 * (dc + roll(dc, -1)), 0.0)
        hv = jnp.where(nv_f > 0.0, 0.5 * (dc + dn), 0.0)
        fm[0, pl.ds(own + W, PR), :] = hu / jnp.maximum(nu_f, 1.0) * (-0.5 * sum_u)
        fm[1, pl.ds(own + W, PR), :] = hv / jnp.maximum(nv_f, 1.0) * (-0.5 * sum_v)
        return 0

    lax.fori_loop(0, N // PR, main_step, 0)

    lane8 = lax.broadcasted_iota(jnp.int32, (8, N), 1)
    for f in range(4):
        for lo in (0, 8 + N):
            x = jnp.zeros((8, N), F32)
            for k in range(LEVELS):
                x = jnp.where(lane8 // 4 == k, roll(fb[f, k, lo:lo + 8, :], 4 * k + 2), x)
            qs[f, lo:lo + 8, :] = x

    wait_recv(cols)

    part_x = lax.rem(lax.broadcasted_iota(jnp.int32, (N + 16, N), 1), 4)
    for f in range(4):
        q = qs[f]
        xe[f] = jnp.where(part_x == 2, roll(got_e[...], 2 - f), q)
        xw[f] = jnp.where(part_x == 1, roll(got_w[...], 1 - f), q)
    for f in range(2):
        q = kd[f]
        b = [jnp.broadcast_to(q[:, j:j + 1], q.shape) for j in (N - 2, N - 1, 0, 1)]
        h_e = jnp.broadcast_to(got_e[:, 124 + f:125 + f], q.shape)
        h_w = jnp.broadcast_to(got_w[:, 124 + f:125 + f], q.shape)
        xe[4 + f] = jnp.where(part_x == 0, b[0], jnp.where(part_x == 1, b[1], h_e))
        xw[4 + f] = jnp.where(part_x == 1, h_w, jnp.where(part_x == 2, b[2], b[3]))

    lev = slot.astype(F32)

    row_i = lax.broadcasted_iota(jnp.int32, (N, N), 0)
    same = lax.rem(row_i, 4) == part
    below = jnp.where(same & (row_i // 4 <= slot), 1.0, 0.0)
    every = jnp.where(same, 1.0, 0.0)

    def mix(x, m):
        return jnp.dot(x, m, precision=lax.Precision.HIGHEST, preferred_element_type=F32)

    def strip_force(x):
        def at(f, off):
            return x[f, 8 + off:8 + off + N, :]

        kc, kn = at(4, 0), at(4, 1)
        dc, dn = at(5, 0), at(5, 1)
        nu_f, nv_f = jnp.minimum(kc, roll(kc, -1)), jnp.minimum(kc, kn)
        h_c = at(3, 0) - 0.5 * at(2, 0)
        h_n = at(3, 1) - 0.5 * at(2, 1)
        q_c = (2.0 * mix(h_c, below) - h_c) * thick(kc, dc)
        q_n = (2.0 * mix(h_n, below) - h_n) * thick(kn, dn)
        g_u, g_v, r_u, r_v = force(nu_f > lev, nv_f > lev, q_c, roll(q_c, -1), q_n,
                                   at(0, 0), at(0, 1), at(0, -1), at(1, 0), at(1, 1), at(1, -1))[:4]
        hu = jnp.where(nu_f > 0.0, -0.25 * (dc + roll(dc, -1)), 0.0) / jnp.maximum(nu_f, 1.0)
        hv = jnp.where(nv_f > 0.0, -0.25 * (dc + dn), 0.0) / jnp.maximum(nv_f, 1.0)
        return hu, hv, g_u, g_v, r_u, r_v

    def strip_tracer(x):
        def at(f, off):
            return x[f, 8 + off:8 + off + N, :]

        kc, kn, ks = at(4, 0), at(4, 1), at(4, -1)
        u_m = jnp.where(jnp.minimum(kc, roll(kc, -1)) > lev, at(0, 0), 0.0)
        u_w = jnp.where(jnp.minimum(kc, roll(kc, 1)) > lev, roll(at(0, 0), 1), 0.0)
        v_m = jnp.where(jnp.minimum(kc, kn) > lev, at(1, 0), 0.0)
        v_s = jnp.where(jnp.minimum(kc, ks) > lev, at(1, -1), 0.0)
        return advect(u_m, u_w, v_m, v_s, ((at(2, 0), at(2, 1), at(2, -1)), (at(3, 0), at(3, 1), at(3, -1))))

    def merge(fn):
        return [jnp.where(part == 1, a, b) for a, b in zip(fn(xe), fn(xw))]

    hu, hv, g_u, g_v, r_u, r_v = merge(strip_force)
    rim = (lane == 0) | (lane == N - 1)
    forces = []
    for f, (hf, g) in enumerate(((hu, g_u), (hv, g_v))):
        x = jnp.where(rim, roll(hf * mix(g, every), 2), fm[f, W:W + N, :])
        fm[f, W:W + N, :] = x
        forces.append(x)
    half = lax.broadcasted_iota(jnp.int32, (h, N), 1) < n2
    for ref, x in zip((fk_e, fk_w), pack(forces)):
        for b in range(N // W):
            ref[h * b:h * b + h, :] = jnp.where(half, x[W * b:W * b + h], roll(x[W * b + h:W * b + W], n2))
    start(forc)
    ed[0] = r_u
    ed[1] = r_v
    t1, s1 = merge(strip_tracer)
    ed[2] = t1
    ed[3] = s1

    lane_q = lax.broadcasted_iota(jnp.int32, (QR, N), 1)
    edge_q = (lane_q == 0) | (lane_q == N - 1)

    def solve_step(g, _):
        own = pl.multiple_of(g * QR, QR)
        base = own + 8
        here = pl.ds(own, QR)
        kc = kd[0, pl.ds(base, QR), :]
        kn = kd[0, pl.ds(base + 1, QR), :]
        nu_f = jnp.minimum(kc, jnp.where(lane_q == N - 1, roll(got_e[pl.ds(base, QR), :], 3), roll(kc, -1)))
        nv_f = jnp.minimum(kc, kn)
        two_ref[0, here, :] = nu_f
        two_ref[1, here, :] = nv_f
        zero = jnp.zeros((QR, N), F32)
        refs = (nu_ref, nv_ref, nt_ref, ns_ref)
        cos = (VISC, VISC, DIFF, DIFF)
        d = [zero] * 4

        def factor(n_f, k, co, nu):
            return jnp.where(n_f > k + 1.0, nu * co[0][k], jnp.where(n_f > float(k), nu * co[1][k], 0.0))

        for k in range(LEVELS):
            f_t = factor(kc, k, DIFF, DIFF_NUM)
            facs = (factor(nu_f, k, VISC, VISC_NUM), factor(nv_f, k, VISC, VISC_NUM), f_t, f_t)
            for q in range(4):
                x = jnp.where(edge_q, roll(ed[q, here, :], 126 - 4 * k), refs[q][k, here, :])
                d[q] = (x + d[q]) * facs[q]
                if k == LEVELS - 1:
                    refs[q][k, here, :] = 0.25 * d[q]
                else:
                    refs[q][k, here, :] = d[q]
        sum_u, sum_v = d[0], d[1]
        for k in range(LEVELS - 2, -1, -1):
            for q in range(4):
                d[q] = refs[q][k, here, :] + cos[q][2][k] * d[q]
                refs[q][k, here, :] = 0.25 * d[q]
            sum_u, sum_v = sum_u + d[0], sum_v + d[1]
        two_ref[2, here, :] = sum_u / (VISC_NUM * jnp.maximum(nu_f, 1.0))
        two_ref[3, here, :] = sum_v / (VISC_NUM * jnp.maximum(nv_f, 1.0))
        return 0

    lax.fori_loop(0, N // QR, solve_step, 0)

    wait_recv(wide_main)
    wait_recv(wide_pass)
    lane_x = lax.broadcasted_iota(jnp.int32, (EXT, N), 1)
    row_x = lax.broadcasted_iota(jnp.int32, (EXT, N), 0)
    real = (row_x >= jnp.where(has_s, 0, W)) & (row_x < jnp.where(has_n, EXT, W + N))
    in_e, in_w = lane_x < W, lane_x >= N - W

    def side(f):
        return jnp.where(in_e, roll(we[...], -W * f), roll(ww[...], -W * (f + 1)))

    dms = (jnp.where(real, wm[3], 0.0), jnp.where(real & (in_e | in_w), side(3), 0.0))
    zero8 = jnp.zeros((8, N), F32)
    for ref in (et, fu, fv):
        for t in range(2):
            ref[t, 0:8, :] = zero8
            ref[t, 8 + EXT:TOP, :] = zero8
    for t in range(2):
        et[t, 8:8 + EXT, :] = dms[t]
    ra, rb = roll(dms[0], -1), roll(dms[1], -1)
    dme = (jnp.where(lane_x == N - 1, rb, ra), jnp.where(lane_x == N - 1, ra, rb))
    for t in range(2):
        d_c = dms[t]
        d_n = et[t, 9:9 + EXT, :]
        wet_u = (d_c > 0.0) & (dme[t] > 0.0)
        wet_v = (d_c > 0.0) & (d_n > 0.0)
        pick = (lambda f: wm[f]) if t == 0 else side
        et[t, 8:8 + EXT, :] = jnp.where(d_c > 0.0, pick(0), 0.0)
        fu[t, 8:8 + EXT, :] = jnp.where(wet_u, 0.5 * pick(1), 0.0)
        fv[t, 8:8 + EXT, :] = jnp.where(wet_v, 0.5 * pick(2), 0.0)
        cu[t] = jnp.where(wet_u, 0.125 * (d_c + dme[t]), 0.0)
        cv[t] = jnp.where(wet_v, 0.125 * (d_c + d_n), 0.0)
    wait_send(rows)
    wait_send(cols)
    wait_send(wide_side)
    wait_send(wide_main)
    wait_send(wide_pass)
    wait_recv(forc)
    fm_out[...] = fm[...]
    for out, got in ((fe_out, fe), (fw_out, fw)):
        for b in range(EXT // W):
            x = got[h * b:h * b + h, :]
            out[W * b:W * b + h, :] = x
            out[W * b + h:W * b + W, :] = roll(x, n2)
    wait_send(forc)


def step_kernel(nu_ref, nv_ref, nt_ref, ns_ref, two_ref, et0, fu0, fv0, cu, cv, fm, fe, fw,
                eta_out, tu_out, tv_out, u_hbm, v_hbm, t_hbm, s_hbm,
                et1, fu1, fv1, pu, pv, mean, ub, vb, flat, osem):
    copies = [pltpu.make_async_copy(nt_ref, t_hbm, osem.at[0]), pltpu.make_async_copy(ns_ref, s_hbm, osem.at[1])]
    for cp in copies:
        cp.start()

    lane = lax.broadcasted_iota(jnp.int32, (EXT, N), 1)

    def side(f):
        e, w = fe[...], fw[...]
        e = pltpu.roll(e, N - W * f, 1) if f else e
        w = pltpu.roll(w, N - W * (f + 1), 1)
        return jnp.where(lane < W, e, w)

    for f, (p, co) in enumerate(((pu, cu), (pv, cv))):
        for t in range(2):
            x = fm[f] if t == 0 else side(f)
            p[t] = jnp.where(co[t] > 0.0, (0.125 / SUBCYCLES) * x, 0.0)
    zero8 = jnp.zeros((8, N), F32)
    for ref in (et1, fv1):
        for t in range(2):
            ref[t, 0:8, :] = zero8
            ref[t, 8 + EXT:TOP, :] = zero8

    wgt = weights()
    lane8 = lax.broadcasted_iota(jnp.int32, (8, N), 1)
    first8, last8 = lane8 == 0, lane8 == N - 1

    def west8(x):
        a, b = pltpu.roll(x[0], 1, 1), pltpu.roll(x[1], 1, 1)
        return jnp.where(first8, b, a), jnp.where(first8, a, b)

    def east8(x):
        a, b = pltpu.roll(x[0], N - 1, 1), pltpu.roll(x[1], N - 1, 1)
        return jnp.where(last8, b, a), jnp.where(last8, a, b)

    for n in range(1, SUBCYCLES + 1):
        lo = 8 * (n // 8)
        groups = range(lo, EXT - lo, 8)
        et, fu, fv = (et1, fu1, fv1) if n > 1 else (et0, fu0, fv0)
        for g in groups:
            us = (fu[0, 8 + g:16 + g, :], fu[1, 8 + g:16 + g, :])
            uw = west8(us)
            for t in range(2):
                et1[t, 8 + g:16 + g, :] = et[t, 8 + g:16 + g, :] - (
                    (us[t] - uw[t]) + (fv[t, 8 + g:16 + g, :] - fv[t, 7 + g:15 + g, :]))
        for g in groups:
            es = (et1[0, 8 + g:16 + g, :], et1[1, 8 + g:16 + g, :])
            ee = east8(es)
            for t in range(2):
                u = fu[t, 8 + g:16 + g, :] - cu[t, g:g + 8, :] * (ee[t] - es[t]) + pu[t, g:g + 8, :]
                v = fv[t, 8 + g:16 + g, :] - cv[t, g:g + 8, :] * (et1[t, 9 + g:17 + g, :] - es[t]) + pv[t, g:g + 8, :]
                fu1[t, 8 + g:16 + g, :] = u
                fv1[t, 8 + g:16 + g, :] = v
                if t == 0 and W <= g < W + N:
                    at = slice(g - W, g - W + 8)
                    w = float(wgt[n - 1])
                    mean[0, at, :] = w * u if n == 1 else mean[0, at, :] + w * u
                    mean[1, at, :] = w * v if n == 1 else mean[1, at, :] + w * v

    mid = slice(8 + W, 8 + W + N)
    flat[0] = et1[0, mid, :]
    flat[1] = 2.0 * fu1[0, mid, :]
    flat[2] = 2.0 * fv1[0, mid, :]
    for i, out in enumerate((eta_out, tu_out, tv_out)):
        cp = pltpu.make_async_copy(flat.at[i], out, osem.at[2 + i])
        cp.start()
        copies.append(cp)
    for i, co in ((0, cu), (1, cv)):
        h = co[0, W:W + N, :]
        mean[i] = mean[i] / jnp.where(h > 0.0, 2.0 * h, 1.0) - two_ref[2 + i]

    for ci, (k0, k1) in enumerate(OUT_CHUNKS):
        for i, (src, buf, dst) in enumerate(((nu_ref, ub, u_hbm), (nv_ref, vb, v_hbm))):
            for g in range(0, N, 8):
                at = slice(g, g + 8)
                n_f, m = two_ref[i, at, :], mean[i, at, :]
                for k in range(k0, k1):
                    buf[k, at, :] = src[k, at, :] + jnp.where(n_f > float(k), m, 0.0)
            cp = pltpu.make_async_copy(buf.at[pl.ds(k0, k1 - k0)], dst.at[pl.ds(k0, k1 - k0)], osem.at[5 + 2 * ci + i])
            cp.start()
            copies.append(cp)
    for cp in copies:
        cp.wait()


def solution(mesh):
    ncol, nrow = mesh.shape['col'], mesh.shape['row']
    vmem = pl.BlockSpec(memory_space=pltpu.VMEM)
    hbm = pl.BlockSpec(memory_space=pl.ANY)
    s3 = jax.ShapeDtypeStruct((LEVELS, N, N), F32)
    s2 = jax.ShapeDtypeStruct((N, N), F32)

    def sds(*shape):
        return jax.ShapeDtypeStruct(shape, F32)

    def ocean_step(vel_u, vel_v, temp, salt, eta, tu, tv, dep, kmt):
        def kernel_a(*refs):
            exchange_kernel(ncol, nrow, *refs)

        def kernel_b(*refs):
            step_kernel(*refs)

        mid = pl.pallas_call(
            kernel_a,
            name='exchange',
            out_shape=(s3, s3, s3, s3, sds(4, N, N), sds(2, TOP, N), sds(2, TOP, N), sds(2, TOP, N), sds(2, EXT, N),
                       sds(2, EXT, N), sds(2, EXT, N), sds(EXT, N), sds(EXT, N)),
            in_specs=[hbm] * 9,
            out_specs=(vmem,) * 13,
            scratch_shapes=[
                pltpu.VMEM((4, LEVELS, N + 16, N), F32),
                pltpu.VMEM((N, N), jnp.int32),
                pltpu.VMEM((2, N + 16, N), F32),
                pltpu.VMEM((4, N + 16, N), F32),
                pltpu.VMEM((N, N), F32), pltpu.VMEM((N, N), F32),
                pltpu.VMEM((N + 16, N), F32), pltpu.VMEM((N + 16, N), F32),
                pltpu.VMEM((6, N + 16, N), F32), pltpu.VMEM((6, N + 16, N), F32),
                pltpu.VMEM((4, N, N), F32),
                pltpu.VMEM((4, EXT, N), F32),
                pltpu.VMEM((N, N), F32), pltpu.VMEM((N, N), F32),
                pltpu.VMEM((EXT, N), F32), pltpu.VMEM((EXT, N), F32),
                pltpu.VMEM((2, EXT, N), F32),
                pltpu.VMEM((N // 2, N), F32), pltpu.VMEM((N // 2, N), F32),
                pltpu.VMEM((EXT // 2, N), F32), pltpu.VMEM((EXT // 2, N), F32),
                pltpu.SemaphoreType.DMA((4, len(CHUNKS))),
                pltpu.SemaphoreType.DMA((5,)),
                pltpu.SemaphoreType.DMA((24,)),
                pltpu.SemaphoreType.DMA((24,)),
            ],
            compiler_params=pltpu.CompilerParams(collective_id=0, has_side_effects=True, vmem_limit_bytes=28 * 2 ** 20),
        )(*[pltpu.with_memory_space_constraint(x, pltpu.HBM) for x in (vel_u, vel_v, temp, salt, eta, tu, tv, dep, kmt)])
        st = pltpu.VMEM((2, TOP, N), F32)
        co = pltpu.VMEM((2, EXT, N), F32)
        out = pl.pallas_call(
            kernel_b,
            name='subcycles',
            out_shape=(s2, s2, s2, s3, s3, s3, s3),
            in_specs=[vmem] * 13,
            out_specs=(hbm,) * 7,
            scratch_shapes=[st, st, st, co, co, pltpu.VMEM((2, N, N), F32),
                            pltpu.VMEM((LEVELS, N, N), F32), pltpu.VMEM((LEVELS, N, N), F32),
                            pltpu.VMEM((3, N, N), F32), pltpu.SemaphoreType.DMA((5 + 2 * len(OUT_CHUNKS),))],
            compiler_params=pltpu.CompilerParams(vmem_limit_bytes=28 * 2 ** 20),
        )(*mid)
        return out

    spec_3d = P(None, 'row', 'col')
    spec_2d = P('row', 'col')
    return jax.shard_map(ocean_step, mesh=mesh, in_specs=(spec_3d,) * 4 + (spec_2d,) * 5,
                         out_specs=(spec_2d,) * 3 + (spec_3d,) * 4, check_vma=False)
```

```python
import jax
import jax.numpy as jnp
import numpy as np
from jax import lax
from jax.experimental import pallas as pl
from jax.experimental.pallas import tpu as pltpu
from jax.sharding import PartitionSpec as P

MESH = pl.DeviceIdType.MESH
F32 = jnp.float32
SUBCYCLES = 30
LEVELS = 31
VISC_NUM = 4.0
DIFF_NUM = 1.0
N = 128
W = 32
EXT = N + 2 * W
TOP = EXT + 16
PR = 16
QR = 32
CHUNKS = ((0, 8), (8, 16), (16, 25), (25, 31))
OUT_CHUNKS = ((0, 3), (3, 9), (9, 17), (17, 25), (25, 31))


def solve_coefs(nu):
    inner, last, back = [], [], []
    c_prev = 0.0
    for k in range(LEVELS):
        lo = nu if k > 0 else 0.0
        piv = 1.0 + nu + lo - lo * c_prev
        inner.append(1.0 / piv)
        last.append(1.0 / (1.0 + lo - lo * c_prev))
        c_prev = nu / piv
        back.append(c_prev)
    return inner, last, back


VISC = solve_coefs(VISC_NUM)
DIFF = solve_coefs(DIFF_NUM)


def weights():
    s = np.arange(1, SUBCYCLES + 1, dtype=np.float64) / (SUBCYCLES + 1)
    w = s ** 2 * (1.0 - s ** 4)
    return (w / w.sum()).astype(np.float32)


def exchange_kernel(ncol, nrow, u_hbm, v_hbm, t_hbm, s_hbm, eta_hbm, tu_hbm, tv_hbm, dep_hbm, kmt_hbm,
                    nu_ref, nv_ref, nt_ref, ns_ref, two_ref, et, fu, fv, cu, cv, fm_out, fe_out, fw_out,
                    fb, ki, kd, qs, msg_e, msg_w, fold_s, fold_r, got_w, got_e, xe, xw, ed,
                    wm, pk_e, pk_w, we, ww, fm, fk_e, fk_w, fe, fw,
                    ld_sem, in_sem, snd, rcv):
    c = lax.axis_index('col')
    r = lax.axis_index('row')
    east = lax.rem(c + 1, ncol)
    west = lax.rem(c + ncol - 1, ncol)
    north = lax.rem(r + 1, nrow)
    south = lax.rem(r + nrow - 1, nrow)
    has_n = r < nrow - 1
    has_s = r > 0

    barrier = pltpu.get_barrier_semaphore()
    places = [(east, r), (west, r), (c, north), (c, south), (east, north), (east, south), (west, north), (west, south)]
    for cc, rr in places:
        pl.semaphore_signal(barrier, inc=1, device_id={'col': cc, 'row': rr}, device_id_type=MESH)

    src3 = (u_hbm, v_hbm, t_hbm, s_hbm)
    small = [pltpu.make_async_copy(kmt_hbm, ki, in_sem.at[0]),
             pltpu.make_async_copy(dep_hbm, kd.at[1, pl.ds(8, N), :], in_sem.at[1]),
             pltpu.make_async_copy(eta_hbm, wm.at[0, pl.ds(W, N), :], in_sem.at[2]),
             pltpu.make_async_copy(tu_hbm, wm.at[1, pl.ds(W, N), :], in_sem.at[3]),
             pltpu.make_async_copy(tv_hbm, wm.at[2, pl.ds(W, N), :], in_sem.at[4])]
    loads = []
    for ci, (k0, k1) in enumerate(CHUNKS):
        row = [pltpu.make_async_copy(src3[f].at[pl.ds(k0, k1 - k0)], fb.at[f, pl.ds(k0, k1 - k0), pl.ds(8, N), :],
                                     ld_sem.at[f, ci]) for f in range(4)]
        loads.append(row)
        for cp in row:
            cp.start()
        if ci == 0:
            for cp in small:
                cp.start()

    def copy(i, src, dst, cc, rr):
        return pltpu.make_async_remote_copy(src_ref=src, dst_ref=dst, send_sem=snd.at[i], recv_sem=rcv.at[i],
                                            device_id={'col': cc, 'row': rr}, device_id_type=MESH)

    rows = [
        (copy(0, fb.at[:, :, pl.ds(8, 1), :], fb.at[:, :, pl.ds(8 + N, 1), :], c, south), has_s, has_n),
        (copy(1, fb.at[:, :, pl.ds(7 + N, 1), :], fb.at[:, :, pl.ds(7, 1), :], c, north), has_n, has_s),
        (copy(2, kd.at[:, pl.ds(8, 1), :], kd.at[:, pl.ds(8 + N, 1), :], c, south), has_s, has_n),
        (copy(3, kd.at[:, pl.ds(7 + N, 1), :], kd.at[:, pl.ds(7, 1), :], c, north), has_n, has_s),
    ]
    cols = [
        (copy(4, fold_s.at[1, 0], fold_r.at[1, 0], east, r), None, None),
        (copy(5, fold_s.at[1, 1], fold_r.at[1, 1], west, r), None, None),
        (copy(6, msg_e.at[pl.ds(0, 8), :], got_w.at[pl.ds(8 + N, 8), :], east, south), has_s, has_n),
        (copy(7, msg_w.at[pl.ds(N - 8, 8), :], got_e.at[pl.ds(0, 8), :], west, north), has_n, has_s),
    ]

    cols_a = [
        (copy(24, fold_s.at[0, 0], fold_r.at[0, 0], east, r), None, None),
        (copy(25, fold_s.at[0, 1], fold_r.at[0, 1], west, r), None, None),
    ]

    def main_rows(base, main):
        return [
            (copy(base, main.at[:, pl.ds(W, W), :], main.at[:, pl.ds(W + N, W), :], c, south), has_s, has_n),
            (copy(base + 1, main.at[:, pl.ds(N, W), :], main.at[:, pl.ds(0, W), :], c, north), has_n, has_s),
        ]

    def side_cols(base, to_e, to_w, in_e, in_w, w, n):
        return [
            (copy(base, to_w, in_e.at[pl.ds(w, n), :], west, r), None, None),
            (copy(base + 1, to_e, in_w.at[pl.ds(w, n), :], east, r), None, None),
        ]

    wide_side = side_cols(8, pk_e, pk_w, we, ww, W, N)
    wide_main = main_rows(10, wm)
    wide_pass = []
    for i, buf in ((12, we), (14, ww)):
        wide_pass += [
            (copy(i, buf.at[pl.ds(W, W), :], buf.at[pl.ds(W + N, W), :], c, south), has_s, has_n),
            (copy(i + 1, buf.at[pl.ds(N, W), :], buf.at[pl.ds(0, W), :], c, north), has_n, has_s),
        ]
    h = W // 2
    n2 = N // 2
    lo, hi = pl.ds(0, h), pl.ds(n2 - h, h)
    forc = side_cols(16, fk_e, fk_w, fe, fw, h, n2) + main_rows(18, fm) + [
        (copy(20, fk_w.at[lo, :], fe.at[pl.ds(h + n2, h), :], west, south), has_s, has_n),
        (copy(21, fk_w.at[hi, :], fe.at[lo, :], west, north), has_n, has_s),
        (copy(22, fk_e.at[lo, :], fw.at[pl.ds(h + n2, h), :], east, south), has_s, has_n),
        (copy(23, fk_e.at[hi, :], fw.at[lo, :], east, north), has_n, has_s),
    ]

    def run(cond, fn):
        if cond is None:
            fn()
        else:
            pl.when(cond)(fn)

    def start(items):
        for cp, s_if, _ in items:
            run(s_if, cp.start)

    def wait_recv(items):
        for cp, _, r_if in items:
            run(r_if, cp.wait_recv)

    def wait_send(items):
        for cp, s_if, _ in items:
            run(s_if, cp.wait_send)

    lane = lax.broadcasted_iota(jnp.int32, (N, N), 1)
    part = lax.rem(lane, 4)
    slot = lane // 4

    def roll(x, s):
        s %= N
        return pltpu.roll(x, s, 1) if s else x

    for cp in small:
        cp.wait()
    kmt_f = ki[...].astype(F32)
    dep = kd[1, 8:8 + N, :]
    kd[0, 8:8 + N, :] = kmt_f
    wm[3, W:W + N, :] = jnp.where(kmt_f > 0.0, dep, 0.0)

    def pack(fields):
        e_acc = jnp.zeros((N, N), F32)
        w_acc = jnp.zeros((N, N), F32)
        for f, x in enumerate(fields):
            here = lane // W == f
            w_acc = jnp.where(here, roll(x, W * f), w_acc)
            e_acc = jnp.where(here, roll(x, W * (f + 1)), e_acc)
        return e_acc, w_acc

    e_acc, w_acc = pack([wm[f, W:W + N, :] for f in range(4)])
    pk_e[...] = e_acc
    pk_w[...] = w_acc

    acc = [jnp.zeros((N, N), F32)] * 4
    low64 = lax.broadcasted_iota(jnp.int32, (N // 2, N), 1) < N // 2

    def messages(k0, k1):
        out = []
        for shift in (1, 2):
            x = jnp.zeros((N, N), F32)
            for f in range(4):
                x = jnp.where((part == f) & (slot >= k0) & (slot < k1), roll(acc[f], f - shift), x)
            out.append(x)
        return out

    for ci, (k0, k1) in enumerate(CHUNKS):
        for cp in loads[ci]:
            cp.wait()
        for f in range(4):
            x = acc[f]
            for k in range(k0, k1):
                x = jnp.where(slot == k, roll(fb[f, k, 8:8 + N, :], 4 * k + 2), x)
            acc[f] = x
        if ci == 1:
            for i, (m, ref) in enumerate(zip(messages(0, 16), (msg_e, msg_w))):
                ref[...] = m
                fold_s[0, i] = jnp.where(low64, m[:N // 2], roll(m[N // 2:], N // 2))
            pl.semaphore_wait(barrier, len(places))
            start(cols_a)
    start(rows)
    hi_m = messages(16, LEVELS)
    ends = (jnp.where(lane == 124, roll(kmt_f, -3), roll(dep, -2)), jnp.where(lane == 124, roll(kmt_f, 124), roll(dep, 125)))
    for i, (m, e, ref) in enumerate(zip(hi_m, ends, (msg_e, msg_w))):
        m = jnp.where(slot == LEVELS, e, m)
        ref[...] = jnp.where(lane < N // 2, ref[...], m)
        fold_s[1, i] = jnp.where(low64, roll(m[:N // 2], N // 2), m[N // 2:])
    for f in range(4):
        qs[f, 8:8 + N, :] = acc[f]

    start(cols)

    @pl.when(jnp.logical_not(has_n))
    def _():
        fb[:, :, 8 + N:9 + N, :] = jnp.zeros((4, LEVELS, 1, N), F32)
        kd[:, 8 + N:9 + N, :] = jnp.zeros((2, 1, N), F32)
        got_w[8 + N:16 + N, :] = jnp.zeros((8, N), F32)

    @pl.when(jnp.logical_not(has_s))
    def _():
        fb[:, :, 7:8, :] = jnp.zeros((4, LEVELS, 1, N), F32)
        kd[:, 7:8, :] = jnp.zeros((2, 1, N), F32)
        got_e[0:8, :] = jnp.zeros((8, N), F32)

    def thick(k, d):
        return 0.6 * d / jnp.maximum(k, 1.0)

    def force(wet_u, wet_v, q_c, q_e, q_n, u_c, u_n, u_s, v_c, v_n, v_s):
        us, vs = u_c + u_n, v_c + v_s
        v_at_u = 0.25 * (vs + roll(vs, -1))
        u_at_v = 0.25 * (us + roll(us, 1))
        u_w = roll(u_c, 1)
        g_u = jnp.where(wet_u, u_c * (roll(u_c, -1) - u_w) + v_at_u * (u_n - u_s) + (q_e - q_c), 0.0)
        g_v = jnp.where(wet_v, u_at_v * (roll(v_c, -1) - roll(v_c, 1)) + v_c * (v_n - v_s) + (q_n - q_c), 0.0)
        u_m, v_m = jnp.where(wet_u, u_c, 0.0), jnp.where(wet_v, v_c, 0.0)
        return g_u, g_v, u_m - 0.125 * g_u, v_m - 0.125 * g_v, u_m, v_m, u_w

    def advect(u_e, u_w, v_n, v_s, tracers):
        a_e, a_w = jnp.minimum(u_e, 0.0), jnp.maximum(u_w, 0.0)
        a_n, a_s = jnp.minimum(v_n, 0.0), jnp.maximum(v_s, 0.0)
        a_c = (jnp.maximum(u_e, 0.0) - jnp.minimum(u_w, 0.0)) + (jnp.maximum(v_n, 0.0) - jnp.minimum(v_s, 0.0))
        b_c = 4.0 - a_c
        return [b_c * x + ((a_w * roll(x, 1) - a_e * roll(x, -1)) + (a_s * x_s - a_n * x_n)) for x, x_n, x_s in tracers]

    def main_step(i, _):
        @pl.when(i == 3)
        def _():
            start(wide_side)
            start(wide_main)

        @pl.when(i == N // PR - 2)
        def _():
            wait_recv(rows)

        own = pl.multiple_of(lax.rem(i + 1, N // PR) * PR, PR)
        base = own + 8

        def at(f, k, off):
            return fb[f, k, pl.ds(base + off, PR), :]

        kc = kd[0, pl.ds(base, PR), :]
        kn = kd[0, pl.ds(base + 1, PR), :]
        ks = kd[0, pl.ds(base - 1, PR), :]
        dc = kd[1, pl.ds(base, PR), :]
        dn = kd[1, pl.ds(base + 1, PR), :]
        th_c, th_n = thick(kc, dc), thick(kn, dn)
        nu_f = jnp.minimum(kc, roll(kc, -1))
        nw_f = jnp.minimum(kc, roll(kc, 1))
        nv_f = jnp.minimum(kc, kn)
        nq_f = jnp.minimum(kc, ks)
        zero = jnp.zeros((PR, N), F32)
        cum_c, cum_n, sum_u, sum_v = zero, zero, zero, zero
        for k in range(LEVELS):
            fk = float(k)
            t_c, s_c = at(2, k, 0), at(3, k, 0)
            t_n, s_n = at(2, k, 1), at(3, k, 1)
            h_c = s_c - 0.5 * t_c
            h_n = s_n - 0.5 * t_n
            mid_c, mid_n = cum_c + h_c, cum_n + h_n
            cum_c, cum_n = mid_c + h_c, mid_n + h_n
            q_c = mid_c * th_c
            u_c, v_c, v_s = at(0, k, 0), at(1, k, 0), at(1, k, -1)
            g_u, g_v, r_u, r_v, u_m, v_m, u_w = force(
                nu_f > fk, nv_f > fk, q_c, roll(q_c, -1), mid_n * th_n,
                u_c, at(0, k, 1), at(0, k, -1), v_c, at(1, k, 1), v_s)
            sum_u, sum_v = sum_u + g_u, sum_v + g_v
            nu_ref[k, pl.ds(own, PR), :] = r_u
            nv_ref[k, pl.ds(own, PR), :] = r_v
            t1, s1 = advect(u_m, jnp.where(nw_f > fk, u_w, 0.0), v_m, jnp.where(nq_f > fk, v_s, 0.0),
                            ((t_c, t_n, at(2, k, -1)), (s_c, s_n, at(3, k, -1))))
            nt_ref[k, pl.ds(own, PR), :] = t1
            ns_ref[k, pl.ds(own, PR), :] = s1
        hu = jnp.where(nu_f > 0.0, 0.5 * (dc + roll(dc, -1)), 0.0)
        hv = jnp.where(nv_f > 0.0, 0.5 * (dc + dn), 0.0)
        fm[0, pl.ds(own + W, PR), :] = hu / jnp.maximum(nu_f, 1.0) * (-0.5 * sum_u)
        fm[1, pl.ds(own + W, PR), :] = hv / jnp.maximum(nv_f, 1.0) * (-0.5 * sum_v)
        return 0

    lax.fori_loop(0, N // PR, main_step, 0)

    lane8 = lax.broadcasted_iota(jnp.int32, (8, N), 1)
    for f in range(4):
        for lo in (0, 8 + N):
            x = jnp.zeros((8, N), F32)
            for k in range(LEVELS):
                x = jnp.where(lane8 // 4 == k, roll(fb[f, k, lo:lo + 8, :], 4 * k + 2), x)
            qs[f, lo:lo + 8, :] = x

    wait_recv(cols_a)
    wait_recv(cols)
    for i, got in ((0, got_w), (1, got_e)):
        a, b = fold_r[0, i], fold_r[1, i]
        got[8:8 + N // 2, :] = jnp.where(low64, a, roll(b, N // 2))
        got[8 + N // 2:8 + N, :] = jnp.where(low64, roll(a, N // 2), b)

    part_x = lax.rem(lax.broadcasted_iota(jnp.int32, (N + 16, N), 1), 4)
    for f in range(4):
        q = qs[f]
        xe[f] = jnp.where(part_x == 2, roll(got_e[...], 2 - f), q)
        xw[f] = jnp.where(part_x == 1, roll(got_w[...], 1 - f), q)
    for f in range(2):
        q = kd[f]
        b = [jnp.broadcast_to(q[:, j:j + 1], q.shape) for j in (N - 2, N - 1, 0, 1)]
        h_e = jnp.broadcast_to(got_e[:, 124 + f:125 + f], q.shape)
        h_w = jnp.broadcast_to(got_w[:, 124 + f:125 + f], q.shape)
        xe[4 + f] = jnp.where(part_x == 0, b[0], jnp.where(part_x == 1, b[1], h_e))
        xw[4 + f] = jnp.where(part_x == 1, h_w, jnp.where(part_x == 2, b[2], b[3]))

    lev = slot.astype(F32)

    row_i = lax.broadcasted_iota(jnp.int32, (N, N), 0)
    same = lax.rem(row_i, 4) == part
    below = jnp.where(same & (row_i // 4 <= slot), 1.0, 0.0)
    every = jnp.where(same, 1.0, 0.0)

    def mix(x, m):
        return jnp.dot(x, m, precision=lax.Precision.HIGHEST, preferred_element_type=F32)

    def strip_force(x):
        def at(f, off):
            return x[f, 8 + off:8 + off + N, :]

        kc, kn = at(4, 0), at(4, 1)
        dc, dn = at(5, 0), at(5, 1)
        nu_f, nv_f = jnp.minimum(kc, roll(kc, -1)), jnp.minimum(kc, kn)
        h_c = at(3, 0) - 0.5 * at(2, 0)
        h_n = at(3, 1) - 0.5 * at(2, 1)
        q_c = (2.0 * mix(h_c, below) - h_c) * thick(kc, dc)
        q_n = (2.0 * mix(h_n, below) - h_n) * thick(kn, dn)
        g_u, g_v, r_u, r_v = force(nu_f > lev, nv_f > lev, q_c, roll(q_c, -1), q_n,
                                   at(0, 0), at(0, 1), at(0, -1), at(1, 0), at(1, 1), at(1, -1))[:4]
        hu = jnp.where(nu_f > 0.0, -0.25 * (dc + roll(dc, -1)), 0.0) / jnp.maximum(nu_f, 1.0)
        hv = jnp.where(nv_f > 0.0, -0.25 * (dc + dn), 0.0) / jnp.maximum(nv_f, 1.0)
        return hu, hv, g_u, g_v, r_u, r_v

    def strip_tracer(x):
        def at(f, off):
            return x[f, 8 + off:8 + off + N, :]

        kc, kn, ks = at(4, 0), at(4, 1), at(4, -1)
        u_m = jnp.where(jnp.minimum(kc, roll(kc, -1)) > lev, at(0, 0), 0.0)
        u_w = jnp.where(jnp.minimum(kc, roll(kc, 1)) > lev, roll(at(0, 0), 1), 0.0)
        v_m = jnp.where(jnp.minimum(kc, kn) > lev, at(1, 0), 0.0)
        v_s = jnp.where(jnp.minimum(kc, ks) > lev, at(1, -1), 0.0)
        return advect(u_m, u_w, v_m, v_s, ((at(2, 0), at(2, 1), at(2, -1)), (at(3, 0), at(3, 1), at(3, -1))))

    def merge(fn):
        return [jnp.where(part == 1, a, b) for a, b in zip(fn(xe), fn(xw))]

    hu, hv, g_u, g_v, r_u, r_v = merge(strip_force)
    rim = (lane == 0) | (lane == N - 1)
    forces = []
    for f, (hf, g) in enumerate(((hu, g_u), (hv, g_v))):
        x = jnp.where(rim, roll(hf * mix(g, every), 2), fm[f, W:W + N, :])
        fm[f, W:W + N, :] = x
        forces.append(x)
    half = lax.broadcasted_iota(jnp.int32, (h, N), 1) < n2
    for ref, x in zip((fk_e, fk_w), pack(forces)):
        for b in range(N // W):
            ref[h * b:h * b + h, :] = jnp.where(half, x[W * b:W * b + h], roll(x[W * b + h:W * b + W], n2))
    start(forc)
    ed[0] = r_u
    ed[1] = r_v
    t1, s1 = merge(strip_tracer)
    ed[2] = t1
    ed[3] = s1
    wait_recv(wide_side)
    start(wide_pass)

    lane_q = lax.broadcasted_iota(jnp.int32, (QR, N), 1)
    edge_q = (lane_q == 0) | (lane_q == N - 1)

    def solve_step(g, _):
        own = pl.multiple_of(g * QR, QR)
        base = own + 8
        here = pl.ds(own, QR)
        kc = kd[0, pl.ds(base, QR), :]
        kn = kd[0, pl.ds(base + 1, QR), :]
        nu_f = jnp.minimum(kc, jnp.where(lane_q == N - 1, roll(got_e[pl.ds(base, QR), :], 3), roll(kc, -1)))
        nv_f = jnp.minimum(kc, kn)
        two_ref[0, here, :] = nu_f
        two_ref[1, here, :] = nv_f
        zero = jnp.zeros((QR, N), F32)
        refs = (nu_ref, nv_ref, nt_ref, ns_ref)
        cos = (VISC, VISC, DIFF, DIFF)
        d = [zero] * 4

        def factor(n_f, k, co, nu):
            return jnp.where(n_f > k + 1.0, nu * co[0][k], jnp.where(n_f > float(k), nu * co[1][k], 0.0))

        for k in range(LEVELS):
            f_t = factor(kc, k, DIFF, DIFF_NUM)
            facs = (factor(nu_f, k, VISC, VISC_NUM), factor(nv_f, k, VISC, VISC_NUM), f_t, f_t)
            for q in range(4):
                x = jnp.where(edge_q, roll(ed[q, here, :], 126 - 4 * k), refs[q][k, here, :])
                d[q] = (x + d[q]) * facs[q]
                if k == LEVELS - 1:
                    refs[q][k, here, :] = 0.25 * d[q]
                else:
                    refs[q][k, here, :] = d[q]
        sum_u, sum_v = d[0], d[1]
        for k in range(LEVELS - 2, -1, -1):
            for q in range(4):
                d[q] = refs[q][k, here, :] + cos[q][2][k] * d[q]
                refs[q][k, here, :] = 0.25 * d[q]
            sum_u, sum_v = sum_u + d[0], sum_v + d[1]
        two_ref[2, here, :] = sum_u / (VISC_NUM * jnp.maximum(nu_f, 1.0))
        two_ref[3, here, :] = sum_v / (VISC_NUM * jnp.maximum(nv_f, 1.0))
        return 0

    lax.fori_loop(0, N // QR, solve_step, 0)

    wait_recv(wide_main)
    wait_recv(wide_pass)
    lane_x = lax.broadcasted_iota(jnp.int32, (EXT, N), 1)
    row_x = lax.broadcasted_iota(jnp.int32, (EXT, N), 0)
    real = (row_x >= jnp.where(has_s, 0, W)) & (row_x < jnp.where(has_n, EXT, W + N))
    in_e, in_w = lane_x < W, lane_x >= N - W

    def side(f):
        return jnp.where(in_e, roll(we[...], -W * f), roll(ww[...], -W * (f + 1)))

    dms = (jnp.where(real, wm[3], 0.0), jnp.where(real & (in_e | in_w), side(3), 0.0))
    zero8 = jnp.zeros((8, N), F32)
    for ref in (et, fu, fv):
        for t in range(2):
            ref[t, 0:8, :] = zero8
            ref[t, 8 + EXT:TOP, :] = zero8
    for t in range(2):
        et[t, 8:8 + EXT, :] = dms[t]
    ra, rb = roll(dms[0], -1), roll(dms[1], -1)
    dme = (jnp.where(lane_x == N - 1, rb, ra), jnp.where(lane_x == N - 1, ra, rb))
    for t in range(2):
        d_c = dms[t]
        d_n = et[t, 9:9 + EXT, :]
        wet_u = (d_c > 0.0) & (dme[t] > 0.0)
        wet_v = (d_c > 0.0) & (d_n > 0.0)
        pick = (lambda f: wm[f]) if t == 0 else side
        et[t, 8:8 + EXT, :] = jnp.where(d_c > 0.0, pick(0), 0.0)
        fu[t, 8:8 + EXT, :] = jnp.where(wet_u, 0.5 * pick(1), 0.0)
        fv[t, 8:8 + EXT, :] = jnp.where(wet_v, 0.5 * pick(2), 0.0)
        cu[t] = jnp.where(wet_u, 0.125 * (d_c + dme[t]), 0.0)
        cv[t] = jnp.where(wet_v, 0.125 * (d_c + d_n), 0.0)
    wait_send(rows)
    wait_send(cols_a)
    wait_send(cols)
    wait_send(wide_side)
    wait_send(wide_main)
    wait_send(wide_pass)
    wait_recv(forc)
    fm_out[...] = fm[...]
    for out, got in ((fe_out, fe), (fw_out, fw)):
        for b in range(EXT // W):
            x = got[h * b:h * b + h, :]
            out[W * b:W * b + h, :] = x
            out[W * b + h:W * b + W, :] = roll(x, n2)
    wait_send(forc)


def step_kernel(nu_ref, nv_ref, nt_ref, ns_ref, two_ref, et0, fu0, fv0, cu, cv, fm, fe, fw,
                eta_out, tu_out, tv_out, u_hbm, v_hbm, t_hbm, s_hbm,
                et1, fu1, fv1, pu, pv, mean, ub, vb, flat, osem):
    copies = [pltpu.make_async_copy(nt_ref, t_hbm, osem.at[0]), pltpu.make_async_copy(ns_ref, s_hbm, osem.at[1])]
    for cp in copies:
        cp.start()

    lane = lax.broadcasted_iota(jnp.int32, (EXT, N), 1)

    def side(f):
        e, w = fe[...], fw[...]
        e = pltpu.roll(e, N - W * f, 1) if f else e
        w = pltpu.roll(w, N - W * (f + 1), 1)
        return jnp.where(lane < W, e, w)

    for f, (p, co) in enumerate(((pu, cu), (pv, cv))):
        for t in range(2):
            x = fm[f] if t == 0 else side(f)
            p[t] = jnp.where(co[t] > 0.0, (0.125 / SUBCYCLES) * x, 0.0)
    zero8 = jnp.zeros((8, N), F32)
    for ref in (et1, fv1):
        for t in range(2):
            ref[t, 0:8, :] = zero8
            ref[t, 8 + EXT:TOP, :] = zero8

    wgt = weights()
    lane8 = lax.broadcasted_iota(jnp.int32, (8, N), 1)
    first8, last8 = lane8 == 0, lane8 == N - 1

    def west8(x):
        a, b = pltpu.roll(x[0], 1, 1), pltpu.roll(x[1], 1, 1)
        return jnp.where(first8, b, a), jnp.where(first8, a, b)

    def east8(x):
        a, b = pltpu.roll(x[0], N - 1, 1), pltpu.roll(x[1], N - 1, 1)
        return jnp.where(last8, b, a), jnp.where(last8, a, b)

    for n in range(1, SUBCYCLES + 1):
        lo = 8 * (n // 8)
        groups = range(lo, EXT - lo, 8)
        et, fu, fv = (et1, fu1, fv1) if n > 1 else (et0, fu0, fv0)
        for g in groups:
            us = (fu[0, 8 + g:16 + g, :], fu[1, 8 + g:16 + g, :])
            uw = west8(us)
            for t in range(2):
                et1[t, 8 + g:16 + g, :] = et[t, 8 + g:16 + g, :] - (
                    (us[t] - uw[t]) + (fv[t, 8 + g:16 + g, :] - fv[t, 7 + g:15 + g, :]))
        for g in groups:
            es = (et1[0, 8 + g:16 + g, :], et1[1, 8 + g:16 + g, :])
            ee = east8(es)
            for t in range(2):
                u = fu[t, 8 + g:16 + g, :] - cu[t, g:g + 8, :] * (ee[t] - es[t]) + pu[t, g:g + 8, :]
                v = fv[t, 8 + g:16 + g, :] - cv[t, g:g + 8, :] * (et1[t, 9 + g:17 + g, :] - es[t]) + pv[t, g:g + 8, :]
                fu1[t, 8 + g:16 + g, :] = u
                fv1[t, 8 + g:16 + g, :] = v
                if t == 0 and W <= g < W + N:
                    at = slice(g - W, g - W + 8)
                    w = float(wgt[n - 1])
                    mean[0, at, :] = w * u if n == 1 else mean[0, at, :] + w * u
                    mean[1, at, :] = w * v if n == 1 else mean[1, at, :] + w * v

    mid = slice(8 + W, 8 + W + N)
    flat[0] = et1[0, mid, :]
    flat[1] = 2.0 * fu1[0, mid, :]
    flat[2] = 2.0 * fv1[0, mid, :]
    for i, out in enumerate((eta_out, tu_out, tv_out)):
        cp = pltpu.make_async_copy(flat.at[i], out, osem.at[2 + i])
        cp.start()
        copies.append(cp)
    for i, co in ((0, cu), (1, cv)):
        h = co[0, W:W + N, :]
        mean[i] = mean[i] / jnp.where(h > 0.0, 2.0 * h, 1.0) - two_ref[2 + i]

    for ci, (k0, k1) in enumerate(OUT_CHUNKS):
        for i, (src, buf, dst) in enumerate(((nu_ref, ub, u_hbm), (nv_ref, vb, v_hbm))):
            for g in range(0, N, 8):
                at = slice(g, g + 8)
                n_f, m = two_ref[i, at, :], mean[i, at, :]
                for k in range(k0, k1):
                    buf[k, at, :] = src[k, at, :] + jnp.where(n_f > float(k), m, 0.0)
            cp = pltpu.make_async_copy(buf.at[pl.ds(k0, k1 - k0)], dst.at[pl.ds(k0, k1 - k0)], osem.at[5 + 2 * ci + i])
            cp.start()
            copies.append(cp)
    for cp in copies:
        cp.wait()


def solution(mesh):
    ncol, nrow = mesh.shape['col'], mesh.shape['row']
    vmem = pl.BlockSpec(memory_space=pltpu.VMEM)
    hbm = pl.BlockSpec(memory_space=pl.ANY)
    s3 = jax.ShapeDtypeStruct((LEVELS, N, N), F32)
    s2 = jax.ShapeDtypeStruct((N, N), F32)

    def sds(*shape):
        return jax.ShapeDtypeStruct(shape, F32)

    def ocean_step(vel_u, vel_v, temp, salt, eta, tu, tv, dep, kmt):
        def kernel_a(*refs):
            exchange_kernel(ncol, nrow, *refs)

        def kernel_b(*refs):
            step_kernel(*refs)

        mid = pl.pallas_call(
            kernel_a,
            name='exchange',
            out_shape=(s3, s3, s3, s3, sds(4, N, N), sds(2, TOP, N), sds(2, TOP, N), sds(2, TOP, N), sds(2, EXT, N),
                       sds(2, EXT, N), sds(2, EXT, N), sds(EXT, N), sds(EXT, N)),
            in_specs=[hbm] * 9,
            out_specs=(vmem,) * 13,
            scratch_shapes=[
                pltpu.VMEM((4, LEVELS, N + 16, N), F32),
                pltpu.VMEM((N, N), jnp.int32),
                pltpu.VMEM((2, N + 16, N), F32),
                pltpu.VMEM((4, N + 16, N), F32),
                pltpu.VMEM((N, N), F32), pltpu.VMEM((N, N), F32),
                pltpu.VMEM((2, 2, N // 2, N), F32), pltpu.VMEM((2, 2, N // 2, N), F32),
                pltpu.VMEM((N + 16, N), F32), pltpu.VMEM((N + 16, N), F32),
                pltpu.VMEM((6, N + 16, N), F32), pltpu.VMEM((6, N + 16, N), F32),
                pltpu.VMEM((4, N, N), F32),
                pltpu.VMEM((4, EXT, N), F32),
                pltpu.VMEM((N, N), F32), pltpu.VMEM((N, N), F32),
                pltpu.VMEM((EXT, N), F32), pltpu.VMEM((EXT, N), F32),
                pltpu.VMEM((2, EXT, N), F32),
                pltpu.VMEM((N // 2, N), F32), pltpu.VMEM((N // 2, N), F32),
                pltpu.VMEM((EXT // 2, N), F32), pltpu.VMEM((EXT // 2, N), F32),
                pltpu.SemaphoreType.DMA((4, len(CHUNKS))),
                pltpu.SemaphoreType.DMA((5,)),
                pltpu.SemaphoreType.DMA((26,)),
                pltpu.SemaphoreType.DMA((26,)),
            ],
            compiler_params=pltpu.CompilerParams(collective_id=0, has_side_effects=True, vmem_limit_bytes=28 * 2 ** 20),
        )(*[pltpu.with_memory_space_constraint(x, pltpu.HBM) for x in (vel_u, vel_v, temp, salt, eta, tu, tv, dep, kmt)])
        st = pltpu.VMEM((2, TOP, N), F32)
        co = pltpu.VMEM((2, EXT, N), F32)
        out = pl.pallas_call(
            kernel_b,
            name='subcycles',
            out_shape=(s2, s2, s2, s3, s3, s3, s3),
            in_specs=[vmem] * 13,
            out_specs=(hbm,) * 7,
            scratch_shapes=[st, st, st, co, co, pltpu.VMEM((2, N, N), F32),
                            pltpu.VMEM((LEVELS, N, N), F32), pltpu.VMEM((LEVELS, N, N), F32),
                            pltpu.VMEM((3, N, N), F32), pltpu.SemaphoreType.DMA((5 + 2 * len(OUT_CHUNKS),))],
            compiler_params=pltpu.CompilerParams(vmem_limit_bytes=28 * 2 ** 20),
        )(*mid)
        return out

    spec_3d = P(None, 'row', 'col')
    spec_2d = P('row', 'col')
    return jax.shard_map(ocean_step, mesh=mesh, in_specs=(spec_3d,) * 4 + (spec_2d,) * 5,
                         out_specs=(spec_2d,) * 3 + (spec_3d,) * 4, check_vma=False)
```

```python
import jax
import jax.numpy as jnp
import numpy as np
from jax import lax
from jax.experimental import pallas as pl
from jax.experimental.pallas import tpu as pltpu
from jax.sharding import PartitionSpec as P

MESH = pl.DeviceIdType.MESH
F32 = jnp.float32
SUBCYCLES = 30
LEVELS = 31
VISC_NUM = 4.0
DIFF_NUM = 1.0
N = 128
W = 32
EXT = N + 2 * W
TOP = EXT + 16
PR = 16
QR = 32
CHUNKS = ((0, 9), (9, 18), (18, 27), (27, 31))
OUT_CHUNKS = ((0, 3), (3, 9), (9, 17), (17, 25), (25, 31))


def solve_coefs(nu):
    inner, last, back = [], [], []
    c_prev = 0.0
    for k in range(LEVELS):
        lo = nu if k > 0 else 0.0
        piv = 1.0 + nu + lo - lo * c_prev
        inner.append(1.0 / piv)
        last.append(1.0 / (1.0 + lo - lo * c_prev))
        c_prev = nu / piv
        back.append(c_prev)
    return inner, last, back


VISC = solve_coefs(VISC_NUM)
DIFF = solve_coefs(DIFF_NUM)


def weights():
    s = np.arange(1, SUBCYCLES + 1, dtype=np.float64) / (SUBCYCLES + 1)
    w = s ** 2 * (1.0 - s ** 4)
    return (w / w.sum()).astype(np.float32)


def exchange_kernel(ncol, nrow, u_hbm, v_hbm, t_hbm, s_hbm, eta_hbm, tu_hbm, tv_hbm, dep_hbm, kmt_hbm,
                    nu_ref, nv_ref, nt_ref, ns_ref, two_ref, et, fu, fv, cu, cv, fm_out, fe_out, fw_out,
                    fb, ki, kd, qs, msg_e, msg_w, got_w, got_e, xe, xw, ed,
                    wm, pk_e, pk_w, we, ww, fm, fk_e, fk_w, fe, fw,
                    ld_sem, in_sem, snd, rcv):
    c = lax.axis_index('col')
    r = lax.axis_index('row')
    east = lax.rem(c + 1, ncol)
    west = lax.rem(c + ncol - 1, ncol)
    north = lax.rem(r + 1, nrow)
    south = lax.rem(r + nrow - 1, nrow)
    has_n = r < nrow - 1
    has_s = r > 0

    barrier = pltpu.get_barrier_semaphore()
    places = [(east, r), (west, r), (c, north), (c, south), (east, north), (east, south), (west, north), (west, south)]
    for cc, rr in places:
        pl.semaphore_signal(barrier, inc=1, device_id={'col': cc, 'row': rr}, device_id_type=MESH)

    src3 = (u_hbm, v_hbm, t_hbm, s_hbm)
    small = [pltpu.make_async_copy(kmt_hbm, ki, in_sem.at[0]),
             pltpu.make_async_copy(dep_hbm, kd.at[1, pl.ds(8, N), :], in_sem.at[1]),
             pltpu.make_async_copy(eta_hbm, wm.at[0, pl.ds(W, N), :], in_sem.at[2]),
             pltpu.make_async_copy(tu_hbm, wm.at[1, pl.ds(W, N), :], in_sem.at[3]),
             pltpu.make_async_copy(tv_hbm, wm.at[2, pl.ds(W, N), :], in_sem.at[4])]
    loads = []
    for ci, (k0, k1) in enumerate(CHUNKS):
        row = [pltpu.make_async_copy(src3[f].at[pl.ds(k0, k1 - k0)], fb.at[f, pl.ds(k0, k1 - k0), pl.ds(8, N), :],
                                     ld_sem.at[f, ci]) for f in range(4)]
        loads.append(row)
        for cp in row:
            cp.start()
        if ci == 0:
            for cp in small:
                cp.start()

    def copy(i, src, dst, cc, rr):
        return pltpu.make_async_remote_copy(src_ref=src, dst_ref=dst, send_sem=snd.at[i], recv_sem=rcv.at[i],
                                            device_id={'col': cc, 'row': rr}, device_id_type=MESH)

    rows = [
        (copy(0, fb.at[:, :, pl.ds(8, 1), :], fb.at[:, :, pl.ds(8 + N, 1), :], c, south), has_s, has_n),
        (copy(1, fb.at[:, :, pl.ds(7 + N, 1), :], fb.at[:, :, pl.ds(7, 1), :], c, north), has_n, has_s),
        (copy(2, kd.at[:, pl.ds(8, 1), :], kd.at[:, pl.ds(8 + N, 1), :], c, south), has_s, has_n),
        (copy(3, kd.at[:, pl.ds(7 + N, 1), :], kd.at[:, pl.ds(7, 1), :], c, north), has_n, has_s),
    ]
    cols = [
        (copy(4, msg_e, got_w.at[pl.ds(8, N), :], east, r), None, None),
        (copy(5, msg_w, got_e.at[pl.ds(8, N), :], west, r), None, None),
        (copy(6, msg_e.at[pl.ds(0, 8), :], got_w.at[pl.ds(8 + N, 8), :], east, south), has_s, has_n),
        (copy(7, msg_w.at[pl.ds(N - 8, 8), :], got_e.at[pl.ds(0, 8), :], west, north), has_n, has_s),
    ]

    def main_rows(base, main):
        return [
            (copy(base, main.at[:, pl.ds(W, W), :], main.at[:, pl.ds(W + N, W), :], c, south), has_s, has_n),
            (copy(base + 1, main.at[:, pl.ds(N, W), :], main.at[:, pl.ds(0, W), :], c, north), has_n, has_s),
        ]

    def side_cols(base, to_e, to_w, in_e, in_w, w, n):
        return [
            (copy(base, to_w, in_e.at[pl.ds(w, n), :], west, r), None, None),
            (copy(base + 1, to_e, in_w.at[pl.ds(w, n), :], east, r), None, None),
        ]

    wide_side = side_cols(8, pk_e, pk_w, we, ww, W, N)
    wide_main = main_rows(10, wm)
    wide_pass = []
    for i, buf in ((12, we), (14, ww)):
        wide_pass += [
            (copy(i, buf.at[pl.ds(W, W), :], buf.at[pl.ds(W + N, W), :], c, south), has_s, has_n),
            (copy(i + 1, buf.at[pl.ds(N, W), :], buf.at[pl.ds(0, W), :], c, north), has_n, has_s),
        ]
    h = W // 2
    n2 = N // 2
    lo, hi = pl.ds(0, h), pl.ds(n2 - h, h)
    forc = side_cols(16, fk_e, fk_w, fe, fw, h, n2) + main_rows(18, fm) + [
        (copy(20, fk_w.at[lo, :], fe.at[pl.ds(h + n2, h), :], west, south), has_s, has_n),
        (copy(21, fk_w.at[hi, :], fe.at[lo, :], west, north), has_n, has_s),
        (copy(22, fk_e.at[lo, :], fw.at[pl.ds(h + n2, h), :], east, south), has_s, has_n),
        (copy(23, fk_e.at[hi, :], fw.at[lo, :], east, north), has_n, has_s),
    ]

    def run(cond, fn):
        if cond is None:
            fn()
        else:
            pl.when(cond)(fn)

    def start(items):
        for cp, s_if, _ in items:
            run(s_if, cp.start)

    def wait_recv(items):
        for cp, _, r_if in items:
            run(r_if, cp.wait_recv)

    def wait_send(items):
        for cp, s_if, _ in items:
            run(s_if, cp.wait_send)

    lane = lax.broadcasted_iota(jnp.int32, (N, N), 1)
    part = lax.rem(lane, 4)
    slot = lane // 4

    def roll(x, s):
        s %= N
        return pltpu.roll(x, s, 1) if s else x

    for cp in small:
        cp.wait()
    kmt_f = ki[...].astype(F32)
    dep = kd[1, 8:8 + N, :]
    kd[0, 8:8 + N, :] = kmt_f
    wm[3, W:W + N, :] = jnp.where(kmt_f > 0.0, dep, 0.0)

    def pack(fields):
        e_acc = jnp.zeros((N, N), F32)
        w_acc = jnp.zeros((N, N), F32)
        for f, x in enumerate(fields):
            here = lane // W == f
            w_acc = jnp.where(here, roll(x, W * f), w_acc)
            e_acc = jnp.where(here, roll(x, W * (f + 1)), e_acc)
        return e_acc, w_acc

    e_acc, w_acc = pack([wm[f, W:W + N, :] for f in range(4)])
    pk_e[...] = e_acc
    pk_w[...] = w_acc

    msg_e[...] = jnp.where(lane == 124, roll(kmt_f, -3), roll(dep, -2))
    msg_w[...] = jnp.where(lane == 124, roll(kmt_f, 124), roll(dep, 125))
    acc = [jnp.zeros((N, N), F32)] * 4
    for ci, (k0, k1) in enumerate(CHUNKS):
        for cp in loads[ci]:
            cp.wait()
        if ci == 0:
            pl.semaphore_wait(barrier, len(places))
            start(wide_side)
            start(wide_main)
        if ci == len(CHUNKS) - 1:
            start(rows)
        for f in range(4):
            x = acc[f]
            for k in range(k0, k1):
                x = jnp.where(slot == k, roll(fb[f, k, 8:8 + N, :], 4 * k + 2), x)
            acc[f] = x
    out_e, out_w = msg_e[...], msg_w[...]
    for f in range(4):
        qs[f, 8:8 + N, :] = acc[f]
        pick = (part == f) & (slot < LEVELS)
        out_e = jnp.where(pick, roll(acc[f], f - 1), out_e)
        out_w = jnp.where(pick, roll(acc[f], f - 2), out_w)
    msg_e[...] = out_e
    msg_w[...] = out_w

    start(cols)

    @pl.when(jnp.logical_not(has_n))
    def _():
        fb[:, :, 8 + N:9 + N, :] = jnp.zeros((4, LEVELS, 1, N), F32)
        kd[:, 8 + N:9 + N, :] = jnp.zeros((2, 1, N), F32)
        got_w[8 + N:16 + N, :] = jnp.zeros((8, N), F32)

    @pl.when(jnp.logical_not(has_s))
    def _():
        fb[:, :, 7:8, :] = jnp.zeros((4, LEVELS, 1, N), F32)
        kd[:, 7:8, :] = jnp.zeros((2, 1, N), F32)
        got_e[0:8, :] = jnp.zeros((8, N), F32)

    def thick(k, d):
        return 0.6 * d / jnp.maximum(k, 1.0)

    def force(wet_u, wet_v, q_c, q_e, q_n, u_c, u_n, u_s, v_c, v_n, v_s):
        us, vs = u_c + u_n, v_c + v_s
        v_at_u = 0.25 * (vs + roll(vs, -1))
        u_at_v = 0.25 * (us + roll(us, 1))
        u_w = roll(u_c, 1)
        g_u = jnp.where(wet_u, u_c * (roll(u_c, -1) - u_w) + v_at_u * (u_n - u_s) + (q_e - q_c), 0.0)
        g_v = jnp.where(wet_v, u_at_v * (roll(v_c, -1) - roll(v_c, 1)) + v_c * (v_n - v_s) + (q_n - q_c), 0.0)
        u_m, v_m = jnp.where(wet_u, u_c, 0.0), jnp.where(wet_v, v_c, 0.0)
        return g_u, g_v, u_m - 0.125 * g_u, v_m - 0.125 * g_v, u_m, v_m, u_w

    def advect(u_e, u_w, v_n, v_s, tracers):
        a_e, a_w = jnp.minimum(u_e, 0.0), jnp.maximum(u_w, 0.0)
        a_n, a_s = jnp.minimum(v_n, 0.0), jnp.maximum(v_s, 0.0)
        a_c = (jnp.maximum(u_e, 0.0) - jnp.minimum(u_w, 0.0)) + (jnp.maximum(v_n, 0.0) - jnp.minimum(v_s, 0.0))
        b_c = 4.0 - a_c
        return [b_c * x + ((a_w * roll(x, 1) - a_e * roll(x, -1)) + (a_s * x_s - a_n * x_n)) for x, x_n, x_s in tracers]

    def main_step(i, _):
        @pl.when(i == N // PR - 2)
        def _():
            wait_recv(rows)
            wait_recv(wide_side)
            start(wide_pass)

        own = pl.multiple_of(lax.rem(i + 1, N // PR) * PR, PR)
        base = own + 8

        def at(f, k, off):
            return fb[f, k, pl.ds(base + off, PR), :]

        kc = kd[0, pl.ds(base, PR), :]
        kn = kd[0, pl.ds(base + 1, PR), :]
        ks = kd[0, pl.ds(base - 1, PR), :]
        dc = kd[1, pl.ds(base, PR), :]
        dn = kd[1, pl.ds(base + 1, PR), :]
        th_c, th_n = thick(kc, dc), thick(kn, dn)
        nu_f = jnp.minimum(kc, roll(kc, -1))
        nw_f = jnp.minimum(kc, roll(kc, 1))
        nv_f = jnp.minimum(kc, kn)
        nq_f = jnp.minimum(kc, ks)
        zero = jnp.zeros((PR, N), F32)
        cum_c, cum_n, sum_u, sum_v = zero, zero, zero, zero
        for k in range(LEVELS):
            fk = float(k)
            t_c, s_c = at(2, k, 0), at(3, k, 0)
            t_n, s_n = at(2, k, 1), at(3, k, 1)
            h_c = s_c - 0.5 * t_c
            h_n = s_n - 0.5 * t_n
            mid_c, mid_n = cum_c + h_c, cum_n + h_n
            cum_c, cum_n = mid_c + h_c, mid_n + h_n
            q_c = mid_c * th_c
            u_c, v_c, v_s = at(0, k, 0), at(1, k, 0), at(1, k, -1)
            g_u, g_v, r_u, r_v, u_m, v_m, u_w = force(
                nu_f > fk, nv_f > fk, q_c, roll(q_c, -1), mid_n * th_n,
                u_c, at(0, k, 1), at(0, k, -1), v_c, at(1, k, 1), v_s)
            sum_u, sum_v = sum_u + g_u, sum_v + g_v
            nu_ref[k, pl.ds(own, PR), :] = r_u
            nv_ref[k, pl.ds(own, PR), :] = r_v
            t1, s1 = advect(u_m, jnp.where(nw_f > fk, u_w, 0.0), v_m, jnp.where(nq_f > fk, v_s, 0.0),
                            ((t_c, t_n, at(2, k, -1)), (s_c, s_n, at(3, k, -1))))
            nt_ref[k, pl.ds(own, PR), :] = t1
            ns_ref[k, pl.ds(own, PR), :] = s1
        hu = jnp.where(nu_f > 0.0, 0.5 * (dc + roll(dc, -1)), 0.0)
        hv = jnp.where(nv_f > 0.0, 0.5 * (dc + dn), 0.0)
        fm[0, pl.ds(own + W, PR), :] = hu / jnp.maximum(nu_f, 1.0) * (-0.5 * sum_u)
        fm[1, pl.ds(own + W, PR), :] = hv / jnp.maximum(nv_f, 1.0) * (-0.5 * sum_v)
        return 0

    lax.fori_loop(0, N // PR, main_step, 0)

    lane8 = lax.broadcasted_iota(jnp.int32, (8, N), 1)
    for f in range(4):
        for lo in (0, 8 + N):
            x = jnp.zeros((8, N), F32)
            for k in range(LEVELS):
                x = jnp.where(lane8 // 4 == k, roll(fb[f, k, lo:lo + 8, :], 4 * k + 2), x)
            qs[f, lo:lo + 8, :] = x

    wait_recv(cols)

    part_x = lax.rem(lax.broadcasted_iota(jnp.int32, (N + 16, N), 1), 4)
    for f in range(4):
        q = qs[f]
        xe[f] = jnp.where(part_x == 2, roll(got_e[...], 2 - f), q)
        xw[f] = jnp.where(part_x == 1, roll(got_w[...], 1 - f), q)
    for f in range(2):
        q = kd[f]
        b = [jnp.broadcast_to(q[:, j:j + 1], q.shape) for j in (N - 2, N - 1, 0, 1)]
        h_e = jnp.broadcast_to(got_e[:, 124 + f:125 + f], q.shape)
        h_w = jnp.broadcast_to(got_w[:, 124 + f:125 + f], q.shape)
        xe[4 + f] = jnp.where(part_x == 0, b[0], jnp.where(part_x == 1, b[1], h_e))
        xw[4 + f] = jnp.where(part_x == 1, h_w, jnp.where(part_x == 2, b[2], b[3]))

    lev = slot.astype(F32)

    row_i = lax.broadcasted_iota(jnp.int32, (N, N), 0)
    same = lax.rem(row_i, 4) == part
    below = jnp.where(same & (row_i // 4 <= slot), 1.0, 0.0)
    every = jnp.where(same, 1.0, 0.0)

    def mix(x, m):
        return jnp.dot(x, m, precision=lax.Precision.HIGHEST, preferred_element_type=F32)

    def strip_force(x):
        def at(f, off):
            return x[f, 8 + off:8 + off + N, :]

        kc, kn = at(4, 0), at(4, 1)
        dc, dn = at(5, 0), at(5, 1)
        nu_f, nv_f = jnp.minimum(kc, roll(kc, -1)), jnp.minimum(kc, kn)
        h_c = at(3, 0) - 0.5 * at(2, 0)
        h_n = at(3, 1) - 0.5 * at(2, 1)
        q_c = (2.0 * mix(h_c, below) - h_c) * thick(kc, dc)
        q_n = (2.0 * mix(h_n, below) - h_n) * thick(kn, dn)
        g_u, g_v, r_u, r_v = force(nu_f > lev, nv_f > lev, q_c, roll(q_c, -1), q_n,
                                   at(0, 0), at(0, 1), at(0, -1), at(1, 0), at(1, 1), at(1, -1))[:4]
        hu = jnp.where(nu_f > 0.0, -0.25 * (dc + roll(dc, -1)), 0.0) / jnp.maximum(nu_f, 1.0)
        hv = jnp.where(nv_f > 0.0, -0.25 * (dc + dn), 0.0) / jnp.maximum(nv_f, 1.0)
        return hu, hv, g_u, g_v, r_u, r_v

    def strip_tracer(x):
        def at(f, off):
            return x[f, 8 + off:8 + off + N, :]

        kc, kn, ks = at(4, 0), at(4, 1), at(4, -1)
        u_m = jnp.where(jnp.minimum(kc, roll(kc, -1)) > lev, at(0, 0), 0.0)
        u_w = jnp.where(jnp.minimum(kc, roll(kc, 1)) > lev, roll(at(0, 0), 1), 0.0)
        v_m = jnp.where(jnp.minimum(kc, kn) > lev, at(1, 0), 0.0)
        v_s = jnp.where(jnp.minimum(kc, ks) > lev, at(1, -1), 0.0)
        return advect(u_m, u_w, v_m, v_s, ((at(2, 0), at(2, 1), at(2, -1)), (at(3, 0), at(3, 1), at(3, -1))))

    def merge(fn):
        return [jnp.where(part == 1, a, b) for a, b in zip(fn(xe), fn(xw))]

    hu, hv, g_u, g_v, r_u, r_v = merge(strip_force)
    rim = (lane == 0) | (lane == N - 1)
    forces = []
    for f, (hf, g) in enumerate(((hu, g_u), (hv, g_v))):
        x = jnp.where(rim, roll(hf * mix(g, every), 2), fm[f, W:W + N, :])
        fm[f, W:W + N, :] = x
        forces.append(x)
    half = lax.broadcasted_iota(jnp.int32, (h, N), 1) < n2
    for ref, x in zip((fk_e, fk_w), pack(forces)):
        for b in range(N // W):
            ref[h * b:h * b + h, :] = jnp.where(half, x[W * b:W * b + h], roll(x[W * b + h:W * b + W], n2))
    start(forc)
    ed[0] = r_u
    ed[1] = r_v
    t1, s1 = merge(strip_tracer)
    ed[2] = t1
    ed[3] = s1

    lane_q = lax.broadcasted_iota(jnp.int32, (QR, N), 1)
    edge_q = (lane_q == 0) | (lane_q == N - 1)

    def solve_step(g, _):
        own = pl.multiple_of(g * QR, QR)
        base = own + 8
        here = pl.ds(own, QR)
        kc = kd[0, pl.ds(base, QR), :]
        kn = kd[0, pl.ds(base + 1, QR), :]
        nu_f = jnp.minimum(kc, jnp.where(lane_q == N - 1, roll(got_e[pl.ds(base, QR), :], 3), roll(kc, -1)))
        nv_f = jnp.minimum(kc, kn)
        two_ref[0, here, :] = nu_f
        two_ref[1, here, :] = nv_f
        zero = jnp.zeros((QR, N), F32)
        refs = (nu_ref, nv_ref, nt_ref, ns_ref)
        cos = (VISC, VISC, DIFF, DIFF)
        d = [zero] * 4

        def factor(n_f, k, co, nu):
            return jnp.where(n_f > k + 1.0, nu * co[0][k], jnp.where(n_f > float(k), nu * co[1][k], 0.0))

        for k in range(LEVELS):
            f_t = factor(kc, k, DIFF, DIFF_NUM)
            facs = (factor(nu_f, k, VISC, VISC_NUM), factor(nv_f, k, VISC, VISC_NUM), f_t, f_t)
            for q in range(4):
                x = jnp.where(edge_q, roll(ed[q, here, :], 126 - 4 * k), refs[q][k, here, :])
                d[q] = (x + d[q]) * facs[q]
                if k == LEVELS - 1:
                    refs[q][k, here, :] = 0.25 * d[q]
                else:
                    refs[q][k, here, :] = d[q]
        sum_u, sum_v = d[0], d[1]
        for k in range(LEVELS - 2, -1, -1):
            for q in range(4):
                d[q] = refs[q][k, here, :] + cos[q][2][k] * d[q]
                refs[q][k, here, :] = 0.25 * d[q]
            sum_u, sum_v = sum_u + d[0], sum_v + d[1]
        two_ref[2, here, :] = sum_u / (VISC_NUM * jnp.maximum(nu_f, 1.0))
        two_ref[3, here, :] = sum_v / (VISC_NUM * jnp.maximum(nv_f, 1.0))
        return 0

    lax.fori_loop(0, N // QR, solve_step, 0)

    wait_recv(wide_main)
    wait_recv(wide_pass)
    lane_x = lax.broadcasted_iota(jnp.int32, (EXT, N), 1)
    row_x = lax.broadcasted_iota(jnp.int32, (EXT, N), 0)
    real = (row_x >= jnp.where(has_s, 0, W)) & (row_x < jnp.where(has_n, EXT, W + N))
    in_e, in_w = lane_x < W, lane_x >= N - W

    def side(f):
        return jnp.where(in_e, roll(we[...], -W * f), roll(ww[...], -W * (f + 1)))

    dms = (jnp.where(real, wm[3], 0.0), jnp.where(real & (in_e | in_w), side(3), 0.0))
    zero8 = jnp.zeros((8, N), F32)
    for ref in (et, fu, fv):
        for t in range(2):
            ref[t, 0:8, :] = zero8
            ref[t, 8 + EXT:TOP, :] = zero8
    for t in range(2):
        et[t, 8:8 + EXT, :] = dms[t]
    ra, rb = roll(dms[0], -1), roll(dms[1], -1)
    dme = (jnp.where(lane_x == N - 1, rb, ra), jnp.where(lane_x == N - 1, ra, rb))
    for t in range(2):
        d_c = dms[t]
        d_n = et[t, 9:9 + EXT, :]
        wet_u = (d_c > 0.0) & (dme[t] > 0.0)
        wet_v = (d_c > 0.0) & (d_n > 0.0)
        pick = (lambda f: wm[f]) if t == 0 else side
        et[t, 8:8 + EXT, :] = jnp.where(d_c > 0.0, pick(0), 0.0)
        fu[t, 8:8 + EXT, :] = jnp.where(wet_u, 0.5 * pick(1), 0.0)
        fv[t, 8:8 + EXT, :] = jnp.where(wet_v, 0.5 * pick(2), 0.0)
        cu[t] = jnp.where(wet_u, 0.125 * (d_c + dme[t]), 0.0)
        cv[t] = jnp.where(wet_v, 0.125 * (d_c + d_n), 0.0)
    wait_send(rows)
    wait_send(cols)
    wait_send(wide_side)
    wait_send(wide_main)
    wait_send(wide_pass)
    wait_recv(forc)
    fm_out[...] = fm[...]
    for out, got in ((fe_out, fe), (fw_out, fw)):
        for b in range(EXT // W):
            x = got[h * b:h * b + h, :]
            out[W * b:W * b + h, :] = x
            out[W * b + h:W * b + W, :] = roll(x, n2)
    wait_send(forc)


def step_kernel(nu_ref, nv_ref, nt_ref, ns_ref, two_ref, et0, fu0, fv0, cu, cv, fm, fe, fw,
                eta_out, tu_out, tv_out, u_hbm, v_hbm, t_hbm, s_hbm,
                et1, fu1, fv1, pu, pv, mean, ub, vb, flat, osem):
    copies = [pltpu.make_async_copy(nt_ref, t_hbm, osem.at[0]), pltpu.make_async_copy(ns_ref, s_hbm, osem.at[1])]
    for cp in copies:
        cp.start()

    lane = lax.broadcasted_iota(jnp.int32, (EXT, N), 1)

    def side(f):
        e, w = fe[...], fw[...]
        e = pltpu.roll(e, N - W * f, 1) if f else e
        w = pltpu.roll(w, N - W * (f + 1), 1)
        return jnp.where(lane < W, e, w)

    for f, (p, co) in enumerate(((pu, cu), (pv, cv))):
        for t in range(2):
            x = fm[f] if t == 0 else side(f)
            p[t] = jnp.where(co[t] > 0.0, (0.125 / SUBCYCLES) * x, 0.0)
    zero8 = jnp.zeros((8, N), F32)
    for ref in (et1, fv1):
        for t in range(2):
            ref[t, 0:8, :] = zero8
            ref[t, 8 + EXT:TOP, :] = zero8

    wgt = weights()
    lane8 = lax.broadcasted_iota(jnp.int32, (8, N), 1)
    first8, last8 = lane8 == 0, lane8 == N - 1

    def west8(x):
        a, b = pltpu.roll(x[0], 1, 1), pltpu.roll(x[1], 1, 1)
        return jnp.where(first8, b, a), jnp.where(first8, a, b)

    def east8(x):
        a, b = pltpu.roll(x[0], N - 1, 1), pltpu.roll(x[1], N - 1, 1)
        return jnp.where(last8, b, a), jnp.where(last8, a, b)

    for n in range(1, SUBCYCLES + 1):
        lo = 8 * (n // 8)
        groups = range(lo, EXT - lo, 8)
        et, fu, fv = (et1, fu1, fv1) if n > 1 else (et0, fu0, fv0)
        for g in groups:
            us = (fu[0, 8 + g:16 + g, :], fu[1, 8 + g:16 + g, :])
            uw = west8(us)
            for t in range(2):
                et1[t, 8 + g:16 + g, :] = et[t, 8 + g:16 + g, :] - (
                    (us[t] - uw[t]) + (fv[t, 8 + g:16 + g, :] - fv[t, 7 + g:15 + g, :]))
        for g in groups:
            es = (et1[0, 8 + g:16 + g, :], et1[1, 8 + g:16 + g, :])
            ee = east8(es)
            for t in range(2):
                u = fu[t, 8 + g:16 + g, :] - cu[t, g:g + 8, :] * (ee[t] - es[t]) + pu[t, g:g + 8, :]
                v = fv[t, 8 + g:16 + g, :] - cv[t, g:g + 8, :] * (et1[t, 9 + g:17 + g, :] - es[t]) + pv[t, g:g + 8, :]
                fu1[t, 8 + g:16 + g, :] = u
                fv1[t, 8 + g:16 + g, :] = v
                if t == 0 and W <= g < W + N:
                    at = slice(g - W, g - W + 8)
                    w = float(wgt[n - 1])
                    mean[0, at, :] = w * u if n == 1 else mean[0, at, :] + w * u
                    mean[1, at, :] = w * v if n == 1 else mean[1, at, :] + w * v

    mid = slice(8 + W, 8 + W + N)
    flat[0] = et1[0, mid, :]
    flat[1] = 2.0 * fu1[0, mid, :]
    flat[2] = 2.0 * fv1[0, mid, :]
    for i, out in enumerate((eta_out, tu_out, tv_out)):
        cp = pltpu.make_async_copy(flat.at[i], out, osem.at[2 + i])
        cp.start()
        copies.append(cp)
    for i, co in ((0, cu), (1, cv)):
        h = co[0, W:W + N, :]
        mean[i] = mean[i] / jnp.where(h > 0.0, 2.0 * h, 1.0) - two_ref[2 + i]

    for ci, (k0, k1) in enumerate(OUT_CHUNKS):
        for i, (src, buf, dst) in enumerate(((nu_ref, ub, u_hbm), (nv_ref, vb, v_hbm))):
            for g in range(0, N, 8):
                at = slice(g, g + 8)
                n_f, m = two_ref[i, at, :], mean[i, at, :]
                for k in range(k0, k1):
                    buf[k, at, :] = src[k, at, :] + jnp.where(n_f > float(k), m, 0.0)
            cp = pltpu.make_async_copy(buf.at[pl.ds(k0, k1 - k0)], dst.at[pl.ds(k0, k1 - k0)], osem.at[5 + 2 * ci + i])
            cp.start()
            copies.append(cp)
    for cp in copies:
        cp.wait()


def solution(mesh):
    ncol, nrow = mesh.shape['col'], mesh.shape['row']
    vmem = pl.BlockSpec(memory_space=pltpu.VMEM)
    hbm = pl.BlockSpec(memory_space=pl.ANY)
    s3 = jax.ShapeDtypeStruct((LEVELS, N, N), F32)
    s2 = jax.ShapeDtypeStruct((N, N), F32)

    def sds(*shape):
        return jax.ShapeDtypeStruct(shape, F32)

    def ocean_step(vel_u, vel_v, temp, salt, eta, tu, tv, dep, kmt):
        def kernel_a(*refs):
            exchange_kernel(ncol, nrow, *refs)

        def kernel_b(*refs):
            step_kernel(*refs)

        mid = pl.pallas_call(
            kernel_a,
            name='exchange',
            out_shape=(s3, s3, s3, s3, sds(4, N, N), sds(2, TOP, N), sds(2, TOP, N), sds(2, TOP, N), sds(2, EXT, N),
                       sds(2, EXT, N), sds(2, EXT, N), sds(EXT, N), sds(EXT, N)),
            in_specs=[hbm] * 9,
            out_specs=(vmem,) * 13,
            scratch_shapes=[
                pltpu.VMEM((4, LEVELS, N + 16, N), F32),
                pltpu.VMEM((N, N), jnp.int32),
                pltpu.VMEM((2, N + 16, N), F32),
                pltpu.VMEM((4, N + 16, N), F32),
                pltpu.VMEM((N, N), F32), pltpu.VMEM((N, N), F32),
                pltpu.VMEM((N + 16, N), F32), pltpu.VMEM((N + 16, N), F32),
                pltpu.VMEM((6, N + 16, N), F32), pltpu.VMEM((6, N + 16, N), F32),
                pltpu.VMEM((4, N, N), F32),
                pltpu.VMEM((4, EXT, N), F32),
                pltpu.VMEM((N, N), F32), pltpu.VMEM((N, N), F32),
                pltpu.VMEM((EXT, N), F32), pltpu.VMEM((EXT, N), F32),
                pltpu.VMEM((2, EXT, N), F32),
                pltpu.VMEM((N // 2, N), F32), pltpu.VMEM((N // 2, N), F32),
                pltpu.VMEM((EXT // 2, N), F32), pltpu.VMEM((EXT // 2, N), F32),
                pltpu.SemaphoreType.DMA((4, len(CHUNKS))),
                pltpu.SemaphoreType.DMA((5,)),
                pltpu.SemaphoreType.DMA((24,)),
                pltpu.SemaphoreType.DMA((24,)),
            ],
            compiler_params=pltpu.CompilerParams(collective_id=0, has_side_effects=True, vmem_limit_bytes=28 * 2 ** 20),
        )(*[pltpu.with_memory_space_constraint(x, pltpu.HBM) for x in (vel_u, vel_v, temp, salt, eta, tu, tv, dep, kmt)])
        st = pltpu.VMEM((2, TOP, N), F32)
        co = pltpu.VMEM((2, EXT, N), F32)
        out = pl.pallas_call(
            kernel_b,
            name='subcycles',
            out_shape=(s2, s2, s2, s3, s3, s3, s3),
            in_specs=[vmem] * 13,
            out_specs=(hbm,) * 7,
            scratch_shapes=[st, st, st, co, co, pltpu.VMEM((2, N, N), F32),
                            pltpu.VMEM((LEVELS, N, N), F32), pltpu.VMEM((LEVELS, N, N), F32),
                            pltpu.VMEM((3, N, N), F32), pltpu.SemaphoreType.DMA((5 + 2 * len(OUT_CHUNKS),))],
            compiler_params=pltpu.CompilerParams(vmem_limit_bytes=28 * 2 ** 20),
        )(*mid)
        return out

    spec_3d = P(None, 'row', 'col')
    spec_2d = P('row', 'col')
    return jax.shard_map(ocean_step, mesh=mesh, in_specs=(spec_3d,) * 4 + (spec_2d,) * 5,
                         out_specs=(spec_2d,) * 3 + (spec_3d,) * 4, check_vma=False)
```
